32 devices in a mesh: dp: 2 (over x), tp: 4 (over z), dm: 4 (over y, core).
Axes of the slice: x: 2, y: 2, z: 4, core: 2. Of those that a mesh axis runs over, the one named last changes fastest.
Arguments:
- tokens: bfloat16 [8192, 3584], P('dp', 'dm'), parts along dimension 0
- positions: int32 [8, 1024], P('dp'), parts along dimension 0
- norm_pre_attn: bfloat16 [3584], P('dm')
- w_query: bfloat16 [3584, 16, 256], P('dm', 'tp')
- w_key: bfloat16 [3584, 8, 256], P('dm', 'tp')
- w_value: bfloat16 [3584, 8, 256], P('dm', 'tp')
- w_out: bfloat16 [16, 256, 3584], P('tp', None, 'dm')
- norm_post_attn: bfloat16 [3584], P('dm')
- norm_pre_ffw: bfloat16 [3584], P('dm')
- w_gate: bfloat16 [3584, 14336], P('dm', 'tp')
- w_up: bfloat16 [3584, 14336], P('dm', 'tp')
- w_down: bfloat16 [14336, 3584], P('tp', 'dm')
- norm_post_ffw: bfloat16 [3584], P('dm')
Outputs:
- output 1: bfloat16 [8192, 3584], P('dp', 'dm'), parts along dimension 0
- output 2: bfloat16 [8192, 8, 256], P('dp', 'tp'), parts along dimension 0
- output 3: bfloat16 [8192, 8, 256], P('dp', 'tp'), parts along dimension 0
There are 2 independent parts. The reference program is written for one: setup_inputs(seed, part) draws one part's arguments, and reference() takes and returns one part's arrays. A program takes and returns all parts, laid end to end along the dimension named above; an argument that names none is the same for every part.
All inputs are finite; a program needn't handle non-finite values.
Results may differ from the reference program's by a relative error of at most 0.02.
Values are sent between devices in bfloat16 or wider.
A program may use at most 1 GiB of HBM per device.

```python
import jax
import jax.numpy as jnp
from jax import lax

MODEL_DIM = 3584
NUM_HEADS = 16
KV_HEADS = 8
HEAD_DIM = 256
FFW_DIM = 14336
NUM_SEQS = 4
SEQ_LEN = 1024
WINDOW_LEN = 4096
NUM_TOKENS = NUM_SEQS * SEQ_LEN
GROUP_SIZE = NUM_HEADS // KV_HEADS
QUERY_BLOCK = min(SEQ_LEN, 128)
NORM_EPS = 1e-6
SOFT_CAP = 50.0
ROPE_BASE = 10000.0
SCORE_SCALE = (MODEL_DIM / NUM_HEADS) ** -0.5


def draw_normal(key, shape, scale):
    return (jax.random.normal(key, shape, jnp.float32) * scale).astype(jnp.bfloat16)


def draw_gain(key, gain_ramp):
    return (jax.random.normal(key, (MODEL_DIM,), jnp.float32) * 0.3 + gain_ramp).astype(jnp.bfloat16)


def setup_inputs(seed: int = 0, part: int = 0) -> dict:
    shared_key, part_root = jax.random.split(jax.random.key(seed))
    part_key = jax.random.fold_in(part_root, part)
    tok_key, start_key, step_key = jax.random.split(part_key, 3)
    weight_keys = jax.random.split(shared_key, 11)
    seq_start = jax.random.randint(start_key, (NUM_SEQS, 1), 0, SEQ_LEN)
    pos_steps = jax.random.randint(step_key, (NUM_SEQS, SEQ_LEN), 1, 4)
    positions = seq_start + jnp.cumsum(pos_steps, axis=1) - pos_steps[:, :1]
    col_pos = jnp.arange(MODEL_DIM, dtype=jnp.float32) / (MODEL_DIM - 1)
    width_ramp = 2.0 ** (3.0 * col_pos - 1.5)
    out_ramp = 2.0 ** (2.0 * col_pos - 1.0)
    gain_ramp = col_pos - 0.5
    model_scale = MODEL_DIM ** -0.5
    tokens = jax.random.normal(tok_key, (NUM_TOKENS, MODEL_DIM), jnp.float32) * width_ramp[None, :]
    w_out = jax.random.normal(weight_keys[4], (NUM_HEADS, HEAD_DIM, MODEL_DIM), jnp.float32) * ((NUM_HEADS * HEAD_DIM) ** -0.5) * out_ramp
    w_down = jax.random.normal(weight_keys[9], (FFW_DIM, MODEL_DIM), jnp.float32) * (FFW_DIM ** -0.5) * out_ramp[None, :]
    return {
        'tokens': tokens.astype(jnp.bfloat16),
        'positions': positions.astype(jnp.int32),
        'norm_pre_attn': draw_gain(weight_keys[0], gain_ramp),
        'w_query': draw_normal(weight_keys[1], (MODEL_DIM, NUM_HEADS, HEAD_DIM), model_scale),
        'w_key': draw_normal(weight_keys[2], (MODEL_DIM, KV_HEADS, HEAD_DIM), model_scale),
        'w_value': draw_normal(weight_keys[3], (MODEL_DIM, KV_HEADS, HEAD_DIM), model_scale),
        'w_out': w_out.astype(jnp.bfloat16),
        'norm_post_attn': draw_gain(weight_keys[5], gain_ramp),
        'norm_pre_ffw': draw_gain(weight_keys[6], gain_ramp),
        'w_gate': draw_normal(weight_keys[7], (MODEL_DIM, FFW_DIM), model_scale),
        'w_up': draw_normal(weight_keys[8], (MODEL_DIM, FFW_DIM), model_scale),
        'w_down': w_down.astype(jnp.bfloat16),
        'norm_post_ffw': draw_gain(weight_keys[10], gain_ramp),
    }


def rms_scale(values, gain_vec):
    vals32 = values.astype(jnp.float32)
    mean_sq = jnp.mean(vals32 * vals32, axis=-1, keepdims=True)
    return vals32 * lax.rsqrt(mean_sq + NORM_EPS) * (1.0 + gain_vec.astype(jnp.float32))


def rotary_tables(positions):
    half_dim = HEAD_DIM // 2
    inv_freq = ROPE_BASE ** (-2.0 * jnp.arange(half_dim, dtype=jnp.float32) / HEAD_DIM)
    angles = positions.reshape(-1).astype(jnp.float32)[:, None] * inv_freq[None, :]
    return jnp.cos(angles)[:, None, :], jnp.sin(angles)[:, None, :]


def apply_rotary(head_vals, cos_tab, sin_tab):
    half_dim = head_vals.shape[-1] // 2
    lower_half = head_vals[..., :half_dim].astype(jnp.float32)
    upper_half = head_vals[..., half_dim:].astype(jnp.float32)
    rotated = jnp.concatenate([lower_half * cos_tab - upper_half * sin_tab, upper_half * cos_tab + lower_half * sin_tab], axis=-1)
    return rotated.astype(jnp.bfloat16)


def attend(query_rows, key_rows, value_rows, positions):
    keys32 = key_rows.astype(jnp.float32)
    values32 = value_rows.astype(jnp.float32)
    key_index = jnp.arange(SEQ_LEN)

    def one_block(block_index):
        row_start = block_index * QUERY_BLOCK
        q_blk = lax.dynamic_slice_in_dim(query_rows, row_start, QUERY_BLOCK, axis=1).astype(jnp.float32)
        q_pos = lax.dynamic_slice_in_dim(positions, row_start, QUERY_BLOCK, axis=1)
        scores = jnp.einsum('bqkgd,bskd->bkgqs', q_blk, keys32) * SCORE_SCALE
        scores = SOFT_CAP * jnp.tanh(scores / SOFT_CAP)
        q_index = row_start + jnp.arange(QUERY_BLOCK)
        allowed = (key_index[None, :] <= q_index[:, None])[None] & (q_pos[:, :, None] - positions[:, None, :] < WINDOW_LEN)
        scores = jnp.where(allowed[:, None, None], scores, -1e30)
        attn_probs = jax.nn.softmax(scores, axis=-1).astype(jnp.bfloat16).astype(jnp.float32)
        return jnp.einsum('bkgqs,bskd->bqkgd', attn_probs, values32).astype(jnp.bfloat16)

    blocks = lax.map(one_block, jnp.arange(SEQ_LEN // QUERY_BLOCK))
    return jnp.moveaxis(blocks, 0, 1).reshape(NUM_TOKENS, NUM_HEADS * HEAD_DIM)


def reference(tokens, positions, norm_pre_attn, w_query, w_key, w_value, w_out, norm_post_attn, norm_pre_ffw, w_gate, w_up, w_down, norm_post_ffw):
    cos_tab, sin_tab = rotary_tables(positions)
    normed = rms_scale(tokens, norm_pre_attn).astype(jnp.bfloat16)
    query_rows = jnp.dot(normed, w_query.reshape(MODEL_DIM, NUM_HEADS * HEAD_DIM), preferred_element_type=jnp.float32).astype(jnp.bfloat16)
    key_rows = jnp.dot(normed, w_key.reshape(MODEL_DIM, KV_HEADS * HEAD_DIM), preferred_element_type=jnp.float32).astype(jnp.bfloat16)
    value_rows = jnp.dot(normed, w_value.reshape(MODEL_DIM, KV_HEADS * HEAD_DIM), preferred_element_type=jnp.float32).astype(jnp.bfloat16)
    query_rows = apply_rotary(query_rows.reshape(NUM_TOKENS, NUM_HEADS, HEAD_DIM), cos_tab, sin_tab)
    key_rows = apply_rotary(key_rows.reshape(NUM_TOKENS, KV_HEADS, HEAD_DIM), cos_tab, sin_tab)
    value_rows = value_rows.reshape(NUM_TOKENS, KV_HEADS, HEAD_DIM)
    attn_rows = attend(query_rows.reshape(NUM_SEQS, SEQ_LEN, KV_HEADS, GROUP_SIZE, HEAD_DIM), key_rows.reshape(NUM_SEQS, SEQ_LEN, KV_HEADS, HEAD_DIM), value_rows.reshape(NUM_SEQS, SEQ_LEN, KV_HEADS, HEAD_DIM), positions)
    attn_out = jnp.dot(attn_rows, w_out.reshape(NUM_HEADS * HEAD_DIM, MODEL_DIM), preferred_element_type=jnp.float32).astype(jnp.bfloat16)
    hidden = (tokens.astype(jnp.float32) + rms_scale(attn_out, norm_post_attn)).astype(jnp.bfloat16)
    ffw_in = rms_scale(hidden, norm_pre_ffw).astype(jnp.bfloat16)
    gate_proj = jnp.dot(ffw_in, w_gate, preferred_element_type=jnp.float32).astype(jnp.bfloat16)
    up_proj = jnp.dot(ffw_in, w_up, preferred_element_type=jnp.float32).astype(jnp.bfloat16)
    gated_act = (jax.nn.gelu(gate_proj.astype(jnp.float32), approximate=True) * up_proj.astype(jnp.float32)).astype(jnp.bfloat16)
    down_proj = jnp.dot(gated_act, w_down, preferred_element_type=jnp.float32).astype(jnp.bfloat16)
    tokens_out = (hidden.astype(jnp.float32) + rms_scale(down_proj, norm_post_ffw)).astype(jnp.bfloat16)
    return (tokens_out, key_rows, value_rows)
```

```python
import functools

import jax
import jax.numpy as jnp
from jax import lax
from jax.experimental import pallas as pl
from jax.experimental.pallas import tpu as pltpu
from jax.sharding import PartitionSpec as P

NORM_EPS = 1e-6
SOFT_CAP = 50.0
ROPE_BASE = 10000.0
WINDOW_LEN = 4096
BF16 = jnp.bfloat16
F32 = jnp.float32

CHUNK = 32
LAG = 2
LINE = 4
VMEM_BYTES = 60 * 1024 * 1024

ANY = pl.BlockSpec(memory_space=pl.ANY)
VMEM = pl.BlockSpec(memory_space=pltpu.VMEM)
DMA = pltpu.SemaphoreType.DMA


def places():
    row = lax.axis_index('dp')
    line = lax.axis_index('tp')
    me = lax.axis_index('dm')
    side = lax.div(me, 2)
    core = me - 2 * side
    return row, line, me, 2 * side + 1 - core, 2 * (1 - side) + core, 2 * (1 - side) + 1 - core


def remote(src, dst, send_sem, recv_sem, device):
    return pltpu.make_async_remote_copy(src_ref=src, dst_ref=dst, send_sem=send_sem, recv_sem=recv_sem, device_id=device, device_id_type=pl.DeviceIdType.MESH)


def meet(peers):
    barrier = pltpu.get_barrier_semaphore()
    for peer in peers:
        pl.semaphore_signal(barrier, inc=1, device_id=peer, device_id_type=pl.DeviceIdType.MESH)
    pl.semaphore_wait(barrier, len(peers))


def line_peers(line):
    return [{'tp': lax.rem(line + 1, LINE)}, {'tp': lax.rem(line + LINE - 1, LINE)}]


class Shard:
    def __init__(self, src, dst, by_rows, pieces):
        self.src, self.dst, self.by_rows, self.pieces = src, dst, by_rows, pieces
        self.rows = src.shape[0]
        self.unit = self.rows // (2 * pieces)

    def own(self, half, piece):
        return self.src.at[pl.ds(pl.multiple_of((half * self.pieces + piece) * self.unit, self.unit), self.unit)]

    def at(self, shard, half, piece):
        start = (half * self.pieces + piece) * self.unit
        if self.by_rows:
            return self.dst.at[pl.ds(pl.multiple_of(shard * self.rows + start, self.unit), self.unit)]
        cols = self.src.shape[1]
        return self.dst.at[pl.ds(pl.multiple_of(start, self.unit), self.unit), pl.ds(pl.multiple_of(shard * cols, cols), cols)]

    def whole(self, shard):
        if self.by_rows:
            return self.dst.at[pl.ds(pl.multiple_of(shard * self.rows, self.rows), self.rows)]
        cols = self.src.shape[1]
        return self.dst.at[:, pl.ds(pl.multiple_of(shard * cols, cols), cols)]


class WeightGather:
    def __init__(self, shards, own_send, own_recv, send, recv):
        self.shards, self.own_send, self.own_recv, self.send, self.recv = shards, own_send, own_recv, send, recv
        self.row, _, self.me, self.mate, self.across, self.cross = places()
        self.units = [(w, p) for w in range(len(shards)) for p in range(shards[w].pieces)]

    def copy(self, k, hop):
        w, p = self.units[k]
        shard = self.shards[w]
        mine, other = self.row, 1 - self.row
        if hop == 0:
            src, dst, device = shard.own(mine, p), shard.at(self.me, mine, p), {'dm': self.across}
        elif hop == 1:
            src = dst = shard.at(self.across, mine, p)
            device = {'dp': other}
        elif hop == 2:
            src = dst = shard.at(self.across, mine, p)
            device = {'dm': self.mate}
        else:
            src = dst = shard.at(self.across, other, p)
            device = {'dm': self.mate}
        return remote(src, dst, self.send.at[k, hop], self.recv.at[k, hop], device)

    def arrival(self, k, hop):
        w, p = self.units[k]
        shard = self.shards[w]
        mine, other = self.row, 1 - self.row
        region = (shard.at(self.across, mine, p), shard.at(self.across, other, p), shard.at(self.cross, mine, p), shard.at(self.cross, other, p))[hop]
        return remote(region, region, self.send.at[k, hop], self.recv.at[k, hop], {'dm': self.mate})

    def own_copy(self, w, shard_index):
        shard = self.shards[w]
        return remote(shard.src, shard.whole(shard_index), self.own_send.at[w], self.own_recv.at[w], {'dm': self.mate})

    def start(self):
        for k in range(len(self.units)):
            self.copy(k, 0).start()
        for w in range(len(self.shards)):
            self.own_copy(w, self.me).start()

    def pass_y(self, k):
        self.arrival(k, 0).wait_recv()
        self.copy(k, 1).start()
        self.copy(k, 2).start()

    def pass_x(self, k):
        self.arrival(k, 1).wait_recv()
        self.copy(k, 3).start()

    def settle(self):
        for k in range(len(self.units)):
            self.arrival(k, 2).wait_recv()
            self.arrival(k, 3).wait_recv()
            for hop in range(4):
                self.copy(k, hop).wait_send()
        for w in range(len(self.shards)):
            self.own_copy(w, self.mate).wait_recv()
            self.own_copy(w, self.me).wait_send()


def fetch_kernel(x_ref, n_ref, wq_ref, wk_ref, wv_ref, wo_ref, xf_ref, nf_ref, wqf_ref, wkf_ref, wvf_ref, wof_ref, x_buf, n_buf, q_buf, k_buf, v_buf, o_buf, load_sem, store_sem, x_send, x_recv, n_send, n_recv, z_send, z_recv, own_send, own_recv, w_send, w_recv):
    row, line, me, mate, across, cross = places()
    seq = xf_ref.shape[0]
    part = seq // LINE
    cols = x_ref.shape[1]
    mine = pl.ds(pl.multiple_of(me * cols, cols), cols)
    shards = [Shard(wq_ref, wqf_ref, True, 1), Shard(wk_ref, wkf_ref, True, 1), Shard(wv_ref, wvf_ref, True, 1), Shard(wo_ref, wof_ref, False, 1)]
    gather = WeightGather(shards, own_send, own_recv, w_send, w_recv)

    def x_copy(hop):
        dev = (mate, across, cross)[hop]
        if hop == 0:
            src = x_ref.at[pl.ds(pl.multiple_of(dev * seq, seq), seq)]
            dst = xf_ref.at[:, mine]
        else:
            src = x_ref.at[pl.ds(pl.multiple_of(dev * seq + line * part, part), part)]
            dst = xf_ref.at[pl.ds(pl.multiple_of(line * part, part), part), mine]
        return remote(src, dst, x_send.at[hop], x_recv.at[hop], {'dm': dev})

    def x_arrival(hop):
        dev = (mate, across, cross)[hop]
        theirs = pl.ds(pl.multiple_of(dev * cols, cols), cols)
        if hop == 0:
            region = xf_ref.at[:, theirs]
        else:
            region = xf_ref.at[pl.ds(pl.multiple_of(line * part, part), part), theirs]
        return remote(region, region, x_send.at[hop], x_recv.at[hop], {'dm': dev})

    far = pl.ds(pl.multiple_of((1 - lax.div(me, 2)) * 2 * cols, 2 * cols), 2 * cols)

    def z_copy(up, block):
        region = xf_ref.at[pl.ds(pl.multiple_of(block * part, part), part), far]
        device = {'tp': line + 1} if up else {'tp': line - 1}
        return remote(region, region, z_send.at[0 if up else 1, block], z_recv.at[block], device)

    def z_step(step):
        below, above = line - step, line + step

        @pl.when(below >= 0)
        def _():
            z_copy(True, below).wait_recv()

            @pl.when(line < LINE - 1)
            def _():
                z_copy(True, below).start()

        @pl.when(above < LINE)
        def _():
            z_copy(False, above).wait_recv()

            @pl.when(line > 0)
            def _():
                z_copy(False, above).start()

    meet([{'dm': mate}, {'dm': across}, {'dm': cross}, {'dp': 1 - row}] + line_peers(line))
    x_copy(1).start()
    x_copy(2).start()
    x_copy(0).start()
    gather.start()
    n_copies = [remote(n_ref, nf_ref.at[me], n_send.at[i], n_recv.at[i], {'dm': dev}) for i, dev in enumerate((mate, across, cross))]
    n_arrivals = [remote(n_ref, nf_ref.at[dev], n_send.at[i], n_recv.at[i], {'dm': dev}) for i, dev in enumerate((mate, across, cross))]
    for copy in n_copies:
        copy.start()
    moves = [
        (x_ref.at[pl.ds(pl.multiple_of(me * seq, seq), seq)], x_buf, xf_ref.at[:, mine]),
        (wq_ref, q_buf, shards[0].whole(me)),
        (wk_ref, k_buf, shards[1].whole(me)),
        (wv_ref, v_buf, shards[2].whole(me)),
        (wo_ref, o_buf, shards[3].whole(me)),
        (n_ref, n_buf, nf_ref.at[me]),
    ]
    loads = [pltpu.make_async_copy(src, buf, load_sem.at[i]) for i, (src, buf, _) in enumerate(moves)]
    stores = [pltpu.make_async_copy(buf, dst, store_sem.at[i]) for i, (_, buf, dst) in enumerate(moves)]
    for load in loads:
        load.start()
    for load, store in zip(loads, stores):
        load.wait()
        store.start()

    x_arrival(1).wait_recv()
    x_arrival(2).wait_recv()

    @pl.when(line < LINE - 1)
    def _():
        z_copy(True, line).start()

    @pl.when(line > 0)
    def _():
        z_copy(False, line).start()

    z_step(1)
    gather.pass_y(0)
    gather.pass_y(1)
    z_step(2)
    gather.pass_y(2)
    gather.pass_x(0)
    gather.pass_x(1)
    z_step(3)
    gather.pass_y(3)
    gather.pass_x(2)
    gather.pass_x(3)
    gather.settle()
    x_arrival(0).wait_recv()
    for copy in n_arrivals:
        copy.wait_recv()
    for copy in n_copies:
        copy.wait_send()
    for hop in range(3):
        x_copy(hop).wait_send()
    for store in stores:
        store.wait()
    for block in range(LINE):

        @pl.when((block <= line) & (line < LINE - 1))
        def _():
            z_copy(True, block).wait_send()

        @pl.when((block >= line) & (line > 0))
        def _():
            z_copy(False, block).wait_send()


class LineSum:
    def __init__(self, p_ref, got, acc, out, sum_send, sum_recv, out_send, out_recv, finish, emit):
        self.p_ref, self.got, self.acc, self.out = p_ref, got, acc, out
        self.sum_send, self.sum_recv, self.out_send, self.out_recv = sum_send, sum_recv, out_send, out_recv
        self.finish, self.emit = finish, emit
        self.half = p_ref.shape[0] // 2
        self.chunks = self.half // CHUNK
        self.steps = self.chunks + 6 * LAG
        self.line = lax.axis_index('tp')

    def way(self, d):
        if d == 0:
            return self.line, {'tp': self.line + 1}, {'tp': self.line - 1}
        return LINE - 1 - self.line, {'tp': self.line - 1}, {'tp': self.line + 1}

    def rows(self, c):
        return pl.ds(pl.multiple_of(c * CHUNK, CHUNK), CHUNK)

    def out_rows(self, d, c):
        return pl.ds(pl.multiple_of(d * self.half + c * CHUNK, CHUNK), CHUNK)

    def sum_copy(self, d, c, first):
        src = self.p_ref.at[self.out_rows(d, c)] if first else self.acc.at[d, self.rows(c)]
        return remote(src, self.got.at[d, self.rows(c)], self.sum_send.at[d, c], self.sum_recv.at[d, c], self.way(d)[1])

    def out_copy(self, d, c):
        region = self.out.at[self.out_rows(d, c)]
        return remote(region, region, self.out_send.at[d, c], self.out_recv.at[d, c], self.way(d)[2])

    def step(self, t):
        for d in range(2):
            self.sum_step(d, t)
        for d in range(2):
            self.out_step(d, t)

    def sum_step(self, d, t):
        pos = self.way(d)[0]
        c = t - LAG * pos

        @pl.when((c >= 0) & (c < self.chunks))
        def _():
            @pl.when(pos == 0)
            def _():
                self.sum_copy(d, c, True).start()

            @pl.when(pos > 0)
            def _():
                self.sum_copy(d, c, False).wait_recv()
                total = self.p_ref[self.out_rows(d, c), :].astype(F32) + self.got[d, self.rows(c), :].astype(F32)

                @pl.when(pos < LINE - 1)
                def _():
                    self.acc[d, self.rows(c), :] = total.astype(BF16)
                    self.sum_copy(d, c, False).start()

                @pl.when(pos == LINE - 1)
                def _():
                    self.finish(self.out_rows(d, c), self.rows(c), total.astype(BF16))
                    self.out_copy(d, c).start()
                    self.emit(self.out_rows(d, c))

    def out_step(self, d, t):
        pos = self.way(d)[0]
        c = t - 3 * LAG - LAG * (LINE - 1 - pos)

        @pl.when((c >= 0) & (c < self.chunks) & (pos < LINE - 1))
        def _():
            self.out_copy(d, c).wait_recv()

            @pl.when(pos > 0)
            def _():
                self.out_copy(d, c).start()

            self.emit(self.out_rows(d, c))

    def run(self, actions):
        marks = sorted(set([0, self.steps] + [t for t in actions if 0 < t < self.steps]))
        for begin, end in zip(marks[:-1], marks[1:]):
            for action in actions.get(begin, ()):
                action()

            def body(t, carry):
                self.step(t)
                return carry

            lax.fori_loop(begin, end, body, 0)

    def settle(self):
        def body(c, carry):
            for d in range(2):
                pos = self.way(d)[0]

                @pl.when(pos < LINE - 1)
                def _():
                    self.sum_copy(d, c, False).wait_send()

                @pl.when(pos > 0)
                def _():
                    self.out_copy(d, c).wait_send()

            return carry

        lax.fori_loop(0, self.chunks, body, 0)


def unit_rows(values, gain):
    mean_sq = jnp.mean(values * values, axis=-1, keepdims=True)
    return values * lax.rsqrt(mean_sq + NORM_EPS) * gain


def middle_kernel(p_ref, xf_ref, n2_ref, n3_ref, wg_ref, wu_ref, wd_ref, m_ref, h_ref, wgf_ref, wuf_ref, wdf_ref, got, acc, m_buf, res_buf, row_buf, col_buf, res_sem, m_sem, h_sem, load_sem, store_sem, sum_send, sum_recv, out_send, out_recv, own_send, own_recv, w_send, w_recv):
    row, line, me, mate, across, cross = places()
    seq = p_ref.shape[0]
    half = seq // 2
    shards = [Shard(wg_ref, wgf_ref, True, 2), Shard(wu_ref, wuf_ref, True, 2), Shard(wd_ref, wdf_ref, False, 2)]
    gather = WeightGather(shards, own_send, own_recv, w_send, w_recv)
    first_row = pl.multiple_of(half * (1 - jnp.minimum(line, 1)), half)
    res_load = pltpu.make_async_copy(xf_ref.at[pl.ds(first_row, half)], res_buf, res_sem)
    h_store = pltpu.make_async_copy(res_buf, h_ref, h_sem)

    def finish(out_rows, rows, total):
        hidden = (res_buf[rows, :].astype(F32) + unit_rows(total.astype(F32), n2_ref[...])).astype(BF16)
        res_buf[rows, :] = hidden
        m_buf[out_rows, :] = unit_rows(hidden.astype(F32), n3_ref[...]).astype(BF16)

    def emit(out_rows):
        pltpu.make_async_copy(m_buf.at[out_rows], m_ref.at[out_rows], m_sem).start()

    sums = LineSum(p_ref, got, acc, m_buf, sum_send, sum_recv, out_send, out_recv, finish, emit)
    bufs = (row_buf, row_buf, col_buf)
    loads = [pltpu.make_async_copy(shard.src, buf, load_sem.at[w]) for w, (shard, buf) in enumerate(zip(shards, bufs))]
    stores = [pltpu.make_async_copy(buf, shard.whole(me), store_sem.at[w]) for w, (shard, buf) in enumerate(zip(shards, bufs))]

    meet([{'dm': mate}, {'dm': across}, {'dp': 1 - row}] + line_peers(line))
    res_load.start()
    loads[0].start()
    loads[2].start()
    gather.start()
    res_load.wait()

    def own_first():
        loads[0].wait()
        stores[0].start()
        loads[2].wait()
        stores[2].start()

    def own_second():
        stores[0].wait()
        loads[1].start()

    def own_third():
        loads[1].wait()
        stores[1].start()

    actions = {
        2: [own_first],
        5: [own_second],
        7: [own_third, functools.partial(gather.pass_y, 0)],
        13: [functools.partial(gather.pass_y, 1)],
        14: [functools.partial(gather.pass_x, 0)],
        18: [functools.partial(gather.pass_y, 2)],
        19: [functools.partial(gather.pass_x, 1)],
        23: [functools.partial(gather.pass_y, 3)],
        24: [functools.partial(gather.pass_x, 2)],
    }
    order = [action for t in sorted(actions) for action in actions[t]]
    sums.run({t: acts for t, acts in actions.items() if t < sums.steps})
    done = [action for t in sorted(actions) if t < sums.steps for action in actions[t]]
    for action in order[len(done):]:
        action()
    gather.pass_y(4)
    gather.pass_x(3)
    gather.pass_y(5)
    gather.pass_x(4)
    gather.pass_x(5)

    @pl.when((line == 0) | (line == LINE - 1))
    def _():
        h_store.start()
        h_store.wait()

    pltpu.make_async_copy(m_buf, m_ref, m_sem).wait()
    sums.settle()
    stores[1].wait()
    stores[2].wait()
    gather.settle()


def last_kernel(p_ref, h_ref, n4_ref, k_ref, v_ref, y_ref, kf_ref, vf_ref, got, acc, y_buf, res_buf, k_buf, v_buf, res_sem, kv_load, kv_store, kv_send, kv_recv, fin_send, fin_recv, own_sem, sum_send, sum_recv, out_send, out_recv):
    row, line, me, mate, across, cross = places()
    seq = p_ref.shape[0]
    cols = y_ref.shape[1]
    res_load = pltpu.make_async_copy(h_ref, res_buf, res_sem)
    ends = (line == 0) | (line == LINE - 1)
    caches = ((k_ref, kf_ref, k_buf), (v_ref, vf_ref, v_buf))

    def block(ref, shard):
        return ref.at[pl.ds(pl.multiple_of(shard * seq, seq), seq)]

    def kv_copy(i, hop):
        src, dst, _ = caches[i]
        if hop == 0:
            return remote(src, block(dst, me), kv_send.at[i, hop], kv_recv.at[i, hop], {'dm': across})
        if hop == 1:
            return remote(src, block(dst, me), kv_send.at[i, hop], kv_recv.at[i, hop], {'dm': mate})
        return remote(block(dst, across), block(dst, across), kv_send.at[i, hop], kv_recv.at[i, hop], {'dm': mate})

    def kv_arrival(i, hop):
        region = block(caches[i][1], (across, mate, cross)[hop])
        return remote(region, region, kv_send.at[i, hop], kv_recv.at[i, hop], {'dm': mate})

    kv_loads = [pltpu.make_async_copy(src, buf, kv_load.at[i]) for i, (src, _, buf) in enumerate(caches)]
    kv_stores = [pltpu.make_async_copy(buf, block(dst, me), kv_store.at[i]) for i, (_, dst, buf) in enumerate(caches)]

    def column(shard):
        return pl.ds(pl.multiple_of(shard * cols, cols), cols)

    def finish(out_rows, rows, total):
        y_buf[out_rows, :] = (res_buf[rows, :].astype(F32) + unit_rows(total.astype(F32), n4_ref[...])).astype(BF16)

    def emit(out_rows):
        start = out_rows.start
        there = pl.ds(pl.multiple_of(me * seq + start, CHUNK), CHUNK)
        for i, dev in enumerate((across, cross, mate)):
            remote(y_buf.at[out_rows, column(dev)], y_ref.at[there], fin_send.at[i], fin_recv.at[i], {'dm': dev}).start()
        pltpu.make_async_copy(y_buf.at[out_rows, column(me)], y_ref.at[there], own_sem).start()

    sums = LineSum(p_ref, got, acc, y_buf, sum_send, sum_recv, out_send, out_recv, finish, emit)

    meet([{'dm': mate}, {'dm': across}, {'dm': cross}] + line_peers(line))

    @pl.when(ends)
    def _():
        res_load.start()

    for i in range(2):
        kv_loads[i].start()
        kv_copy(i, 0).start()
        kv_copy(i, 1).start()

    @pl.when(ends)
    def _():
        res_load.wait()

    def keep_own():
        for i in range(2):
            kv_loads[i].wait()
            kv_stores[i].start()

    def pass_kv(i):
        kv_arrival(i, 0).wait_recv()
        kv_copy(i, 2).start()

    last = sums.steps - 1
    actions = {min(1, last): [keep_own], min(9, last): [functools.partial(pass_kv, 0), functools.partial(pass_kv, 1)]}
    if len(actions) == 1:
        actions = {last: [keep_own, functools.partial(pass_kv, 0), functools.partial(pass_kv, 1)]}
    sums.run(actions)
    sums.settle()
    for i in range(2):
        kv_stores[i].wait()
        for hop in range(3):
            kv_copy(i, hop).wait_send()
        kv_arrival(i, 1).wait_recv()
        kv_arrival(i, 2).wait_recv()
    for i, dev in enumerate((across, cross, mate)):
        done = remote(y_buf.at[:, column(dev)], block(y_ref, dev), fin_send.at[i], fin_recv.at[i], {'dm': dev})
        done.wait_send()
        done.wait_recv()
    pltpu.make_async_copy(y_buf.at[:, column(me)], block(y_ref, me), own_sem).wait()


def rotate(values, cos_tab, sin_tab):
    half_dim = values.shape[-1] // 2
    lower = values[:, :half_dim].astype(F32)
    upper = values[:, half_dim:].astype(F32)
    return jnp.concatenate([lower * cos_tab - upper * sin_tab, upper * cos_tab + lower * sin_tab], axis=-1).astype(BF16)


def attend_kernel(scale, q_ref, k_ref, v_ref, cos_ref, sin_ref, pos_col_ref, pos_row_ref, o_ref, k_out_ref, q_rot):
    seq = q_ref.shape[1]
    block = min(seq, 256)
    q_rot[...] = rotate(q_ref[0], cos_ref[...], sin_ref[...])
    k_out_ref[0] = rotate(k_ref[0], cos_ref[...], sin_ref[...])
    for i in range(seq // block):
        rows = slice(i * block, (i + 1) * block)
        span = (i + 1) * block
        scores = lax.dot_general(q_rot[rows, :], k_out_ref[0, :span, :], (((1,), (1,)), ((), ())), preferred_element_type=F32)
        capped = SOFT_CAP * jnp.tanh(scores * scale / SOFT_CAP)
        q_index = i * block + lax.broadcasted_iota(jnp.int32, (block, span), 0)
        key_index = lax.broadcasted_iota(jnp.int32, (block, span), 1)
        allowed = (key_index <= q_index) & (pos_col_ref[rows, :] - pos_row_ref[:, :span] < WINDOW_LEN)
        weights = jnp.where(allowed, jnp.exp(capped), 0.0)
        probs = (weights / jnp.sum(weights, axis=-1, keepdims=True)).astype(BF16)
        o_ref[rows, :] = jnp.dot(probs, v_ref[0, :span, :], preferred_element_type=F32).astype(BF16)


def gate_kernel(m_ref, wg_ref, wu_ref, z_ref):
    block = min(m_ref.shape[0], 512)

    def body(i, carry):
        rows = pl.ds(pl.multiple_of(i * block, block), block)
        gate = jnp.dot(m_ref[rows, :], wg_ref[...], preferred_element_type=F32).astype(BF16).astype(F32)
        up = jnp.dot(m_ref[rows, :], wu_ref[...], preferred_element_type=F32).astype(BF16).astype(F32)
        z_ref[rows, :] = (jax.nn.gelu(gate, approximate=True) * up).astype(BF16)
        return carry

    lax.fori_loop(0, m_ref.shape[0] // block, body, 0)


def like(*shape, dtype=BF16):
    return jax.ShapeDtypeStruct(shape, dtype)


def params(collective_id):
    return pltpu.CompilerParams(collective_id=collective_id, has_side_effects=True, vmem_limit_bytes=VMEM_BYTES)


def fetch(x, norms, wq, wk, wv, wo, seq):
    shard_rows, cols = wq.shape[0], x.shape[1]
    dim = 4 * cols
    return pl.pallas_call(
        fetch_kernel,
        name='fetch',
        out_shape=(like(seq, dim), like(4, *norms.shape), like(4 * shard_rows, *wq.shape[1:]), like(4 * shard_rows, *wk.shape[1:]), like(4 * shard_rows, *wv.shape[1:]), like(wo.shape[0], dim)),
        in_specs=[ANY] * 6,
        out_specs=(ANY,) * 6,
        scratch_shapes=[
            pltpu.VMEM((seq, cols), BF16), pltpu.VMEM(norms.shape, BF16), pltpu.VMEM(wq.shape, BF16), pltpu.VMEM(wk.shape, BF16), pltpu.VMEM(wv.shape, BF16), pltpu.VMEM(wo.shape, BF16),
            DMA((6,)), DMA((6,)), DMA((3,)), DMA((3,)), DMA((3,)), DMA((3,)), DMA((2, LINE)), DMA((LINE,)), DMA((4,)), DMA((4,)), DMA((4, 4)), DMA((4, 4)),
        ],
        compiler_params=params(0),
    )(x, norms, wq, wk, wv, wo)


def line_scratch(seq, dim):
    chunks = seq // 2 // CHUNK
    bufs = [pltpu.VMEM((2, seq // 2, dim), BF16), pltpu.VMEM((2, seq // 2, dim), BF16), pltpu.VMEM((seq, dim), BF16), pltpu.VMEM((seq // 2, dim), BF16)]
    return bufs, [DMA((2, chunks))] * 4


def middle(part, xf, gain2, gain3, wg, wu, wd):
    seq, dim = part.shape
    bufs, sems = line_scratch(seq, dim)
    return pl.pallas_call(
        middle_kernel,
        name='middle',
        out_shape=(like(seq, dim), like(seq // 2, dim), like(4 * wg.shape[0], wg.shape[1]), like(4 * wu.shape[0], wu.shape[1]), like(wd.shape[0], 4 * wd.shape[1])),
        in_specs=[VMEM, ANY, VMEM, VMEM, ANY, ANY, ANY],
        out_specs=(ANY,) * 5,
        scratch_shapes=bufs + [pltpu.VMEM(wg.shape, BF16), pltpu.VMEM(wd.shape, BF16), DMA, DMA, DMA, DMA((3,)), DMA((3,))] + sems + [DMA((3,)), DMA((3,)), DMA((6, 4)), DMA((6, 4))],
        compiler_params=params(1),
    )(part, xf, gain2, gain3, wg, wu, wd)


def last(part, hidden, gain4, k_own, v_own):
    seq, dim = part.shape
    bufs, sems = line_scratch(seq, dim)
    return pl.pallas_call(
        last_kernel,
        name='last',
        out_shape=(like(4 * seq, dim // 4), like(4 * seq, *k_own.shape[1:]), like(4 * seq, *v_own.shape[1:])),
        in_specs=[VMEM, ANY, VMEM, ANY, ANY],
        out_specs=(ANY,) * 3,
        scratch_shapes=bufs + [pltpu.VMEM(k_own.shape, BF16), pltpu.VMEM(v_own.shape, BF16), DMA, DMA((2,)), DMA((2,)), DMA((2, 3)), DMA((2, 3)), DMA((3,)), DMA((3,)), DMA] + sems,
        compiler_params=params(2),
    )(part, hidden, gain4, k_own, v_own)


def attend(q, k, v, cos_tab, sin_tab, pos, scale):
    heads, seq, head_dim = q.shape
    group = heads // k.shape[0]
    full = lambda shape: pl.BlockSpec(shape, lambda h: (0,) * len(shape))
    kv_spec = pl.BlockSpec((1, seq, head_dim), lambda h: (h // group, 0, 0))
    return pl.pallas_call(
        functools.partial(attend_kernel, scale),
        name='attend',
        grid=(heads,),
        out_shape=(like(seq, heads * head_dim), like(*k.shape)),
        in_specs=[pl.BlockSpec((1, seq, head_dim), lambda h: (h, 0, 0)), kv_spec, kv_spec, full(cos_tab.shape), full(sin_tab.shape), full((seq, 1)), full((1, seq))],
        out_specs=(pl.BlockSpec((seq, head_dim), lambda h: (0, h)), kv_spec),
        scratch_shapes=[pltpu.VMEM((seq, head_dim), BF16)],
        compiler_params=pltpu.CompilerParams(vmem_limit_bytes=VMEM_BYTES),
        cost_estimate=pl.CostEstimate(flops=4 * heads * seq * seq * head_dim, bytes_accessed=6 * heads * seq * head_dim, transcendentals=2 * heads * seq * seq),
    )(q, k, v, cos_tab, sin_tab, pos[:, None], pos[None, :])


def gate_up(m, wg, wu):
    seq, dim = m.shape
    hidden = wg.shape[1]
    tile = min(hidden, 512)
    w_spec = pl.BlockSpec((dim, tile), lambda f: (0, f))
    return pl.pallas_call(
        gate_kernel,
        name='gate_up',
        grid=(hidden // tile,),
        out_shape=like(seq, hidden),
        in_specs=[pl.BlockSpec((seq, dim), lambda f: (0, 0)), w_spec, w_spec],
        out_specs=pl.BlockSpec((seq, tile), lambda f: (0, f)),
        compiler_params=pltpu.CompilerParams(vmem_limit_bytes=VMEM_BYTES),
        cost_estimate=pl.CostEstimate(flops=4 * seq * dim * hidden, bytes_accessed=4 * dim * hidden, transcendentals=seq * hidden),
    )(m, wg, wu)


def solution(mesh):
    tp_size = mesh.shape['tp']

    def layer(tokens, positions, norm_pre_attn, w_query, w_key, w_value, w_out, norm_post_attn, norm_pre_ffw, w_gate, w_up, w_down, norm_post_ffw):
        seq = positions.shape[1]
        heads, head_dim, cols = w_out.shape
        dim = 4 * cols
        scale = (dim / (heads * tp_size)) ** -0.5
        norms = jnp.stack([norm_pre_attn, norm_post_attn, norm_pre_ffw, norm_post_ffw])
        xf, norms_all, wq, wk, wv, wo = fetch(tokens, norms, w_query, w_key, w_value, w_out.reshape(heads * head_dim, cols), seq)
        gains = 1.0 + jnp.swapaxes(norms_all, 0, 1).reshape(4, 1, dim).astype(F32)

        normed = lax.optimization_barrier(unit_rows(xf.astype(F32), gains[0]).astype(BF16))
        q, k, v = (jnp.einsum('nd,dhk->hnk', normed, w, preferred_element_type=F32).astype(BF16) for w in (wq, wk, wv))
        pos = lax.dynamic_index_in_dim(positions, lax.axis_index('dm'), 0, keepdims=False)
        half_dim = head_dim // 2
        inv_freq = ROPE_BASE ** (-2.0 * jnp.arange(half_dim, dtype=F32) / head_dim)
        angles = pos.astype(F32)[:, None] * inv_freq[None, :]
        attn_rows, k_rot = attend(q, k, v, jnp.cos(angles), jnp.sin(angles), pos, scale)

        attn_part = jnp.dot(attn_rows, wo, preferred_element_type=F32).astype(BF16)
        ffw_in, hidden, wg, wu, wd = middle(attn_part, xf, gains[1], gains[2], w_gate, w_up, w_down)
        gated = gate_up(ffw_in, wg, wu)
        down_part = jnp.dot(gated, wd, preferred_element_type=F32).astype(BF16)
        k_own, v_own = jnp.swapaxes(k_rot, 0, 1), jnp.swapaxes(v, 0, 1)
        return last(down_part, hidden, gains[3], k_own, v_own)

    width_spec = P('dm')
    in_specs = (P('dp', 'dm'), P('dp', None), width_spec, P('dm', 'tp', None), P('dm', 'tp', None), P('dm', 'tp', None), P('tp', None, 'dm'), width_spec, width_spec, P('dm', 'tp'), P('dm', 'tp'), P('tp', 'dm'), width_spec)
    out_specs = (P('dp', 'dm'), P('dp', 'tp', None), P('dp', 'tp', None))
    return jax.shard_map(layer, mesh=mesh, in_specs=in_specs, out_specs=out_specs, check_vma=False)
```

```python
import functools

import jax
import jax.numpy as jnp
from jax import lax
from jax.experimental import pallas as pl
from jax.experimental.pallas import tpu as pltpu
from jax.sharding import PartitionSpec as P

NORM_EPS = 1e-6
SOFT_CAP = 50.0
ROPE_BASE = 10000.0
WINDOW_LEN = 4096
BF16 = jnp.bfloat16
F32 = jnp.float32

CHUNK = 16
LAG = 2
LINE = 4
VMEM_BYTES = 62 * 1024 * 1024

ANY = pl.BlockSpec(memory_space=pl.ANY)
VMEM = pl.BlockSpec(memory_space=pltpu.VMEM)
DMA = pltpu.SemaphoreType.DMA


def places():
    row = lax.axis_index('dp')
    line = lax.axis_index('tp')
    me = lax.axis_index('dm')
    side = lax.div(me, 2)
    core = me - 2 * side
    return row, line, me, 2 * side + 1 - core, 2 * (1 - side) + core, 2 * (1 - side) + 1 - core


def remote(src, dst, send_sem, recv_sem, device):
    return pltpu.make_async_remote_copy(src_ref=src, dst_ref=dst, send_sem=send_sem, recv_sem=recv_sem, device_id=device, device_id_type=pl.DeviceIdType.MESH)


def meet(peers):
    barrier = pltpu.get_barrier_semaphore()
    for peer in peers:
        pl.semaphore_signal(barrier, inc=1, device_id=peer, device_id_type=pl.DeviceIdType.MESH)
    pl.semaphore_wait(barrier, len(peers))


def line_peers(line):
    return [{'tp': lax.rem(line + 1, LINE)}, {'tp': lax.rem(line + LINE - 1, LINE)}]


class Shard:
    def __init__(self, src, dst, by_rows, pieces):
        self.src, self.dst, self.by_rows, self.pieces = src, dst, by_rows, pieces
        self.rows = src.shape[0]
        self.unit = self.rows // (2 * pieces)

    def own(self, half, piece):
        return self.src.at[pl.ds(pl.multiple_of((half * self.pieces + piece) * self.unit, self.unit), self.unit)]

    def at(self, shard, half, piece):
        start = (half * self.pieces + piece) * self.unit
        if self.by_rows:
            return self.dst.at[pl.ds(pl.multiple_of(shard * self.rows + start, self.unit), self.unit)]
        cols = self.src.shape[1]
        return self.dst.at[pl.ds(pl.multiple_of(start, self.unit), self.unit), pl.ds(pl.multiple_of(shard * cols, cols), cols)]

    def whole(self, shard):
        if self.by_rows:
            return self.dst.at[pl.ds(pl.multiple_of(shard * self.rows, self.rows), self.rows)]
        cols = self.src.shape[1]
        return self.dst.at[:, pl.ds(pl.multiple_of(shard * cols, cols), cols)]


class WeightGather:
    def __init__(self, shards, own_send, own_recv, send, recv):
        self.shards, self.own_send, self.own_recv, self.send, self.recv = shards, own_send, own_recv, send, recv
        self.row, _, self.me, self.mate, self.across, self.cross = places()
        self.units = [(w, p) for w in range(len(shards)) for p in range(shards[w].pieces)]

    def copy(self, k, hop):
        w, p = self.units[k]
        shard = self.shards[w]
        mine, other = self.row, 1 - self.row
        if hop == 0:
            src, dst, device = shard.own(mine, p), shard.at(self.me, mine, p), {'dm': self.across}
        elif hop == 1:
            src = dst = shard.at(self.across, mine, p)
            device = {'dp': other}
        elif hop == 2:
            src = dst = shard.at(self.across, mine, p)
            device = {'dm': self.mate}
        else:
            src = dst = shard.at(self.across, other, p)
            device = {'dm': self.mate}
        return remote(src, dst, self.send.at[k, hop], self.recv.at[k, hop], device)

    def arrival(self, k, hop):
        w, p = self.units[k]
        shard = self.shards[w]
        mine, other = self.row, 1 - self.row
        region = (shard.at(self.across, mine, p), shard.at(self.across, other, p), shard.at(self.cross, mine, p), shard.at(self.cross, other, p))[hop]
        return remote(region, region, self.send.at[k, hop], self.recv.at[k, hop], {'dm': self.mate})

    def own_copy(self, w, shard_index):
        shard = self.shards[w]
        return remote(shard.src, shard.whole(shard_index), self.own_send.at[w], self.own_recv.at[w], {'dm': self.mate})

    def start(self):
        for k in range(len(self.units)):
            self.copy(k, 0).start()
        for w in range(len(self.shards)):
            self.own_copy(w, self.me).start()

    def pass_y(self, k):
        self.arrival(k, 0).wait_recv()
        self.copy(k, 1).start()
        self.copy(k, 2).start()

    def pass_x(self, k):
        self.arrival(k, 1).wait_recv()
        self.copy(k, 3).start()

    def settle_units(self, units, weights):
        for k in units:
            self.arrival(k, 2).wait_recv()
            self.arrival(k, 3).wait_recv()
            for hop in range(4):
                self.copy(k, hop).wait_send()
        for w in weights:
            self.own_copy(w, self.mate).wait_recv()
            self.own_copy(w, self.me).wait_send()


class LineSum:
    def __init__(self, p_buf, got, out, sum_send, sum_recv, out_send, out_recv, finish, emit):
        self.p_buf, self.got, self.out = p_buf, got, out
        self.sum_send, self.sum_recv, self.out_send, self.out_recv = sum_send, sum_recv, out_send, out_recv
        self.finish, self.emit = finish, emit
        self.half = p_buf.shape[0] // 2
        self.chunks = self.half // CHUNK
        self.steps = self.chunks + 6 * LAG
        self.line = lax.axis_index('tp')

    def way(self, d):
        if d == 0:
            return self.line, {'tp': self.line + 1}, {'tp': self.line - 1}
        return LINE - 1 - self.line, {'tp': self.line - 1}, {'tp': self.line + 1}

    def rows(self, c):
        return pl.ds(pl.multiple_of(c * CHUNK, CHUNK), CHUNK)

    def out_rows(self, d, c):
        return pl.ds(pl.multiple_of(d * self.half + c * CHUNK, CHUNK), CHUNK)

    def sum_copy(self, d, c):
        return remote(self.p_buf.at[self.out_rows(d, c)], self.got.at[d, self.rows(c)], self.sum_send.at[d, c], self.sum_recv.at[d, c], self.way(d)[1])

    def out_copy(self, d, c):
        region = self.out.at[self.out_rows(d, c)]
        return remote(region, region, self.out_send.at[d, c], self.out_recv.at[d, c], self.way(d)[2])

    def step(self, t):
        for d in range(2):
            self.sum_step(d, t)
        for d in range(2):
            self.out_step(d, t)

    def sum_step(self, d, t):
        pos = self.way(d)[0]
        c = t - LAG * pos

        @pl.when((c >= 0) & (c < self.chunks))
        def _():
            @pl.when(pos == 0)
            def _():
                self.sum_copy(d, c).start()

            @pl.when(pos > 0)
            def _():
                self.sum_copy(d, c).wait_recv()
                total = self.p_buf[self.out_rows(d, c), :].astype(F32) + self.got[d, self.rows(c), :].astype(F32)

                @pl.when(pos < LINE - 1)
                def _():
                    self.p_buf[self.out_rows(d, c), :] = total.astype(BF16)
                    self.sum_copy(d, c).start()

                @pl.when(pos == LINE - 1)
                def _():
                    self.finish(self.out_rows(d, c), self.rows(c), total.astype(BF16))
                    self.out_copy(d, c).start()
                    self.emit(self.out_rows(d, c))

    def out_step(self, d, t):
        pos = self.way(d)[0]
        c = t - 3 * LAG - LAG * (LINE - 1 - pos)

        @pl.when((c >= 0) & (c < self.chunks) & (pos < LINE - 1))
        def _():
            self.out_copy(d, c).wait_recv()

            @pl.when(pos > 0)
            def _():
                self.out_copy(d, c).start()

            self.emit(self.out_rows(d, c))

    def run(self, actions):
        def body(t, carry):
            for turn in sorted(actions):

                @pl.when(t == turn)
                def _():
                    for action in actions[turn]:
                        action()

            self.step(t)
            return carry

        lax.fori_loop(0, self.steps, body, 0)

    def settle(self):
        def body(c, carry):
            for d in range(2):
                pos = self.way(d)[0]

                @pl.when(pos < LINE - 1)
                def _():
                    self.sum_copy(d, c).wait_send()

                @pl.when(pos > 0)
                def _():
                    self.out_copy(d, c).wait_send()

            return carry

        lax.fori_loop(0, self.chunks, body, 0)


def unit_rows(values, gain):
    mean_sq = jnp.mean(values * values, axis=-1, keepdims=True)
    return values * lax.rsqrt(mean_sq + NORM_EPS) * gain


def rotate(values, cos_tab, sin_tab):
    half_dim = values.shape[-1] // 2
    lower = values[:, :half_dim].astype(F32)
    upper = values[:, half_dim:].astype(F32)
    return jnp.concatenate([lower * cos_tab - upper * sin_tab, upper * cos_tab + lower * sin_tab], axis=-1).astype(BF16)


def front_kernel(scale, kv_heads, head_dim, x_ref, n_ref, wqkv_ref, wo_ref, wg_ref, wu_ref, wd_ref, cos_ref, sin_ref, pos_col_ref, pos_row_ref, m_ref, h_ref, k_out_ref, v_out_ref, gain_ref, wgf_ref, wuf_ref, wdf_ref, xm_buf, w_buf, wo_buf, qkv_buf, o_buf, p_buf, got, res_buf, n_buf, x_send, x_recv, n_send, n_recv, z_send, z_recv, own_send, own_recv, w_send, w_recv, load_sem, keep_load, keep_store, m_sem, h_sem, kv_sem, sum_send, sum_recv, out_send, out_recv):
    row, line, me, mate, across, cross = places()
    seq, dim = xm_buf.shape
    cols = dim // 4
    half = seq // 2
    quarter = seq // LINE
    sub = quarter // 2
    heads = wo_ref.shape[0] // head_dim
    group = heads // kv_heads
    mine = pl.ds(pl.multiple_of(me * cols, cols), cols)
    shards = [Shard(wqkv_ref, w_buf, True, 4), Shard(wo_ref, wo_buf, False, 2), Shard(wg_ref, wgf_ref, True, 4), Shard(wu_ref, wuf_ref, True, 4), Shard(wd_ref, wdf_ref, False, 4)]
    gather = WeightGather(shards, own_send, own_recv, w_send, w_recv)
    first, out_first, ffw_first, units = 0, 4, 6, 18
    peers = (mate, across, cross)

    def x_copy(hop, s):
        dev = peers[hop]
        if hop == 0:
            src, dst = x_ref.at[pl.ds(pl.multiple_of(dev * seq, seq), seq)], xm_buf.at[:, mine]
        else:
            start = line * quarter + s * sub
            src = x_ref.at[pl.ds(pl.multiple_of(dev * seq + start, sub), sub)]
            dst = xm_buf.at[pl.ds(pl.multiple_of(start, sub), sub), mine]
        return remote(src, dst, x_send.at[hop, s], x_recv.at[hop, s], {'dm': dev})

    def x_arrival(hop, s):
        dev = peers[hop]
        theirs = pl.ds(pl.multiple_of(dev * cols, cols), cols)
        region = xm_buf.at[:, theirs] if hop == 0 else xm_buf.at[pl.ds(pl.multiple_of(line * quarter + s * sub, sub), sub), theirs]
        return remote(region, region, x_send.at[hop, s], x_recv.at[hop, s], {'dm': dev})

    far = pl.ds(pl.multiple_of((1 - lax.div(me, 2)) * 2 * cols, 2 * cols), 2 * cols)

    def z_copy(up, block, s):
        index = 2 * block + s
        region = xm_buf.at[pl.ds(pl.multiple_of(index * sub, sub), sub), far]
        device = {'tp': line + 1} if up else {'tp': line - 1}
        return remote(region, region, z_send.at[0 if up else 1, index], z_recv.at[index], device)

    def z_first(s):
        x_arrival(1, s).wait_recv()
        x_arrival(2, s).wait_recv()

        @pl.when(line < LINE - 1)
        def _():
            z_copy(True, line, s).start()

        @pl.when(line > 0)
        def _():
            z_copy(False, line, s).start()

    def z_step(step, s):
        below, above = line - step, line + step

        @pl.when(below >= 0)
        def _():
            z_copy(True, below, s).wait_recv()

            @pl.when(line < LINE - 1)
            def _():
                z_copy(True, below, s).start()

        @pl.when(above < LINE)
        def _():
            z_copy(False, above, s).wait_recv()

            @pl.when(line > 0)
            def _():
                z_copy(False, above, s).start()

    n_copies = [remote(n_ref, n_buf.at[me], n_send.at[i], n_recv.at[i], {'dm': dev}) for i, dev in enumerate(peers)]
    n_arrivals = [remote(n_ref, n_buf.at[dev], n_send.at[i], n_recv.at[i], {'dm': dev}) for i, dev in enumerate(peers)]
    loads = [
        pltpu.make_async_copy(x_ref.at[pl.ds(pl.multiple_of(me * seq, seq), seq)], xm_buf.at[:, mine], load_sem.at[0]),
        pltpu.make_async_copy(wqkv_ref, shards[0].whole(me), load_sem.at[1]),
        pltpu.make_async_copy(wo_ref, shards[1].whole(me), load_sem.at[2]),
        pltpu.make_async_copy(n_ref, n_buf.at[me], load_sem.at[3]),
    ]
    rows = wg_ref.shape[0]
    down_rows = wd_ref.shape[0] // 4
    keeps = []
    for w in (2, 3):
        keeps.append([(shards[w].src, p_buf.at[:rows], shards[w].whole(me))])
    keeps.append([(wd_ref.at[pl.ds(i * down_rows, down_rows)], p_buf.at[:down_rows, pl.ds(i * cols, cols)], wdf_ref.at[pl.ds(i * down_rows, down_rows), mine]) for i in range(4)])

    def keep(i, storing):
        moves = keeps[i]
        return [pltpu.make_async_copy(buf, dst, keep_store.at[n]) if storing else pltpu.make_async_copy(src, buf, keep_load.at[n]) for n, (src, buf, dst) in enumerate(moves)]

    def keep_load_start(i):
        for copy in keep(i, False):
            copy.start()

    def keep_store_start(i):
        for copy in keep(i, False):
            copy.wait()
        for copy in keep(i, True):
            copy.start()

    def keep_done(i):
        for copy in keep(i, True):
            copy.wait()

    meet([{'dm': mate}, {'dm': across}, {'dm': cross}, {'dp': 1 - row}] + line_peers(line))
    for s in range(2):
        x_copy(1, s).start()
        x_copy(2, s).start()
    x_copy(0, 0).start()
    for copy in n_copies:
        copy.start()
    gather.start()
    for load in loads:
        load.start()
    keep_load_start(0)
    z_first(0)
    keep_store_start(0)
    z_first(1)
    keep_done(0)
    keep_load_start(1)
    z_step(1, 0)
    gather.pass_y(0)
    keep_store_start(1)
    z_step(1, 1)
    gather.pass_y(1)
    keep_done(1)
    keep_load_start(2)
    z_step(2, 0)
    gather.pass_x(0)
    gather.pass_y(2)
    keep_store_start(2)
    z_step(2, 1)
    gather.pass_x(1)
    gather.pass_y(3)
    z_step(3, 0)
    gather.pass_x(2)
    for copy in n_arrivals:
        copy.wait_recv()
    for load in loads:
        load.wait()
    for shard in range(4):
        gain_ref[:, shard * cols:(shard + 1) * cols] = 1.0 + n_buf[shard]
    x_arrival(0, 0).wait_recv()
    z_step(3, 1)
    gather.pass_x(3)

    for block in range(LINE):
        for s in range(2):

            @pl.when((block <= line) & (line < LINE - 1))
            def _():
                z_copy(True, block, s).wait_send()

            @pl.when((block >= line) & (line > 0))
            def _():
                z_copy(False, block, s).wait_send()

    first_row = pl.multiple_of(half * (1 - jnp.minimum(line, 1)), half)
    res_buf[...] = xm_buf[pl.ds(first_row, half), :]
    norm_rows = min(seq, 64)

    def norm_body(i, carry):
        part = pl.ds(pl.multiple_of(i * norm_rows, norm_rows), norm_rows)
        xm_buf[part, :] = unit_rows(xm_buf[part, :].astype(F32), gain_ref[0:1, :]).astype(BF16)
        return carry

    lax.fori_loop(0, seq // norm_rows, norm_body, 0)
    gather.settle_units(range(0, 4), [0])
    gather.pass_y(4)
    gather.pass_y(5)
    keep_done(2)

    big = min(seq, 512)
    width = qkv_buf.shape[1]
    tile = min(width, 512)

    def qkv_body(i, carry):
        column = pl.ds(pl.multiple_of(lax.rem(i, width // tile) * tile, tile), tile)
        part = pl.ds(pl.multiple_of(lax.div(i, width // tile) * big, big), big)
        qkv_buf[part, column] = jnp.dot(xm_buf[part, :], w_buf[:, column], preferred_element_type=F32).astype(BF16)
        return carry

    lax.fori_loop(0, (width // tile) * (seq // big), qkv_body, 0)
    gather.pass_x(4)
    gather.pass_x(5)
    gather.pass_y(6)

    def rotate_body(i, carry):
        column = pl.ds(pl.multiple_of(i * head_dim, head_dim), head_dim)
        qkv_buf[:, column] = rotate(qkv_buf[:, column], cos_ref[...], sin_ref[...])
        return carry

    lax.fori_loop(0, heads + kv_heads, rotate_body, 0)
    kv_copies = []
    for i in range(kv_heads):
        for n, ref in enumerate((k_out_ref, v_out_ref)):
            start = (heads + n * kv_heads + i) * head_dim
            kv_copies.append(pltpu.make_async_copy(qkv_buf.at[:, pl.ds(start, head_dim)], ref.at[i], kv_sem.at[n, i]))
    for copy in kv_copies:
        copy.start()

    block = seq // 8
    d_tile = min(dim, 512)

    def attend_block(i):
        part = slice(i * block, (i + 1) * block)
        span = (i + 1) * block
        q_index = i * block + lax.broadcasted_iota(jnp.int32, (block, span), 0)
        key_index = lax.broadcasted_iota(jnp.int32, (block, span), 1)
        allowed = (key_index <= q_index) & (pos_col_ref[part, :] - pos_row_ref[:, :span] < WINDOW_LEN)

        def head_body(h, carry):
            q_cols = pl.ds(pl.multiple_of(h * head_dim, head_dim), head_dim)
            k_cols = pl.ds(pl.multiple_of((heads + lax.div(h, group)) * head_dim, head_dim), head_dim)
            v_cols = pl.ds(pl.multiple_of((heads + kv_heads + lax.div(h, group)) * head_dim, head_dim), head_dim)
            scores = lax.dot_general(qkv_buf[part, q_cols], qkv_buf[:span, k_cols], (((1,), (1,)), ((), ())), preferred_element_type=F32)
            capped = SOFT_CAP * jnp.tanh(scores * scale / SOFT_CAP)
            weights = jnp.where(allowed, jnp.exp(capped), 0.0)
            probs = (weights / jnp.sum(weights, axis=-1, keepdims=True)).astype(BF16)
            o_buf[part, q_cols] = jnp.dot(probs, qkv_buf[:span, v_cols], preferred_element_type=F32).astype(BF16)
            return carry

        lax.fori_loop(0, heads, head_body, 0)

    def out_block(i):
        part = slice(i * block, (i + 1) * block)

        def out_body(n, carry):
            column = pl.ds(pl.multiple_of(n * d_tile, d_tile), d_tile)
            p_buf[part, column] = jnp.dot(o_buf[part, :], wo_buf[:, column], preferred_element_type=F32).astype(BF16)
            return carry

        lax.fori_loop(0, dim // d_tile, out_body, 0)

    attend_block(0)
    attend_block(4)
    gather.settle_units(range(4, 6), [1])
    out_block(0)
    out_block(4)
    gather.pass_y(7)

    def finish(out_rows, rows, total):
        hidden = (res_buf[rows, :].astype(F32) + unit_rows(total.astype(F32), gain_ref[1:2, :])).astype(BF16)
        res_buf[rows, :] = hidden
        xm_buf[out_rows, :] = unit_rows(hidden.astype(F32), gain_ref[2:3, :]).astype(BF16)

    def emit(out_rows):
        pltpu.make_async_copy(xm_buf.at[out_rows], m_ref.at[out_rows], m_sem).start()

    sums = LineSum(p_buf, got, xm_buf, sum_send, sum_recv, out_send, out_recv, finish, emit)

    ahead = block // CHUNK
    actions = {}

    def at(t, action):
        actions.setdefault(min(max(t, 0), sums.steps - 1), []).append(action)

    def both(i):
        attend_block(i)
        out_block(i)

    for i in range(1, 4):
        at(i * ahead - (5 * ahead) // 8, functools.partial(both, i))
        at(i * ahead - (3 * ahead) // 8, functools.partial(both, 4 + i))
    turn = sums.steps / 44.0
    y_turns = (8, 11, 15, 18, 22, 25, 29, 32, 36, 41)
    for k in range(8, units):
        at(int(y_turns[k - 8] * turn), functools.partial(gather.pass_y, k))
    x_turns = (4, 9, 12, 16, 19, 23, 26, 30, 33, 38, 43)
    for k in range(6, units - 1):
        at(int(x_turns[k - 6] * turn), functools.partial(gather.pass_x, k))
    sums.run(actions)
    gather.pass_x(units - 1)

    h_store = pltpu.make_async_copy(res_buf, h_ref, h_sem)
    ends = (line == 0) | (line == LINE - 1)

    @pl.when(ends)
    def _():
        h_store.start()

    pltpu.make_async_copy(xm_buf, m_ref, m_sem).wait()
    sums.settle()
    gather.settle_units(range(6, units), [2, 3, 4])
    for copy in kv_copies:
        copy.wait()
    for copy in n_copies:
        copy.wait_send()
    x_copy(0, 0).wait_send()
    for s in range(2):
        x_copy(1, s).wait_send()
        x_copy(2, s).wait_send()

    @pl.when(ends)
    def _():
        h_store.wait()


def last_kernel(p_ref, h_ref, n4_ref, k_ref, v_ref, y_ref, kf_ref, vf_ref, p_buf, got, y_buf, res_buf, k_buf, v_buf, res_sem, kv_load, kv_store, kv_send, kv_recv, fin_send, fin_recv, own_sem, p_sem, sum_send, sum_recv, out_send, out_recv):
    row, line, me, mate, across, cross = places()
    seq = p_ref.shape[0]
    cols = y_ref.shape[1]
    res_load = pltpu.make_async_copy(h_ref, res_buf, res_sem)
    p_load = pltpu.make_async_copy(p_ref, p_buf, p_sem)
    ends = (line == 0) | (line == LINE - 1)
    caches = ((k_ref, kf_ref, k_buf), (v_ref, vf_ref, v_buf))

    def block(ref, shard):
        return ref.at[pl.ds(pl.multiple_of(shard * seq, seq), seq)]

    def kv_copy(i, hop):
        src, dst, _ = caches[i]
        if hop == 0:
            return remote(src, block(dst, me), kv_send.at[i, hop], kv_recv.at[i, hop], {'dm': across})
        if hop == 1:
            return remote(src, block(dst, me), kv_send.at[i, hop], kv_recv.at[i, hop], {'dm': mate})
        return remote(block(dst, across), block(dst, across), kv_send.at[i, hop], kv_recv.at[i, hop], {'dm': mate})

    def kv_arrival(i, hop):
        region = block(caches[i][1], (across, mate, cross)[hop])
        return remote(region, region, kv_send.at[i, hop], kv_recv.at[i, hop], {'dm': mate})

    kv_loads = [pltpu.make_async_copy(src, buf, kv_load.at[i]) for i, (src, _, buf) in enumerate(caches)]
    kv_stores = [pltpu.make_async_copy(buf, block(dst, me), kv_store.at[i]) for i, (_, dst, buf) in enumerate(caches)]

    def column(shard):
        return pl.ds(pl.multiple_of(shard * cols, cols), cols)

    def finish(out_rows, rows, total):
        y_buf[out_rows, :] = (res_buf[rows, :].astype(F32) + unit_rows(total.astype(F32), n4_ref[3:4, :])).astype(BF16)

    def emit(out_rows):
        start = out_rows.start
        there = pl.ds(pl.multiple_of(me * seq + start, CHUNK), CHUNK)
        for i, dev in enumerate((across, cross, mate)):
            remote(y_buf.at[out_rows, column(dev)], y_ref.at[there], fin_send.at[i], fin_recv.at[i], {'dm': dev}).start()
        pltpu.make_async_copy(y_buf.at[out_rows, column(me)], y_ref.at[there], own_sem).start()

    sums = LineSum(p_buf, got, y_buf, sum_send, sum_recv, out_send, out_recv, finish, emit)

    p_load.start()
    meet([{'dm': mate}, {'dm': across}, {'dm': cross}] + line_peers(line))

    @pl.when(ends)
    def _():
        res_load.start()

    for i in range(2):
        kv_loads[i].start()
        kv_copy(i, 0).start()
        kv_copy(i, 1).start()

    @pl.when(ends)
    def _():
        res_load.wait()

    p_load.wait()

    def keep_own():
        for i in range(2):
            kv_loads[i].wait()
            kv_stores[i].start()

    def pass_kv(i):
        kv_arrival(i, 0).wait_recv()
        kv_copy(i, 2).start()

    actions = {1: [keep_own], min(14, sums.steps - 2): [functools.partial(pass_kv, 0)], min(17, sums.steps - 1): [functools.partial(pass_kv, 1)]}
    sums.run(actions)
    sums.settle()
    for i in range(2):
        kv_stores[i].wait()
        for hop in range(3):
            kv_copy(i, hop).wait_send()
        kv_arrival(i, 1).wait_recv()
        kv_arrival(i, 2).wait_recv()
    for i, dev in enumerate((across, cross, mate)):
        done = remote(y_buf.at[:, column(dev)], block(y_ref, dev), fin_send.at[i], fin_recv.at[i], {'dm': dev})
        done.wait_send()
        done.wait_recv()
    pltpu.make_async_copy(y_buf.at[:, column(me)], block(y_ref, me), own_sem).wait()


def gate_kernel(m_ref, wg_ref, wu_ref, z_ref):
    block = min(m_ref.shape[0], 512)

    def body(i, carry):
        rows = pl.ds(pl.multiple_of(i * block, block), block)
        gate = jnp.dot(m_ref[rows, :], wg_ref[...], preferred_element_type=F32).astype(BF16).astype(F32)
        up = jnp.dot(m_ref[rows, :], wu_ref[...], preferred_element_type=F32).astype(BF16).astype(F32)
        z_ref[rows, :] = (jax.nn.gelu(gate, approximate=True) * up).astype(BF16)
        return carry

    lax.fori_loop(0, m_ref.shape[0] // block, body, 0)


def like(*shape, dtype=BF16):
    return jax.ShapeDtypeStruct(shape, dtype)


def params(collective_id):
    return pltpu.CompilerParams(collective_id=collective_id, has_side_effects=True, vmem_limit_bytes=VMEM_BYTES)


def line_scratch(seq, dim):
    chunks = seq // 2 // CHUNK
    return [DMA((2, chunks))] * 4


def front(x, norms, wqkv, wo, wg, wu, wd, cos_tab, sin_tab, pos, scale, kv_heads, head_dim):
    seq = pos.shape[0]
    cols = x.shape[1]
    dim = 4 * cols
    width = wqkv.shape[1]
    units = 18
    return pl.pallas_call(
        functools.partial(front_kernel, scale, kv_heads, head_dim),
        name='front',
        out_shape=(like(seq, dim), like(seq // 2, dim), like(kv_heads, seq, head_dim), like(kv_heads, seq, head_dim), like(8, dim, dtype=F32), like(4 * wg.shape[0], wg.shape[1]), like(4 * wu.shape[0], wu.shape[1]), like(wd.shape[0], 4 * wd.shape[1])),
        in_specs=[ANY] * 7 + [VMEM] * 4,
        out_specs=(ANY,) * 4 + (VMEM,) + (ANY,) * 3,
        scratch_shapes=[
            pltpu.VMEM((seq, dim), BF16), pltpu.VMEM((dim, width), BF16), pltpu.VMEM((wo.shape[0], dim), BF16), pltpu.VMEM((seq, width), BF16), pltpu.VMEM((seq, wo.shape[0]), BF16),
            pltpu.VMEM((seq, dim), BF16), pltpu.VMEM((2, seq // 2, dim), BF16), pltpu.VMEM((seq // 2, dim), BF16), pltpu.VMEM((4,) + norms.shape, F32),
            DMA((3, 2)), DMA((3, 2)), DMA((3,)), DMA((3,)), DMA((2, 2 * LINE)), DMA((2 * LINE,)), DMA((5,)), DMA((5,)), DMA((units, 4)), DMA((units, 4)), DMA((4,)), DMA((4,)), DMA((4,)), DMA, DMA, DMA((2, kv_heads)),
        ] + line_scratch(seq, dim),
        compiler_params=params(0),
    )(x, norms, wqkv, wo, wg, wu, wd, cos_tab, sin_tab, pos[:, None], pos[None, :])


def last(part, hidden, gains, k_own, v_own):
    seq, dim = part.shape
    return pl.pallas_call(
        last_kernel,
        name='last',
        out_shape=(like(4 * seq, dim // 4), like(4 * seq, *k_own.shape[1:]), like(4 * seq, *v_own.shape[1:])),
        in_specs=[ANY, ANY, VMEM, ANY, ANY],
        out_specs=(ANY,) * 3,
        scratch_shapes=[pltpu.VMEM((seq, dim), BF16), pltpu.VMEM((2, seq // 2, dim), BF16), pltpu.VMEM((seq, dim), BF16), pltpu.VMEM((seq // 2, dim), BF16), pltpu.VMEM(k_own.shape, BF16), pltpu.VMEM(v_own.shape, BF16), DMA, DMA((2,)), DMA((2,)), DMA((2, 3)), DMA((2, 3)), DMA((3,)), DMA((3,)), DMA, DMA] + line_scratch(seq, dim),
        compiler_params=params(2),
    )(part, hidden, gains, k_own, v_own)


def gate_up(m, wg, wu):
    seq, dim = m.shape
    hidden = wg.shape[1]
    tile = min(hidden, 512)
    w_spec = pl.BlockSpec((dim, tile), lambda f: (0, f))
    return pl.pallas_call(
        gate_kernel,
        name='gate_up',
        grid=(hidden // tile,),
        out_shape=like(seq, hidden),
        in_specs=[pl.BlockSpec((seq, dim), lambda f: (0, 0)), w_spec, w_spec],
        out_specs=pl.BlockSpec((seq, tile), lambda f: (0, f)),
        compiler_params=pltpu.CompilerParams(vmem_limit_bytes=VMEM_BYTES),
        cost_estimate=pl.CostEstimate(flops=4 * seq * dim * hidden, bytes_accessed=4 * dim * hidden, transcendentals=seq * hidden),
    )(m, wg, wu)


def solution(mesh):
    tp_size = mesh.shape['tp']

    def layer(tokens, positions, norm_pre_attn, w_query, w_key, w_value, w_out, norm_post_attn, norm_pre_ffw, w_gate, w_up, w_down, norm_post_ffw):
        seq = positions.shape[1]
        heads, head_dim, cols = w_out.shape
        dim = 4 * cols
        scale = (dim / (heads * tp_size)) ** -0.5
        norms = jnp.stack([norm_pre_attn, norm_post_attn, norm_pre_ffw, norm_post_ffw]).astype(F32)
        norms = jnp.concatenate([norms, jnp.zeros_like(norms)])
        wqkv = jnp.concatenate([w.reshape(w.shape[0], -1) for w in (w_query, w_key, w_value)], axis=1)
        pos = lax.dynamic_index_in_dim(positions, lax.axis_index('dm'), 0, keepdims=False)
        half_dim = head_dim // 2
        inv_freq = ROPE_BASE ** (-2.0 * jnp.arange(half_dim, dtype=F32) / head_dim)
        angles = pos.astype(F32)[:, None] * inv_freq[None, :]
        ffw_in, hidden, k_rot, v, gains, wg, wu, wd = front(tokens, norms, wqkv, w_out.reshape(heads * head_dim, cols), w_gate, w_up, w_down, jnp.cos(angles), jnp.sin(angles), pos, scale, w_key.shape[1], head_dim)
        gated = gate_up(ffw_in, wg, wu)
        down_part = jnp.dot(gated, wd, preferred_element_type=F32).astype(BF16)
        k_own, v_own = jnp.swapaxes(k_rot, 0, 1), jnp.swapaxes(v, 0, 1)
        return last(down_part, hidden, gains, k_own, v_own)

    width_spec = P('dm')
    in_specs = (P('dp', 'dm'), P('dp', None), width_spec, P('dm', 'tp', None), P('dm', 'tp', None), P('dm', 'tp', None), P('tp', None, 'dm'), width_spec, width_spec, P('dm', 'tp'), P('dm', 'tp'), P('tp', 'dm'), width_spec)
    out_specs = (P('dp', 'dm'), P('dp', 'tp', None), P('dp', 'tp', None))
    return jax.shard_map(layer, mesh=mesh, in_specs=in_specs, out_specs=out_specs, check_vma=False)
```

```python
import functools

import jax
import jax.numpy as jnp
from jax import lax
from jax.experimental import pallas as pl
from jax.experimental.pallas import tpu as pltpu
from jax.sharding import PartitionSpec as P

NORM_EPS = 1e-6
SOFT_CAP = 50.0
ROPE_BASE = 10000.0
WINDOW_LEN = 4096
BF16 = jnp.bfloat16
F32 = jnp.float32

CHUNK = 16
LAG = 2
LINE = 4
VMEM_BYTES = 67043328

ANY = pl.BlockSpec(memory_space=pl.ANY)
VMEM = pl.BlockSpec(memory_space=pltpu.VMEM)
DMA = pltpu.SemaphoreType.DMA


def places():
    row = lax.axis_index('dp')
    line = lax.axis_index('tp')
    me = lax.axis_index('dm')
    side = lax.div(me, 2)
    core = me - 2 * side
    return row, line, me, 2 * side + 1 - core, 2 * (1 - side) + core, 2 * (1 - side) + 1 - core


def remote(src, dst, send_sem, recv_sem, device):
    return pltpu.make_async_remote_copy(src_ref=src, dst_ref=dst, send_sem=send_sem, recv_sem=recv_sem, device_id=device, device_id_type=pl.DeviceIdType.MESH)


def meet(peers):
    barrier = pltpu.get_barrier_semaphore()
    for peer in peers:
        pl.semaphore_signal(barrier, inc=1, device_id=peer, device_id_type=pl.DeviceIdType.MESH)
    pl.semaphore_wait(barrier, len(peers))


def line_peers(line):
    return [{'tp': lax.rem(line + 1, LINE)}, {'tp': lax.rem(line + LINE - 1, LINE)}]


class Shard:
    def __init__(self, src, dst, by_rows, pieces):
        self.src, self.dst, self.by_rows, self.pieces = src, dst, by_rows, pieces
        self.rows = src.shape[0]
        self.unit = self.rows // (2 * pieces)

    def own(self, half, piece):
        return self.src.at[pl.ds(pl.multiple_of((half * self.pieces + piece) * self.unit, self.unit), self.unit)]

    def at(self, shard, half, piece):
        start = (half * self.pieces + piece) * self.unit
        if self.by_rows:
            return self.dst.at[pl.ds(pl.multiple_of(shard * self.rows + start, self.unit), self.unit)]
        cols = self.src.shape[1]
        return self.dst.at[pl.ds(pl.multiple_of(start, self.unit), self.unit), pl.ds(pl.multiple_of(shard * cols, cols), cols)]

    def whole(self, shard):
        if self.by_rows:
            return self.dst.at[pl.ds(pl.multiple_of(shard * self.rows, self.rows), self.rows)]
        cols = self.src.shape[1]
        return self.dst.at[:, pl.ds(pl.multiple_of(shard * cols, cols), cols)]


class WeightGather:
    def __init__(self, shards, own_send, own_recv, send, recv):
        self.shards, self.own_send, self.own_recv, self.send, self.recv = shards, own_send, own_recv, send, recv
        self.row, _, self.me, self.mate, self.across, self.cross = places()
        self.units = [(w, p) for w in range(len(shards)) for p in range(shards[w].pieces)]

    def copy(self, k, hop):
        w, p = self.units[k]
        shard = self.shards[w]
        mine, other = self.row, 1 - self.row
        if hop == 0:
            src, dst, device = shard.own(mine, p), shard.at(self.me, mine, p), {'dm': self.across}
        elif hop == 1:
            src = dst = shard.at(self.across, mine, p)
            device = {'dp': other}
        elif hop == 2:
            src = dst = shard.at(self.across, mine, p)
            device = {'dm': self.mate}
        else:
            src = dst = shard.at(self.across, other, p)
            device = {'dm': self.mate}
        return remote(src, dst, self.send.at[k, hop], self.recv.at[k, hop], device)

    def arrival(self, k, hop):
        w, p = self.units[k]
        shard = self.shards[w]
        mine, other = self.row, 1 - self.row
        region = (shard.at(self.across, mine, p), shard.at(self.across, other, p), shard.at(self.cross, mine, p), shard.at(self.cross, other, p))[hop]
        return remote(region, region, self.send.at[k, hop], self.recv.at[k, hop], {'dm': self.mate})

    def own_copy(self, w, shard_index):
        shard = self.shards[w]
        return remote(shard.src, shard.whole(shard_index), self.own_send.at[w], self.own_recv.at[w], {'dm': self.mate})

    def start(self):
        for k in range(len(self.units)):
            self.copy(k, 0).start()
        for w in range(len(self.shards)):
            self.own_copy(w, self.me).start()

    def pass_y(self, k):
        self.arrival(k, 0).wait_recv()
        self.copy(k, 1).start()
        self.copy(k, 2).start()

    def pass_x(self, k):
        self.arrival(k, 1).wait_recv()
        self.copy(k, 3).start()

    def settle_units(self, units, weights):
        for k in units:
            self.arrival(k, 2).wait_recv()
            self.arrival(k, 3).wait_recv()
            for hop in range(4):
                self.copy(k, hop).wait_send()
        for w in weights:
            self.own_copy(w, self.mate).wait_recv()
            self.own_copy(w, self.me).wait_send()


class LineSum:
    def __init__(self, p_buf, got, out, sum_send, sum_recv, out_send, out_recv, finish, emit):
        self.p_buf, self.got, self.out = p_buf, got, out
        self.sum_send, self.sum_recv, self.out_send, self.out_recv = sum_send, sum_recv, out_send, out_recv
        self.finish, self.emit = finish, emit
        self.half = p_buf.shape[0] // 2
        self.chunks = self.half // CHUNK
        self.steps = self.chunks + 6 * LAG
        self.line = lax.axis_index('tp')

    def way(self, d):
        if d == 0:
            return self.line, {'tp': self.line + 1}, {'tp': self.line - 1}
        return LINE - 1 - self.line, {'tp': self.line - 1}, {'tp': self.line + 1}

    def rows(self, c):
        return pl.ds(pl.multiple_of(c * CHUNK, CHUNK), CHUNK)

    def out_rows(self, d, c):
        return pl.ds(pl.multiple_of(d * self.half + c * CHUNK, CHUNK), CHUNK)

    def sum_copy(self, d, c):
        return remote(self.p_buf.at[self.out_rows(d, c)], self.got.at[d, self.rows(c)], self.sum_send.at[d, c], self.sum_recv.at[d, c], self.way(d)[1])

    def out_copy(self, d, c):
        region = self.out.at[self.out_rows(d, c)]
        return remote(region, region, self.out_send.at[d, c], self.out_recv.at[d, c], self.way(d)[2])

    def step(self, t):
        for d in range(2):
            self.sum_step(d, t)
        for d in range(2):
            self.out_step(d, t)

    def sum_step(self, d, t):
        pos = self.way(d)[0]
        c = t - LAG * pos

        @pl.when((c >= 0) & (c < self.chunks))
        def _():
            @pl.when(pos == 0)
            def _():
                self.sum_copy(d, c).start()

            @pl.when(pos > 0)
            def _():
                self.sum_copy(d, c).wait_recv()
                total = self.p_buf[self.out_rows(d, c), :].astype(F32) + self.got[d, self.rows(c), :].astype(F32)

                @pl.when(pos < LINE - 1)
                def _():
                    self.p_buf[self.out_rows(d, c), :] = total.astype(BF16)
                    self.sum_copy(d, c).start()

                @pl.when(pos == LINE - 1)
                def _():
                    self.finish(self.out_rows(d, c), self.rows(c), total.astype(BF16))
                    self.out_copy(d, c).start()
                    self.emit(self.out_rows(d, c))

    def out_step(self, d, t):
        pos = self.way(d)[0]
        c = t - 3 * LAG - LAG * (LINE - 1 - pos)

        @pl.when((c >= 0) & (c < self.chunks) & (pos < LINE - 1))
        def _():
            self.out_copy(d, c).wait_recv()

            @pl.when(pos > 0)
            def _():
                self.out_copy(d, c).start()

            self.emit(self.out_rows(d, c))

    def run(self, actions, each):
        def body(t, carry):
            for turn in sorted(actions):

                @pl.when(t == turn)
                def _():
                    for action in actions[turn]:
                        action()

            each(t)
            self.step(t)
            return carry

        lax.fori_loop(0, self.steps, body, 0)

    def settle(self):
        def body(c, carry):
            for d in range(2):
                pos = self.way(d)[0]

                @pl.when(pos < LINE - 1)
                def _():
                    self.sum_copy(d, c).wait_send()

                @pl.when(pos > 0)
                def _():
                    self.out_copy(d, c).wait_send()

            return carry

        lax.fori_loop(0, self.chunks, body, 0)


def unit_rows(values, gain):
    mean_sq = jnp.mean(values * values, axis=-1, keepdims=True)
    return values * lax.rsqrt(mean_sq + NORM_EPS) * gain


def rotate(values, cos_tab, sin_tab):
    half_dim = values.shape[-1] // 2
    lower = values[:, :half_dim].astype(F32)
    upper = values[:, half_dim:].astype(F32)
    return jnp.concatenate([lower * cos_tab - upper * sin_tab, upper * cos_tab + lower * sin_tab], axis=-1).astype(BF16)


def layer_kernel(scale, kv_heads, head_dim, x_ref, n_ref, wq_ref, wk_ref, wv_ref, wo_ref, wg_ref, wu_ref, wd_ref, cos_ref, sin_ref, pos_col_ref, pos_row_ref, y_ref, kf_ref, vf_ref, wgf_ref, wuf_ref, wdf_ref, xm_buf, w_buf, wo_buf, qkv_buf, p_buf, got, res_buf, n_buf, gain_buf, wq_buf, wk_buf, wv_buf, k_buf, v_buf, x_send, x_recv, n_send, n_recv, z_send, z_recv, own_send, own_recv, w_send, w_recv, load_sem, keep_load, keep_store, tile_sem, kv_store, kv_send, kv_recv, fin_send, fin_recv, fin_own, *line_sems):
    row, line, me, mate, across, cross = places()
    seq, dim = xm_buf.shape
    cols = dim // 4
    half = seq // 2
    quarter = seq // LINE
    sub = quarter // 2
    heads = wo_ref.shape[0] // head_dim
    group = heads // kv_heads
    mine = pl.ds(pl.multiple_of(me * cols, cols), cols)
    own_rows = w_buf.at[pl.ds(pl.multiple_of(me * cols, cols), cols)]
    shards = [Shard(own_rows, w_buf, True, 4), Shard(wo_ref, wo_buf, False, 2), Shard(wg_ref, wgf_ref, True, 4), Shard(wu_ref, wuf_ref, True, 4), Shard(wd_ref, wdf_ref, False, 4)]
    gather = WeightGather(shards, own_send, own_recv, w_send, w_recv)
    units = 18
    peers = (mate, across, cross)

    def x_copy(hop, s):
        dev = peers[hop]
        if hop == 0:
            src, dst = x_ref.at[pl.ds(pl.multiple_of(dev * seq, seq), seq)], xm_buf.at[:, mine]
        else:
            start = line * quarter + s * sub
            src = x_ref.at[pl.ds(pl.multiple_of(dev * seq + start, sub), sub)]
            dst = xm_buf.at[pl.ds(pl.multiple_of(start, sub), sub), mine]
        return remote(src, dst, x_send.at[hop, s], x_recv.at[hop, s], {'dm': dev})

    def x_arrival(hop, s):
        dev = peers[hop]
        theirs = pl.ds(pl.multiple_of(dev * cols, cols), cols)
        region = xm_buf.at[:, theirs] if hop == 0 else xm_buf.at[pl.ds(pl.multiple_of(line * quarter + s * sub, sub), sub), theirs]
        return remote(region, region, x_send.at[hop, s], x_recv.at[hop, s], {'dm': dev})

    far = pl.ds(pl.multiple_of((1 - lax.div(me, 2)) * 2 * cols, 2 * cols), 2 * cols)

    def z_copy(up, block, s):
        index = 2 * block + s
        region = xm_buf.at[pl.ds(pl.multiple_of(index * sub, sub), sub), far]
        device = {'tp': line + 1} if up else {'tp': line - 1}
        return remote(region, region, z_send.at[0 if up else 1, index], z_recv.at[index], device)

    def z_first(s):
        x_arrival(1, s).wait_recv()
        x_arrival(2, s).wait_recv()

        @pl.when(line < LINE - 1)
        def _():
            z_copy(True, line, s).start()

        @pl.when(line > 0)
        def _():
            z_copy(False, line, s).start()

    def z_step(step, s):
        below, above = line - step, line + step

        @pl.when(below >= 0)
        def _():
            z_copy(True, below, s).wait_recv()

            @pl.when(line < LINE - 1)
            def _():
                z_copy(True, below, s).start()

        @pl.when(above < LINE)
        def _():
            z_copy(False, above, s).wait_recv()

            @pl.when(line > 0)
            def _():
                z_copy(False, above, s).start()

    n_copies = [remote(n_ref, n_buf.at[me], n_send.at[i], n_recv.at[i], {'dm': dev}) for i, dev in enumerate(peers)]
    n_arrivals = [remote(n_ref, n_buf.at[dev], n_send.at[i], n_recv.at[i], {'dm': dev}) for i, dev in enumerate(peers)]
    loads = [
        pltpu.make_async_copy(x_ref.at[pl.ds(pl.multiple_of(me * seq, seq), seq)], xm_buf.at[:, mine], load_sem.at[0]),
        pltpu.make_async_copy(wo_ref, shards[1].whole(me), load_sem.at[1]),
        pltpu.make_async_copy(n_ref, n_buf.at[me], load_sem.at[2]),
    ]
    thirds = ((wq_ref, wq_buf), (wk_ref, wk_buf), (wv_ref, wv_buf))
    third_loads = [pltpu.make_async_copy(src, buf, load_sem.at[3 + i]) for i, (src, buf) in enumerate(thirds)]

    def flatten_own():
        for load in third_loads:
            load.wait()
        flat_rows = min(cols, 64)

        def body(i, carry):
            part = pl.ds(pl.multiple_of(i * flat_rows, flat_rows), flat_rows)
            there = pl.ds(pl.multiple_of(me * cols + i * flat_rows, flat_rows), flat_rows)
            start = 0
            for _, buf in thirds:
                wide = buf.shape[1] * buf.shape[2]
                w_buf[there, start:start + wide] = buf[part].reshape(flat_rows, wide)
                start += wide
            return carry

        lax.fori_loop(0, cols // flat_rows, body, 0)

    rows = wg_ref.shape[0]
    down_rows = wd_ref.shape[0] // 4
    keeps = []
    for w in (2, 3):
        keeps.append([(shards[w].src, p_buf.at[:rows], shards[w].whole(me))])
    keeps.append([(wd_ref.at[pl.ds(i * down_rows, down_rows)], p_buf.at[:down_rows, pl.ds(i * cols, cols)], wdf_ref.at[pl.ds(i * down_rows, down_rows), mine]) for i in range(4)])

    def keep(i, storing):
        moves = keeps[i]
        return [pltpu.make_async_copy(buf, dst, keep_store.at[n]) if storing else pltpu.make_async_copy(src, buf, keep_load.at[n]) for n, (src, buf, dst) in enumerate(moves)]

    def keep_load_start(i):
        for copy in keep(i, False):
            copy.start()

    def keep_store_start(i):
        for copy in keep(i, False):
            copy.wait()
        for copy in keep(i, True):
            copy.start()

    def keep_done(i):
        for copy in keep(i, True):
            copy.wait()

    for load in third_loads:
        load.start()
    meet([{'dm': mate}, {'dm': across}, {'dm': cross}, {'dp': 1 - row}] + line_peers(line))
    for s in range(2):
        x_copy(1, s).start()
        x_copy(2, s).start()
    x_copy(0, 0).start()
    for copy in n_copies:
        copy.start()
    for load in loads:
        load.start()
    flatten_own()
    gather.start()
    keep_load_start(0)
    z_first(0)
    keep_store_start(0)
    z_first(1)
    keep_done(0)
    keep_load_start(1)
    z_step(1, 0)
    gather.pass_y(0)
    keep_store_start(1)
    z_step(1, 1)
    gather.pass_y(1)
    keep_done(1)
    keep_load_start(2)
    z_step(2, 0)
    gather.pass_x(0)
    gather.pass_y(2)
    keep_store_start(2)
    z_step(2, 1)
    gather.pass_x(1)
    gather.pass_y(3)
    z_step(3, 0)
    gather.pass_x(2)
    for copy in n_arrivals:
        copy.wait_recv()
    for load in loads:
        load.wait()
    for shard in range(4):
        gain_buf[:, shard * cols:(shard + 1) * cols] = 1.0 + n_buf[shard]
    x_arrival(0, 0).wait_recv()
    z_step(3, 1)
    gather.pass_x(3)

    for block in range(LINE):
        for s in range(2):

            @pl.when((block <= line) & (line < LINE - 1))
            def _():
                z_copy(True, block, s).wait_send()

            @pl.when((block >= line) & (line > 0))
            def _():
                z_copy(False, block, s).wait_send()

    first_row = pl.multiple_of(half * (1 - jnp.minimum(line, 1)), half)
    res_buf[...] = xm_buf[pl.ds(first_row, half), :]
    norm_rows = min(seq, 64)

    def norm_body(i, carry):
        part = pl.ds(pl.multiple_of(i * norm_rows, norm_rows), norm_rows)
        xm_buf[part, :] = unit_rows(xm_buf[part, :].astype(F32), gain_buf[0:1, :]).astype(BF16)
        return carry

    lax.fori_loop(0, seq // norm_rows, norm_body, 0)
    gather.settle_units(range(0, 4), [0])
    gather.pass_y(4)
    gather.pass_y(5)
    keep_done(2)

    big = min(seq, 512)
    width = qkv_buf.shape[1]
    tile = min(width, 512)

    def qkv_body(i, carry):
        column = pl.ds(pl.multiple_of(lax.rem(i, width // tile) * tile, tile), tile)
        part = pl.ds(pl.multiple_of(lax.div(i, width // tile) * big, big), big)
        qkv_buf[part, column] = jnp.dot(xm_buf[part, :], w_buf[:, column], preferred_element_type=F32).astype(BF16)
        return carry

    lax.fori_loop(0, (width // tile) * (seq // big), qkv_body, 0)
    gather.pass_x(4)
    gather.pass_x(5)
    gather.pass_y(6)

    def rotate_body(i, carry):
        column = pl.ds(pl.multiple_of(i * head_dim, head_dim), head_dim)
        qkv_buf[:, column] = rotate(qkv_buf[:, column], cos_ref[...], sin_ref[...])
        return carry

    lax.fori_loop(0, heads + kv_heads, rotate_body, 0)
    def cache_body(i, carry):
        part = pl.ds(pl.multiple_of(i * norm_rows, norm_rows), norm_rows)
        wide = kv_heads * head_dim
        for n, buf in enumerate((k_buf, v_buf)):
            start = heads * head_dim + n * wide
            buf[part] = qkv_buf[part, start:start + wide].reshape(norm_rows, kv_heads, head_dim)
        return carry

    lax.fori_loop(0, seq // norm_rows, cache_body, 0)

    block = seq // 8
    d_tile = min(dim, 512)

    def attend_block(i):
        part = slice(i * block, (i + 1) * block)
        span = (i + 1) * block
        q_index = i * block + lax.broadcasted_iota(jnp.int32, (block, span), 0)
        key_index = lax.broadcasted_iota(jnp.int32, (block, span), 1)
        allowed = (key_index <= q_index) & (pos_col_ref[part, :] - pos_row_ref[:, :span] < WINDOW_LEN)

        def head_body(h, carry):
            q_cols = pl.ds(pl.multiple_of(h * head_dim, head_dim), head_dim)
            k_cols = pl.ds(pl.multiple_of((heads + lax.div(h, group)) * head_dim, head_dim), head_dim)
            v_cols = pl.ds(pl.multiple_of((heads + kv_heads + lax.div(h, group)) * head_dim, head_dim), head_dim)
            scores = lax.dot_general(qkv_buf[part, q_cols], qkv_buf[:span, k_cols], (((1,), (1,)), ((), ())), preferred_element_type=F32)
            capped = SOFT_CAP * jnp.tanh(scores * scale / SOFT_CAP)
            weights = jnp.where(allowed, jnp.exp(capped), 0.0)
            probs = (weights / jnp.sum(weights, axis=-1, keepdims=True)).astype(BF16)
            qkv_buf[part, q_cols] = jnp.dot(probs, qkv_buf[:span, v_cols], preferred_element_type=F32).astype(BF16)
            return carry

        lax.fori_loop(0, heads, head_body, 0)

    def out_block(i):
        part = slice(i * block, (i + 1) * block)

        def out_body(n, carry):
            column = pl.ds(pl.multiple_of(n * d_tile, d_tile), d_tile)
            p_buf[part, column] = jnp.dot(qkv_buf[part, :heads * head_dim], wo_buf[:, column], preferred_element_type=F32).astype(BF16)
            return carry

        lax.fori_loop(0, dim // d_tile, out_body, 0)

    attend_block(0)
    attend_block(4)
    gather.settle_units(range(4, 6), [1])
    out_block(0)
    out_block(4)
    gather.pass_y(7)

    def finish(out_rows, rows, total):
        hidden = (res_buf[rows, :].astype(F32) + unit_rows(total.astype(F32), gain_buf[1:2, :])).astype(BF16)
        res_buf[rows, :] = hidden
        xm_buf[out_rows, :] = unit_rows(hidden.astype(F32), gain_buf[2:3, :]).astype(BF16)

    sums = LineSum(p_buf, got, xm_buf, *line_sems[:4], finish, lambda out_rows: None)

    ahead = block // CHUNK
    actions = {}

    def at(t, action):
        actions.setdefault(min(max(t, 0), sums.steps - 1), []).append(action)

    def both(i):
        attend_block(i)
        out_block(i)

    for i in range(1, 4):
        at(i * ahead - (5 * ahead) // 8, functools.partial(both, i))
        at(i * ahead - (3 * ahead) // 8, functools.partial(both, 4 + i))

    hidden_cols = wgf_ref.shape[1]
    tile = min(hidden_cols // 2, 512)
    tiles = hidden_cols // tile
    span_rows = half // 4
    z_buf = wo_buf

    def group_rows(g):
        return [pl.ds(pl.multiple_of(d * half + g * span_rows, span_rows), span_rows) for d in range(2)]

    def slot_cols(slot):
        return pl.ds(pl.multiple_of(slot * tile, tile), tile)

    def gate_loads(i):
        column = pl.ds(pl.multiple_of(lax.rem(i, tiles) * tile, tile), tile)
        slot = 2 * lax.rem(i, 2)
        return [pltpu.make_async_copy(ref.at[:, column], w_buf.at[:, slot_cols(slot + n)], tile_sem.at[slot + n]) for n, ref in enumerate((wgf_ref, wuf_ref))]

    def gate_item(i):
        for load in gate_loads(i):
            load.wait()

        @pl.when(i + 1 < 4 * tiles)
        def _():
            for load in gate_loads(i + 1):
                load.start()

        slot = 2 * lax.rem(i, 2)
        parts = group_rows(lax.div(i, tiles))
        column = pl.ds(pl.multiple_of(lax.rem(i, tiles) * tile, tile), tile)
        ffw_in = jnp.concatenate([xm_buf[part, :] for part in parts], axis=0)
        gate = jnp.dot(ffw_in, w_buf[:, slot_cols(slot)], preferred_element_type=F32).astype(BF16).astype(F32)
        up = jnp.dot(ffw_in, w_buf[:, slot_cols(slot + 1)], preferred_element_type=F32).astype(BF16).astype(F32)
        gated = (jax.nn.gelu(gate, approximate=True) * up).astype(BF16)
        for d, part in enumerate(parts):
            z_buf[part, column] = gated[d * span_rows:(d + 1) * span_rows]

    ready = [(g + 1) * (sums.chunks // 4) + 6 * LAG for g in range(3)]
    gate_start = max(max(ready[g] - (tiles * g) // 2 for g in range(3)), int(29 * sums.steps / 44))
    gate_inside = max(0, min(3 * tiles, 2 * (sums.steps - gate_start)))

    def open_gate():
        gather.settle_units(range(6, 14), [2, 3])
        for load in gate_loads(0):
            load.start()

    turn = sums.steps / 44.0
    y_turns = (8, 11, 15, 18, 22, 25, 29, 31, 34, 37)
    for k in range(8, units):
        at(int(y_turns[k - 8] * turn), functools.partial(gather.pass_y, k))
    x_turns = (4, 9, 12, 16, 19, 23, 26, 28, 31, 34, 37, 40)
    for k in range(6, units):
        at(int(x_turns[k - 6] * turn), functools.partial(gather.pass_x, k))
    at(gate_start, open_gate)

    def each_first(t):
        for n in range(2):
            i = 2 * (t - gate_start) + n

            @pl.when((i >= 0) & (i < gate_inside))
            def _():
                gate_item(i)

    sums.run(actions, each_first)

    def gate_body(i, carry):
        gate_item(i)
        return carry

    lax.fori_loop(gate_inside, 4 * tiles, gate_body, 0)
    sums.settle()
    gather.settle_units(range(14, units), [4])

    d_tiles = dim // tile

    def down_load(i):
        column = pl.ds(pl.multiple_of(lax.rem(i, d_tiles) * tile, tile), tile)
        slot = lax.rem(i, 4)
        return pltpu.make_async_copy(wdf_ref.at[:, column], w_buf.at[:, slot_cols(slot)], tile_sem.at[slot])

    def down_item(i):
        down_load(i).wait()

        @pl.when(i + 2 < 4 * d_tiles)
        def _():
            down_load(i + 2).start()

        parts = group_rows(lax.div(i, d_tiles))
        column = pl.ds(pl.multiple_of(lax.rem(i, d_tiles) * tile, tile), tile)
        gated = jnp.concatenate([z_buf[part, :] for part in parts], axis=0)
        down = jnp.dot(gated, w_buf[:, slot_cols(lax.rem(i, 4))], preferred_element_type=F32).astype(BF16)
        for d, part in enumerate(parts):
            p_buf[part, column] = down[d * span_rows:(d + 1) * span_rows]

    down_load(0).start()
    down_load(1).start()

    caches = ((k_buf, kf_ref), (v_buf, vf_ref))

    def rows_of(ref, shard):
        return ref.at[pl.ds(pl.multiple_of(shard * seq, seq), seq)]

    def kv_copy(i, hop):
        src, dst = caches[i]
        if hop == 0:
            return remote(src, rows_of(dst, me), kv_send.at[i, hop], kv_recv.at[i, hop], {'dm': across})
        if hop == 1:
            return remote(src, rows_of(dst, me), kv_send.at[i, hop], kv_recv.at[i, hop], {'dm': mate})
        return remote(rows_of(dst, across), rows_of(dst, across), kv_send.at[i, hop], kv_recv.at[i, hop], {'dm': mate})

    def kv_arrival(i, hop):
        region = rows_of(caches[i][1], (across, mate, cross)[hop])
        return remote(region, region, kv_send.at[i, hop], kv_recv.at[i, hop], {'dm': mate})

    kv_stores = [pltpu.make_async_copy(src, rows_of(dst, me), kv_store.at[i]) for i, (src, dst) in enumerate(caches)]
    for i in range(2):
        kv_copy(i, 0).start()
        kv_copy(i, 1).start()
        kv_stores[i].start()

    def down_body(i, carry):
        down_item(i)
        return carry

    lax.fori_loop(0, d_tiles, down_body, 0)

    def column_of(shard):
        return pl.ds(pl.multiple_of(shard * cols, cols), cols)

    def finish_last(out_rows, rows, total):
        xm_buf[out_rows, :] = (res_buf[rows, :].astype(F32) + unit_rows(total.astype(F32), gain_buf[3:4, :])).astype(BF16)

    def emit_last(out_rows):
        there = pl.ds(pl.multiple_of(me * seq + out_rows.start, CHUNK), CHUNK)
        for i, dev in enumerate((across, cross, mate)):
            remote(xm_buf.at[out_rows, column_of(dev)], y_ref.at[there], fin_send.at[i], fin_recv.at[i], {'dm': dev}).start()
        pltpu.make_async_copy(xm_buf.at[out_rows, column_of(me)], y_ref.at[there], fin_own).start()

    last_sums = LineSum(p_buf, got, xm_buf, *line_sems[4:], finish_last, emit_last)

    def pass_kv(i):
        kv_arrival(i, 0).wait_recv()
        kv_copy(i, 2).start()

    def each_last(t):
        @pl.when(t < 3 * d_tiles)
        def _():
            down_item(t + d_tiles)

    last_sums.run({min(14, sums.steps - 2): [functools.partial(pass_kv, 0)], min(17, sums.steps - 1): [functools.partial(pass_kv, 1)]}, each_last)
    last_sums.settle()
    for i in range(2):
        kv_stores[i].wait()
        for hop in range(3):
            kv_copy(i, hop).wait_send()
        kv_arrival(i, 1).wait_recv()
        kv_arrival(i, 2).wait_recv()
    for i, dev in enumerate((across, cross, mate)):
        done = remote(xm_buf.at[:, column_of(dev)], rows_of(y_ref, dev), fin_send.at[i], fin_recv.at[i], {'dm': dev})
        done.wait_send()
        done.wait_recv()
    pltpu.make_async_copy(xm_buf.at[:, column_of(me)], rows_of(y_ref, me), fin_own).wait()
    for copy in n_copies:
        copy.wait_send()
    x_copy(0, 0).wait_send()
    for s in range(2):
        x_copy(1, s).wait_send()
        x_copy(2, s).wait_send()


def like(*shape, dtype=BF16):
    return jax.ShapeDtypeStruct(shape, dtype)


def params(collective_id):
    return pltpu.CompilerParams(collective_id=collective_id, has_side_effects=True, vmem_limit_bytes=VMEM_BYTES)


def run_layer(x, norms, wq, wk, wv, wo, wg, wu, wd, cos_tab, sin_tab, pos, scale):
    seq = pos.shape[0]
    cols = x.shape[1]
    dim = 4 * cols
    kv_heads, head_dim = wk.shape[1:]
    width = wo.shape[0] + 2 * kv_heads * head_dim
    units = 18
    chunks = seq // 2 // CHUNK
    cache = (seq, kv_heads, head_dim)
    return pl.pallas_call(
        functools.partial(layer_kernel, scale, kv_heads, head_dim),
        name='layer',
        out_shape=(like(4 * seq, cols), like(4 * seq, kv_heads, head_dim), like(4 * seq, kv_heads, head_dim), like(4 * wg.shape[0], wg.shape[1]), like(4 * wu.shape[0], wu.shape[1]), like(wd.shape[0], 4 * wd.shape[1])),
        in_specs=[ANY] * 9 + [VMEM] * 4,
        out_specs=(ANY,) * 6,
        scratch_shapes=[
            pltpu.VMEM((seq, dim), BF16), pltpu.VMEM((dim, width), BF16), pltpu.VMEM((wo.shape[0], dim), BF16), pltpu.VMEM((seq, width), BF16),
            pltpu.VMEM((seq, dim), BF16), pltpu.VMEM((2, seq // 2, dim), BF16), pltpu.VMEM((seq // 2, dim), BF16), pltpu.VMEM((4,) + norms.shape, F32), pltpu.VMEM((8, dim), F32),
            pltpu.VMEM(wq.shape, BF16), pltpu.VMEM(wk.shape, BF16), pltpu.VMEM(wv.shape, BF16), pltpu.VMEM(cache, BF16), pltpu.VMEM(cache, BF16),
            DMA((3, 2)), DMA((3, 2)), DMA((3,)), DMA((3,)), DMA((2, 2 * LINE)), DMA((2 * LINE,)), DMA((5,)), DMA((5,)), DMA((units, 4)), DMA((units, 4)), DMA((6,)), DMA((4,)), DMA((4,)),
            DMA((4,)), DMA((2,)), DMA((2, 3)), DMA((2, 3)), DMA((3,)), DMA((3,)), DMA,
        ] + [DMA((2, chunks))] * 8,
        compiler_params=params(0),
    )(x, norms, wq, wk, wv, wo, wg, wu, wd, cos_tab, sin_tab, pos[:, None], pos[None, :])


def solution(mesh):
    tp_size = mesh.shape['tp']

    def layer(tokens, positions, norm_pre_attn, w_query, w_key, w_value, w_out, norm_post_attn, norm_pre_ffw, w_gate, w_up, w_down, norm_post_ffw):
        seq = positions.shape[1]
        heads, head_dim, cols = w_out.shape
        dim = 4 * cols
        scale = (dim / (heads * tp_size)) ** -0.5
        norms = jnp.stack([norm_pre_attn, norm_post_attn, norm_pre_ffw, norm_post_ffw]).astype(F32)
        norms = jnp.concatenate([norms, jnp.zeros_like(norms)])
        pos = lax.dynamic_index_in_dim(positions, lax.axis_index('dm'), 0, keepdims=False)
        half_dim = head_dim // 2
        inv_freq = ROPE_BASE ** (-2.0 * jnp.arange(half_dim, dtype=F32) / head_dim)
        angles = pos.astype(F32)[:, None] * inv_freq[None, :]
        outs = run_layer(tokens, norms, w_query, w_key, w_value, w_out.reshape(heads * head_dim, cols), w_gate, w_up, w_down, jnp.cos(angles), jnp.sin(angles), pos, scale)
        return outs[:3]

    width_spec = P('dm')
    in_specs = (P('dp', 'dm'), P('dp', None), width_spec, P('dm', 'tp', None), P('dm', 'tp', None), P('dm', 'tp', None), P('tp', None, 'dm'), width_spec, width_spec, P('dm', 'tp'), P('dm', 'tp'), P('tp', 'dm'), width_spec)
    out_specs = (P('dp', 'dm'), P('dp', 'tp', None), P('dp', 'tp', None))
    return jax.shard_map(layer, mesh=mesh, in_specs=in_specs, out_specs=out_specs, check_vma=False)
```

```python
import functools

import jax
import jax.numpy as jnp
from jax import lax
from jax.experimental import pallas as pl
from jax.experimental.pallas import tpu as pltpu
from jax.sharding import PartitionSpec as P

NORM_EPS = 1e-6
SOFT_CAP = 50.0
ROPE_BASE = 10000.0
WINDOW_LEN = 4096
BF16 = jnp.bfloat16
F32 = jnp.float32

CHUNK = 16
LAG = 2
LINE = 4
VMEM_BYTES = 67043328

PASS_Y = [(0, 0), (3, 0), (5, 1), (9, 0), (11, 0), (13, 0), (15, 0), (17, 0), (19, 0), (20, 1), (23, 0), (25, 0), (27, 0), (29, 0), (30, 0), (31, 0), (32, 0), (33, 0), (33, 1), (34, 1), (35, 1), (36, 1), (37, 0), (37, 1), (38, 1), (39, 1), (40, 1), (42, 0)]
PASS_X = [(3, 1), (8, 0), (11, 0), (13, 0), (13, 1), (17, 0), (18, 0), (19, 1), (22, 0), (25, 0), (26, 1), (29, 0), (30, 1), (32, 0), (33, 0), (33, 1), (34, 1), (35, 1), (36, 1), (37, 1), (37, 1), (38, 1), (39, 1), (40, 1), (43, 0), None, None, None]
GATE_TURNS = [20, 20, 21, 26, 30, 33, 33, 34, 34, 35, 35, 36, 36, 37, 37, 38, 38, 39, 39, 40, 40]

ANY = pl.BlockSpec(memory_space=pl.ANY)
VMEM = pl.BlockSpec(memory_space=pltpu.VMEM)
DMA = pltpu.SemaphoreType.DMA


def places():
    row = lax.axis_index('dp')
    line = lax.axis_index('tp')
    me = lax.axis_index('dm')
    side = lax.div(me, 2)
    core = me - 2 * side
    return row, line, me, 2 * side + 1 - core, 2 * (1 - side) + core, 2 * (1 - side) + 1 - core


def times(value, unit):
    return value if isinstance(value, int) else pl.multiple_of(value, unit)


def remote(src, dst, send_sem, recv_sem, device):
    return pltpu.make_async_remote_copy(src_ref=src, dst_ref=dst, send_sem=send_sem, recv_sem=recv_sem, device_id=device, device_id_type=pl.DeviceIdType.MESH)


def meet(peers):
    barrier = pltpu.get_barrier_semaphore()
    for peer in peers:
        pl.semaphore_signal(barrier, inc=1, device_id=peer, device_id_type=pl.DeviceIdType.MESH)
    pl.semaphore_wait(barrier, len(peers))


def line_peers(line):
    return [{'tp': lax.rem(line + 1, LINE)}, {'tp': lax.rem(line + LINE - 1, LINE)}]


QKV, OUT, GATE, UP, DOWN = range(5)


class WeightGather:
    def __init__(self, refs, pieces, tile, own_send, own_recv, send, recv):
        self.refs, self.pieces, self.tile = refs, pieces, tile
        self.own_send, self.own_recv, self.send, self.recv = own_send, own_recv, send, recv
        self.row, _, self.me, self.mate, self.across, self.cross = places()
        self.order = [(QKV, p) for p in range(pieces[QKV])] + [(OUT, p) for p in range(pieces[OUT])]
        self.order += [(part, p) for p in range(pieces[GATE]) for part in (GATE, UP)]
        self.order += [(DOWN, p) for p in range(pieces[DOWN])]

    def index(self, part, p):
        first = {QKV: 0, OUT: self.pieces[QKV]}
        ffw = self.pieces[QKV] + self.pieces[OUT]
        if part in first:
            return first[part] + p
        if part == DOWN:
            return ffw + 2 * self.pieces[GATE] + p
        return ffw + 2 * p + (part - GATE)

    def direct(self, part, p):
        return part == DOWN and p == self.pieces[DOWN] - 1

    def cut(self, part, half, p):
        size = self.refs[part][0].shape[0] // (2 * self.pieces[part])
        return pl.ds(pl.multiple_of((half * self.pieces[part] + p) * size, size), size)

    def own(self, part, half, p):
        src = self.refs[part][0]
        if part in (GATE, UP):
            size = self.tile // 2
            return src.at[:, pl.ds(pl.multiple_of(p * self.tile + half * size, size), size)]
        return src.at[self.cut(part, half, p)]

    def at(self, part, shard, half, p):
        src, dst = self.refs[part]
        if part == QKV:
            size = src.shape[0] // (2 * self.pieces[part])
            return dst.at[pl.ds(pl.multiple_of(shard * src.shape[0] + (half * self.pieces[part] + p) * size, size), size)]
        if part == OUT:
            return dst.at[self.cut(part, half, p), pl.ds(pl.multiple_of(shard * src.shape[1], src.shape[1]), src.shape[1])]
        if part == DOWN:
            return dst.at[shard, self.cut(part, half, p)]
        size = self.tile // 2
        return dst.at[p, pl.ds(pl.multiple_of(shard * src.shape[0], src.shape[0]), src.shape[0]), pl.ds(pl.multiple_of(half * size, size), size)]

    def copy(self, part, p, hop):
        mine, other = self.row, 1 - self.row
        k = self.index(part, p)
        device = {'dm': self.mate}
        if hop == 0 or (hop == 1 and self.direct(part, p)):
            half = mine if hop == 0 else other
            src, dst, device = self.own(part, half, p), self.at(part, self.me, half, p), {'dm': self.across}
        else:
            src = dst = self.at(part, self.across, other if hop == 3 else mine, p)
            if hop == 1:
                device = {'dp': other}
        return remote(src, dst, self.send.at[k, hop], self.recv.at[k, hop], device)

    def arrival(self, part, p, hop):
        k = self.index(part, p)
        region = self.at(part, self.across if hop < 2 else self.cross, 1 - self.row if hop % 2 else self.row, p)
        return remote(region, region, self.send.at[k, hop], self.recv.at[k, hop], {'dm': self.mate})

    def own_copy(self, part, p, shard):
        src, dst = self.refs[part]
        if part in (GATE, UP):
            src = src.at[:, pl.ds(times(p * self.tile, self.tile), self.tile)]
            dst = dst.at[p, pl.ds(pl.multiple_of(shard * src.shape[0], src.shape[0]), src.shape[0])]
            k = 3 + 2 * p + part - GATE
        else:
            k = (QKV, OUT, DOWN).index(part)
            if part == DOWN:
                dst = dst.at[shard]
            elif part == OUT:
                dst = dst.at[:, pl.ds(pl.multiple_of(shard * src.shape[1], src.shape[1]), src.shape[1])]
            else:
                dst = dst.at[pl.ds(pl.multiple_of(shard * src.shape[0], src.shape[0]), src.shape[0])]
        return remote(src, dst, self.own_send.at[k], self.own_recv.at[k], {'dm': self.mate})

    def start(self):
        for part, p in self.order:
            self.copy(part, p, 0).start()
            if self.direct(part, p):
                self.copy(part, p, 1).start()

    def pass_y(self, part, p):
        self.arrival(part, p, 0).wait_recv()
        if not self.direct(part, p):
            self.copy(part, p, 1).start()
        self.copy(part, p, 2).start()

    def pass_x(self, part, p):
        self.arrival(part, p, 1).wait_recv()
        self.copy(part, p, 3).start()

    def landed(self, part, p):
        self.arrival(part, p, 2).wait_recv()
        self.arrival(part, p, 3).wait_recv()

    def sent(self, part, p):
        for hop in range(4):
            self.copy(part, p, hop).wait_send()

    def own_start(self, part, p=0):
        self.own_copy(part, p, self.me).start()

    def own_landed(self, part, p=0):
        self.own_copy(part, p, self.mate).wait_recv()

    def own_sent(self, part, p=0):
        self.own_copy(part, p, self.me).wait_send()


class LineSum:
    def __init__(self, p_buf, got, out, sum_send, sum_recv, out_send, out_recv, finish, emit):
        self.p_buf, self.got, self.out = p_buf, got, out
        self.sum_send, self.sum_recv, self.out_send, self.out_recv = sum_send, sum_recv, out_send, out_recv
        self.finish, self.emit = finish, emit
        self.half = p_buf.shape[0] // 2
        self.chunks = self.half // CHUNK
        self.steps = self.chunks + 6 * LAG
        self.line = lax.axis_index('tp')

    def way(self, d):
        if d == 0:
            return self.line, {'tp': self.line + 1}, {'tp': self.line - 1}
        return LINE - 1 - self.line, {'tp': self.line - 1}, {'tp': self.line + 1}

    def rows(self, c):
        return pl.ds(pl.multiple_of(c * CHUNK, CHUNK), CHUNK)

    def out_rows(self, d, c):
        return pl.ds(pl.multiple_of(d * self.half + c * CHUNK, CHUNK), CHUNK)

    def sum_copy(self, d, c):
        return remote(self.p_buf.at[self.out_rows(d, c)], self.got.at[d, self.rows(c)], self.sum_send.at[d, c], self.sum_recv.at[d, c], self.way(d)[1])

    def out_copy(self, d, c):
        region = self.out.at[self.out_rows(d, c)]
        return remote(region, region, self.out_send.at[d, c], self.out_recv.at[d, c], self.way(d)[2])

    def step(self, t):
        for d in range(2):
            with jax.named_scope(f'sum{d}'):
                self.sum_step(d, t)
        for d in range(2):
            with jax.named_scope(f'out{d}'):
                self.out_step(d, t)

    def sum_step(self, d, t):
        pos = self.way(d)[0]
        c = t - LAG * pos

        @pl.when((c >= 0) & (c < self.chunks))
        def _():
            @pl.when(pos == 0)
            def _():
                self.sum_copy(d, c).start()

            @pl.when(pos > 0)
            def _():
                self.sum_copy(d, c).wait_recv()
                total = self.p_buf[self.out_rows(d, c), :].astype(F32) + self.got[d, self.rows(c), :].astype(F32)

                @pl.when(pos < LINE - 1)
                def _():
                    self.p_buf[self.out_rows(d, c), :] = total.astype(BF16)
                    self.sum_copy(d, c).start()

                @pl.when(pos == LINE - 1)
                def _():
                    self.finish(self.out_rows(d, c), self.rows(c), total.astype(BF16))
                    self.out_copy(d, c).start()
                    self.emit(self.out_rows(d, c))

    def out_step(self, d, t):
        pos = self.way(d)[0]
        c = t - 3 * LAG - LAG * (LINE - 1 - pos)

        @pl.when((c >= 0) & (c < self.chunks) & (pos < LINE - 1))
        def _():
            self.out_copy(d, c).wait_recv()

            @pl.when(pos > 0)
            def _():
                self.out_copy(d, c).start()

            self.emit(self.out_rows(d, c))

    def run(self, before, each, after):
        def body(t, carry):
            def act(actions):
                for turn in sorted(actions):

                    @pl.when(t == turn)
                    def _():
                        for action in actions[turn]:
                            action()

            with jax.named_scope('before'):
                act(before)
            with jax.named_scope('each'):
                each(t)
            with jax.named_scope('after'):
                act(after)
            self.step(t)
            return carry

        lax.fori_loop(0, self.steps, body, 0)

    def settle(self):
        def body(c, carry):
            for d in range(2):
                pos = self.way(d)[0]

                @pl.when(pos < LINE - 1)
                def _():
                    self.sum_copy(d, c).wait_send()

                @pl.when(pos > 0)
                def _():
                    self.out_copy(d, c).wait_send()

            return carry

        lax.fori_loop(0, self.chunks, body, 0)


def unit_rows(values, gain):
    mean_sq = jnp.mean(values * values, axis=-1, keepdims=True)
    return values * lax.rsqrt(mean_sq + NORM_EPS) * gain


def rotate(values, cos_tab, sin_tab):
    half_dim = values.shape[-1] // 2
    lower = values[:, :half_dim].astype(F32)
    upper = values[:, half_dim:].astype(F32)
    return jnp.concatenate([lower * cos_tab - upper * sin_tab, upper * cos_tab + lower * sin_tab], axis=-1).astype(BF16)


def turns_of(table, t):
    first = sum([jnp.where(t > turn, 1, 0) for turn in table], 0)
    return first, first + sum([jnp.where(t == turn, 1, 0) for turn in table], 0)


def layer_kernel(scale, kv_heads, head_dim, pieces, x_ref, n_ref, wq_ref, wk_ref, wv_ref, wo_ref, wg_ref, wu_ref, wd_ref, cos_ref, sin_ref, pos_col_ref, pos_row_ref, y_ref, kf_ref, vf_ref, wgf_ref, wuf_ref, wdf_ref, xm_buf, w_buf, wo_buf, qkv_buf, p_buf, got, res_buf, n_buf, gain_buf, wq_buf, wk_buf, wv_buf, k_buf, v_buf, x_send, x_recv, n_send, n_recv, z_send, z_recv, own_send, own_recv, w_send, w_recv, load_sem, gate_sem, down_sem, kv_store, kv_send, kv_recv, fin_send, fin_recv, fin_own, *line_sems):
    row, line, me, mate, across, cross = places()
    seq, dim = xm_buf.shape
    cols = dim // 4
    half = seq // 2
    quarter = seq // LINE
    sub = quarter // 2
    heads = wo_ref.shape[0] // head_dim
    group = heads // kv_heads
    tiles, _, tile = wgf_ref.shape
    peers = (mate, across, cross)

    def shard_span(shard):
        return pl.ds(pl.multiple_of(shard * cols, cols), cols)

    mine = shard_span(me)
    refs = ((w_buf.at[mine], w_buf), (wo_ref, wo_buf), (wg_ref, wgf_ref), (wu_ref, wuf_ref), (wd_ref, wdf_ref))
    gather = WeightGather(refs, pieces, tile, own_send, own_recv, w_send, w_recv)
    pass_y, pass_x = gather.pass_y, gather.pass_x

    def x_copy(hop, s):
        dev = peers[hop]
        if hop == 0:
            src, dst = x_ref.at[pl.ds(pl.multiple_of(dev * seq, seq), seq)], xm_buf.at[:, mine]
        else:
            start = line * quarter + s * sub
            src = x_ref.at[pl.ds(pl.multiple_of(dev * seq + start, sub), sub)]
            dst = xm_buf.at[pl.ds(pl.multiple_of(start, sub), sub), mine]
        return remote(src, dst, x_send.at[hop, s], x_recv.at[hop, s], {'dm': dev})

    def x_arrival(hop, s):
        theirs = shard_span(peers[hop])
        region = xm_buf.at[:, theirs] if hop == 0 else xm_buf.at[pl.ds(pl.multiple_of(line * quarter + s * sub, sub), sub), theirs]
        return remote(region, region, x_send.at[hop, s], x_recv.at[hop, s], {'dm': mate})

    far = pl.ds(pl.multiple_of((1 - lax.div(me, 2)) * 2 * cols, 2 * cols), 2 * cols)

    def z_copy(up, block, s):
        index = 2 * block + s
        region = xm_buf.at[pl.ds(pl.multiple_of(index * sub, sub), sub), far]
        device = {'tp': line + 1} if up else {'tp': line - 1}
        return remote(region, region, z_send.at[0 if up else 1, index], z_recv.at[index], device)

    def z_first(s):
        x_arrival(1, s).wait_recv()
        x_arrival(2, s).wait_recv()

        @pl.when(line < LINE - 1)
        def _():
            z_copy(True, line, s).start()

        @pl.when(line > 0)
        def _():
            z_copy(False, line, s).start()

    def z_step(step, s):
        below, above = line - step, line + step

        @pl.when(below >= 0)
        def _():
            z_copy(True, below, s).wait_recv()

            @pl.when(line < LINE - 1)
            def _():
                z_copy(True, below, s).start()

        @pl.when(above < LINE)
        def _():
            z_copy(False, above, s).wait_recv()

            @pl.when(line > 0)
            def _():
                z_copy(False, above, s).start()

    n_copies = [remote(n_ref, n_buf.at[me], n_send.at[i], n_recv.at[i], {'dm': dev}) for i, dev in enumerate(peers)]
    n_arrivals = [remote(n_ref, n_buf.at[dev], n_send.at[i], n_recv.at[i], {'dm': dev}) for i, dev in enumerate(peers)]
    loads = [
        pltpu.make_async_copy(x_ref.at[pl.ds(pl.multiple_of(me * seq, seq), seq)], xm_buf.at[:, mine], load_sem.at[0]),
        pltpu.make_async_copy(wo_ref, wo_buf.at[:, mine], load_sem.at[1]),
        pltpu.make_async_copy(n_ref, n_buf.at[me], load_sem.at[2]),
    ]
    thirds = ((wq_ref, wq_buf), (wk_ref, wk_buf), (wv_ref, wv_buf))
    third_loads = [pltpu.make_async_copy(src, buf, load_sem.at[3 + i]) for i, (src, buf) in enumerate(thirds)]

    def flatten_own():
        for load in third_loads:
            load.wait()
        flat_rows = min(cols, 64)

        def body(i, carry):
            part = pl.ds(pl.multiple_of(i * flat_rows, flat_rows), flat_rows)
            there = pl.ds(pl.multiple_of(me * cols + i * flat_rows, flat_rows), flat_rows)
            start = 0
            for _, buf in thirds:
                wide = buf.shape[1] * buf.shape[2]
                w_buf[there, start:start + wide] = buf[part].reshape(flat_rows, wide)
                start += wide
            return carry

        lax.fori_loop(0, cols // flat_rows, body, 0)

    def spread(part, share):
        count = pieces[part]
        return [p for p in range(count) if (4 * p) // count == share]

    for load in third_loads:
        load.start()
    with jax.named_scope('meet'):
        meet([{'dm': mate}, {'dm': across}, {'dm': cross}, {'dp': 1 - row}] + line_peers(line))
    for s in range(2):
        x_copy(1, s).start()
        x_copy(2, s).start()
    with jax.named_scope('flatten'):
        flatten_own()
    gather.start()
    x_copy(0, 0).start()
    for copy in n_copies:
        copy.start()
    for load in loads:
        load.start()
    gather.own_start(QKV)
    gather.own_start(OUT)
    with jax.named_scope('z0'):
        z_first(0)
        z_first(1)
        z_step(1, 0)
    with jax.named_scope('z1'):
        for p in spread(QKV, 0)[:1]:
            pass_y(QKV, p)
        z_step(1, 1)
        for p in spread(QKV, 0)[1:]:
            pass_y(QKV, p)
        for p in spread(QKV, 0)[:1]:
            pass_x(QKV, p)
        z_step(2, 0)
    with jax.named_scope('z2'):
        for p in spread(QKV, 1):
            pass_y(QKV, p)
        for p in spread(QKV, 0)[1:]:
            pass_x(QKV, p)
        z_step(2, 1)
        for p in spread(QKV, 2):
            pass_y(QKV, p)
        for p in spread(QKV, 1):
            pass_x(QKV, p)
        z_step(3, 0)
    with jax.named_scope('z3'):
        for p in spread(QKV, 3):
            pass_y(QKV, p)
        for p in spread(QKV, 2):
            pass_x(QKV, p)
        for copy in n_arrivals:
            copy.wait_recv()
        for load in loads:
            load.wait()
        for shard in range(4):
            gain_buf[:, shard * cols:(shard + 1) * cols] = 1.0 + n_buf[shard]
        x_arrival(0, 0).wait_recv()
        z_step(3, 1)

    for block in range(LINE):
        for s in range(2):

            @pl.when((block <= line) & (line < LINE - 1))
            def _():
                z_copy(True, block, s).wait_send()

            @pl.when((block >= line) & (line > 0))
            def _():
                z_copy(False, block, s).wait_send()

    first_row = pl.multiple_of(half * (1 - jnp.minimum(line, 1)), half)
    res_buf[...] = xm_buf[pl.ds(first_row, half), :]
    norm_rows = min(seq, 64)

    def norm_body(i, carry):
        part = pl.ds(pl.multiple_of(i * norm_rows, norm_rows), norm_rows)
        xm_buf[part, :] = unit_rows(xm_buf[part, :].astype(F32), gain_buf[0:1, :]).astype(BF16)
        return carry

    with jax.named_scope('norm'):
        lax.fori_loop(0, seq // norm_rows, norm_body, 0)
    with jax.named_scope('settle_qkv'):
        for p in spread(QKV, 3):
            pass_x(QKV, p)
        for part in (GATE, UP):
            for p in range(tiles):
                gather.own_start(part, p)
        gather.own_start(DOWN)
        for p in range(pieces[QKV]):
            gather.landed(QKV, p)
            gather.sent(QKV, p)
        gather.own_landed(QKV)
        gather.own_sent(QKV)

    big = min(seq, 512)
    width = qkv_buf.shape[1]
    q_tile = min(width, 512)
    q_steps = (width // q_tile) * (seq // big)
    stops = {0: [(pass_y, 0)], 1: [(pass_y, 1)], 2: [(pass_y, 2)], 4: [(pass_x, 0)], 5: [(pass_y, 3), (pass_x, 1)], 7: [(pass_x, 2)]}

    def qkv_body(i, carry):
        for stop in range(q_steps):
            todo = [move for turn, moves in stops.items() if min(turn, q_steps - 1) == stop for move in moves]
            if todo:

                @pl.when(i == stop)
                def _():
                    for move, p in todo:
                        move(OUT, p)

        column = pl.ds(pl.multiple_of(lax.rem(i, width // q_tile) * q_tile, q_tile), q_tile)
        part = pl.ds(pl.multiple_of(lax.div(i, width // q_tile) * big, big), big)
        qkv_buf[part, column] = jnp.dot(xm_buf[part, :], w_buf[:, column], preferred_element_type=F32).astype(BF16)
        return carry

    with jax.named_scope('qkv'):
        lax.fori_loop(0, q_steps, qkv_body, 0)
    with jax.named_scope('pass_out'):
        pass_x(OUT, 3)

    def rotate_body(i, carry):
        column = pl.ds(pl.multiple_of(i * head_dim, head_dim), head_dim)
        qkv_buf[:, column] = rotate(qkv_buf[:, column], cos_ref[...], sin_ref[...])
        return carry

    with jax.named_scope('rotate'):
        lax.fori_loop(0, heads + kv_heads, rotate_body, 0)

    def keep_caches():
        def cache_body(i, carry):
            part = pl.ds(pl.multiple_of(i * norm_rows, norm_rows), norm_rows)
            wide = kv_heads * head_dim
            for n, buf in enumerate((k_buf, v_buf)):
                start = heads * head_dim + n * wide
                buf[part] = qkv_buf[part, start:start + wide].reshape(norm_rows, kv_heads, head_dim)
            return carry

        lax.fori_loop(0, seq // norm_rows, cache_body, 0)

    block = seq // 8
    d_tile = min(dim, 512)

    def attend_block(i):
        part = slice(i * block, (i + 1) * block)
        span = (i + 1) * block
        q_index = i * block + lax.broadcasted_iota(jnp.int32, (block, span), 0)
        key_index = lax.broadcasted_iota(jnp.int32, (block, span), 1)
        allowed = (key_index <= q_index) & (pos_col_ref[part, :] - pos_row_ref[:, :span] < WINDOW_LEN)

        def head_body(h, carry):
            q_cols = pl.ds(pl.multiple_of(h * head_dim, head_dim), head_dim)
            k_cols = pl.ds(pl.multiple_of((heads + lax.div(h, group)) * head_dim, head_dim), head_dim)
            v_cols = pl.ds(pl.multiple_of((heads + kv_heads + lax.div(h, group)) * head_dim, head_dim), head_dim)
            scores = lax.dot_general(qkv_buf[part, q_cols], qkv_buf[:span, k_cols], (((1,), (1,)), ((), ())), preferred_element_type=F32)
            capped = SOFT_CAP * jnp.tanh(scores * scale / SOFT_CAP)
            weights = jnp.where(allowed, jnp.exp(capped), 0.0)
            probs = (weights / jnp.sum(weights, axis=-1, keepdims=True)).astype(BF16)
            qkv_buf[part, q_cols] = jnp.dot(probs, qkv_buf[:span, v_cols], preferred_element_type=F32).astype(BF16)
            return carry

        lax.fori_loop(0, heads, head_body, 0)

    def out_block(i):
        part = slice(i * block, (i + 1) * block)

        def out_body(n, carry):
            column = pl.ds(pl.multiple_of(n * d_tile, d_tile), d_tile)
            p_buf[part, column] = jnp.dot(qkv_buf[part, :heads * head_dim], wo_buf[:, column], preferred_element_type=F32).astype(BF16)
            return carry

        lax.fori_loop(0, dim // d_tile, out_body, 0)

    def both(i):
        attend_block(i)
        out_block(i)

    with jax.named_scope('attend0'):
        attend_block(0)
        attend_block(4)
        pass_y(GATE, 0)
    with jax.named_scope('settle_out'):
        for p in range(pieces[OUT]):
            gather.landed(OUT, p)
            gather.sent(OUT, p)
        gather.own_landed(OUT)
        gather.own_sent(OUT)
    with jax.named_scope('out0'):
        out_block(0)
        out_block(4)

    def finish(out_rows, rows, total):
        hidden = (res_buf[rows, :].astype(F32) + unit_rows(total.astype(F32), gain_buf[1:2, :])).astype(BF16)
        res_buf[rows, :] = hidden
        xm_buf[out_rows, :] = unit_rows(hidden.astype(F32), gain_buf[2:3, :]).astype(BF16)

    sums = LineSum(p_buf, got, xm_buf, *line_sems[:4], finish, lambda out_rows: None)
    last = sums.steps - 1
    ahead = sums.chunks // 4

    span_rows = half // 4
    z_buf = wo_buf
    pair = 2 * tile

    def group_rows(g):
        return [pl.ds(times(d * half + g * span_rows, span_rows), span_rows) for d in range(2)]

    def gate_loads(f, base):
        copies = []
        for n, (src, dst) in enumerate(((wg_ref, wgf_ref), (wu_ref, wuf_ref))):
            column = pl.ds(times(base + n * tile, tile), tile)
            for r, shard in enumerate((me, mate, across, cross)):
                part = src.at[:, pl.ds(times(f * tile, tile), tile)] if r == 0 else dst.at[f, shard_span(shard)]
                copies.append(pltpu.make_async_copy(part, w_buf.at[shard_span(shard), column], gate_sem.at[base // pair if isinstance(base, int) else lax.div(base, pair), n, r]))
        return copies

    def gate_fetch(f, base):
        for load in gate_loads(f, base):
            load.start()

    def gate_settle(f):
        for part in (GATE, UP):
            gather.landed(part, f)
            gather.own_landed(part, f)

    def gate_work(g, f, base):
        for load in gate_loads(f, base):
            load.wait()
        parts = group_rows(g)
        ffw_in = jnp.concatenate([xm_buf[part, :] for part in parts], axis=0)
        gate = jnp.dot(ffw_in, w_buf[:, pl.ds(times(base, tile), tile)], preferred_element_type=F32).astype(BF16).astype(F32)
        up = jnp.dot(ffw_in, w_buf[:, pl.ds(times(base + tile, tile), tile)], preferred_element_type=F32).astype(BF16).astype(F32)
        gated = (jax.nn.gelu(gate, approximate=True) * up).astype(BF16)
        for d, part in enumerate(parts):
            z_buf[part, pl.ds(times(f * tile, tile), tile)] = gated[d * span_rows:(d + 1) * span_rows]

    def gate_item(i, carry):
        base = lax.rem(i, 2) * pair
        ahead_f = lax.rem(i + 1, tiles)

        @pl.when(i + 1 < tiles)
        def _():
            gate_settle(ahead_f)

        @pl.when(i + 1 < 3 * tiles)
        def _():
            gate_fetch(ahead_f, pair - base)

        gate_work(lax.div(i, tiles), lax.rem(i, tiles), base)
        return carry

    ffw = gather.order[pieces[QKV] + pieces[OUT]:]
    if len(ffw) == len(PASS_Y):
        y_turns, x_turns, gate_turns = PASS_Y, PASS_X, GATE_TURNS
    else:
        y_turns = [(min(3 + 2 * k, last), 0) for k in range(len(ffw))]
        x_turns = [(min(4 + 2 * k, last), 0) for k in range(len(ffw))]
        gate_turns = [0] * (3 * tiles)
    before, after, tail = {}, {}, []

    def at(turn, action):
        if turn is None:
            tail.append(action)
        else:
            (after if turn[1] else before).setdefault(turn[0], []).append(action)

    moves = [(turn, 0, k) for k, turn in enumerate(y_turns) if k > 0] + [(turn, 1, k) for k, turn in enumerate(x_turns)]
    for turn, way, k in sorted(moves, key=lambda move: ((99, 0) if move[0] is None else move[0], move[2] + move[1], move[1])):
        at(turn, functools.partial((pass_y, pass_x)[way], *ffw[k]))
    at((min(1, last), 1), keep_caches)
    for i in range(1, 4):
        early = (2 * ahead) // 8 if i == 3 else 0
        at((min(i * ahead - (5 * ahead) // 8 - early, last), 0), functools.partial(both, i))
        at((min(i * ahead - (3 * ahead) // 8 - early, last), 0), functools.partial(both, 4 + i))
    gate_ready = [max(x_turns[k][0] + x_turns[k][1] for k in (2 * f, 2 * f + 1)) for f in range(tiles)]
    gate_table = []
    for i in range(3 * tiles):
        turn = max(gate_turns[i], (i // tiles + 1) * ahead + 6 * LAG, gate_ready[min(i + 1, tiles - 1)])
        gate_table.append(max(turn, gate_table[-1] if gate_table else 0))

    def open_gate():
        gate_settle(0)
        gate_fetch(0, 0)

    at((min(gate_table[0], last), 0), open_gate)

    def each_first(t):
        lax.fori_loop(*turns_of([turn for turn in gate_table if turn <= last], t), gate_item, 0)

    with jax.named_scope('chain1'):
        sums.run(before, each_first, after)
    with jax.named_scope('gate_rest'):
        lax.fori_loop(len([turn for turn in gate_table if turn <= last]), 3 * tiles, gate_item, 0)
    shards = (me, mate, across, cross)

    def down_load(r, base):
        column = pl.ds(base, cols)
        sem = down_sem.at[0 if base else 1]
        return pltpu.make_async_copy(wd_ref if r == 0 else wdf_ref.at[shards[r]], w_buf.at[:, column], sem)

    def down_fetch(r, base):
        if isinstance(r, int):
            down_load(r, base).start()
            return
        for n in range(4):

            @pl.when(r == n)
            def _():
                down_load(n, base).start()

    def down_work(g, r, base):
        down_load(0, base).wait()
        parts = group_rows(g)
        gated = jnp.concatenate([z_buf[part, :] for part in parts], axis=0)
        down = jnp.dot(gated, w_buf[:, pl.ds(base, cols)], preferred_element_type=F32).astype(BF16)
        if isinstance(r, int):
            shard = shards[r]
        else:
            shard = jnp.where(r == 0, me, jnp.where(r == 1, mate, jnp.where(r == 2, across, cross)))
        for d, part in enumerate(parts):
            p_buf[part, shard_span(shard)] = down[d * span_rows:(d + 1) * span_rows]

    with jax.named_scope('tail'):
        down_fetch(0, pair)
        for action in tail:
            action()
        gather.own_landed(DOWN)
        down_fetch(1, 0)
        sums.settle()
    with jax.named_scope('down_near'):
        down_work(0, 0, pair)
        down_work(0, 1, 0)

    caches = ((k_buf, kf_ref), (v_buf, vf_ref))

    def rows_of(ref, shard):
        return ref.at[pl.ds(pl.multiple_of(shard * seq, seq), seq)]

    def kv_copy(i, hop):
        src, dst = caches[i]
        if hop == 0:
            return remote(src, rows_of(dst, me), kv_send.at[i, hop], kv_recv.at[i, hop], {'dm': across})
        if hop == 1:
            return remote(src, rows_of(dst, me), kv_send.at[i, hop], kv_recv.at[i, hop], {'dm': mate})
        return remote(rows_of(dst, across), rows_of(dst, across), kv_send.at[i, hop], kv_recv.at[i, hop], {'dm': mate})

    def kv_arrival(i, hop):
        region = rows_of(caches[i][1], (across, mate, cross)[hop])
        return remote(region, region, kv_send.at[i, hop], kv_recv.at[i, hop], {'dm': mate})

    with jax.named_scope('settle_down'):
        for p in range(pieces[DOWN]):
            gather.landed(DOWN, p)
    down_fetch(2, pair)
    down_fetch(3, 0)
    kv_stores = [pltpu.make_async_copy(src, rows_of(dst, me), kv_store.at[i]) for i, (src, dst) in enumerate(caches)]
    for i in range(2):
        kv_copy(i, 0).start()
        kv_copy(i, 1).start()
        kv_stores[i].start()
    with jax.named_scope('down_far'):
        down_work(0, 2, pair)
        down_fetch(0, pair)
        down_work(0, 3, 0)
        gate_fetch(0, 0)

    def finish_last(out_rows, rows, total):
        xm_buf[out_rows, :] = (res_buf[rows, :].astype(F32) + unit_rows(total.astype(F32), gain_buf[3:4, :])).astype(BF16)

    def emit_last(out_rows):
        there = pl.ds(pl.multiple_of(me * seq + out_rows.start, CHUNK), CHUNK)
        for i, dev in enumerate((across, cross, mate)):
            remote(xm_buf.at[out_rows, shard_span(dev)], y_ref.at[there], fin_send.at[i], fin_recv.at[i], {'dm': dev}).start()
        pltpu.make_async_copy(xm_buf.at[out_rows, mine], y_ref.at[there], fin_own).start()

    last_sums = LineSum(p_buf, got, xm_buf, *line_sems[4:], finish_last, emit_last)

    def pass_kv(i):
        kv_arrival(i, 0).wait_recv()
        kv_copy(i, 2).start()

    late_gates = [int((f + 0.5) * 2 * ahead / (tiles + 1)) for f in range(tiles)]
    late_downs = [(n * ahead) // 4 for n in range(12)]

    def late_gate(f, carry):
        gate_work(3, f, 0)

        @pl.when(f + 1 < tiles)
        def _():
            gate_fetch(f + 1, 0)

        return carry

    def late_down(n, carry):
        down_work(1 + lax.div(n, 4), lax.rem(n, 4), pair)

        @pl.when(n + 1 < 12)
        def _():
            down_fetch(lax.rem(n + 1, 4), pair)

        return carry

    def each_last(t):
        lax.fori_loop(*turns_of(late_gates, t), late_gate, 0)
        lax.fori_loop(*turns_of(late_downs, t), late_down, 0)

    with jax.named_scope('chain2'):
        last_sums.run({min(14, last - 1): [functools.partial(pass_kv, 0)], min(17, last): [functools.partial(pass_kv, 1)]}, each_last, {})
    with jax.named_scope('close'):
        last_sums.settle()
        for i in range(2):
            kv_stores[i].wait()
            for hop in range(3):
                kv_copy(i, hop).wait_send()
            kv_arrival(i, 1).wait_recv()
            kv_arrival(i, 2).wait_recv()
        for i, dev in enumerate((across, cross, mate)):
            done = remote(xm_buf.at[:, shard_span(dev)], rows_of(y_ref, dev), fin_send.at[i], fin_recv.at[i], {'dm': dev})
            done.wait_send()
            done.wait_recv()
        pltpu.make_async_copy(xm_buf.at[:, mine], rows_of(y_ref, me), fin_own).wait()
        for part in (GATE, UP):
            for p in range(tiles):
                gather.sent(part, p)
                gather.own_sent(part, p)
        for p in range(pieces[DOWN]):
            gather.sent(DOWN, p)
        gather.own_sent(DOWN)
        for copy in n_copies:
            copy.wait_send()
        x_copy(0, 0).wait_send()
        for s in range(2):
            x_copy(1, s).wait_send()
            x_copy(2, s).wait_send()


def like(*shape, dtype=BF16):
    return jax.ShapeDtypeStruct(shape, dtype)


def params(collective_id):
    return pltpu.CompilerParams(collective_id=collective_id, has_side_effects=True, vmem_limit_bytes=VMEM_BYTES)


def run_layer(x, norms, wq, wk, wv, wo, wg, wu, wd, cos_tab, sin_tab, pos, scale):
    seq = pos.shape[0]
    cols = x.shape[1]
    dim = 4 * cols
    kv_heads, head_dim = wk.shape[1:]
    width = wo.shape[0] + 2 * kv_heads * head_dim
    chunks = seq // 2 // CHUNK
    cache = (seq, kv_heads, head_dim)
    hidden = wg.shape[1]
    tile = min(hidden // 2, 512)
    tiles = hidden // tile

    def count(rows, most):
        return most if rows % (32 * most) == 0 else 2

    pieces = (count(cols, 7), 4, tiles, tiles, count(wd.shape[0], 14))
    units = sum(pieces)
    return pl.pallas_call(
        functools.partial(layer_kernel, scale, kv_heads, head_dim, pieces),
        name='layer',
        out_shape=(like(4 * seq, cols), like(4 * seq, kv_heads, head_dim), like(4 * seq, kv_heads, head_dim), like(tiles, dim, tile), like(tiles, dim, tile), like(4, *wd.shape)),
        in_specs=[ANY] * 9 + [VMEM] * 4,
        out_specs=(ANY,) * 6,
        scratch_shapes=[
            pltpu.VMEM((seq, dim), BF16), pltpu.VMEM((dim, width), BF16), pltpu.VMEM((wo.shape[0], dim), BF16), pltpu.VMEM((seq, width), BF16),
            pltpu.VMEM((seq, dim), BF16), pltpu.VMEM((2, seq // 2, dim), BF16), pltpu.VMEM((seq // 2, dim), BF16), pltpu.VMEM((4,) + norms.shape, F32), pltpu.VMEM((8, dim), F32),
            pltpu.VMEM(wq.shape, BF16), pltpu.VMEM(wk.shape, BF16), pltpu.VMEM(wv.shape, BF16), pltpu.VMEM(cache, BF16), pltpu.VMEM(cache, BF16),
            DMA((3, 2)), DMA((3, 2)), DMA((3,)), DMA((3,)), DMA((2, 2 * LINE)), DMA((2 * LINE,)), DMA((3 + 2 * tiles,)), DMA((3 + 2 * tiles,)), DMA((units, 4)), DMA((units, 4)), DMA((6,)),
            DMA((2, 2, 4)), DMA((2,)), DMA((2,)), DMA((2, 3)), DMA((2, 3)), DMA((3,)), DMA((3,)), DMA,
        ] + [DMA((2, chunks))] * 8,
        compiler_params=params(0),
    )(x, norms, wq, wk, wv, wo, wg, wu, wd, cos_tab, sin_tab, pos[:, None], pos[None, :])


def solution(mesh):
    tp_size = mesh.shape['tp']

    def layer(tokens, positions, norm_pre_attn, w_query, w_key, w_value, w_out, norm_post_attn, norm_pre_ffw, w_gate, w_up, w_down, norm_post_ffw):
        seq = positions.shape[1]
        heads, head_dim, cols = w_out.shape
        dim = 4 * cols
        scale = (dim / (heads * tp_size)) ** -0.5
        norms = jnp.stack([norm_pre_attn, norm_post_attn, norm_pre_ffw, norm_post_ffw]).astype(F32)
        norms = jnp.concatenate([norms, jnp.zeros_like(norms)])
        pos = lax.dynamic_index_in_dim(positions, lax.axis_index('dm'), 0, keepdims=False)
        half_dim = head_dim // 2
        inv_freq = ROPE_BASE ** (-2.0 * jnp.arange(half_dim, dtype=F32) / head_dim)
        angles = pos.astype(F32)[:, None] * inv_freq[None, :]
        outs = run_layer(tokens, norms, w_query, w_key, w_value, w_out.reshape(heads * head_dim, cols), w_gate, w_up, w_down, jnp.cos(angles), jnp.sin(angles), pos, scale)
        return outs[:3]

    width_spec = P('dm')
    in_specs = (P('dp', 'dm'), P('dp', None), width_spec, P('dm', 'tp', None), P('dm', 'tp', None), P('dm', 'tp', None), P('tp', None, 'dm'), width_spec, width_spec, P('dm', 'tp'), P('dm', 'tp'), P('tp', 'dm'), width_spec)
    out_specs = (P('dp', 'dm'), P('dp', 'tp', None), P('dp', 'tp', None))
    return jax.shard_map(layer, mesh=mesh, in_specs=in_specs, out_specs=out_specs, check_vma=False)
```

```python
import functools

import jax
import jax.numpy as jnp
from jax import lax
from jax.experimental import pallas as pl
from jax.experimental.pallas import tpu as pltpu
from jax.sharding import PartitionSpec as P

NORM_EPS = 1e-6
SOFT_CAP = 50.0
ROPE_BASE = 10000.0
WINDOW_LEN = 4096
BF16 = jnp.bfloat16
F32 = jnp.float32

CHUNK = 16
LAG = 2
LINE = 4
VMEM_BYTES = 67043328

PASS_Y = [(0, 0), (3, 0), (5, 1), (9, 0), (11, 0), (13, 0), (15, 0), (17, 0), (19, 0), (20, 1), (23, 0), (25, 0), (27, 0), (29, 0), (30, 0), (31, 0), (32, 0), (33, 0), (33, 1), (34, 1), (35, 1), (36, 1), (37, 0), (37, 1), (38, 1), (39, 1), (40, 1), (42, 0)]
PASS_X = [(3, 1), (8, 0), (11, 0), (13, 0), (13, 1), (17, 0), (18, 0), (19, 1), (22, 0), (25, 0), (26, 1), (29, 0), (30, 1), (32, 0), (33, 0), (33, 1), (34, 1), (35, 1), (36, 1), (37, 1), (37, 1), (38, 1), (39, 1), (40, 1), (43, 0), None, None, None]
GATE_TURNS = [20, 20, 21, 26, 30, 33, 33, 34, 34, 35, 35, 36, 36, 37, 37, 38, 38, 39, 39, 40, 40]

ANY = pl.BlockSpec(memory_space=pl.ANY)
VMEM = pl.BlockSpec(memory_space=pltpu.VMEM)
DMA = pltpu.SemaphoreType.DMA


def places():
    row = lax.axis_index('dp')
    line = lax.axis_index('tp')
    me = lax.axis_index('dm')
    side = lax.div(me, 2)
    core = me - 2 * side
    return row, line, me, 2 * side + 1 - core, 2 * (1 - side) + core, 2 * (1 - side) + 1 - core


def times(value, unit):
    return value if isinstance(value, int) else pl.multiple_of(value, unit)


def remote(src, dst, send_sem, recv_sem, device):
    return pltpu.make_async_remote_copy(src_ref=src, dst_ref=dst, send_sem=send_sem, recv_sem=recv_sem, device_id=device, device_id_type=pl.DeviceIdType.MESH)


def meet(peers):
    barrier = pltpu.get_barrier_semaphore()
    for peer in peers:
        pl.semaphore_signal(barrier, inc=1, device_id=peer, device_id_type=pl.DeviceIdType.MESH)
    pl.semaphore_wait(barrier, len(peers))


def line_peers(line):
    return [{'tp': lax.rem(line + 1, LINE)}, {'tp': lax.rem(line + LINE - 1, LINE)}]


QKV, OUT, GATE, UP, DOWN = range(5)


class WeightGather:
    def __init__(self, refs, pieces, tile, own_send, own_recv, send, recv):
        self.refs, self.pieces, self.tile = refs, pieces, tile
        self.own_send, self.own_recv, self.send, self.recv = own_send, own_recv, send, recv
        self.row, _, self.me, self.mate, self.across, self.cross = places()
        self.order = [(QKV, p) for p in range(pieces[QKV])] + [(OUT, p) for p in range(pieces[OUT])]
        self.order += [(part, p) for p in range(pieces[GATE]) for part in (GATE, UP)]
        self.order += [(DOWN, p) for p in range(pieces[DOWN])]

    def index(self, part, p):
        first = {QKV: 0, OUT: self.pieces[QKV]}
        ffw = self.pieces[QKV] + self.pieces[OUT]
        if part in first:
            return first[part] + p
        if part == DOWN:
            return ffw + 2 * self.pieces[GATE] + p
        return ffw + 2 * p + (part - GATE)

    def direct(self, part, p):
        return part == DOWN and p == self.pieces[DOWN] - 1

    def cut(self, part, half, p):
        size = self.refs[part][0].shape[0] // (2 * self.pieces[part])
        return pl.ds(pl.multiple_of((half * self.pieces[part] + p) * size, size), size)

    def own(self, part, half, p):
        src = self.refs[part][0]
        if part in (GATE, UP):
            size = self.tile // 2
            return src.at[:, pl.ds(pl.multiple_of(p * self.tile + half * size, size), size)]
        return src.at[self.cut(part, half, p)]

    def at(self, part, shard, half, p):
        src, dst = self.refs[part]
        if part == QKV:
            size = src.shape[0] // (2 * self.pieces[part])
            return dst.at[pl.ds(pl.multiple_of(shard * src.shape[0] + (half * self.pieces[part] + p) * size, size), size)]
        if part == OUT:
            return dst.at[self.cut(part, half, p), pl.ds(pl.multiple_of(shard * src.shape[1], src.shape[1]), src.shape[1])]
        if part == DOWN:
            return dst.at[shard, self.cut(part, half, p)]
        size = self.tile // 2
        return dst.at[p, pl.ds(pl.multiple_of(shard * src.shape[0], src.shape[0]), src.shape[0]), pl.ds(pl.multiple_of(half * size, size), size)]

    def copy(self, part, p, hop):
        mine, other = self.row, 1 - self.row
        k = self.index(part, p)
        device = {'dm': self.mate}
        if hop == 0 or (hop == 1 and self.direct(part, p)):
            half = mine if hop == 0 else other
            src, dst, device = self.own(part, half, p), self.at(part, self.me, half, p), {'dm': self.across}
        else:
            src = dst = self.at(part, self.across, other if hop == 3 else mine, p)
            if hop == 1:
                device = {'dp': other}
        return remote(src, dst, self.send.at[k, hop], self.recv.at[k, hop], device)

    def arrival(self, part, p, hop):
        k = self.index(part, p)
        region = self.at(part, self.across if hop < 2 else self.cross, 1 - self.row if hop % 2 else self.row, p)
        return remote(region, region, self.send.at[k, hop], self.recv.at[k, hop], {'dm': self.mate})

    def own_copy(self, part, p, shard):
        src, dst = self.refs[part]
        if part in (GATE, UP):
            src = src.at[:, pl.ds(times(p * self.tile, self.tile), self.tile)]
            dst = dst.at[p, pl.ds(pl.multiple_of(shard * src.shape[0], src.shape[0]), src.shape[0])]
            k = 3 + 2 * p + part - GATE
        else:
            k = (QKV, OUT, DOWN).index(part)
            if part == DOWN:
                dst = dst.at[shard]
            elif part == OUT:
                dst = dst.at[:, pl.ds(pl.multiple_of(shard * src.shape[1], src.shape[1]), src.shape[1])]
            else:
                dst = dst.at[pl.ds(pl.multiple_of(shard * src.shape[0], src.shape[0]), src.shape[0])]
        return remote(src, dst, self.own_send.at[k], self.own_recv.at[k], {'dm': self.mate})

    def start(self):
        for part, p in self.order:
            self.copy(part, p, 0).start()
            if self.direct(part, p):
                self.copy(part, p, 1).start()

    def pass_y(self, part, p):
        self.arrival(part, p, 0).wait_recv()
        if not self.direct(part, p):
            self.copy(part, p, 1).start()
        self.copy(part, p, 2).start()

    def pass_x(self, part, p):
        self.arrival(part, p, 1).wait_recv()
        self.copy(part, p, 3).start()

    def landed(self, part, p):
        self.arrival(part, p, 2).wait_recv()
        self.arrival(part, p, 3).wait_recv()

    def sent(self, part, p):
        for hop in range(4):
            self.copy(part, p, hop).wait_send()

    def own_start(self, part, p=0):
        self.own_copy(part, p, self.me).start()

    def own_landed(self, part, p=0):
        self.own_copy(part, p, self.mate).wait_recv()

    def own_sent(self, part, p=0):
        self.own_copy(part, p, self.me).wait_send()


class LineSum:
    def __init__(self, p_buf, got, out, sum_send, sum_recv, out_send, out_recv, finish, emit):
        self.p_buf, self.got, self.out = p_buf, got, out
        self.sum_send, self.sum_recv, self.out_send, self.out_recv = sum_send, sum_recv, out_send, out_recv
        self.finish, self.emit = finish, emit
        self.half = p_buf.shape[0] // 2
        self.chunks = self.half // CHUNK
        self.steps = self.chunks + 6 * LAG
        self.line = lax.axis_index('tp')

    def way(self, d):
        if d == 0:
            return self.line, {'tp': self.line + 1}, {'tp': self.line - 1}
        return LINE - 1 - self.line, {'tp': self.line - 1}, {'tp': self.line + 1}

    def rows(self, c):
        return pl.ds(pl.multiple_of(c * CHUNK, CHUNK), CHUNK)

    def out_rows(self, d, c):
        return pl.ds(pl.multiple_of(d * self.half + c * CHUNK, CHUNK), CHUNK)

    def sum_copy(self, d, c):
        return remote(self.p_buf.at[self.out_rows(d, c)], self.got.at[d, self.rows(c)], self.sum_send.at[d, c], self.sum_recv.at[d, c], self.way(d)[1])

    def out_copy(self, d, c):
        region = self.out.at[self.out_rows(d, c)]
        return remote(region, region, self.out_send.at[d, c], self.out_recv.at[d, c], self.way(d)[2])

    def step(self, t):
        for d in range(2):
            with jax.named_scope(f'sum{d}'):
                self.sum_step(d, t)
        for d in range(2):
            with jax.named_scope(f'out{d}'):
                self.out_step(d, t)

    def sum_step(self, d, t):
        pos = self.way(d)[0]
        c = t - LAG * pos

        @pl.when((c >= 0) & (c < self.chunks))
        def _():
            @pl.when(pos == 0)
            def _():
                self.sum_copy(d, c).start()

            @pl.when(pos > 0)
            def _():
                self.sum_copy(d, c).wait_recv()
                total = self.p_buf[self.out_rows(d, c), :].astype(F32) + self.got[d, self.rows(c), :].astype(F32)

                @pl.when(pos < LINE - 1)
                def _():
                    self.p_buf[self.out_rows(d, c), :] = total.astype(BF16)
                    self.sum_copy(d, c).start()

                @pl.when(pos == LINE - 1)
                def _():
                    self.finish(self.out_rows(d, c), self.rows(c), total.astype(BF16))
                    self.out_copy(d, c).start()
                    self.emit(self.out_rows(d, c))

    def out_step(self, d, t):
        pos = self.way(d)[0]
        c = t - 3 * LAG - LAG * (LINE - 1 - pos)

        @pl.when((c >= 0) & (c < self.chunks) & (pos < LINE - 1))
        def _():
            self.out_copy(d, c).wait_recv()

            @pl.when(pos > 0)
            def _():
                self.out_copy(d, c).start()

            self.emit(self.out_rows(d, c))

    def run(self, before, each, after):
        def body(t, carry):
            def act(actions):
                for turn in sorted(actions):

                    @pl.when(t == turn)
                    def _():
                        for action in actions[turn]:
                            action()

            with jax.named_scope('before'):
                act(before)
            with jax.named_scope('each'):
                each(t)
            with jax.named_scope('after'):
                act(after)
            self.step(t)
            return carry

        lax.fori_loop(0, self.steps, body, 0)

    def settle(self):
        def body(c, carry):
            for d in range(2):
                pos = self.way(d)[0]

                @pl.when(pos < LINE - 1)
                def _():
                    self.sum_copy(d, c).wait_send()

                @pl.when(pos > 0)
                def _():
                    self.out_copy(d, c).wait_send()

            return carry

        lax.fori_loop(0, self.chunks, body, 0)


def unit_rows(values, gain):
    mean_sq = jnp.mean(values * values, axis=-1, keepdims=True)
    return values * lax.rsqrt(mean_sq + NORM_EPS) * gain


def rotate(values, cos_tab, sin_tab):
    half_dim = values.shape[-1] // 2
    lower = values[:, :half_dim].astype(F32)
    upper = values[:, half_dim:].astype(F32)
    return jnp.concatenate([lower * cos_tab - upper * sin_tab, upper * cos_tab + lower * sin_tab], axis=-1).astype(BF16)


def turns_of(table, t):
    first = sum([jnp.where(t > turn, 1, 0) for turn in table], 0)
    return first, first + sum([jnp.where(t == turn, 1, 0) for turn in table], 0)


def layer_kernel(scale, kv_heads, head_dim, pieces, x_ref, n_ref, wq_ref, wk_ref, wv_ref, wo_ref, wg_ref, wu_ref, wd_ref, cos_ref, sin_ref, pos_col_ref, pos_row_ref, y_ref, kf_ref, vf_ref, wgf_ref, wuf_ref, wdf_ref, xm_buf, w_buf, wo_buf, qkv_buf, p_buf, got, res_buf, n_buf, gain_buf, wq_buf, wk_buf, wv_buf, k_buf, v_buf, x_send, x_recv, n_send, n_recv, z_send, z_recv, own_send, own_recv, w_send, w_recv, load_sem, gate_sem, down_sem, kv_store, kv_send, kv_recv, fin_send, fin_recv, fin_own, *line_sems):
    row, line, me, mate, across, cross = places()
    seq, dim = xm_buf.shape
    cols = dim // 4
    half = seq // 2
    quarter = seq // LINE
    sub = quarter // 2
    heads = wo_ref.shape[0] // head_dim
    group = heads // kv_heads
    tiles, _, tile = wgf_ref.shape
    peers = (mate, across, cross)

    def shard_span(shard):
        return pl.ds(pl.multiple_of(shard * cols, cols), cols)

    mine = shard_span(me)
    refs = ((w_buf.at[mine], w_buf), (wo_ref, wo_buf), (wg_ref, wgf_ref), (wu_ref, wuf_ref), (wd_ref, wdf_ref))
    gather = WeightGather(refs, pieces, tile, own_send, own_recv, w_send, w_recv)
    pass_y, pass_x = gather.pass_y, gather.pass_x

    def x_copy(hop, s):
        dev = peers[hop]
        if hop == 0:
            src, dst = x_ref.at[pl.ds(pl.multiple_of(dev * seq, seq), seq)], xm_buf.at[:, mine]
        else:
            start = line * quarter + s * sub
            src = x_ref.at[pl.ds(pl.multiple_of(dev * seq + start, sub), sub)]
            dst = xm_buf.at[pl.ds(pl.multiple_of(start, sub), sub), mine]
        return remote(src, dst, x_send.at[hop, s], x_recv.at[hop, s], {'dm': dev})

    def x_arrival(hop, s):
        theirs = shard_span(peers[hop])
        region = xm_buf.at[:, theirs] if hop == 0 else xm_buf.at[pl.ds(pl.multiple_of(line * quarter + s * sub, sub), sub), theirs]
        return remote(region, region, x_send.at[hop, s], x_recv.at[hop, s], {'dm': mate})

    far = pl.ds(pl.multiple_of((1 - lax.div(me, 2)) * 2 * cols, 2 * cols), 2 * cols)

    def z_copy(up, block, s):
        index = 2 * block + s
        region = xm_buf.at[pl.ds(pl.multiple_of(index * sub, sub), sub), far]
        device = {'tp': line + 1} if up else {'tp': line - 1}
        return remote(region, region, z_send.at[0 if up else 1, index], z_recv.at[index], device)

    def z_first(s):
        x_arrival(1, s).wait_recv()
        x_arrival(2, s).wait_recv()

        @pl.when(line < LINE - 1)
        def _():
            z_copy(True, line, s).start()

        @pl.when(line > 0)
        def _():
            z_copy(False, line, s).start()

    def z_step(step, s):
        below, above = line - step, line + step

        @pl.when(below >= 0)
        def _():
            z_copy(True, below, s).wait_recv()

            @pl.when(line < LINE - 1)
            def _():
                z_copy(True, below, s).start()

        @pl.when(above < LINE)
        def _():
            z_copy(False, above, s).wait_recv()

            @pl.when(line > 0)
            def _():
                z_copy(False, above, s).start()

    n_copies = [remote(n_ref, n_buf.at[me], n_send.at[i], n_recv.at[i], {'dm': dev}) for i, dev in enumerate(peers)]
    n_arrivals = [remote(n_ref, n_buf.at[dev], n_send.at[i], n_recv.at[i], {'dm': dev}) for i, dev in enumerate(peers)]
    loads = [
        pltpu.make_async_copy(x_ref.at[pl.ds(pl.multiple_of(me * seq, seq), seq)], xm_buf.at[:, mine], load_sem.at[0]),
        pltpu.make_async_copy(wo_ref, wo_buf.at[:, mine], load_sem.at[1]),
        pltpu.make_async_copy(n_ref, n_buf.at[me], load_sem.at[2]),
    ]
    thirds = ((wq_ref, wq_buf), (wk_ref, wk_buf), (wv_ref, wv_buf))
    third_loads = [pltpu.make_async_copy(src, buf, load_sem.at[3 + i]) for i, (src, buf) in enumerate(thirds)]

    def flatten_own():
        for load in third_loads:
            load.wait()
        flat_rows = min(cols, 64)

        def body(i, carry):
            part = pl.ds(pl.multiple_of(i * flat_rows, flat_rows), flat_rows)
            there = pl.ds(pl.multiple_of(me * cols + i * flat_rows, flat_rows), flat_rows)
            start = 0
            for _, buf in thirds:
                wide = buf.shape[1] * buf.shape[2]
                w_buf[there, start:start + wide] = buf[part].reshape(flat_rows, wide)
                start += wide
            return carry

        lax.fori_loop(0, cols // flat_rows, body, 0)

    def spread(part, share):
        count = pieces[part]
        return [p for p in range(count) if (4 * p) // count == share]

    for load in third_loads:
        load.start()
    with jax.named_scope('meet'):
        meet([{'dm': mate}, {'dm': across}, {'dm': cross}, {'dp': 1 - row}] + line_peers(line))
    for s in range(2):
        x_copy(1, s).start()
        x_copy(2, s).start()
    for copy in n_copies:
        copy.start()
    with jax.named_scope('flatten'):
        flatten_own()
    gather.start()
    x_copy(0, 0).start()
    for load in loads:
        load.start()
    gather.own_start(QKV)
    gather.own_start(OUT)
    with jax.named_scope('z0'):
        z_first(0)
        z_first(1)
        z_step(1, 0)
    with jax.named_scope('z1'):
        for p in spread(QKV, 0)[:1]:
            pass_y(QKV, p)
        z_step(1, 1)
        for p in spread(QKV, 0)[1:]:
            pass_y(QKV, p)
        for p in spread(QKV, 0)[:1]:
            pass_x(QKV, p)
        z_step(2, 0)
    with jax.named_scope('z2'):
        for p in spread(QKV, 1):
            pass_y(QKV, p)
        for p in spread(QKV, 0)[1:]:
            pass_x(QKV, p)
        z_step(2, 1)
        for p in spread(QKV, 2):
            pass_y(QKV, p)
        for p in spread(QKV, 1):
            pass_x(QKV, p)
        z_step(3, 0)
    with jax.named_scope('z3'):
        for p in spread(QKV, 3):
            pass_y(QKV, p)
        for p in spread(QKV, 2):
            pass_x(QKV, p)
        for copy in n_arrivals:
            copy.wait_recv()
        for load in loads:
            load.wait()
        for shard in range(4):
            gain_buf[:, shard * cols:(shard + 1) * cols] = 1.0 + n_buf[shard]
        x_arrival(0, 0).wait_recv()
        z_step(3, 1)

    for block in range(LINE):
        for s in range(2):

            @pl.when((block <= line) & (line < LINE - 1))
            def _():
                z_copy(True, block, s).wait_send()

            @pl.when((block >= line) & (line > 0))
            def _():
                z_copy(False, block, s).wait_send()

    first_row = pl.multiple_of(half * (1 - jnp.minimum(line, 1)), half)
    res_buf[...] = xm_buf[pl.ds(first_row, half), :]
    norm_rows = min(seq, 64)

    def norm_body(i, carry):
        part = pl.ds(pl.multiple_of(i * norm_rows, norm_rows), norm_rows)
        xm_buf[part, :] = unit_rows(xm_buf[part, :].astype(F32), gain_buf[0:1, :]).astype(BF16)
        return carry

    with jax.named_scope('norm'):
        lax.fori_loop(0, seq // norm_rows, norm_body, 0)
    with jax.named_scope('settle_qkv'):
        for p in spread(QKV, 3):
            pass_x(QKV, p)
        for part in (GATE, UP):
            for p in range(tiles):
                gather.own_start(part, p)
        gather.own_start(DOWN)
        for p in range(pieces[QKV]):
            gather.landed(QKV, p)
            gather.sent(QKV, p)
        gather.own_landed(QKV)
        gather.own_sent(QKV)

    big = min(seq, 512)
    width = qkv_buf.shape[1]
    q_tile = min(width, 512)
    q_steps = (width // q_tile) * (seq // big)

    def qkv_body(i, carry):
        column = pl.ds(pl.multiple_of(lax.rem(i, width // q_tile) * q_tile, q_tile), q_tile)
        part = pl.ds(pl.multiple_of(lax.div(i, width // q_tile) * big, big), big)
        qkv_buf[part, column] = jnp.dot(xm_buf[part, :], w_buf[:, column], preferred_element_type=F32).astype(BF16)
        return carry

    with jax.named_scope('qkv'):
        pass_y(OUT, 0)
        pass_y(OUT, 1)
        lax.fori_loop(0, q_steps // 2, qkv_body, 0)
        pass_y(OUT, 2)
        pass_x(OUT, 0)
        pass_y(OUT, 3)
        lax.fori_loop(q_steps // 2, q_steps, qkv_body, 0)
        pass_x(OUT, 1)
        pass_x(OUT, 2)
    with jax.named_scope('pass_out'):
        pass_x(OUT, 3)

    def rotate_body(i, carry):
        column = pl.ds(pl.multiple_of(i * head_dim, head_dim), head_dim)
        qkv_buf[:, column] = rotate(qkv_buf[:, column], cos_ref[...], sin_ref[...])
        return carry

    with jax.named_scope('rotate'):
        lax.fori_loop(0, heads + kv_heads, rotate_body, 0)

    def keep_caches():
        def cache_body(i, carry):
            part = pl.ds(pl.multiple_of(i * norm_rows, norm_rows), norm_rows)
            wide = kv_heads * head_dim
            for n, buf in enumerate((k_buf, v_buf)):
                start = heads * head_dim + n * wide
                buf[part] = qkv_buf[part, start:start + wide].reshape(norm_rows, kv_heads, head_dim)
            return carry

        lax.fori_loop(0, seq // norm_rows, cache_body, 0)

    block = seq // 8
    d_tile = min(dim, 512)

    def attend_block(i):
        part = slice(i * block, (i + 1) * block)
        span = (i + 1) * block
        q_index = i * block + lax.broadcasted_iota(jnp.int32, (block, span), 0)
        key_index = lax.broadcasted_iota(jnp.int32, (block, span), 1)
        allowed = (key_index <= q_index) & (pos_col_ref[part, :] - pos_row_ref[:, :span] < WINDOW_LEN)

        def head_body(h, carry):
            q_cols = pl.ds(pl.multiple_of(h * head_dim, head_dim), head_dim)
            k_cols = pl.ds(pl.multiple_of((heads + lax.div(h, group)) * head_dim, head_dim), head_dim)
            v_cols = pl.ds(pl.multiple_of((heads + kv_heads + lax.div(h, group)) * head_dim, head_dim), head_dim)
            scores = lax.dot_general(qkv_buf[part, q_cols], qkv_buf[:span, k_cols], (((1,), (1,)), ((), ())), preferred_element_type=F32)
            capped = SOFT_CAP * jnp.tanh(scores * scale / SOFT_CAP)
            weights = jnp.where(allowed, jnp.exp(capped), 0.0)
            probs = (weights / jnp.sum(weights, axis=-1, keepdims=True)).astype(BF16)
            qkv_buf[part, q_cols] = jnp.dot(probs, qkv_buf[:span, v_cols], preferred_element_type=F32).astype(BF16)
            return carry

        lax.fori_loop(0, heads, head_body, 0)

    def out_block(i):
        part = slice(i * block, (i + 1) * block)

        def out_body(n, carry):
            column = pl.ds(pl.multiple_of(n * d_tile, d_tile), d_tile)
            p_buf[part, column] = jnp.dot(qkv_buf[part, :heads * head_dim], wo_buf[:, column], preferred_element_type=F32).astype(BF16)
            return carry

        lax.fori_loop(0, dim // d_tile, out_body, 0)

    def both(i):
        attend_block(i)
        out_block(i)

    with jax.named_scope('attend0'):
        attend_block(0)
        attend_block(4)
        pass_y(GATE, 0)
    with jax.named_scope('settle_out'):
        for p in range(pieces[OUT]):
            gather.landed(OUT, p)
            gather.sent(OUT, p)
        gather.own_landed(OUT)
        gather.own_sent(OUT)
    with jax.named_scope('out0'):
        out_block(0)
        out_block(4)

    def finish(out_rows, rows, total):
        hidden = (res_buf[rows, :].astype(F32) + unit_rows(total.astype(F32), gain_buf[1:2, :])).astype(BF16)
        res_buf[rows, :] = hidden
        xm_buf[out_rows, :] = unit_rows(hidden.astype(F32), gain_buf[2:3, :]).astype(BF16)

    sums = LineSum(p_buf, got, xm_buf, *line_sems[:4], finish, lambda out_rows: None)
    last = sums.steps - 1
    ahead = sums.chunks // 4

    span_rows = half // 4
    z_buf = wo_buf
    pair = 2 * tile

    def group_rows(g):
        return [pl.ds(times(d * half + g * span_rows, span_rows), span_rows) for d in range(2)]

    def gate_loads(f, base):
        copies = []
        for n, (src, dst) in enumerate(((wg_ref, wgf_ref), (wu_ref, wuf_ref))):
            column = pl.ds(times(base + n * tile, tile), tile)
            for r, shard in enumerate((me, mate, across, cross)):
                part = src.at[:, pl.ds(times(f * tile, tile), tile)] if r == 0 else dst.at[f, shard_span(shard)]
                copies.append(pltpu.make_async_copy(part, w_buf.at[shard_span(shard), column], gate_sem.at[base // pair if isinstance(base, int) else lax.div(base, pair), n, r]))
        return copies

    def gate_fetch(f, base):
        for load in gate_loads(f, base):
            load.start()

    def gate_settle(f):
        for part in (GATE, UP):
            gather.landed(part, f)
            gather.own_landed(part, f)

    def gate_work(g, f, base):
        for load in gate_loads(f, base):
            load.wait()
        parts = group_rows(g)
        ffw_in = jnp.concatenate([xm_buf[part, :] for part in parts], axis=0)
        gate = jnp.dot(ffw_in, w_buf[:, pl.ds(times(base, tile), tile)], preferred_element_type=F32).astype(BF16).astype(F32)
        up = jnp.dot(ffw_in, w_buf[:, pl.ds(times(base + tile, tile), tile)], preferred_element_type=F32).astype(BF16).astype(F32)
        gated = (jax.nn.gelu(gate, approximate=True) * up).astype(BF16)
        for d, part in enumerate(parts):
            z_buf[part, pl.ds(times(f * tile, tile), tile)] = gated[d * span_rows:(d + 1) * span_rows]

    def gate_item(i, carry):
        base = lax.rem(i, 2) * pair
        ahead_f = lax.rem(i + 1, tiles)

        @pl.when(i + 1 < tiles)
        def _():
            gate_settle(ahead_f)

        @pl.when(i + 1 < 3 * tiles)
        def _():
            gate_fetch(ahead_f, pair - base)

        gate_work(lax.div(i, tiles), lax.rem(i, tiles), base)
        return carry

    ffw = gather.order[pieces[QKV] + pieces[OUT]:]
    if len(ffw) == len(PASS_Y):
        y_turns, x_turns, gate_turns = PASS_Y, PASS_X, GATE_TURNS
    else:
        y_turns = [(min(3 + 2 * k, last), 0) for k in range(len(ffw))]
        x_turns = [(min(4 + 2 * k, last), 0) for k in range(len(ffw))]
        gate_turns = [0] * (3 * tiles)
    before, after, tail = {}, {}, []

    def at(turn, action):
        if turn is None:
            tail.append(action)
        else:
            (after if turn[1] else before).setdefault(turn[0], []).append(action)

    moves = [(turn, 0, k) for k, turn in enumerate(y_turns) if k > 0] + [(turn, 1, k) for k, turn in enumerate(x_turns)]
    for turn, way, k in sorted(moves, key=lambda move: ((99, 0) if move[0] is None else move[0], move[2] + move[1], move[1])):
        at(turn, functools.partial((pass_y, pass_x)[way], *ffw[k]))
    at((min(1, last), 1), keep_caches)
    for i in range(1, 4):
        early = (2 * ahead) // 8 if i == 3 else 0
        at((min(i * ahead - (5 * ahead) // 8 - early, last), 0), functools.partial(both, i))
        at((min(i * ahead - (3 * ahead) // 8 - early, last), 0), functools.partial(both, 4 + i))
    gate_ready = [max(x_turns[k][0] + x_turns[k][1] for k in (2 * f, 2 * f + 1)) for f in range(tiles)]
    gate_table = []
    for i in range(3 * tiles):
        turn = max(gate_turns[i], (i // tiles + 1) * ahead + 6 * LAG, gate_ready[min(i + 1, tiles - 1)])
        gate_table.append(max(turn, gate_table[-1] if gate_table else 0))

    def open_gate():
        gate_settle(0)
        gate_fetch(0, 0)

    at((min(gate_table[0], last), 0), open_gate)

    def each_first(t):
        lax.fori_loop(*turns_of([turn for turn in gate_table if turn <= last], t), gate_item, 0)

    with jax.named_scope('chain1'):
        sums.run(before, each_first, after)
    with jax.named_scope('gate_rest'):
        lax.fori_loop(len([turn for turn in gate_table if turn <= last]), 3 * tiles, gate_item, 0)
    shards = (me, mate, across, cross)

    def down_load(r, base):
        column = pl.ds(base, cols)
        sem = down_sem.at[0 if base else 1]
        return pltpu.make_async_copy(wd_ref if r == 0 else wdf_ref.at[shards[r]], w_buf.at[:, column], sem)

    def down_fetch(r, base):
        if isinstance(r, int):
            down_load(r, base).start()
            return
        for n in range(4):

            @pl.when(r == n)
            def _():
                down_load(n, base).start()

    def down_work(g, r, base):
        down_load(0, base).wait()
        parts = group_rows(g)
        gated = jnp.concatenate([z_buf[part, :] for part in parts], axis=0)
        down = jnp.dot(gated, w_buf[:, pl.ds(base, cols)], preferred_element_type=F32).astype(BF16)
        if isinstance(r, int):
            shard = shards[r]
        else:
            shard = jnp.where(r == 0, me, jnp.where(r == 1, mate, jnp.where(r == 2, across, cross)))
        for d, part in enumerate(parts):
            p_buf[part, shard_span(shard)] = down[d * span_rows:(d + 1) * span_rows]

    with jax.named_scope('tail'):
        down_fetch(0, pair)
        for action in tail:
            action()
        gather.own_landed(DOWN)
        down_fetch(1, 0)
        sums.settle()
    with jax.named_scope('down_near'):
        down_work(0, 0, pair)
        down_work(0, 1, 0)

    caches = ((k_buf, kf_ref), (v_buf, vf_ref))

    def rows_of(ref, shard):
        return ref.at[pl.ds(pl.multiple_of(shard * seq, seq), seq)]

    def kv_copy(i, hop):
        src, dst = caches[i]
        if hop == 0:
            return remote(src, rows_of(dst, me), kv_send.at[i, hop], kv_recv.at[i, hop], {'dm': across})
        if hop == 1:
            return remote(src, rows_of(dst, me), kv_send.at[i, hop], kv_recv.at[i, hop], {'dm': mate})
        return remote(rows_of(dst, across), rows_of(dst, across), kv_send.at[i, hop], kv_recv.at[i, hop], {'dm': mate})

    def kv_arrival(i, hop):
        region = rows_of(caches[i][1], (across, mate, cross)[hop])
        return remote(region, region, kv_send.at[i, hop], kv_recv.at[i, hop], {'dm': mate})

    with jax.named_scope('settle_down'):
        for p in range(pieces[DOWN]):
            gather.landed(DOWN, p)
    down_fetch(2, pair)
    down_fetch(3, 0)
    kv_stores = [pltpu.make_async_copy(src, rows_of(dst, me), kv_store.at[i]) for i, (src, dst) in enumerate(caches)]
    for i in range(2):
        kv_copy(i, 0).start()
        kv_copy(i, 1).start()
        kv_stores[i].start()
    with jax.named_scope('down_far'):
        down_work(0, 2, pair)
        down_fetch(0, pair)
        down_work(0, 3, 0)
        gate_fetch(0, 0)

    def finish_last(out_rows, rows, total):
        xm_buf[out_rows, :] = (res_buf[rows, :].astype(F32) + unit_rows(total.astype(F32), gain_buf[3:4, :])).astype(BF16)

    def emit_last(out_rows):
        there = pl.ds(pl.multiple_of(me * seq + out_rows.start, CHUNK), CHUNK)
        for i, dev in enumerate((across, cross, mate)):
            remote(xm_buf.at[out_rows, shard_span(dev)], y_ref.at[there], fin_send.at[i], fin_recv.at[i], {'dm': dev}).start()
        pltpu.make_async_copy(xm_buf.at[out_rows, mine], y_ref.at[there], fin_own).start()

    last_sums = LineSum(p_buf, got, xm_buf, *line_sems[4:], finish_last, emit_last)

    def pass_kv(i):
        kv_arrival(i, 0).wait_recv()
        kv_copy(i, 2).start()

    late_gates = [int((f + 0.5) * 2 * ahead / (tiles + 1)) for f in range(tiles)]
    late_downs = [(n * ahead) // 4 for n in range(12)]

    def late_gate(f, carry):
        gate_work(3, f, 0)

        @pl.when(f + 1 < tiles)
        def _():
            gate_fetch(f + 1, 0)

        return carry

    def late_down(n, carry):
        down_work(1 + lax.div(n, 4), lax.rem(n, 4), pair)

        @pl.when(n + 1 < 12)
        def _():
            down_fetch(lax.rem(n + 1, 4), pair)

        return carry

    def each_last(t):
        lax.fori_loop(*turns_of(late_gates, t), late_gate, 0)
        lax.fori_loop(*turns_of(late_downs, t), late_down, 0)

    with jax.named_scope('chain2'):
        last_sums.run({min(14, last - 1): [functools.partial(pass_kv, 0)], min(17, last): [functools.partial(pass_kv, 1)]}, each_last, {})
    with jax.named_scope('close'):
        last_sums.settle()
        for i in range(2):
            kv_stores[i].wait()
            for hop in range(3):
                kv_copy(i, hop).wait_send()
            kv_arrival(i, 1).wait_recv()
            kv_arrival(i, 2).wait_recv()
        for i, dev in enumerate((across, cross, mate)):
            done = remote(xm_buf.at[:, shard_span(dev)], rows_of(y_ref, dev), fin_send.at[i], fin_recv.at[i], {'dm': dev})
            done.wait_send()
            done.wait_recv()
        pltpu.make_async_copy(xm_buf.at[:, mine], rows_of(y_ref, me), fin_own).wait()
        for part in (GATE, UP):
            for p in range(tiles):
                gather.sent(part, p)
                gather.own_sent(part, p)
        for p in range(pieces[DOWN]):
            gather.sent(DOWN, p)
        gather.own_sent(DOWN)
        for copy in n_copies:
            copy.wait_send()
        x_copy(0, 0).wait_send()
        for s in range(2):
            x_copy(1, s).wait_send()
            x_copy(2, s).wait_send()


def like(*shape, dtype=BF16):
    return jax.ShapeDtypeStruct(shape, dtype)


def params(collective_id):
    return pltpu.CompilerParams(collective_id=collective_id, has_side_effects=True, vmem_limit_bytes=VMEM_BYTES)


def run_layer(x, norms, wq, wk, wv, wo, wg, wu, wd, cos_tab, sin_tab, pos, scale):
    seq = pos.shape[0]
    cols = x.shape[1]
    dim = 4 * cols
    kv_heads, head_dim = wk.shape[1:]
    width = wo.shape[0] + 2 * kv_heads * head_dim
    chunks = seq // 2 // CHUNK
    cache = (seq, kv_heads, head_dim)
    hidden = wg.shape[1]
    tile = min(hidden // 2, 512)
    tiles = hidden // tile

    def count(rows, most):
        return most if rows % (32 * most) == 0 else 2

    pieces = (count(cols, 7), 4, tiles, tiles, count(wd.shape[0], 14))
    units = sum(pieces)
    return pl.pallas_call(
        functools.partial(layer_kernel, scale, kv_heads, head_dim, pieces),
        name='layer',
        out_shape=(like(4 * seq, cols), like(4 * seq, kv_heads, head_dim), like(4 * seq, kv_heads, head_dim), like(tiles, dim, tile), like(tiles, dim, tile), like(4, *wd.shape)),
        in_specs=[ANY] * 9 + [VMEM] * 4,
        out_specs=(ANY,) * 6,
        scratch_shapes=[
            pltpu.VMEM((seq, dim), BF16), pltpu.VMEM((dim, width), BF16), pltpu.VMEM((wo.shape[0], dim), BF16), pltpu.VMEM((seq, width), BF16),
            pltpu.VMEM((seq, dim), BF16), pltpu.VMEM((2, seq // 2, dim), BF16), pltpu.VMEM((seq // 2, dim), BF16), pltpu.VMEM((4,) + norms.shape, F32), pltpu.VMEM((8, dim), F32),
            pltpu.VMEM(wq.shape, BF16), pltpu.VMEM(wk.shape, BF16), pltpu.VMEM(wv.shape, BF16), pltpu.VMEM(cache, BF16), pltpu.VMEM(cache, BF16),
            DMA((3, 2)), DMA((3, 2)), DMA((3,)), DMA((3,)), DMA((2, 2 * LINE)), DMA((2 * LINE,)), DMA((3 + 2 * tiles,)), DMA((3 + 2 * tiles,)), DMA((units, 4)), DMA((units, 4)), DMA((6,)),
            DMA((2, 2, 4)), DMA((2,)), DMA((2,)), DMA((2, 3)), DMA((2, 3)), DMA((3,)), DMA((3,)), DMA,
        ] + [DMA((2, chunks))] * 8,
        compiler_params=params(0),
    )(x, norms, wq, wk, wv, wo, wg, wu, wd, cos_tab, sin_tab, pos[:, None], pos[None, :])


def solution(mesh):
    tp_size = mesh.shape['tp']

    def layer(tokens, positions, norm_pre_attn, w_query, w_key, w_value, w_out, norm_post_attn, norm_pre_ffw, w_gate, w_up, w_down, norm_post_ffw):
        seq = positions.shape[1]
        heads, head_dim, cols = w_out.shape
        dim = 4 * cols
        scale = (dim / (heads * tp_size)) ** -0.5
        norms = jnp.stack([norm_pre_attn, norm_post_attn, norm_pre_ffw, norm_post_ffw]).astype(F32)
        norms = jnp.concatenate([norms, jnp.zeros_like(norms)])
        pos = lax.dynamic_index_in_dim(positions, lax.axis_index('dm'), 0, keepdims=False)
        half_dim = head_dim // 2
        inv_freq = ROPE_BASE ** (-2.0 * jnp.arange(half_dim, dtype=F32) / head_dim)
        angles = pos.astype(F32)[:, None] * inv_freq[None, :]
        outs = run_layer(tokens, norms, w_query, w_key, w_value, w_out.reshape(heads * head_dim, cols), w_gate, w_up, w_down, jnp.cos(angles), jnp.sin(angles), pos, scale)
        return outs[:3]

    width_spec = P('dm')
    in_specs = (P('dp', 'dm'), P('dp', None), width_spec, P('dm', 'tp', None), P('dm', 'tp', None), P('dm', 'tp', None), P('tp', None, 'dm'), width_spec, width_spec, P('dm', 'tp'), P('dm', 'tp'), P('tp', 'dm'), width_spec)
    out_specs = (P('dp', 'dm'), P('dp', 'tp', None), P('dp', 'tp', None))
    return jax.shard_map(layer, mesh=mesh, in_specs=in_specs, out_specs=out_specs, check_vma=False)
```

```python
import functools

import jax
import jax.numpy as jnp
from jax import lax
from jax.experimental import pallas as pl
from jax.experimental.pallas import tpu as pltpu
from jax.sharding import PartitionSpec as P

NORM_EPS = 1e-6
SOFT_CAP = 50.0
ROPE_BASE = 10000.0
WINDOW_LEN = 4096
BF16 = jnp.bfloat16
F32 = jnp.float32

CHUNK = 16
LAG = 2
LINE = 4
VMEM_BYTES = 67043328

PASS_Y = [(0, 0), (0, 0), (3, 1), (8, 0), (11, 0), (12, 0), (13, 1), (17, 0), (18, 0), (19, 1), (22, 0), (25, 0), (27, 0), (29, 0), (29, 1), (29, 1), (30, 1), (31, 1), (32, 1), (33, 1), (34, 0), (36, 0), (36, 1), (37, 1), (38, 1), (38, 1), (42, 0), (43, 0)]
PASS_X = [(3, 0), (5, 1), (9, 0), (11, 0), (13, 1), (16, 0), (17, 1), (19, 1), (21, 0), (24, 0), (25, 1), (28, 0), (29, 1), (31, 0), (31, 1), (32, 1), (33, 1), (35, 0), (36, 0), (36, 1), (37, 1), (38, 1), (39, 1), (42, 0), None, None, None, None]
GATE_TURNS = [20, 20, 21, 25, 29, 29, 30, 30, 31, 31, 32, 32, 33, 33, 36, 36, 37, 37, 38, 38, 39]

ANY = pl.BlockSpec(memory_space=pl.ANY)
VMEM = pl.BlockSpec(memory_space=pltpu.VMEM)
DMA = pltpu.SemaphoreType.DMA


def places():
    row = lax.axis_index('dp')
    line = lax.axis_index('tp')
    me = lax.axis_index('dm')
    side = lax.div(me, 2)
    core = me - 2 * side
    return row, line, me, 2 * side + 1 - core, 2 * (1 - side) + core, 2 * (1 - side) + 1 - core


def times(value, unit):
    return value if isinstance(value, int) else pl.multiple_of(value, unit)


def remote(src, dst, send_sem, recv_sem, device):
    return pltpu.make_async_remote_copy(src_ref=src, dst_ref=dst, send_sem=send_sem, recv_sem=recv_sem, device_id=device, device_id_type=pl.DeviceIdType.MESH)


def meet(peers):
    barrier = pltpu.get_barrier_semaphore()
    for peer in peers:
        pl.semaphore_signal(barrier, inc=1, device_id=peer, device_id_type=pl.DeviceIdType.MESH)
    pl.semaphore_wait(barrier, len(peers))


def line_peers(line):
    return [{'tp': lax.rem(line + 1, LINE)}, {'tp': lax.rem(line + LINE - 1, LINE)}]


QKV, OUT, GATE, UP, DOWN = range(5)


class WeightGather:
    def __init__(self, refs, pieces, tile, own_send, own_recv, send, recv):
        self.refs, self.pieces, self.tile = refs, pieces, tile
        self.own_send, self.own_recv, self.send, self.recv = own_send, own_recv, send, recv
        self.row, _, self.me, self.mate, self.across, self.cross = places()
        self.order = [(QKV, p) for p in range(pieces[QKV])] + [(OUT, p) for p in range(pieces[OUT])]
        self.order += [(part, p) for p in range(pieces[GATE]) for part in (GATE, UP)]
        self.order += [(DOWN, p) for p in range(pieces[DOWN])]

    def index(self, part, p):
        first = {QKV: 0, OUT: self.pieces[QKV]}
        ffw = self.pieces[QKV] + self.pieces[OUT]
        if part in first:
            return first[part] + p
        if part == DOWN:
            return ffw + 2 * self.pieces[GATE] + p
        return ffw + 2 * p + (part - GATE)

    def direct(self, part, p):
        return part == DOWN and p == self.pieces[DOWN] - 1

    def cut(self, part, half, p):
        size = self.refs[part][0].shape[0] // (2 * self.pieces[part])
        return pl.ds(pl.multiple_of((half * self.pieces[part] + p) * size, size), size)

    def own(self, part, half, p):
        src = self.refs[part][0]
        if part in (GATE, UP):
            size = self.tile // 2
            return src.at[:, pl.ds(pl.multiple_of(p * self.tile + half * size, size), size)]
        return src.at[self.cut(part, half, p)]

    def at(self, part, shard, half, p):
        src, dst = self.refs[part]
        if part == QKV:
            size = src.shape[0] // (2 * self.pieces[part])
            return dst.at[pl.ds(pl.multiple_of(shard * src.shape[0] + (half * self.pieces[part] + p) * size, size), size)]
        if part == OUT:
            return dst.at[self.cut(part, half, p), pl.ds(pl.multiple_of(shard * src.shape[1], src.shape[1]), src.shape[1])]
        if part == DOWN:
            return dst.at[shard, self.cut(part, half, p)]
        size = self.tile // 2
        return dst.at[p, pl.ds(pl.multiple_of(shard * src.shape[0], src.shape[0]), src.shape[0]), pl.ds(pl.multiple_of(half * size, size), size)]

    def copy(self, part, p, hop):
        mine, other = self.row, 1 - self.row
        k = self.index(part, p)
        device = {'dm': self.mate}
        if hop == 0 or (hop == 1 and self.direct(part, p)):
            half = mine if hop == 0 else other
            src, dst, device = self.own(part, half, p), self.at(part, self.me, half, p), {'dm': self.across}
        else:
            src = dst = self.at(part, self.across, other if hop == 3 else mine, p)
            if hop == 1:
                device = {'dp': other}
        return remote(src, dst, self.send.at[k, hop], self.recv.at[k, hop], device)

    def arrival(self, part, p, hop):
        k = self.index(part, p)
        region = self.at(part, self.across if hop < 2 else self.cross, 1 - self.row if hop % 2 else self.row, p)
        return remote(region, region, self.send.at[k, hop], self.recv.at[k, hop], {'dm': self.mate})

    def own_copy(self, part, p, shard):
        src, dst = self.refs[part]
        if part in (GATE, UP):
            src = src.at[:, pl.ds(times(p * self.tile, self.tile), self.tile)]
            dst = dst.at[p, pl.ds(pl.multiple_of(shard * src.shape[0], src.shape[0]), src.shape[0])]
            k = 3 + 2 * p + part - GATE
        else:
            k = (QKV, OUT, DOWN).index(part)
            if part == DOWN:
                dst = dst.at[shard]
            elif part == OUT:
                dst = dst.at[:, pl.ds(pl.multiple_of(shard * src.shape[1], src.shape[1]), src.shape[1])]
            else:
                dst = dst.at[pl.ds(pl.multiple_of(shard * src.shape[0], src.shape[0]), src.shape[0])]
        return remote(src, dst, self.own_send.at[k], self.own_recv.at[k], {'dm': self.mate})

    def start(self):
        for part, p in self.order:
            self.copy(part, p, 0).start()
            if self.direct(part, p):
                self.copy(part, p, 1).start()

    def pass_y(self, part, p):
        self.arrival(part, p, 0).wait_recv()
        if not self.direct(part, p):
            self.copy(part, p, 1).start()
        self.copy(part, p, 2).start()

    def pass_x(self, part, p):
        self.arrival(part, p, 1).wait_recv()
        self.copy(part, p, 3).start()

    def landed(self, part, p):
        self.arrival(part, p, 2).wait_recv()
        self.arrival(part, p, 3).wait_recv()

    def sent(self, part, p):
        for hop in range(4):
            self.copy(part, p, hop).wait_send()

    def own_start(self, part, p=0):
        self.own_copy(part, p, self.me).start()

    def own_landed(self, part, p=0):
        self.own_copy(part, p, self.mate).wait_recv()

    def own_sent(self, part, p=0):
        self.own_copy(part, p, self.me).wait_send()


class LineSum:
    def __init__(self, p_buf, got, out, sum_send, sum_recv, out_send, out_recv, finish, emit):
        self.p_buf, self.got, self.out = p_buf, got, out
        self.sum_send, self.sum_recv, self.out_send, self.out_recv = sum_send, sum_recv, out_send, out_recv
        self.finish, self.emit = finish, emit
        self.half = p_buf.shape[0] // 2
        self.chunks = self.half // CHUNK
        self.steps = self.chunks + 6 * LAG
        self.line = lax.axis_index('tp')

    def way(self, d):
        if d == 0:
            return self.line, {'tp': self.line + 1}, {'tp': self.line - 1}
        return LINE - 1 - self.line, {'tp': self.line - 1}, {'tp': self.line + 1}

    def rows(self, c):
        return pl.ds(pl.multiple_of(c * CHUNK, CHUNK), CHUNK)

    def out_rows(self, d, c):
        return pl.ds(pl.multiple_of(d * self.half + c * CHUNK, CHUNK), CHUNK)

    def sum_copy(self, d, c):
        return remote(self.p_buf.at[self.out_rows(d, c)], self.got.at[d, self.rows(c)], self.sum_send.at[d, c], self.sum_recv.at[d, c], self.way(d)[1])

    def out_copy(self, d, c):
        region = self.out.at[self.out_rows(d, c)]
        return remote(region, region, self.out_send.at[d, c], self.out_recv.at[d, c], self.way(d)[2])

    def step(self, t):
        for d in range(2):
            with jax.named_scope(f'sum{d}'):
                self.sum_step(d, t)
        for d in range(2):
            with jax.named_scope(f'out{d}'):
                self.out_step(d, t)

    def sum_step(self, d, t):
        pos = self.way(d)[0]
        c = t - LAG * pos

        @pl.when((c >= 0) & (c < self.chunks))
        def _():
            @pl.when(pos == 0)
            def _():
                self.sum_copy(d, c).start()

            @pl.when(pos > 0)
            def _():
                self.sum_copy(d, c).wait_recv()
                total = self.p_buf[self.out_rows(d, c), :].astype(F32) + self.got[d, self.rows(c), :].astype(F32)

                @pl.when(pos < LINE - 1)
                def _():
                    self.p_buf[self.out_rows(d, c), :] = total.astype(BF16)
                    self.sum_copy(d, c).start()

                @pl.when(pos == LINE - 1)
                def _():
                    self.finish(self.out_rows(d, c), self.rows(c), total.astype(BF16))
                    self.out_copy(d, c).start()
                    self.emit(self.out_rows(d, c))

    def out_step(self, d, t):
        pos = self.way(d)[0]
        c = t - 3 * LAG - LAG * (LINE - 1 - pos)

        @pl.when((c >= 0) & (c < self.chunks) & (pos < LINE - 1))
        def _():
            self.out_copy(d, c).wait_recv()

            @pl.when(pos > 0)
            def _():
                self.out_copy(d, c).start()

            self.emit(self.out_rows(d, c))

    def run(self, before, each, after):
        def body(t, carry):
            def act(actions):
                for turn in sorted(actions):

                    @pl.when(t == turn)
                    def _():
                        for action in actions[turn]:
                            action()

            with jax.named_scope('before'):
                act(before)
            with jax.named_scope('each'):
                each(t)
            with jax.named_scope('after'):
                act(after)
            self.step(t)
            return carry

        lax.fori_loop(0, self.steps, body, 0)

    def settle(self):
        def body(c, carry):
            for d in range(2):
                pos = self.way(d)[0]

                @pl.when(pos < LINE - 1)
                def _():
                    self.sum_copy(d, c).wait_send()

                @pl.when(pos > 0)
                def _():
                    self.out_copy(d, c).wait_send()

            return carry

        lax.fori_loop(0, self.chunks, body, 0)


def unit_rows(values, gain):
    mean_sq = jnp.mean(values * values, axis=-1, keepdims=True)
    return values * lax.rsqrt(mean_sq + NORM_EPS) * gain


def rotate(values, cos_tab, sin_tab):
    half_dim = values.shape[-1] // 2
    lower = values[:, :half_dim].astype(F32)
    upper = values[:, half_dim:].astype(F32)
    return jnp.concatenate([lower * cos_tab - upper * sin_tab, upper * cos_tab + lower * sin_tab], axis=-1).astype(BF16)


def turns_of(table, t):
    first = sum([jnp.where(t > turn, 1, 0) for turn in table], 0)
    return first, first + sum([jnp.where(t == turn, 1, 0) for turn in table], 0)


def layer_kernel(scale, kv_heads, head_dim, pieces, x_ref, n_ref, wq_ref, wk_ref, wv_ref, wo_ref, wg_ref, wu_ref, wd_ref, cos_ref, sin_ref, pos_col_ref, pos_row_ref, y_ref, kf_ref, vf_ref, wgf_ref, wuf_ref, wdf_ref, xm_buf, w_buf, wo_buf, qkv_buf, p_buf, got, res_buf, n_buf, gain_buf, wq_buf, wk_buf, wv_buf, k_buf, v_buf, far_buf, x_send, x_recv, n_send, n_recv, z_send, z_recv, own_send, own_recv, w_send, w_recv, load_sem, gate_sem, down_sem, far_sem, kv_store, kv_send, kv_recv, fin_send, fin_recv, fin_own, *line_sems):
    row, line, me, mate, across, cross = places()
    seq, dim = xm_buf.shape
    cols = dim // 4
    half = seq // 2
    quarter = seq // LINE
    sub = quarter // 2
    heads = wo_ref.shape[0] // head_dim
    group = heads // kv_heads
    tiles, _, tile = wgf_ref.shape
    peers = (mate, across, cross)

    def shard_span(shard):
        return pl.ds(pl.multiple_of(shard * cols, cols), cols)

    mine = shard_span(me)
    refs = ((w_buf.at[mine], w_buf), (wo_ref, wo_buf), (wg_ref, wgf_ref), (wu_ref, wuf_ref), (wd_ref, wdf_ref))
    gather = WeightGather(refs, pieces, tile, own_send, own_recv, w_send, w_recv)
    pass_y, pass_x = gather.pass_y, gather.pass_x

    def x_copy(hop, s):
        dev = peers[hop]
        if hop == 0:
            src, dst = x_ref.at[pl.ds(pl.multiple_of(dev * seq, seq), seq)], xm_buf.at[:, mine]
        else:
            start = line * quarter + s * sub
            src = x_ref.at[pl.ds(pl.multiple_of(dev * seq + start, sub), sub)]
            dst = xm_buf.at[pl.ds(pl.multiple_of(start, sub), sub), mine]
        return remote(src, dst, x_send.at[hop, s], x_recv.at[hop, s], {'dm': dev})

    def x_arrival(hop, s):
        theirs = shard_span(peers[hop])
        region = xm_buf.at[:, theirs] if hop == 0 else xm_buf.at[pl.ds(pl.multiple_of(line * quarter + s * sub, sub), sub), theirs]
        return remote(region, region, x_send.at[hop, s], x_recv.at[hop, s], {'dm': mate})

    far = pl.ds(pl.multiple_of((1 - lax.div(me, 2)) * 2 * cols, 2 * cols), 2 * cols)

    def z_copy(up, block, s):
        index = 2 * block + s
        region = xm_buf.at[pl.ds(pl.multiple_of(index * sub, sub), sub), far]
        device = {'tp': line + 1} if up else {'tp': line - 1}
        return remote(region, region, z_send.at[0 if up else 1, index], z_recv.at[index], device)

    def z_first(s):
        x_arrival(1, s).wait_recv()
        x_arrival(2, s).wait_recv()

        @pl.when(line < LINE - 1)
        def _():
            z_copy(True, line, s).start()

        @pl.when(line > 0)
        def _():
            z_copy(False, line, s).start()

    def z_step(step, s):
        below, above = line - step, line + step

        @pl.when(below >= 0)
        def _():
            z_copy(True, below, s).wait_recv()

            @pl.when(line < LINE - 1)
            def _():
                z_copy(True, below, s).start()

        @pl.when(above < LINE)
        def _():
            z_copy(False, above, s).wait_recv()

            @pl.when(line > 0)
            def _():
                z_copy(False, above, s).start()

    n_copies = [remote(n_ref, n_buf.at[me], n_send.at[i], n_recv.at[i], {'dm': dev}) for i, dev in enumerate(peers)]
    n_arrivals = [remote(n_ref, n_buf.at[dev], n_send.at[i], n_recv.at[i], {'dm': dev}) for i, dev in enumerate(peers)]
    loads = [
        pltpu.make_async_copy(x_ref.at[pl.ds(pl.multiple_of(me * seq, seq), seq)], xm_buf.at[:, mine], load_sem.at[0]),
        pltpu.make_async_copy(wo_ref, wo_buf.at[:, mine], load_sem.at[1]),
        pltpu.make_async_copy(n_ref, n_buf.at[me], load_sem.at[2]),
    ]
    thirds = ((wq_ref, wq_buf), (wk_ref, wk_buf), (wv_ref, wv_buf))
    third_loads = [pltpu.make_async_copy(src, buf, load_sem.at[3 + i]) for i, (src, buf) in enumerate(thirds)]

    def flatten_own():
        for load in third_loads:
            load.wait()
        flat_rows = min(cols, 64)

        def body(i, carry):
            part = pl.ds(pl.multiple_of(i * flat_rows, flat_rows), flat_rows)
            there = pl.ds(pl.multiple_of(me * cols + i * flat_rows, flat_rows), flat_rows)
            start = 0
            for _, buf in thirds:
                wide = buf.shape[1] * buf.shape[2]
                w_buf[there, start:start + wide] = buf[part].reshape(flat_rows, wide)
                start += wide
            return carry

        lax.fori_loop(0, cols // flat_rows, body, 0)

    def spread(part, share):
        count = pieces[part]
        return [p for p in range(count) if (4 * p) // count == share]

    for load in third_loads:
        load.start()
    with jax.named_scope('meet'):
        meet([{'dm': mate}, {'dm': across}, {'dm': cross}, {'dp': 1 - row}] + line_peers(line))
    for s in range(2):
        x_copy(1, s).start()
        x_copy(2, s).start()
    for copy in n_copies:
        copy.start()
    with jax.named_scope('flatten'):
        flatten_own()
    gather.start()
    x_copy(0, 0).start()
    for load in loads:
        load.start()
    gather.own_start(QKV)
    gather.own_start(OUT)
    with jax.named_scope('z0'):
        z_first(0)
        z_first(1)
        z_step(1, 0)
    with jax.named_scope('z1'):
        for p in spread(QKV, 0)[:1]:
            pass_y(QKV, p)
        z_step(1, 1)
        for p in spread(QKV, 0)[1:]:
            pass_y(QKV, p)
        for p in spread(QKV, 0)[:1]:
            pass_x(QKV, p)
        z_step(2, 0)
    with jax.named_scope('z2'):
        for p in spread(QKV, 1):
            pass_y(QKV, p)
        for p in spread(QKV, 0)[1:]:
            pass_x(QKV, p)
        z_step(2, 1)
        for p in spread(QKV, 2):
            pass_y(QKV, p)
        for p in spread(QKV, 1):
            pass_x(QKV, p)
        z_step(3, 0)
    with jax.named_scope('z3'):
        for p in spread(QKV, 3):
            pass_y(QKV, p)
        for p in spread(QKV, 2):
            pass_x(QKV, p)
        for copy in n_arrivals:
            copy.wait_recv()
        for load in loads:
            load.wait()
        for shard in range(4):
            gain_buf[:, shard * cols:(shard + 1) * cols] = 1.0 + n_buf[shard]
        x_arrival(0, 0).wait_recv()
        z_step(3, 1)

    for block in range(LINE):
        for s in range(2):

            @pl.when((block <= line) & (line < LINE - 1))
            def _():
                z_copy(True, block, s).wait_send()

            @pl.when((block >= line) & (line > 0))
            def _():
                z_copy(False, block, s).wait_send()

    first_row = pl.multiple_of(half * (1 - jnp.minimum(line, 1)), half)
    res_buf[...] = xm_buf[pl.ds(first_row, half), :]
    norm_rows = min(seq, 64)

    def norm_body(i, carry):
        part = pl.ds(pl.multiple_of(i * norm_rows, norm_rows), norm_rows)
        xm_buf[part, :] = unit_rows(xm_buf[part, :].astype(F32), gain_buf[0:1, :]).astype(BF16)
        return carry

    with jax.named_scope('norm'):
        lax.fori_loop(0, seq // norm_rows, norm_body, 0)
    with jax.named_scope('settle_qkv'):
        for p in spread(QKV, 3):
            pass_x(QKV, p)
        for p in range(pieces[QKV]):
            gather.landed(QKV, p)
            gather.sent(QKV, p)
        gather.own_landed(QKV)
        gather.own_sent(QKV)

    big = min(seq, 512)
    width = qkv_buf.shape[1]
    q_tile = min(width, 512)
    q_steps = (width // q_tile) * (seq // big)

    def qkv_body(i, carry):
        column = pl.ds(pl.multiple_of(lax.rem(i, width // q_tile) * q_tile, q_tile), q_tile)
        part = pl.ds(pl.multiple_of(lax.div(i, width // q_tile) * big, big), big)
        qkv_buf[part, column] = jnp.dot(xm_buf[part, :], w_buf[:, column], preferred_element_type=F32).astype(BF16)
        return carry

    with jax.named_scope('qkv'):
        pass_y(OUT, 0)
        pass_y(OUT, 1)
        lax.fori_loop(0, q_steps // 2, qkv_body, 0)
        pass_y(OUT, 2)
        pass_x(OUT, 0)
        pass_y(OUT, 3)
        lax.fori_loop(q_steps // 2, q_steps, qkv_body, 0)
        pass_x(OUT, 1)
        pass_x(OUT, 2)
        pass_y(GATE, 0)
    with jax.named_scope('pass_out'):
        pass_x(OUT, 3)

    def rotate_body(i, carry):
        column = pl.ds(pl.multiple_of(i * head_dim, head_dim), head_dim)
        qkv_buf[:, column] = rotate(qkv_buf[:, column], cos_ref[...], sin_ref[...])
        return carry

    with jax.named_scope('rotate'):
        lax.fori_loop(0, heads + kv_heads, rotate_body, 0)

    def keep_caches():
        def cache_body(i, carry):
            part = pl.ds(pl.multiple_of(i * norm_rows, norm_rows), norm_rows)
            wide = kv_heads * head_dim
            for n, buf in enumerate((k_buf, v_buf)):
                start = heads * head_dim + n * wide
                buf[part] = qkv_buf[part, start:start + wide].reshape(norm_rows, kv_heads, head_dim)
            return carry

        lax.fori_loop(0, seq // norm_rows, cache_body, 0)

    block = seq // 8
    d_tile = min(dim, 512)

    def attend_block(i):
        part = slice(i * block, (i + 1) * block)
        span = (i + 1) * block
        q_index = i * block + lax.broadcasted_iota(jnp.int32, (block, span), 0)
        key_index = lax.broadcasted_iota(jnp.int32, (block, span), 1)
        allowed = (key_index <= q_index) & (pos_col_ref[part, :] - pos_row_ref[:, :span] < WINDOW_LEN)

        def head_body(h, carry):
            q_cols = pl.ds(pl.multiple_of(h * head_dim, head_dim), head_dim)
            k_cols = pl.ds(pl.multiple_of((heads + lax.div(h, group)) * head_dim, head_dim), head_dim)
            v_cols = pl.ds(pl.multiple_of((heads + kv_heads + lax.div(h, group)) * head_dim, head_dim), head_dim)
            scores = lax.dot_general(qkv_buf[part, q_cols], qkv_buf[:span, k_cols], (((1,), (1,)), ((), ())), preferred_element_type=F32)
            capped = SOFT_CAP * jnp.tanh(scores * scale / SOFT_CAP)
            weights = jnp.where(allowed, jnp.exp(capped), 0.0)
            probs = (weights / jnp.sum(weights, axis=-1, keepdims=True)).astype(BF16)
            qkv_buf[part, q_cols] = jnp.dot(probs, qkv_buf[:span, v_cols], preferred_element_type=F32).astype(BF16)
            return carry

        lax.fori_loop(0, heads, head_body, 0)

    def out_block(i):
        part = slice(i * block, (i + 1) * block)

        def out_body(n, carry):
            column = pl.ds(pl.multiple_of(n * d_tile, d_tile), d_tile)
            p_buf[part, column] = jnp.dot(qkv_buf[part, :heads * head_dim], wo_buf[:, column], preferred_element_type=F32).astype(BF16)
            return carry

        lax.fori_loop(0, dim // d_tile, out_body, 0)

    def both(i):
        attend_block(i)
        out_block(i)

    with jax.named_scope('attend0'):
        attend_block(0)
        attend_block(4)
    with jax.named_scope('settle_out'):
        for p in range(pieces[OUT]):
            gather.landed(OUT, p)
            gather.sent(OUT, p)
        gather.own_landed(OUT)
        gather.own_sent(OUT)
        for part in (GATE, UP):
            for p in range(tiles):
                gather.own_start(part, p)
        gather.own_start(DOWN)
    with jax.named_scope('out0'):
        out_block(0)
        out_block(4)

    def finish(out_rows, rows, total):
        hidden = (res_buf[rows, :].astype(F32) + unit_rows(total.astype(F32), gain_buf[1:2, :])).astype(BF16)
        res_buf[rows, :] = hidden
        xm_buf[out_rows, :] = unit_rows(hidden.astype(F32), gain_buf[2:3, :]).astype(BF16)

    sums = LineSum(p_buf, got, xm_buf, *line_sems[:4], finish, lambda out_rows: None)
    last = sums.steps - 1
    ahead = sums.chunks // 4

    span_rows = half // 4
    z_buf = wo_buf
    pair = 2 * tile

    def group_rows(g):
        return [pl.ds(times(d * half + g * span_rows, span_rows), span_rows) for d in range(2)]

    def gate_loads(f, base):
        copies = []
        for n, (src, dst) in enumerate(((wg_ref, wgf_ref), (wu_ref, wuf_ref))):
            column = pl.ds(times(base + n * tile, tile), tile)
            for r, shard in enumerate((me, mate, across, cross)):
                part = src.at[:, pl.ds(times(f * tile, tile), tile)] if r == 0 else dst.at[f, shard_span(shard)]
                copies.append(pltpu.make_async_copy(part, w_buf.at[shard_span(shard), column], gate_sem.at[base // pair if isinstance(base, int) else lax.div(base, pair), n, r]))
        return copies

    def gate_fetch(f, base):
        for load in gate_loads(f, base):
            load.start()

    def gate_settle(f):
        for part in (GATE, UP):
            gather.landed(part, f)
            gather.own_landed(part, f)

    def gate_work(g, f, base):
        for load in gate_loads(f, base):
            load.wait()
        parts = group_rows(g)
        ffw_in = jnp.concatenate([xm_buf[part, :] for part in parts], axis=0)
        gate = jnp.dot(ffw_in, w_buf[:, pl.ds(times(base, tile), tile)], preferred_element_type=F32).astype(BF16).astype(F32)
        up = jnp.dot(ffw_in, w_buf[:, pl.ds(times(base + tile, tile), tile)], preferred_element_type=F32).astype(BF16).astype(F32)
        gated = (jax.nn.gelu(gate, approximate=True) * up).astype(BF16)
        for d, part in enumerate(parts):
            z_buf[part, pl.ds(times(f * tile, tile), tile)] = gated[d * span_rows:(d + 1) * span_rows]

    def gate_place(i):
        early = tiles - 1
        if isinstance(i, int):
            if i < 2 * early:
                return i // early, i % early
            return (i - 2 * early, early) if i < 2 * tiles else (2, i - 2 * tiles)
        g = jnp.where(i < 2 * early, lax.div(i, early), jnp.where(i < 2 * tiles, i - 2 * early, 2))
        return g, jnp.where(i < 2 * early, lax.rem(i, early), jnp.where(i < 2 * tiles, early, i - 2 * tiles))

    def gate_item(i, carry):
        base = lax.rem(i, 2) * pair
        ahead_g, ahead_f = gate_place(i + 1)

        @pl.when(ahead_g == 0)
        def _():
            gate_settle(ahead_f)

        @pl.when(i + 1 < 3 * tiles)
        def _():
            gate_fetch(ahead_f, pair - base)

        gate_work(*gate_place(i), base)
        return carry

    ffw = gather.order[pieces[QKV] + pieces[OUT]:]
    if len(ffw) == len(PASS_Y):
        y_turns, x_turns, gate_turns = PASS_Y, PASS_X, GATE_TURNS
    else:
        y_turns = [(min(3 + 2 * k, last), 0) for k in range(len(ffw))]
        x_turns = [(min(4 + 2 * k, last), 0) for k in range(len(ffw))]
        gate_turns = [0] * (3 * tiles)
    before, after, tail = {}, {}, []

    def at(turn, action):
        (after if turn[1] else before).setdefault(turn[0], []).append(action)

    late_pieces = max(1, min(3, pieces[DOWN] - 1))
    edge = pieces[DOWN] - late_pieces

    moves = [(turn, 0, k) for k, turn in enumerate(y_turns) if k > 0] + [(turn, 1, k) for k, turn in enumerate(x_turns)]
    for turn, way, k in sorted(moves, key=lambda move: ((99, 0) if move[0] is None else move[0], move[2] + move[1], move[1])):
        move = functools.partial((pass_y, pass_x)[way], *ffw[k])
        if turn is None:
            tail.append((ffw[k], move))
        else:
            at(turn, move)
    at((min(1, last), 1), keep_caches)
    for i in range(1, 4):
        early = (2 * ahead) // 8 if i == 3 else 0
        at((min(i * ahead - (5 * ahead) // 8 - early, last), 0), functools.partial(both, i))
        at((min(i * ahead - (3 * ahead) // 8 - early, last), 0), functools.partial(both, 4 + i))
    gate_ready = [max(x_turns[k][0] + x_turns[k][1] for k in (2 * f, 2 * f + 1)) for f in range(tiles)]
    gate_table = []
    for i in range(3 * tiles):
        (g, f), (next_g, next_f) = gate_place(i), gate_place(min(i + 1, 3 * tiles - 1))
        turn = max(gate_turns[i], (g + 1) * ahead + 6 * LAG, gate_ready[next_f] if next_g == 0 else 0)
        gate_table.append(max(turn, gate_table[-1] if gate_table else 0))

    def open_gate():
        gate_settle(0)
        gate_fetch(0, 0)

    at((min(gate_table[0], last), 0), open_gate)

    def each_first(t):
        lax.fori_loop(*turns_of([turn for turn in gate_table if turn <= last], t), gate_item, 0)

    with jax.named_scope('chain1'):
        sums.run(before, each_first, after)
    with jax.named_scope('gate_rest'):
        lax.fori_loop(len([turn for turn in gate_table if turn <= last]), 3 * tiles, gate_item, 0)
    shards = (me, mate, across, cross)

    def down_load(r, base):
        column = pl.ds(base, cols)
        sem = down_sem.at[0 if base else 1]
        return pltpu.make_async_copy(wd_ref if r == 0 else wdf_ref.at[shards[r]], w_buf.at[:, column], sem)

    def down_fetch(r, base):
        if isinstance(r, int):
            down_load(r, base).start()
            return
        for n in range(4):

            @pl.when(r == n)
            def _():
                down_load(n, base).start()

    def down_work(g, r, base):
        down_load(0, base).wait()
        parts = group_rows(g)
        gated = jnp.concatenate([z_buf[part, :] for part in parts], axis=0)
        down = jnp.dot(gated, w_buf[:, pl.ds(base, cols)], preferred_element_type=F32).astype(BF16)
        if isinstance(r, int):
            shard = shards[r]
        else:
            shard = jnp.where(r == 0, me, jnp.where(r == 1, mate, jnp.where(r == 2, across, cross)))
        for d, part in enumerate(parts):
            p_buf[part, shard_span(shard)] = down[d * span_rows:(d + 1) * span_rows]

    rows_each = wd_ref.shape[0] // (2 * pieces[DOWN])
    half_hidden = wd_ref.shape[0] // 2
    spans = (((0, edge * rows_each), (half_hidden, edge * rows_each)), ((edge * rows_each, late_pieces * rows_each), (half_hidden + edge * rows_each, late_pieces * rows_each)))

    def far_loads(r, base, late):
        column = pl.ds(base, cols)
        return [pltpu.make_async_copy(wdf_ref.at[shards[r], pl.ds(start, size)], w_buf.at[pl.ds(start, size), column], far_sem.at[r - 2, n]) for n, (start, size) in enumerate(spans[late])]

    def far_product(base, late):
        gated = [jnp.concatenate([z_buf[part, start:start + size] for part in group_rows(0)], axis=0) for start, size in spans[late]]
        return sum(jnp.dot(rows, w_buf[start:start + size, pl.ds(base, cols)], preferred_element_type=F32) for rows, (start, size) in zip(gated, spans[late]))

    def far_early(r, base):
        for load in far_loads(r, base, 0):
            load.wait()
        far_buf[r - 2] = far_product(base, 0)

    def far_late(r, base):
        for load in far_loads(r, base, 1):
            load.wait()
        down = (far_buf[r - 2] + far_product(base, 1)).astype(BF16)
        for d, part in enumerate(group_rows(0)):
            p_buf[part, shard_span(shards[r])] = down[d * span_rows:(d + 1) * span_rows]

    def far_start(r, base, late):
        for load in far_loads(r, base, late):
            load.start()

    with jax.named_scope('tail'):
        down_fetch(0, pair)
        gather.own_landed(DOWN)
        down_fetch(1, 0)
        sums.settle()
    with jax.named_scope('down_near'):
        down_work(0, 0, pair)
        down_work(0, 1, 0)
    with jax.named_scope('pass_early'):
        for (part, p), move in tail:
            if part != DOWN or p < edge:
                move()
        for p in range(edge):
            gather.landed(DOWN, p)
        far_start(2, pair, 0)
        far_start(3, 0, 0)
    with jax.named_scope('far_early'):
        far_early(2, pair)
        far_early(3, 0)
    with jax.named_scope('pass_late'):
        for (part, p), move in tail:
            if part == DOWN and p >= edge:
                move()

    caches = ((k_buf, kf_ref), (v_buf, vf_ref))

    def rows_of(ref, shard):
        return ref.at[pl.ds(pl.multiple_of(shard * seq, seq), seq)]

    def kv_copy(i, hop):
        src, dst = caches[i]
        if hop == 0:
            return remote(src, rows_of(dst, me), kv_send.at[i, hop], kv_recv.at[i, hop], {'dm': across})
        if hop == 1:
            return remote(src, rows_of(dst, me), kv_send.at[i, hop], kv_recv.at[i, hop], {'dm': mate})
        return remote(rows_of(dst, across), rows_of(dst, across), kv_send.at[i, hop], kv_recv.at[i, hop], {'dm': mate})

    def kv_arrival(i, hop):
        region = rows_of(caches[i][1], (across, mate, cross)[hop])
        return remote(region, region, kv_send.at[i, hop], kv_recv.at[i, hop], {'dm': mate})

    with jax.named_scope('settle_down'):
        for p in range(edge, pieces[DOWN]):
            gather.landed(DOWN, p)
    far_start(2, pair, 1)
    far_start(3, 0, 1)
    kv_stores = [pltpu.make_async_copy(src, rows_of(dst, me), kv_store.at[i]) for i, (src, dst) in enumerate(caches)]
    for i in range(2):
        kv_copy(i, 0).start()
        kv_copy(i, 1).start()
        kv_stores[i].start()
    with jax.named_scope('far_late'):
        far_late(2, pair)
        down_fetch(0, pair)
        far_late(3, 0)
        gate_fetch(0, 0)

    def finish_last(out_rows, rows, total):
        xm_buf[out_rows, :] = (res_buf[rows, :].astype(F32) + unit_rows(total.astype(F32), gain_buf[3:4, :])).astype(BF16)

    def emit_last(out_rows):
        there = pl.ds(pl.multiple_of(me * seq + out_rows.start, CHUNK), CHUNK)
        for i, dev in enumerate((across, cross, mate)):
            remote(xm_buf.at[out_rows, shard_span(dev)], y_ref.at[there], fin_send.at[i], fin_recv.at[i], {'dm': dev}).start()
        pltpu.make_async_copy(xm_buf.at[out_rows, mine], y_ref.at[there], fin_own).start()

    last_sums = LineSum(p_buf, got, xm_buf, *line_sems[4:], finish_last, emit_last)

    def pass_kv(i):
        kv_arrival(i, 0).wait_recv()
        kv_copy(i, 2).start()

    late_gates = [int((f + 0.5) * 2 * ahead / (tiles + 1)) for f in range(tiles)]
    late_downs = [(n * ahead) // 4 for n in range(12)]

    def late_gate(f, carry):
        gate_work(3, f, 0)

        @pl.when(f + 1 < tiles)
        def _():
            gate_fetch(f + 1, 0)

        return carry

    def late_down(n, carry):
        down_work(1 + lax.div(n, 4), lax.rem(n, 4), pair)

        @pl.when(n + 1 < 12)
        def _():
            down_fetch(lax.rem(n + 1, 4), pair)

        return carry

    def each_last(t):
        lax.fori_loop(*turns_of(late_gates, t), late_gate, 0)
        lax.fori_loop(*turns_of(late_downs, t), late_down, 0)

    with jax.named_scope('chain2'):
        last_sums.run({min(14, last - 1): [functools.partial(pass_kv, 0)], min(17, last): [functools.partial(pass_kv, 1)]}, each_last, {})
    with jax.named_scope('close'):
        last_sums.settle()
        for i in range(2):
            kv_stores[i].wait()
            for hop in range(3):
                kv_copy(i, hop).wait_send()
            kv_arrival(i, 1).wait_recv()
            kv_arrival(i, 2).wait_recv()
        for i, dev in enumerate((across, cross, mate)):
            done = remote(xm_buf.at[:, shard_span(dev)], rows_of(y_ref, dev), fin_send.at[i], fin_recv.at[i], {'dm': dev})
            done.wait_send()
            done.wait_recv()
        pltpu.make_async_copy(xm_buf.at[:, mine], rows_of(y_ref, me), fin_own).wait()
        for part in (GATE, UP):
            for p in range(tiles):
                gather.sent(part, p)
                gather.own_sent(part, p)
        for p in range(pieces[DOWN]):
            gather.sent(DOWN, p)
        gather.own_sent(DOWN)
        for copy in n_copies:
            copy.wait_send()
        x_copy(0, 0).wait_send()
        for s in range(2):
            x_copy(1, s).wait_send()
            x_copy(2, s).wait_send()


def like(*shape, dtype=BF16):
    return jax.ShapeDtypeStruct(shape, dtype)


def params(collective_id):
    return pltpu.CompilerParams(collective_id=collective_id, has_side_effects=True, vmem_limit_bytes=VMEM_BYTES)


def run_layer(x, norms, wq, wk, wv, wo, wg, wu, wd, cos_tab, sin_tab, pos, scale):
    seq = pos.shape[0]
    cols = x.shape[1]
    dim = 4 * cols
    kv_heads, head_dim = wk.shape[1:]
    width = wo.shape[0] + 2 * kv_heads * head_dim
    chunks = seq // 2 // CHUNK
    cache = (seq, kv_heads, head_dim)
    hidden = wg.shape[1]
    tile = min(hidden // 2, 512)
    tiles = hidden // tile

    def count(rows, most):
        return most if rows % (32 * most) == 0 else 2

    pieces = (count(cols, 7), 4, tiles, tiles, count(wd.shape[0], 14))
    units = sum(pieces)
    return pl.pallas_call(
        functools.partial(layer_kernel, scale, kv_heads, head_dim, pieces),
        name='layer',
        out_shape=(like(4 * seq, cols), like(4 * seq, kv_heads, head_dim), like(4 * seq, kv_heads, head_dim), like(tiles, dim, tile), like(tiles, dim, tile), like(4, *wd.shape)),
        in_specs=[ANY] * 9 + [VMEM] * 4,
        out_specs=(ANY,) * 6,
        scratch_shapes=[
            pltpu.VMEM((seq, dim), BF16), pltpu.VMEM((dim, width), BF16), pltpu.VMEM((wo.shape[0], dim), BF16), pltpu.VMEM((seq, width), BF16),
            pltpu.VMEM((seq, dim), BF16), pltpu.VMEM((2, seq // 2, dim), BF16), pltpu.VMEM((seq // 2, dim), BF16), pltpu.VMEM((4,) + norms.shape, F32), pltpu.VMEM((8, dim), F32),
            pltpu.VMEM(wq.shape, BF16), pltpu.VMEM(wk.shape, BF16), pltpu.VMEM(wv.shape, BF16), pltpu.VMEM(cache, BF16), pltpu.VMEM(cache, BF16), pltpu.VMEM((2, seq // 4, cols), F32),
            DMA((3, 2)), DMA((3, 2)), DMA((3,)), DMA((3,)), DMA((2, 2 * LINE)), DMA((2 * LINE,)), DMA((3 + 2 * tiles,)), DMA((3 + 2 * tiles,)), DMA((units, 4)), DMA((units, 4)), DMA((6,)),
            DMA((2, 2, 4)), DMA((2,)), DMA((2, 2)), DMA((2,)), DMA((2, 3)), DMA((2, 3)), DMA((3,)), DMA((3,)), DMA,
        ] + [DMA((2, chunks))] * 8,
        compiler_params=params(0),
    )(x, norms, wq, wk, wv, wo, wg, wu, wd, cos_tab, sin_tab, pos[:, None], pos[None, :])


def solution(mesh):
    tp_size = mesh.shape['tp']

    def layer(tokens, positions, norm_pre_attn, w_query, w_key, w_value, w_out, norm_post_attn, norm_pre_ffw, w_gate, w_up, w_down, norm_post_ffw):
        seq = positions.shape[1]
        heads, head_dim, cols = w_out.shape
        dim = 4 * cols
        scale = (dim / (heads * tp_size)) ** -0.5
        norms = jnp.stack([norm_pre_attn, norm_post_attn, norm_pre_ffw, norm_post_ffw]).astype(F32)
        norms = jnp.concatenate([norms, jnp.zeros_like(norms)])
        pos = lax.dynamic_index_in_dim(positions, lax.axis_index('dm'), 0, keepdims=False)
        half_dim = head_dim // 2
        inv_freq = ROPE_BASE ** (-2.0 * jnp.arange(half_dim, dtype=F32) / head_dim)
        angles = pos.astype(F32)[:, None] * inv_freq[None, :]
        outs = run_layer(tokens, norms, w_query, w_key, w_value, w_out.reshape(heads * head_dim, cols), w_gate, w_up, w_down, jnp.cos(angles), jnp.sin(angles), pos, scale)
        return outs[:3]

    width_spec = P('dm')
    in_specs = (P('dp', 'dm'), P('dp', None), width_spec, P('dm', 'tp', None), P('dm', 'tp', None), P('dm', 'tp', None), P('tp', None, 'dm'), width_spec, width_spec, P('dm', 'tp'), P('dm', 'tp'), P('tp', 'dm'), width_spec)
    out_specs = (P('dp', 'dm'), P('dp', 'tp', None), P('dp', 'tp', None))
    return jax.shard_map(layer, mesh=mesh, in_specs=in_specs, out_specs=out_specs, check_vma=False)
```

```python
import functools

import jax
import jax.numpy as jnp
from jax import lax
from jax.experimental import pallas as pl
from jax.experimental.pallas import tpu as pltpu
from jax.sharding import PartitionSpec as P

NORM_EPS = 1e-6
SOFT_CAP = 50.0
ROPE_BASE = 10000.0
WINDOW_LEN = 4096
BF16 = jnp.bfloat16
F32 = jnp.float32

CHUNK = 16
LAG = 2
LINE = 4
VMEM_BYTES = 67043328

PASS_Y = [(0, 0), (0, 0), (5, 0), (8, 0), (11, 0), (13, 0), (15, 0), (17, 0), (19, 0), (20, 0), (23, 0), (25, 0), (27, 0), (29, 0), (29, 1), (30, 1), (31, 1), (32, 0), (32, 1), (33, 1), (34, 1), (36, 1), (37, 1), (38, 0), (38, 1), (41, 0), (43, 0), None]
PASS_X = [(3, 0), (5, 1), (10, 0), (11, 1), (13, 1), (16, 0), (17, 1), (19, 1), (21, 0), (24, 0), (25, 1), (28, 0), (29, 1), (31, 1), (32, 0), (32, 1), (33, 1), (34, 1), (36, 1), (37, 1), (38, 0), (38, 1), (41, 0), (43, 0), None, None, None, None]
GATE_TURNS = [20, 20, 25, 29, 29, 30, 30, 31, 31, 32, 32, 33, 33, 34, 36, 36, 37, 37, 38, 38, 39]

ANY = pl.BlockSpec(memory_space=pl.ANY)
VMEM = pl.BlockSpec(memory_space=pltpu.VMEM)
DMA = pltpu.SemaphoreType.DMA


def places():
    row = lax.axis_index('dp')
    line = lax.axis_index('tp')
    me = lax.axis_index('dm')
    side = lax.div(me, 2)
    core = me - 2 * side
    return row, line, me, 2 * side + 1 - core, 2 * (1 - side) + core, 2 * (1 - side) + 1 - core


def times(value, unit):
    return value if isinstance(value, int) else pl.multiple_of(value, unit)


def remote(src, dst, send_sem, recv_sem, device):
    return pltpu.make_async_remote_copy(src_ref=src, dst_ref=dst, send_sem=send_sem, recv_sem=recv_sem, device_id=device, device_id_type=pl.DeviceIdType.MESH)


def meet(peers):
    barrier = pltpu.get_barrier_semaphore()
    for peer in peers:
        pl.semaphore_signal(barrier, inc=1, device_id=peer, device_id_type=pl.DeviceIdType.MESH)
    pl.semaphore_wait(barrier, len(peers))


def line_peers(line):
    return [{'tp': lax.rem(line + 1, LINE)}, {'tp': lax.rem(line + LINE - 1, LINE)}]


QKV, OUT, GATE, UP, DOWN = range(5)


class WeightGather:
    def __init__(self, refs, pieces, tile, own_send, own_recv, send, recv):
        self.refs, self.pieces, self.tile = refs, pieces, tile
        self.own_send, self.own_recv, self.send, self.recv = own_send, own_recv, send, recv
        self.row, _, self.me, self.mate, self.across, self.cross = places()
        self.order = [(QKV, p) for p in range(pieces[QKV])] + [(OUT, p) for p in range(pieces[OUT])]
        self.order += [(part, p) for p in range(pieces[GATE]) for part in (GATE, UP)]
        self.order += [(DOWN, p) for p in range(pieces[DOWN])]

    def index(self, part, p):
        first = {QKV: 0, OUT: self.pieces[QKV]}
        ffw = self.pieces[QKV] + self.pieces[OUT]
        if part in first:
            return first[part] + p
        if part == DOWN:
            return ffw + 2 * self.pieces[GATE] + p
        return ffw + 2 * p + (part - GATE)

    def direct(self, part, p):
        return part == DOWN and p == self.pieces[DOWN] - 1

    def cut(self, part, half, p):
        size = self.refs[part][0].shape[0] // (2 * self.pieces[part])
        return pl.ds(pl.multiple_of((half * self.pieces[part] + p) * size, size), size)

    def own(self, part, half, p):
        src = self.refs[part][0]
        if part in (GATE, UP):
            size = self.tile // 2
            return src.at[:, pl.ds(pl.multiple_of(p * self.tile + half * size, size), size)]
        return src.at[self.cut(part, half, p)]

    def at(self, part, shard, half, p):
        src, dst = self.refs[part]
        if part == QKV:
            size = src.shape[0] // (2 * self.pieces[part])
            return dst.at[pl.ds(pl.multiple_of(shard * src.shape[0] + (half * self.pieces[part] + p) * size, size), size)]
        if part == OUT:
            return dst.at[self.cut(part, half, p), pl.ds(pl.multiple_of(shard * src.shape[1], src.shape[1]), src.shape[1])]
        if part == DOWN:
            return dst.at[shard, self.cut(part, half, p)]
        size = self.tile // 2
        return dst.at[p, pl.ds(pl.multiple_of(shard * src.shape[0], src.shape[0]), src.shape[0]), pl.ds(pl.multiple_of(half * size, size), size)]

    def copy(self, part, p, hop):
        mine, other = self.row, 1 - self.row
        k = self.index(part, p)
        device = {'dm': self.mate}
        if hop == 0 or (hop == 1 and self.direct(part, p)):
            half = mine if hop == 0 else other
            src, dst, device = self.own(part, half, p), self.at(part, self.me, half, p), {'dm': self.across}
        else:
            src = dst = self.at(part, self.across, other if hop == 3 else mine, p)
            if hop == 1:
                device = {'dp': other}
        return remote(src, dst, self.send.at[k, hop], self.recv.at[k, hop], device)

    def arrival(self, part, p, hop):
        k = self.index(part, p)
        region = self.at(part, self.across if hop < 2 else self.cross, 1 - self.row if hop % 2 else self.row, p)
        return remote(region, region, self.send.at[k, hop], self.recv.at[k, hop], {'dm': self.mate})

    def own_copy(self, part, p, shard):
        src, dst = self.refs[part]
        if part in (GATE, UP):
            src = src.at[:, pl.ds(times(p * self.tile, self.tile), self.tile)]
            dst = dst.at[p, pl.ds(pl.multiple_of(shard * src.shape[0], src.shape[0]), src.shape[0])]
            k = 3 + 2 * p + part - GATE
        else:
            k = (QKV, OUT, DOWN).index(part)
            if part == DOWN:
                dst = dst.at[shard]
            elif part == OUT:
                dst = dst.at[:, pl.ds(pl.multiple_of(shard * src.shape[1], src.shape[1]), src.shape[1])]
            else:
                dst = dst.at[pl.ds(pl.multiple_of(shard * src.shape[0], src.shape[0]), src.shape[0])]
        return remote(src, dst, self.own_send.at[k], self.own_recv.at[k], {'dm': self.mate})

    def start(self):
        for part, p in self.order:
            self.copy(part, p, 0).start()
            if self.direct(part, p):
                self.copy(part, p, 1).start()

    def pass_y(self, part, p):
        self.arrival(part, p, 0).wait_recv()
        if not self.direct(part, p):
            self.copy(part, p, 1).start()
        self.copy(part, p, 2).start()

    def pass_x(self, part, p):
        self.arrival(part, p, 1).wait_recv()
        self.copy(part, p, 3).start()

    def landed(self, part, p):
        self.arrival(part, p, 2).wait_recv()
        self.arrival(part, p, 3).wait_recv()

    def sent(self, part, p):
        for hop in range(4):
            self.copy(part, p, hop).wait_send()

    def own_start(self, part, p=0):
        self.own_copy(part, p, self.me).start()

    def own_landed(self, part, p=0):
        self.own_copy(part, p, self.mate).wait_recv()

    def own_sent(self, part, p=0):
        self.own_copy(part, p, self.me).wait_send()


class LineSum:
    def __init__(self, p_buf, got, out, sum_send, sum_recv, out_send, out_recv, finish, emit):
        self.p_buf, self.got, self.out = p_buf, got, out
        self.sum_send, self.sum_recv, self.out_send, self.out_recv = sum_send, sum_recv, out_send, out_recv
        self.finish, self.emit = finish, emit
        self.half = p_buf.shape[0] // 2
        self.chunks = self.half // CHUNK
        self.steps = self.chunks + 6 * LAG
        self.line = lax.axis_index('tp')

    def way(self, d):
        if d == 0:
            return self.line, {'tp': self.line + 1}, {'tp': self.line - 1}
        return LINE - 1 - self.line, {'tp': self.line - 1}, {'tp': self.line + 1}

    def rows(self, c):
        return pl.ds(pl.multiple_of(c * CHUNK, CHUNK), CHUNK)

    def out_rows(self, d, c):
        return pl.ds(pl.multiple_of(d * self.half + c * CHUNK, CHUNK), CHUNK)

    def sum_copy(self, d, c):
        return remote(self.p_buf.at[self.out_rows(d, c)], self.got.at[d, self.rows(c)], self.sum_send.at[d, c], self.sum_recv.at[d, c], self.way(d)[1])

    def out_copy(self, d, c):
        region = self.out.at[self.out_rows(d, c)]
        return remote(region, region, self.out_send.at[d, c], self.out_recv.at[d, c], self.way(d)[2])

    def step(self, t):
        for d in range(2):
            with jax.named_scope(f'sum{d}'):
                self.sum_step(d, t)
        for d in range(2):
            with jax.named_scope(f'out{d}'):
                self.out_step(d, t)

    def sum_step(self, d, t):
        pos = self.way(d)[0]
        c = t - LAG * pos

        @pl.when((c >= 0) & (c < self.chunks))
        def _():
            @pl.when(pos == 0)
            def _():
                self.sum_copy(d, c).start()

            @pl.when(pos > 0)
            def _():
                self.sum_copy(d, c).wait_recv()
                total = self.p_buf[self.out_rows(d, c), :].astype(F32) + self.got[d, self.rows(c), :].astype(F32)

                @pl.when(pos < LINE - 1)
                def _():
                    self.p_buf[self.out_rows(d, c), :] = total.astype(BF16)
                    self.sum_copy(d, c).start()

                @pl.when(pos == LINE - 1)
                def _():
                    self.finish(self.out_rows(d, c), self.rows(c), total.astype(BF16))
                    self.out_copy(d, c).start()
                    self.emit(self.out_rows(d, c))

    def out_step(self, d, t):
        pos = self.way(d)[0]
        c = t - 3 * LAG - LAG * (LINE - 1 - pos)

        @pl.when((c >= 0) & (c < self.chunks) & (pos < LINE - 1))
        def _():
            self.out_copy(d, c).wait_recv()

            @pl.when(pos > 0)
            def _():
                self.out_copy(d, c).start()

            self.emit(self.out_rows(d, c))

    def run(self, before, each, after):
        def body(t, carry):
            def act(actions):
                for turn in sorted(actions):

                    @pl.when(t == turn)
                    def _():
                        for action in actions[turn]:
                            action()

            with jax.named_scope('before'):
                act(before)
            with jax.named_scope('each'):
                each(t)
            with jax.named_scope('after'):
                act(after)
            self.step(t)
            return carry

        lax.fori_loop(0, self.steps, body, 0)

    def settle(self):
        def body(c, carry):
            for d in range(2):
                pos = self.way(d)[0]

                @pl.when(pos < LINE - 1)
                def _():
                    self.sum_copy(d, c).wait_send()

                @pl.when(pos > 0)
                def _():
                    self.out_copy(d, c).wait_send()

            return carry

        lax.fori_loop(0, self.chunks, body, 0)


def unit_rows(values, gain):
    mean_sq = jnp.mean(values * values, axis=-1, keepdims=True)
    return values * lax.rsqrt(mean_sq + NORM_EPS) * gain


def rotate(values, cos_tab, sin_tab):
    half_dim = values.shape[-1] // 2
    lower = values[:, :half_dim].astype(F32)
    upper = values[:, half_dim:].astype(F32)
    return jnp.concatenate([lower * cos_tab - upper * sin_tab, upper * cos_tab + lower * sin_tab], axis=-1).astype(BF16)


def turns_of(table, t):
    first = sum([jnp.where(t > turn, 1, 0) for turn in table], 0)
    return first, first + sum([jnp.where(t == turn, 1, 0) for turn in table], 0)


def layer_kernel(scale, kv_heads, head_dim, pieces, x_ref, n_ref, wq_ref, wk_ref, wv_ref, wo_ref, wg_ref, wu_ref, wd_ref, cos_ref, sin_ref, pos_col_ref, pos_row_ref, y_ref, kf_ref, vf_ref, wgf_ref, wuf_ref, wdf_ref, xm_buf, w_buf, wo_buf, qkv_buf, p_buf, got, res_buf, n_buf, gain_buf, wq_buf, wk_buf, wv_buf, k_buf, v_buf, far_buf, gate_tile, x_send, x_recv, n_send, n_recv, z_send, z_recv, own_send, own_recv, w_send, w_recv, load_sem, gate_sem, down_sem, far_sem, kv_store, kv_send, kv_recv, fin_send, fin_recv, fin_own, *line_sems):
    row, line, me, mate, across, cross = places()
    seq, dim = xm_buf.shape
    cols = dim // 4
    half = seq // 2
    quarter = seq // LINE
    sub = quarter // 2
    heads = wo_ref.shape[0] // head_dim
    group = heads // kv_heads
    tiles, _, tile = wgf_ref.shape
    peers = (mate, across, cross)

    def shard_span(shard):
        return pl.ds(pl.multiple_of(shard * cols, cols), cols)

    mine = shard_span(me)
    refs = ((w_buf.at[mine], w_buf), (wo_ref, wo_buf), (wg_ref, wgf_ref), (wu_ref, wuf_ref), (wd_ref, wdf_ref))
    gather = WeightGather(refs, pieces, tile, own_send, own_recv, w_send, w_recv)
    pass_y, pass_x = gather.pass_y, gather.pass_x

    def x_copy(hop, s):
        dev = peers[hop]
        if hop == 0:
            src, dst = x_ref.at[pl.ds(pl.multiple_of(dev * seq, seq), seq)], xm_buf.at[:, mine]
        else:
            start = line * quarter + s * sub
            src = x_ref.at[pl.ds(pl.multiple_of(dev * seq + start, sub), sub)]
            dst = xm_buf.at[pl.ds(pl.multiple_of(start, sub), sub), mine]
        return remote(src, dst, x_send.at[hop, s], x_recv.at[hop, s], {'dm': dev})

    def x_arrival(hop, s):
        theirs = shard_span(peers[hop])
        region = xm_buf.at[:, theirs] if hop == 0 else xm_buf.at[pl.ds(pl.multiple_of(line * quarter + s * sub, sub), sub), theirs]
        return remote(region, region, x_send.at[hop, s], x_recv.at[hop, s], {'dm': mate})

    far = pl.ds(pl.multiple_of((1 - lax.div(me, 2)) * 2 * cols, 2 * cols), 2 * cols)

    def z_copy(up, block, s):
        index = 2 * block + s
        region = xm_buf.at[pl.ds(pl.multiple_of(index * sub, sub), sub), far]
        device = {'tp': line + 1} if up else {'tp': line - 1}
        return remote(region, region, z_send.at[0 if up else 1, index], z_recv.at[index], device)

    def z_first(s):
        x_arrival(1, s).wait_recv()
        x_arrival(2, s).wait_recv()

        @pl.when(line < LINE - 1)
        def _():
            z_copy(True, line, s).start()

        @pl.when(line > 0)
        def _():
            z_copy(False, line, s).start()

    def z_step(step, s):
        below, above = line - step, line + step

        @pl.when(below >= 0)
        def _():
            z_copy(True, below, s).wait_recv()

            @pl.when(line < LINE - 1)
            def _():
                z_copy(True, below, s).start()

        @pl.when(above < LINE)
        def _():
            z_copy(False, above, s).wait_recv()

            @pl.when(line > 0)
            def _():
                z_copy(False, above, s).start()

    n_copies = [remote(n_ref, n_buf.at[me], n_send.at[i], n_recv.at[i], {'dm': dev}) for i, dev in enumerate(peers)]
    n_arrivals = [remote(n_ref, n_buf.at[dev], n_send.at[i], n_recv.at[i], {'dm': dev}) for i, dev in enumerate(peers)]
    loads = [
        pltpu.make_async_copy(x_ref.at[pl.ds(pl.multiple_of(me * seq, seq), seq)], xm_buf.at[:, mine], load_sem.at[0]),
        pltpu.make_async_copy(wo_ref, wo_buf.at[:, mine], load_sem.at[1]),
        pltpu.make_async_copy(n_ref, n_buf.at[me], load_sem.at[2]),
    ]
    thirds = ((wq_ref, wq_buf), (wk_ref, wk_buf), (wv_ref, wv_buf))
    third_loads = [pltpu.make_async_copy(src, buf, load_sem.at[3 + i]) for i, (src, buf) in enumerate(thirds)]

    def flatten_own():
        for load in third_loads:
            load.wait()
        flat_rows = min(cols, 64)

        def body(i, carry):
            part = pl.ds(pl.multiple_of(i * flat_rows, flat_rows), flat_rows)
            there = pl.ds(pl.multiple_of(me * cols + i * flat_rows, flat_rows), flat_rows)
            start = 0
            for _, buf in thirds:
                wide = buf.shape[1] * buf.shape[2]
                w_buf[there, start:start + wide] = buf[part].reshape(flat_rows, wide)
                start += wide
            return carry

        lax.fori_loop(0, cols // flat_rows, body, 0)

    def spread(part, share):
        count = pieces[part]
        return [p for p in range(count) if (4 * p) // count == share]

    for load in third_loads:
        load.start()
    with jax.named_scope('meet'):
        meet([{'dm': mate}, {'dm': across}, {'dm': cross}, {'dp': 1 - row}] + line_peers(line))
    for s in range(2):
        x_copy(1, s).start()
        x_copy(2, s).start()
    for copy in n_copies:
        copy.start()
    with jax.named_scope('flatten'):
        flatten_own()
    gather.start()
    x_copy(0, 0).start()
    for load in loads:
        load.start()
    gather.own_start(QKV)
    gather.own_start(OUT)
    with jax.named_scope('z0'):
        z_first(0)
        z_first(1)
        z_step(1, 0)
    with jax.named_scope('z1'):
        for p in spread(QKV, 0)[:1]:
            pass_y(QKV, p)
        z_step(1, 1)
        for p in spread(QKV, 0)[1:]:
            pass_y(QKV, p)
        for p in spread(QKV, 0)[:1]:
            pass_x(QKV, p)
        z_step(2, 0)
    with jax.named_scope('z2'):
        for p in spread(QKV, 1):
            pass_y(QKV, p)
        for p in spread(QKV, 0)[1:]:
            pass_x(QKV, p)
        z_step(2, 1)
        for p in spread(QKV, 2):
            pass_y(QKV, p)
        for p in spread(QKV, 1):
            pass_x(QKV, p)
        z_step(3, 0)
    with jax.named_scope('z3'):
        for p in spread(QKV, 3):
            pass_y(QKV, p)
        for p in spread(QKV, 2):
            pass_x(QKV, p)
        for copy in n_arrivals:
            copy.wait_recv()
        for load in loads:
            load.wait()
        for shard in range(4):
            gain_buf[:, shard * cols:(shard + 1) * cols] = 1.0 + n_buf[shard]
        x_arrival(0, 0).wait_recv()
        z_step(3, 1)

    for block in range(LINE):
        for s in range(2):

            @pl.when((block <= line) & (line < LINE - 1))
            def _():
                z_copy(True, block, s).wait_send()

            @pl.when((block >= line) & (line > 0))
            def _():
                z_copy(False, block, s).wait_send()

    first_row = pl.multiple_of(half * (1 - jnp.minimum(line, 1)), half)
    res_buf[...] = xm_buf[pl.ds(first_row, half), :]
    norm_rows = min(seq, 64)

    def norm_body(i, carry):
        part = pl.ds(pl.multiple_of(i * norm_rows, norm_rows), norm_rows)
        xm_buf[part, :] = unit_rows(xm_buf[part, :].astype(F32), gain_buf[0:1, :]).astype(BF16)
        return carry

    pass_y(OUT, 0)
    with jax.named_scope('norm'):
        lax.fori_loop(0, seq // norm_rows, norm_body, 0)
    with jax.named_scope('settle_qkv'):
        pass_y(OUT, 1)
        for p in spread(QKV, 3):
            pass_x(QKV, p)
        for p in range(pieces[QKV]):
            gather.landed(QKV, p)
            gather.sent(QKV, p)
        gather.own_landed(QKV)
        gather.own_sent(QKV)

    big = min(seq, 512)
    width = qkv_buf.shape[1]
    q_tile = min(width, 512)
    q_steps = (width // q_tile) * (seq // big)

    def qkv_body(i, carry):
        column = pl.ds(pl.multiple_of(lax.rem(i, width // q_tile) * q_tile, q_tile), q_tile)
        part = pl.ds(pl.multiple_of(lax.div(i, width // q_tile) * big, big), big)
        qkv_buf[part, column] = jnp.dot(xm_buf[part, :], w_buf[:, column], preferred_element_type=F32).astype(BF16)
        return carry

    with jax.named_scope('qkv'):
        lax.fori_loop(0, q_steps // 4, qkv_body, 0)
        pass_y(OUT, 2)
        pass_x(OUT, 0)
        lax.fori_loop(q_steps // 4, q_steps // 2, qkv_body, 0)
        pass_y(OUT, 3)
        pass_x(OUT, 1)
        lax.fori_loop(q_steps // 2, q_steps, qkv_body, 0)
        pass_x(OUT, 2)
        pass_y(GATE, 0)
    with jax.named_scope('pass_out'):
        pass_x(OUT, 3)

    def rotate_body(i, carry):
        column = pl.ds(pl.multiple_of(i * head_dim, head_dim), head_dim)
        qkv_buf[:, column] = rotate(qkv_buf[:, column], cos_ref[...], sin_ref[...])
        return carry

    with jax.named_scope('rotate'):
        lax.fori_loop(0, heads + kv_heads, rotate_body, 0)

    def keep_caches():
        def cache_body(i, carry):
            part = pl.ds(pl.multiple_of(i * norm_rows, norm_rows), norm_rows)
            wide = kv_heads * head_dim
            for n, buf in enumerate((k_buf, v_buf)):
                start = heads * head_dim + n * wide
                buf[part] = qkv_buf[part, start:start + wide].reshape(norm_rows, kv_heads, head_dim)
            return carry

        lax.fori_loop(0, seq // norm_rows, cache_body, 0)

    block = seq // 8
    d_tile = min(dim, 512)

    def attend_block(i):
        part = slice(i * block, (i + 1) * block)
        span = (i + 1) * block
        q_index = i * block + lax.broadcasted_iota(jnp.int32, (block, span), 0)
        key_index = lax.broadcasted_iota(jnp.int32, (block, span), 1)
        allowed = (key_index <= q_index) & (pos_col_ref[part, :] - pos_row_ref[:, :span] < WINDOW_LEN)

        def head_body(h, carry):
            q_cols = pl.ds(pl.multiple_of(h * head_dim, head_dim), head_dim)
            k_cols = pl.ds(pl.multiple_of((heads + lax.div(h, group)) * head_dim, head_dim), head_dim)
            v_cols = pl.ds(pl.multiple_of((heads + kv_heads + lax.div(h, group)) * head_dim, head_dim), head_dim)
            scores = lax.dot_general(qkv_buf[part, q_cols], qkv_buf[:span, k_cols], (((1,), (1,)), ((), ())), preferred_element_type=F32)
            capped = SOFT_CAP * jnp.tanh(scores * scale / SOFT_CAP)
            weights = jnp.where(allowed, jnp.exp(capped), 0.0)
            probs = (weights / jnp.sum(weights, axis=-1, keepdims=True)).astype(BF16)
            qkv_buf[part, q_cols] = jnp.dot(probs, qkv_buf[:span, v_cols], preferred_element_type=F32).astype(BF16)
            return carry

        lax.fori_loop(0, heads, head_body, 0)

    def out_pair(i):
        parts = [slice(n * block, (n + 1) * block) for n in (i, 4 + i)]

        def out_body(n, carry):
            column = pl.ds(pl.multiple_of(n * d_tile, d_tile), d_tile)
            rows = jnp.concatenate([qkv_buf[part, :heads * head_dim] for part in parts], axis=0)
            sums = jnp.dot(rows, wo_buf[:, column], preferred_element_type=F32).astype(BF16)
            for d, part in enumerate(parts):
                p_buf[part, column] = sums[d * block:(d + 1) * block]
            return carry

        lax.fori_loop(0, dim // d_tile, out_body, 0)

    def second(i):
        attend_block(4 + i)
        out_pair(i)

    with jax.named_scope('attend0'):
        attend_block(0)
        attend_block(4)
    with jax.named_scope('settle_out'):
        for p in range(pieces[OUT]):
            gather.landed(OUT, p)
            gather.sent(OUT, p)
        gather.own_landed(OUT)
        gather.own_sent(OUT)
        for part in (GATE, UP):
            for p in range(tiles):
                gather.own_start(part, p)
        gather.own_start(DOWN)
    with jax.named_scope('out0'):
        out_pair(0)

    def finish(out_rows, rows, total):
        hidden = (res_buf[rows, :].astype(F32) + unit_rows(total.astype(F32), gain_buf[1:2, :])).astype(BF16)
        res_buf[rows, :] = hidden
        xm_buf[out_rows, :] = unit_rows(hidden.astype(F32), gain_buf[2:3, :]).astype(BF16)

    sums = LineSum(p_buf, got, xm_buf, *line_sems[:4], finish, lambda out_rows: None)
    last = sums.steps - 1
    ahead = sums.chunks // 4

    span_rows = half // 4
    z_buf = wo_buf
    pair = 2 * tile

    def group_rows(g):
        return [pl.ds(times(d * half + g * span_rows, span_rows), span_rows) for d in range(2)]

    def gate_loads(f, base):
        copies = []
        for n, (src, dst) in enumerate(((wg_ref, wgf_ref), (wu_ref, wuf_ref))):
            column = pl.ds(times(base + n * tile, tile), tile)
            for r, shard in enumerate((me, mate, across, cross)):
                part = src.at[:, pl.ds(times(f * tile, tile), tile)] if r == 0 else dst.at[f, shard_span(shard)]
                copies.append(pltpu.make_async_copy(part, w_buf.at[shard_span(shard), column], gate_sem.at[base // pair if isinstance(base, int) else lax.div(base, pair), n, r]))
        return copies

    def gate_fetch(f, base, which=(0, 1)):
        for n in which:
            for load in gate_loads(f, base)[4 * n:4 * n + 4]:
                load.start()

    def gate_settle(f):
        for part in (GATE, UP):
            gather.landed(part, f)
            gather.own_landed(part, f)

    def gate_work(g, f, base, refill):
        parts = group_rows(g)
        ffw_in = jnp.concatenate([xm_buf[part, :] for part in parts], axis=0)
        for load in gate_loads(f, base)[:4]:
            load.wait()
        gate_tile[...] = jnp.dot(ffw_in, w_buf[:, pl.ds(times(base, tile), tile)], preferred_element_type=F32).astype(BF16)
        refill(0)
        for load in gate_loads(f, base)[4:]:
            load.wait()
        up = jnp.dot(ffw_in, w_buf[:, pl.ds(times(base + tile, tile), tile)], preferred_element_type=F32).astype(BF16).astype(F32)
        gated = (jax.nn.gelu(gate_tile[...].astype(F32), approximate=True) * up).astype(BF16)
        refill(1)
        for d, part in enumerate(parts):
            z_buf[part, pl.ds(times(f * tile, tile), tile)] = gated[d * span_rows:(d + 1) * span_rows]

    def gate_place(i):
        early = tiles - 1
        if isinstance(i, int):
            if i < 2 * early:
                return i // early, i % early
            return (i - 2 * early, early) if i < 2 * tiles else (2, i - 2 * tiles)
        g = jnp.where(i < 2 * early, lax.div(i, early), jnp.where(i < 2 * tiles, i - 2 * early, 2))
        return g, jnp.where(i < 2 * early, lax.rem(i, early), jnp.where(i < 2 * tiles, early, i - 2 * tiles))

    def gate_item(i, carry):
        base = lax.rem(i, 2) * pair
        ahead_g, ahead_f = gate_place(i + 2)

        @pl.when(ahead_g == 0)
        def _():
            gate_settle(ahead_f)

        def refill(n):
            @pl.when(i + 2 < 3 * tiles)
            def _():
                gate_fetch(ahead_f, base, (n,))

        gate_work(*gate_place(i), base, refill)
        return carry

    ffw = gather.order[pieces[QKV] + pieces[OUT]:]
    if len(ffw) == len(PASS_Y):
        y_turns, x_turns, gate_turns = PASS_Y, PASS_X, GATE_TURNS
    else:
        y_turns = [(min(3 + 2 * k, last), 0) for k in range(len(ffw))]
        x_turns = [(min(4 + 2 * k, last), 0) for k in range(len(ffw))]
        gate_turns = [0] * (3 * tiles)
    before, after, tail = {}, {}, []

    def at(turn, action):
        (after if turn[1] else before).setdefault(turn[0], []).append(action)

    late_pieces = max(1, min(3, pieces[DOWN] - 1))
    edge = pieces[DOWN] - late_pieces

    moves = [(turn, 0, k) for k, turn in enumerate(y_turns) if k > 0] + [(turn, 1, k) for k, turn in enumerate(x_turns)]
    for turn, way, k in sorted(moves, key=lambda move: ((99, 0) if move[0] is None else move[0], move[2] + move[1], move[1])):
        move = functools.partial((pass_y, pass_x)[way], *ffw[k])
        if turn is None:
            tail.append((ffw[k], move))
        else:
            at(turn, move)
    at((min(1, last), 1), keep_caches)
    for i in range(1, 4):
        early = (2 * ahead) // 8 if i == 3 else 0
        at((min(i * ahead - (5 * ahead) // 8 - early, last), 0), functools.partial(attend_block, i))
        at((min(i * ahead - (3 * ahead) // 8 - early, last), 0), functools.partial(second, i))
    gate_ready = [max(x_turns[k][0] + x_turns[k][1] for k in (2 * f, 2 * f + 1)) for f in range(tiles)]
    gate_table = []
    for i in range(3 * tiles):
        coming = [gate_place(min(i + n, 3 * tiles - 1)) for n in (0, 1, 2)]
        turn = max([gate_turns[i], (coming[0][0] + 1) * ahead + 6 * LAG] + [gate_ready[f] for g, f in coming if g == 0])
        gate_table.append(max(turn, gate_table[-1] if gate_table else 0))

    def open_gate():
        for i in range(2):
            if gate_place(i)[0] == 0:
                gate_settle(gate_place(i)[1])
            gate_fetch(gate_place(i)[1], i * pair)

    at((min(gate_table[0], last), 0), open_gate)

    def each_first(t):
        lax.fori_loop(*turns_of([turn for turn in gate_table if turn <= last], t), gate_item, 0)

    with jax.named_scope('chain1'):
        sums.run(before, each_first, after)
    with jax.named_scope('gate_rest'):
        lax.fori_loop(len([turn for turn in gate_table if turn <= last]), 3 * tiles, gate_item, 0)
    shards = (me, mate, across, cross)

    def down_load(r, base):
        column = pl.ds(base, cols)
        sem = down_sem.at[0 if base else 1]
        return pltpu.make_async_copy(wd_ref if r == 0 else wdf_ref.at[shards[r]], w_buf.at[:, column], sem)

    def down_fetch(r, base):
        if isinstance(r, int):
            down_load(r, base).start()
            return
        for n in range(4):

            @pl.when(r == n)
            def _():
                down_load(n, base).start()

    def down_work(g, r, base):
        down_load(0, base).wait()
        parts = group_rows(g)
        gated = jnp.concatenate([z_buf[part, :] for part in parts], axis=0)
        down = jnp.dot(gated, w_buf[:, pl.ds(base, cols)], preferred_element_type=F32).astype(BF16)
        if isinstance(r, int):
            shard = shards[r]
        else:
            shard = jnp.where(r == 0, me, jnp.where(r == 1, mate, jnp.where(r == 2, across, cross)))
        for d, part in enumerate(parts):
            p_buf[part, shard_span(shard)] = down[d * span_rows:(d + 1) * span_rows]

    rows_each = wd_ref.shape[0] // (2 * pieces[DOWN])
    half_hidden = wd_ref.shape[0] // 2
    spans = (((0, edge * rows_each), (half_hidden, edge * rows_each)), ((edge * rows_each, late_pieces * rows_each), (half_hidden + edge * rows_each, late_pieces * rows_each)))

    def far_loads(r, base, late):
        column = pl.ds(base, cols)
        return [pltpu.make_async_copy(wdf_ref.at[shards[r], pl.ds(start, size)], w_buf.at[pl.ds(start, size), column], far_sem.at[r - 2, n]) for n, (start, size) in enumerate(spans[late])]

    def far_product(base, late):
        gated = [jnp.concatenate([z_buf[part, start:start + size] for part in group_rows(0)], axis=0) for start, size in spans[late]]
        return sum(jnp.dot(rows, w_buf[start:start + size, pl.ds(base, cols)], preferred_element_type=F32) for rows, (start, size) in zip(gated, spans[late]))

    def far_early(r, base):
        for load in far_loads(r, base, 0):
            load.wait()
        far_buf[r - 2] = far_product(base, 0)

    def far_late(r, base):
        for load in far_loads(r, base, 1):
            load.wait()
        down = (far_buf[r - 2] + far_product(base, 1)).astype(BF16)
        for d, part in enumerate(group_rows(0)):
            p_buf[part, shard_span(shards[r])] = down[d * span_rows:(d + 1) * span_rows]

    def far_start(r, base, late):
        for load in far_loads(r, base, late):
            load.start()

    with jax.named_scope('tail'):
        down_fetch(0, pair)
        for (part, p), move in tail:
            if part != DOWN or p < edge:
                move()
        gather.own_landed(DOWN)
        down_fetch(1, 0)
        sums.settle()
    with jax.named_scope('down_near'):
        down_work(0, 0, pair)
        for (part, p), move in tail:
            if part == DOWN and p >= edge:
                move()
        down_work(0, 1, 0)
    with jax.named_scope('far_early'):
        for p in range(edge):
            gather.landed(DOWN, p)
        far_start(2, pair, 0)
        far_start(3, 0, 0)
        far_early(2, pair)
        far_early(3, 0)

    caches = ((k_buf, kf_ref), (v_buf, vf_ref))

    def rows_of(ref, shard):
        return ref.at[pl.ds(pl.multiple_of(shard * seq, seq), seq)]

    def kv_copy(i, hop):
        src, dst = caches[i]
        if hop == 0:
            return remote(src, rows_of(dst, me), kv_send.at[i, hop], kv_recv.at[i, hop], {'dm': across})
        if hop == 1:
            return remote(src, rows_of(dst, me), kv_send.at[i, hop], kv_recv.at[i, hop], {'dm': mate})
        return remote(rows_of(dst, across), rows_of(dst, across), kv_send.at[i, hop], kv_recv.at[i, hop], {'dm': mate})

    def kv_arrival(i, hop):
        region = rows_of(caches[i][1], (across, mate, cross)[hop])
        return remote(region, region, kv_send.at[i, hop], kv_recv.at[i, hop], {'dm': mate})

    with jax.named_scope('settle_down'):
        for p in range(edge, pieces[DOWN]):
            gather.landed(DOWN, p)
    far_start(2, pair, 1)
    far_start(3, 0, 1)
    kv_stores = [pltpu.make_async_copy(src, rows_of(dst, me), kv_store.at[i]) for i, (src, dst) in enumerate(caches)]
    for i in range(2):
        kv_copy(i, 0).start()
        kv_copy(i, 1).start()
        kv_stores[i].start()
    with jax.named_scope('far_late'):
        far_late(2, pair)
        down_fetch(0, pair)
        far_late(3, 0)
        gate_fetch(0, 0)

    def finish_last(out_rows, rows, total):
        xm_buf[out_rows, :] = (res_buf[rows, :].astype(F32) + unit_rows(total.astype(F32), gain_buf[3:4, :])).astype(BF16)

    def emit_last(out_rows):
        there = pl.ds(pl.multiple_of(me * seq + out_rows.start, CHUNK), CHUNK)
        for i, dev in enumerate((across, cross, mate)):
            remote(xm_buf.at[out_rows, shard_span(dev)], y_ref.at[there], fin_send.at[i], fin_recv.at[i], {'dm': dev}).start()
        pltpu.make_async_copy(xm_buf.at[out_rows, mine], y_ref.at[there], fin_own).start()

    last_sums = LineSum(p_buf, got, xm_buf, *line_sems[4:], finish_last, emit_last)

    def pass_kv(i):
        kv_arrival(i, 0).wait_recv()
        kv_copy(i, 2).start()

    late_gates = [int((f + 0.5) * 2 * ahead / (tiles + 1)) for f in range(tiles)]
    late_downs = [(n * ahead) // 4 for n in range(12)]

    def late_gate(f, carry):
        def refill(n):
            @pl.when(f + 1 < tiles)
            def _():
                gate_fetch(f + 1, 0, (n,))

        gate_work(3, f, 0, refill)
        return carry

    def late_down(n, carry):
        down_work(1 + lax.div(n, 4), lax.rem(n, 4), pair)

        @pl.when(n + 1 < 12)
        def _():
            down_fetch(lax.rem(n + 1, 4), pair)

        return carry

    def each_last(t):
        lax.fori_loop(*turns_of(late_gates, t), late_gate, 0)
        lax.fori_loop(*turns_of(late_downs, t), late_down, 0)

    with jax.named_scope('chain2'):
        last_sums.run({min(14, last - 1): [functools.partial(pass_kv, 0)], min(17, last): [functools.partial(pass_kv, 1)]}, each_last, {})
    with jax.named_scope('close'):
        last_sums.settle()
        for i in range(2):
            kv_stores[i].wait()
            for hop in range(3):
                kv_copy(i, hop).wait_send()
            kv_arrival(i, 1).wait_recv()
            kv_arrival(i, 2).wait_recv()
        for i, dev in enumerate((across, cross, mate)):
            done = remote(xm_buf.at[:, shard_span(dev)], rows_of(y_ref, dev), fin_send.at[i], fin_recv.at[i], {'dm': dev})
            done.wait_send()
            done.wait_recv()
        pltpu.make_async_copy(xm_buf.at[:, mine], rows_of(y_ref, me), fin_own).wait()
        for part in (GATE, UP):
            for p in range(tiles):
                gather.sent(part, p)
                gather.own_sent(part, p)
        for p in range(pieces[DOWN]):
            gather.sent(DOWN, p)
        gather.own_sent(DOWN)
        for copy in n_copies:
            copy.wait_send()
        x_copy(0, 0).wait_send()
        for s in range(2):
            x_copy(1, s).wait_send()
            x_copy(2, s).wait_send()


def like(*shape, dtype=BF16):
    return jax.ShapeDtypeStruct(shape, dtype)


def params(collective_id):
    return pltpu.CompilerParams(collective_id=collective_id, has_side_effects=True, vmem_limit_bytes=VMEM_BYTES)


def run_layer(x, norms, wq, wk, wv, wo, wg, wu, wd, cos_tab, sin_tab, pos, scale):
    seq = pos.shape[0]
    cols = x.shape[1]
    dim = 4 * cols
    kv_heads, head_dim = wk.shape[1:]
    width = wo.shape[0] + 2 * kv_heads * head_dim
    chunks = seq // 2 // CHUNK
    cache = (seq, kv_heads, head_dim)
    hidden = wg.shape[1]
    tile = min(hidden // 2, 512)
    tiles = hidden // tile

    def count(rows, most):
        return most if rows % (32 * most) == 0 else 2

    pieces = (count(cols, 7), 4, tiles, tiles, count(wd.shape[0], 14))
    units = sum(pieces)
    return pl.pallas_call(
        functools.partial(layer_kernel, scale, kv_heads, head_dim, pieces),
        name='layer',
        out_shape=(like(4 * seq, cols), like(4 * seq, kv_heads, head_dim), like(4 * seq, kv_heads, head_dim), like(tiles, dim, tile), like(tiles, dim, tile), like(4, *wd.shape)),
        in_specs=[ANY] * 9 + [VMEM] * 4,
        out_specs=(ANY,) * 6,
        scratch_shapes=[
            pltpu.VMEM((seq, dim), BF16), pltpu.VMEM((dim, width), BF16), pltpu.VMEM((wo.shape[0], dim), BF16), pltpu.VMEM((seq, width), BF16),
            pltpu.VMEM((seq, dim), BF16), pltpu.VMEM((2, seq // 2, dim), BF16), pltpu.VMEM((seq // 2, dim), BF16), pltpu.VMEM((4,) + norms.shape, F32), pltpu.VMEM((8, dim), F32),
            pltpu.VMEM(wq.shape, BF16), pltpu.VMEM(wk.shape, BF16), pltpu.VMEM(wv.shape, BF16), pltpu.VMEM(cache, BF16), pltpu.VMEM(cache, BF16), pltpu.VMEM((2, seq // 4, cols), F32), pltpu.VMEM((seq // 4, tile), BF16),
            DMA((3, 2)), DMA((3, 2)), DMA((3,)), DMA((3,)), DMA((2, 2 * LINE)), DMA((2 * LINE,)), DMA((3 + 2 * tiles,)), DMA((3 + 2 * tiles,)), DMA((units, 4)), DMA((units, 4)), DMA((6,)),
            DMA((2, 2, 4)), DMA((2,)), DMA((2, 2)), DMA((2,)), DMA((2, 3)), DMA((2, 3)), DMA((3,)), DMA((3,)), DMA,
        ] + [DMA((2, chunks))] * 8,
        compiler_params=params(0),
    )(x, norms, wq, wk, wv, wo, wg, wu, wd, cos_tab, sin_tab, pos[:, None], pos[None, :])


def solution(mesh):
    tp_size = mesh.shape['tp']

    def layer(tokens, positions, norm_pre_attn, w_query, w_key, w_value, w_out, norm_post_attn, norm_pre_ffw, w_gate, w_up, w_down, norm_post_ffw):
        seq = positions.shape[1]
        heads, head_dim, cols = w_out.shape
        dim = 4 * cols
        scale = (dim / (heads * tp_size)) ** -0.5
        norms = jnp.stack([norm_pre_attn, norm_post_attn, norm_pre_ffw, norm_post_ffw]).astype(F32)
        norms = jnp.concatenate([norms, jnp.zeros_like(norms)])
        pos = lax.dynamic_index_in_dim(positions, lax.axis_index('dm'), 0, keepdims=False)
        half_dim = head_dim // 2
        inv_freq = ROPE_BASE ** (-2.0 * jnp.arange(half_dim, dtype=F32) / head_dim)
        angles = pos.astype(F32)[:, None] * inv_freq[None, :]
        outs = run_layer(tokens, norms, w_query, w_key, w_value, w_out.reshape(heads * head_dim, cols), w_gate, w_up, w_down, jnp.cos(angles), jnp.sin(angles), pos, scale)
        return outs[:3]

    width_spec = P('dm')
    in_specs = (P('dp', 'dm'), P('dp', None), width_spec, P('dm', 'tp', None), P('dm', 'tp', None), P('dm', 'tp', None), P('tp', None, 'dm'), width_spec, width_spec, P('dm', 'tp'), P('dm', 'tp'), P('tp', 'dm'), width_spec)
    out_specs = (P('dp', 'dm'), P('dp', 'tp', None), P('dp', 'tp', None))
    return jax.shard_map(layer, mesh=mesh, in_specs=in_specs, out_specs=out_specs, check_vma=False)
```

```python
import functools

import jax
import jax.numpy as jnp
from jax import lax
from jax.experimental import pallas as pl
from jax.experimental.pallas import tpu as pltpu
from jax.sharding import PartitionSpec as P

NORM_EPS = 1e-6
SOFT_CAP = 50.0
ROPE_BASE = 10000.0
WINDOW_LEN = 4096
BF16 = jnp.bfloat16
F32 = jnp.float32

CHUNK = 16
LAG = 2
LINE = 4
VMEM_BYTES = 67043328

PASS_Y = [(0, 0), (0, 0), (5, 0), (8, 0), (11, 0), (13, 0), (15, 0), (17, 0), (19, 0), (20, 0), (23, 0), (25, 0), (27, 0), (29, 0), (29, 1), (30, 1), (31, 1), (32, 0), (32, 1), (33, 1), (34, 1), (36, 1), (37, 1), (38, 0), (38, 1), (41, 0), (43, 0), None]
PASS_X = [(3, 0), (5, 1), (10, 0), (11, 1), (13, 1), (16, 0), (17, 1), (19, 1), (21, 0), (24, 0), (25, 1), (28, 0), (29, 1), (31, 1), (32, 0), (32, 1), (33, 1), (34, 1), (36, 1), (37, 1), (38, 0), (38, 1), (41, 0), (43, 0), None, None, None, None]
GATE_TURNS = [20, 20, 25, 29, 29, 30, 30, 31, 31, 32, 32, 33, 33, 34, 36, 36, 37, 37, 38, 38, 39]

ANY = pl.BlockSpec(memory_space=pl.ANY)
VMEM = pl.BlockSpec(memory_space=pltpu.VMEM)
DMA = pltpu.SemaphoreType.DMA


def places():
    row = lax.axis_index('dp')
    line = lax.axis_index('tp')
    me = lax.axis_index('dm')
    side = lax.div(me, 2)
    core = me - 2 * side
    return row, line, me, 2 * side + 1 - core, 2 * (1 - side) + core, 2 * (1 - side) + 1 - core


def times(value, unit):
    return value if isinstance(value, int) else pl.multiple_of(value, unit)


def remote(src, dst, send_sem, recv_sem, device):
    return pltpu.make_async_remote_copy(src_ref=src, dst_ref=dst, send_sem=send_sem, recv_sem=recv_sem, device_id=device, device_id_type=pl.DeviceIdType.MESH)


def meet(peers):
    barrier = pltpu.get_barrier_semaphore()
    for peer in peers:
        pl.semaphore_signal(barrier, inc=1, device_id=peer, device_id_type=pl.DeviceIdType.MESH)
    pl.semaphore_wait(barrier, len(peers))


def line_peers(line):
    return [{'tp': lax.rem(line + 1, LINE)}, {'tp': lax.rem(line + LINE - 1, LINE)}]


QKV, OUT, GATE, UP, DOWN = range(5)


class WeightGather:
    def __init__(self, refs, pieces, tile, own_send, own_recv, send, recv):
        self.refs, self.pieces, self.tile = refs, pieces, tile
        self.own_send, self.own_recv, self.send, self.recv = own_send, own_recv, send, recv
        self.row, _, self.me, self.mate, self.across, self.cross = places()
        self.order = [(QKV, p) for p in range(pieces[QKV])] + [(OUT, p) for p in range(pieces[OUT])]
        self.order += [(part, p) for p in range(pieces[GATE]) for part in (GATE, UP)]
        self.order += [(DOWN, p) for p in range(pieces[DOWN])]

    def index(self, part, p):
        first = {QKV: 0, OUT: self.pieces[QKV]}
        ffw = self.pieces[QKV] + self.pieces[OUT]
        if part in first:
            return first[part] + p
        if part == DOWN:
            return ffw + 2 * self.pieces[GATE] + p
        return ffw + 2 * p + (part - GATE)

    def direct(self, part, p):
        return part == DOWN and p == self.pieces[DOWN] - 1

    def cut(self, part, half, p):
        size = self.refs[part][0].shape[0] // (2 * self.pieces[part])
        return pl.ds(pl.multiple_of((half * self.pieces[part] + p) * size, size), size)

    def own(self, part, half, p):
        src = self.refs[part][0]
        if part in (GATE, UP):
            size = self.tile // 2
            return src.at[:, pl.ds(pl.multiple_of(p * self.tile + half * size, size), size)]
        return src.at[self.cut(part, half, p)]

    def at(self, part, shard, half, p):
        src, dst = self.refs[part]
        if part == QKV:
            size = src.shape[0] // (2 * self.pieces[part])
            return dst.at[pl.ds(pl.multiple_of(shard * src.shape[0] + (half * self.pieces[part] + p) * size, size), size)]
        if part == OUT:
            return dst.at[self.cut(part, half, p), pl.ds(pl.multiple_of(shard * src.shape[1], src.shape[1]), src.shape[1])]
        if part == DOWN:
            return dst.at[shard, self.cut(part, half, p)]
        size = self.tile // 2
        return dst.at[p, pl.ds(pl.multiple_of(shard * src.shape[0], src.shape[0]), src.shape[0]), pl.ds(pl.multiple_of(half * size, size), size)]

    def copy(self, part, p, hop):
        mine, other = self.row, 1 - self.row
        k = self.index(part, p)
        device = {'dm': self.mate}
        if hop == 0 or (hop == 1 and self.direct(part, p)):
            half = mine if hop == 0 else other
            src, dst, device = self.own(part, half, p), self.at(part, self.me, half, p), {'dm': self.across}
        else:
            src = dst = self.at(part, self.across, other if hop == 3 else mine, p)
            if hop == 1:
                device = {'dp': other}
        return remote(src, dst, self.send.at[k, hop], self.recv.at[k, hop], device)

    def arrival(self, part, p, hop):
        k = self.index(part, p)
        region = self.at(part, self.across if hop < 2 else self.cross, 1 - self.row if hop % 2 else self.row, p)
        return remote(region, region, self.send.at[k, hop], self.recv.at[k, hop], {'dm': self.mate})

    def own_copy(self, part, p, shard):
        src, dst = self.refs[part]
        if part in (GATE, UP):
            src = src.at[:, pl.ds(times(p * self.tile, self.tile), self.tile)]
            dst = dst.at[p, pl.ds(pl.multiple_of(shard * src.shape[0], src.shape[0]), src.shape[0])]
            k = 3 + 2 * p + part - GATE
        else:
            k = (QKV, OUT, DOWN).index(part)
            if part == DOWN:
                dst = dst.at[shard]
            elif part == OUT:
                dst = dst.at[:, pl.ds(pl.multiple_of(shard * src.shape[1], src.shape[1]), src.shape[1])]
            else:
                dst = dst.at[pl.ds(pl.multiple_of(shard * src.shape[0], src.shape[0]), src.shape[0])]
        return remote(src, dst, self.own_send.at[k], self.own_recv.at[k], {'dm': self.mate})

    def start(self):
        for part, p in self.order:
            self.copy(part, p, 0).start()
            if self.direct(part, p):
                self.copy(part, p, 1).start()

    def pass_y(self, part, p):
        self.arrival(part, p, 0).wait_recv()
        if not self.direct(part, p):
            self.copy(part, p, 1).start()
        self.copy(part, p, 2).start()

    def pass_x(self, part, p):
        self.arrival(part, p, 1).wait_recv()
        self.copy(part, p, 3).start()

    def landed(self, part, p):
        self.arrival(part, p, 2).wait_recv()
        self.arrival(part, p, 3).wait_recv()

    def sent(self, part, p):
        for hop in range(4):
            self.copy(part, p, hop).wait_send()

    def own_start(self, part, p=0):
        self.own_copy(part, p, self.me).start()

    def own_landed(self, part, p=0):
        self.own_copy(part, p, self.mate).wait_recv()

    def own_sent(self, part, p=0):
        self.own_copy(part, p, self.me).wait_send()


class LineSum:
    def __init__(self, p_buf, got, out, sum_send, sum_recv, out_send, out_recv, finish, emit):
        self.p_buf, self.got, self.out = p_buf, got, out
        self.sum_send, self.sum_recv, self.out_send, self.out_recv = sum_send, sum_recv, out_send, out_recv
        self.finish, self.emit = finish, emit
        self.half = p_buf.shape[0] // 2
        self.chunks = self.half // CHUNK
        self.steps = self.chunks + 6 * LAG
        self.line = lax.axis_index('tp')

    def way(self, d):
        if d == 0:
            return self.line, {'tp': self.line + 1}, {'tp': self.line - 1}
        return LINE - 1 - self.line, {'tp': self.line - 1}, {'tp': self.line + 1}

    def rows(self, c):
        return pl.ds(pl.multiple_of(c * CHUNK, CHUNK), CHUNK)

    def out_rows(self, d, c):
        return pl.ds(pl.multiple_of(d * self.half + c * CHUNK, CHUNK), CHUNK)

    def sum_copy(self, d, c):
        return remote(self.p_buf.at[self.out_rows(d, c)], self.got.at[d, self.rows(c)], self.sum_send.at[d, c], self.sum_recv.at[d, c], self.way(d)[1])

    def out_copy(self, d, c):
        region = self.out.at[self.out_rows(d, c)]
        return remote(region, region, self.out_send.at[d, c], self.out_recv.at[d, c], self.way(d)[2])

    def step(self, t):
        for d in range(2):
            with jax.named_scope(f'sum{d}'):
                self.sum_step(d, t)
        for d in range(2):
            with jax.named_scope(f'out{d}'):
                self.out_step(d, t)

    def sum_step(self, d, t):
        pos = self.way(d)[0]
        c = t - LAG * pos

        @pl.when((c >= 0) & (c < self.chunks))
        def _():
            @pl.when(pos == 0)
            def _():
                self.sum_copy(d, c).start()

            @pl.when(pos > 0)
            def _():
                self.sum_copy(d, c).wait_recv()
                total = self.p_buf[self.out_rows(d, c), :].astype(F32) + self.got[d, self.rows(c), :].astype(F32)

                @pl.when(pos < LINE - 1)
                def _():
                    self.p_buf[self.out_rows(d, c), :] = total.astype(BF16)
                    self.sum_copy(d, c).start()

                @pl.when(pos == LINE - 1)
                def _():
                    self.finish(self.out_rows(d, c), self.rows(c), total.astype(BF16))
                    self.out_copy(d, c).start()
                    self.emit(self.out_rows(d, c))

    def out_step(self, d, t):
        pos = self.way(d)[0]
        c = t - 3 * LAG - LAG * (LINE - 1 - pos)

        @pl.when((c >= 0) & (c < self.chunks) & (pos < LINE - 1))
        def _():
            self.out_copy(d, c).wait_recv()

            @pl.when(pos > 0)
            def _():
                self.out_copy(d, c).start()

            self.emit(self.out_rows(d, c))

    def run(self, before, each, after):
        def body(t, carry):
            def act(actions):
                for turn in sorted(actions):

                    @pl.when(t == turn)
                    def _():
                        for action in actions[turn]:
                            action()

            with jax.named_scope('before'):
                act(before)
            with jax.named_scope('each'):
                each(t)
            with jax.named_scope('after'):
                act(after)
            self.step(t)
            return carry

        lax.fori_loop(0, self.steps, body, 0)

    def settle(self):
        def body(c, carry):
            for d in range(2):
                pos = self.way(d)[0]

                @pl.when(pos < LINE - 1)
                def _():
                    self.sum_copy(d, c).wait_send()

                @pl.when(pos > 0)
                def _():
                    self.out_copy(d, c).wait_send()

            return carry

        lax.fori_loop(0, self.chunks, body, 0)


def unit_rows(values, gain):
    mean_sq = jnp.mean(values * values, axis=-1, keepdims=True)
    return values * lax.rsqrt(mean_sq + NORM_EPS) * gain


def rotate(values, cos_tab, sin_tab):
    half_dim = values.shape[-1] // 2
    lower = values[:, :half_dim].astype(F32)
    upper = values[:, half_dim:].astype(F32)
    return jnp.concatenate([lower * cos_tab - upper * sin_tab, upper * cos_tab + lower * sin_tab], axis=-1).astype(BF16)


def turns_of(table, t):
    first = sum([jnp.where(t > turn, 1, 0) for turn in table], 0)
    return first, first + sum([jnp.where(t == turn, 1, 0) for turn in table], 0)


def layer_kernel(scale, kv_heads, head_dim, pieces, x_ref, n_ref, wq_ref, wk_ref, wv_ref, wo_ref, wg_ref, wu_ref, wd_ref, cos_ref, sin_ref, pos_col_ref, pos_row_ref, y_ref, kf_ref, vf_ref, wgf_ref, wuf_ref, wdf_ref, xm_buf, w_buf, wo_buf, qkv_buf, p_buf, got, res_buf, n_buf, gain_buf, wq_buf, wk_buf, wv_buf, k_buf, v_buf, far_buf, gate_tile, x_send, x_recv, n_send, n_recv, z_send, z_recv, own_send, own_recv, w_send, w_recv, load_sem, gate_sem, down_sem, far_sem, kv_store, kv_send, kv_recv, fin_send, fin_recv, fin_own, *line_sems):
    row, line, me, mate, across, cross = places()
    seq, dim = xm_buf.shape
    cols = dim // 4
    half = seq // 2
    quarter = seq // LINE
    sub = quarter // 2
    heads = wo_ref.shape[0] // head_dim
    group = heads // kv_heads
    tiles, _, tile = wgf_ref.shape
    peers = (mate, across, cross)

    def shard_span(shard):
        return pl.ds(pl.multiple_of(shard * cols, cols), cols)

    mine = shard_span(me)
    refs = ((w_buf.at[mine], w_buf), (wo_ref, wo_buf), (wg_ref, wgf_ref), (wu_ref, wuf_ref), (wd_ref, wdf_ref))
    gather = WeightGather(refs, pieces, tile, own_send, own_recv, w_send, w_recv)
    pass_y, pass_x = gather.pass_y, gather.pass_x

    def x_copy(hop, s):
        dev = peers[hop]
        if hop == 0:
            src, dst = x_ref.at[pl.ds(pl.multiple_of(dev * seq, seq), seq)], xm_buf.at[:, mine]
        else:
            start = line * quarter + s * sub
            src = x_ref.at[pl.ds(pl.multiple_of(dev * seq + start, sub), sub)]
            dst = xm_buf.at[pl.ds(pl.multiple_of(start, sub), sub), mine]
        return remote(src, dst, x_send.at[hop, s], x_recv.at[hop, s], {'dm': dev})

    def x_arrival(hop, s):
        theirs = shard_span(peers[hop])
        region = xm_buf.at[:, theirs] if hop == 0 else xm_buf.at[pl.ds(pl.multiple_of(line * quarter + s * sub, sub), sub), theirs]
        return remote(region, region, x_send.at[hop, s], x_recv.at[hop, s], {'dm': mate})

    far = pl.ds(pl.multiple_of((1 - lax.div(me, 2)) * 2 * cols, 2 * cols), 2 * cols)

    def z_copy(up, block, s):
        index = 2 * block + s
        region = xm_buf.at[pl.ds(pl.multiple_of(index * sub, sub), sub), far]
        device = {'tp': line + 1} if up else {'tp': line - 1}
        return remote(region, region, z_send.at[0 if up else 1, index], z_recv.at[index], device)

    def z_first(s):
        x_arrival(1, s).wait_recv()
        x_arrival(2, s).wait_recv()

        @pl.when(line < LINE - 1)
        def _():
            z_copy(True, line, s).start()

        @pl.when(line > 0)
        def _():
            z_copy(False, line, s).start()

    def z_step(step, s):
        below, above = line - step, line + step

        @pl.when(below >= 0)
        def _():
            z_copy(True, below, s).wait_recv()

            @pl.when(line < LINE - 1)
            def _():
                z_copy(True, below, s).start()

        @pl.when(above < LINE)
        def _():
            z_copy(False, above, s).wait_recv()

            @pl.when(line > 0)
            def _():
                z_copy(False, above, s).start()

    n_copies = [remote(n_ref, n_buf.at[me], n_send.at[i], n_recv.at[i], {'dm': dev}) for i, dev in enumerate(peers)]
    n_arrivals = [remote(n_ref, n_buf.at[dev], n_send.at[i], n_recv.at[i], {'dm': dev}) for i, dev in enumerate(peers)]
    loads = [
        pltpu.make_async_copy(x_ref.at[pl.ds(pl.multiple_of(me * seq, seq), seq)], xm_buf.at[:, mine], load_sem.at[0]),
        pltpu.make_async_copy(wo_ref, wo_buf.at[:, mine], load_sem.at[1]),
        pltpu.make_async_copy(n_ref, n_buf.at[me], load_sem.at[2]),
    ]
    thirds = ((wq_ref, wq_buf), (wk_ref, wk_buf), (wv_ref, wv_buf))
    third_loads = [pltpu.make_async_copy(src, buf, load_sem.at[3 + i]) for i, (src, buf) in enumerate(thirds)]

    def flatten_own():
        for load in third_loads:
            load.wait()
        flat_rows = min(cols, 64)

        def body(i, carry):
            part = pl.ds(pl.multiple_of(i * flat_rows, flat_rows), flat_rows)
            there = pl.ds(pl.multiple_of(me * cols + i * flat_rows, flat_rows), flat_rows)
            start = 0
            for _, buf in thirds:
                wide = buf.shape[1] * buf.shape[2]
                w_buf[there, start:start + wide] = buf[part].reshape(flat_rows, wide)
                start += wide
            return carry

        lax.fori_loop(0, cols // flat_rows, body, 0)

    def spread(part, share):
        count = pieces[part]
        return [p for p in range(count) if (4 * p) // count == share]

    for load in third_loads:
        load.start()
    with jax.named_scope('meet'):
        meet([{'dm': mate}, {'dm': across}, {'dm': cross}, {'dp': 1 - row}] + line_peers(line))
    for s in range(2):
        x_copy(1, s).start()
        x_copy(2, s).start()
    for copy in n_copies:
        copy.start()
    with jax.named_scope('flatten'):
        flatten_own()
    gather.start()
    x_copy(0, 0).start()
    for load in loads:
        load.start()
    gather.own_start(QKV)
    gather.own_start(OUT)
    with jax.named_scope('z0'):
        z_first(0)
        z_first(1)
        z_step(1, 0)
    with jax.named_scope('z1'):
        for p in spread(QKV, 0)[:1]:
            pass_y(QKV, p)
        z_step(1, 1)
        for p in spread(QKV, 0)[1:]:
            pass_y(QKV, p)
        for p in spread(QKV, 0)[:1]:
            pass_x(QKV, p)
        z_step(2, 0)
    with jax.named_scope('z2'):
        for p in spread(QKV, 1):
            pass_y(QKV, p)
        for p in spread(QKV, 0)[1:]:
            pass_x(QKV, p)
        z_step(2, 1)
        for p in spread(QKV, 2):
            pass_y(QKV, p)
        for p in spread(QKV, 1):
            pass_x(QKV, p)
        z_step(3, 0)
    with jax.named_scope('z3'):
        for p in spread(QKV, 3):
            pass_y(QKV, p)
        for p in spread(QKV, 2):
            pass_x(QKV, p)
        for copy in n_arrivals:
            copy.wait_recv()
        for load in loads:
            load.wait()
        for shard in range(4):
            gain_buf[:, shard * cols:(shard + 1) * cols] = 1.0 + n_buf[shard]
        x_arrival(0, 0).wait_recv()
        z_step(3, 1)

    for block in range(LINE):
        for s in range(2):

            @pl.when((block <= line) & (line < LINE - 1))
            def _():
                z_copy(True, block, s).wait_send()

            @pl.when((block >= line) & (line > 0))
            def _():
                z_copy(False, block, s).wait_send()

    first_row = pl.multiple_of(half * (1 - jnp.minimum(line, 1)), half)
    res_buf[...] = xm_buf[pl.ds(first_row, half), :]
    norm_rows = min(seq, 64)

    def norm_body(i, carry):
        part = pl.ds(pl.multiple_of(i * norm_rows, norm_rows), norm_rows)
        xm_buf[part, :] = unit_rows(xm_buf[part, :].astype(F32), gain_buf[0:1, :]).astype(BF16)
        return carry

    pass_y(OUT, 0)
    with jax.named_scope('norm'):
        lax.fori_loop(0, seq // norm_rows, norm_body, 0)
    with jax.named_scope('settle_qkv'):
        pass_y(OUT, 1)
        for p in spread(QKV, 3):
            pass_x(QKV, p)
        for p in range(pieces[QKV]):
            gather.landed(QKV, p)
            gather.sent(QKV, p)
        gather.own_landed(QKV)
        gather.own_sent(QKV)

    big = min(seq, 512)
    width = qkv_buf.shape[1]
    q_tile = min(width, 512)
    q_steps = (width // q_tile) * (seq // big)

    def qkv_body(i, carry):
        column = pl.ds(pl.multiple_of(lax.rem(i, width // q_tile) * q_tile, q_tile), q_tile)
        part = pl.ds(pl.multiple_of(lax.div(i, width // q_tile) * big, big), big)
        qkv_buf[part, column] = jnp.dot(xm_buf[part, :], w_buf[:, column], preferred_element_type=F32).astype(BF16)
        return carry

    with jax.named_scope('qkv'):
        lax.fori_loop(0, q_steps // 4, qkv_body, 0)
        pass_y(OUT, 2)
        pass_x(OUT, 0)
        lax.fori_loop(q_steps // 4, q_steps // 2, qkv_body, 0)
        pass_y(OUT, 3)
        pass_x(OUT, 1)
        lax.fori_loop(q_steps // 2, q_steps, qkv_body, 0)
        pass_x(OUT, 2)
        pass_y(GATE, 0)
    with jax.named_scope('pass_out'):
        pass_x(OUT, 3)

    def rotate_body(i, carry):
        column = pl.ds(pl.multiple_of(i * head_dim, head_dim), head_dim)
        qkv_buf[:, column] = rotate(qkv_buf[:, column], cos_ref[...], sin_ref[...])
        return carry

    with jax.named_scope('rotate'):
        lax.fori_loop(0, heads + kv_heads, rotate_body, 0)

    def keep_caches():
        def cache_body(i, carry):
            part = pl.ds(pl.multiple_of(i * norm_rows, norm_rows), norm_rows)
            wide = kv_heads * head_dim
            for n, buf in enumerate((k_buf, v_buf)):
                start = heads * head_dim + n * wide
                buf[part] = qkv_buf[part, start:start + wide].reshape(norm_rows, kv_heads, head_dim)
            return carry

        lax.fori_loop(0, seq // norm_rows, cache_body, 0)

    block = seq // 8
    d_tile = min(dim, 512)

    def attend_block(i):
        part = slice(i * block, (i + 1) * block)
        span = (i + 1) * block
        q_index = i * block + lax.broadcasted_iota(jnp.int32, (block, span), 0)
        key_index = lax.broadcasted_iota(jnp.int32, (block, span), 1)
        allowed = (key_index <= q_index) & (pos_col_ref[part, :] - pos_row_ref[:, :span] < WINDOW_LEN)

        def head_body(h, carry):
            q_cols = pl.ds(pl.multiple_of(h * head_dim, head_dim), head_dim)
            k_cols = pl.ds(pl.multiple_of((heads + lax.div(h, group)) * head_dim, head_dim), head_dim)
            v_cols = pl.ds(pl.multiple_of((heads + kv_heads + lax.div(h, group)) * head_dim, head_dim), head_dim)
            scores = lax.dot_general(qkv_buf[part, q_cols], qkv_buf[:span, k_cols], (((1,), (1,)), ((), ())), preferred_element_type=F32)
            capped = SOFT_CAP * jnp.tanh(scores * scale / SOFT_CAP)
            weights = jnp.where(allowed, jnp.exp(capped), 0.0)
            probs = (weights / jnp.sum(weights, axis=-1, keepdims=True)).astype(BF16)
            qkv_buf[part, q_cols] = jnp.dot(probs, qkv_buf[:span, v_cols], preferred_element_type=F32).astype(BF16)
            return carry

        lax.fori_loop(0, heads, head_body, 0)

    def out_pair(i):
        parts = [slice(n * block, (n + 1) * block) for n in (i, 4 + i)]

        def out_body(n, carry):
            column = pl.ds(pl.multiple_of(n * d_tile, d_tile), d_tile)
            rows = jnp.concatenate([qkv_buf[part, :heads * head_dim] for part in parts], axis=0)
            sums = jnp.dot(rows, wo_buf[:, column], preferred_element_type=F32).astype(BF16)
            for d, part in enumerate(parts):
                p_buf[part, column] = sums[d * block:(d + 1) * block]
            return carry

        lax.fori_loop(0, dim // d_tile, out_body, 0)

    def second(i):
        attend_block(4 + i)
        out_pair(i)

    with jax.named_scope('attend0'):
        attend_block(0)
        attend_block(4)
    with jax.named_scope('settle_out'):
        for p in range(pieces[OUT]):
            gather.landed(OUT, p)
            gather.sent(OUT, p)
        gather.own_landed(OUT)
        gather.own_sent(OUT)
        for part in (GATE, UP):
            for p in range(tiles):
                gather.own_start(part, p)
        gather.own_start(DOWN)
    with jax.named_scope('out0'):
        out_pair(0)

    def finish(out_rows, rows, total):
        hidden = (res_buf[rows, :].astype(F32) + unit_rows(total.astype(F32), gain_buf[1:2, :])).astype(BF16)
        res_buf[rows, :] = hidden
        xm_buf[out_rows, :] = unit_rows(hidden.astype(F32), gain_buf[2:3, :]).astype(BF16)

    sums = LineSum(p_buf, got, xm_buf, *line_sems[:4], finish, lambda out_rows: None)
    last = sums.steps - 1
    ahead = sums.chunks // 4

    span_rows = half // 4
    z_buf = wo_buf
    pair = 2 * tile

    def group_rows(g):
        return [pl.ds(times(d * half + g * span_rows, span_rows), span_rows) for d in range(2)]

    def gate_loads(f, base):
        copies = []
        for n, (src, dst) in enumerate(((wg_ref, wgf_ref), (wu_ref, wuf_ref))):
            column = pl.ds(times(base + n * tile, tile), tile)
            for r, shard in enumerate((me, mate, across, cross)):
                part = src.at[:, pl.ds(times(f * tile, tile), tile)] if r == 0 else dst.at[f, shard_span(shard)]
                copies.append(pltpu.make_async_copy(part, w_buf.at[shard_span(shard), column], gate_sem.at[base // pair if isinstance(base, int) else lax.div(base, pair), n, r]))
        return copies

    def gate_fetch(f, base, which=(0, 1)):
        for n in which:
            for load in gate_loads(f, base)[4 * n:4 * n + 4]:
                load.start()

    def gate_settle(f):
        for part in (GATE, UP):
            gather.landed(part, f)
            gather.own_landed(part, f)

    def gate_work(g, f, base, refill):
        parts = group_rows(g)
        ffw_in = jnp.concatenate([xm_buf[part, :] for part in parts], axis=0)
        for load in gate_loads(f, base)[:4]:
            load.wait()
        gate_tile[...] = jnp.dot(ffw_in, w_buf[:, pl.ds(times(base, tile), tile)], preferred_element_type=F32).astype(BF16)
        refill(0)
        for load in gate_loads(f, base)[4:]:
            load.wait()
        up = jnp.dot(ffw_in, w_buf[:, pl.ds(times(base + tile, tile), tile)], preferred_element_type=F32).astype(BF16).astype(F32)
        gated = (jax.nn.gelu(gate_tile[...].astype(F32), approximate=True) * up).astype(BF16)
        refill(1)
        for d, part in enumerate(parts):
            z_buf[part, pl.ds(times(f * tile, tile), tile)] = gated[d * span_rows:(d + 1) * span_rows]

    def gate_place(i):
        early = tiles - 1
        if isinstance(i, int):
            if i < 2 * early:
                return i // early, i % early
            return (i - 2 * early, early) if i < 2 * tiles else (2, i - 2 * tiles)
        g = jnp.where(i < 2 * early, lax.div(i, early), jnp.where(i < 2 * tiles, i - 2 * early, 2))
        return g, jnp.where(i < 2 * early, lax.rem(i, early), jnp.where(i < 2 * tiles, early, i - 2 * tiles))

    def gate_item(i, carry):
        base = lax.rem(i, 2) * pair
        ahead_g, ahead_f = gate_place(i + 2)

        @pl.when(ahead_g == 0)
        def _():
            gate_settle(ahead_f)

        def refill(n):
            @pl.when(i + 2 < 3 * tiles)
            def _():
                gate_fetch(ahead_f, base, (n,))

        gate_work(*gate_place(i), base, refill)
        return carry

    ffw = gather.order[pieces[QKV] + pieces[OUT]:]
    if len(ffw) == len(PASS_Y):
        y_turns, x_turns, gate_turns = PASS_Y, PASS_X, GATE_TURNS
    else:
        y_turns = [(min(3 + 2 * k, last), 0) for k in range(len(ffw))]
        x_turns = [(min(4 + 2 * k, last), 0) for k in range(len(ffw))]
        gate_turns = [0] * (3 * tiles)
    before, after, tail = {}, {}, []

    def at(turn, action):
        (after if turn[1] else before).setdefault(turn[0], []).append(action)

    late_pieces = max(1, min(2, pieces[DOWN] - 1))
    edge = pieces[DOWN] - late_pieces

    moves = [(turn, 0, k) for k, turn in enumerate(y_turns) if k > 0] + [(turn, 1, k) for k, turn in enumerate(x_turns)]
    for turn, way, k in sorted(moves, key=lambda move: ((99, 0) if move[0] is None else move[0], move[2] + move[1], move[1])):
        move = functools.partial((pass_y, pass_x)[way], *ffw[k])
        if turn is None:
            tail.append((ffw[k], move))
        else:
            at(turn, move)
    at((min(1, last), 1), keep_caches)
    for i in range(1, 4):
        early = (2 * ahead) // 8 if i == 3 else 0
        at((min(i * ahead - (5 * ahead) // 8 - early, last), 0), functools.partial(attend_block, i))
        at((min(i * ahead - (3 * ahead) // 8 - early, last), 0), functools.partial(second, i))
    gate_ready = [max(x_turns[k][0] + x_turns[k][1] for k in (2 * f, 2 * f + 1)) for f in range(tiles)]
    gate_table = []
    for i in range(3 * tiles):
        coming = [gate_place(min(i + n, 3 * tiles - 1)) for n in (0, 1, 2)]
        turn = max([gate_turns[i], (coming[0][0] + 1) * ahead + 6 * LAG] + [gate_ready[f] for g, f in coming if g == 0])
        gate_table.append(max(turn, gate_table[-1] if gate_table else 0))

    def open_gate():
        for i in range(2):
            if gate_place(i)[0] == 0:
                gate_settle(gate_place(i)[1])
            gate_fetch(gate_place(i)[1], i * pair)

    at((min(gate_table[0], last), 0), open_gate)

    def each_first(t):
        lax.fori_loop(*turns_of([turn for turn in gate_table if turn <= last], t), gate_item, 0)

    with jax.named_scope('chain1'):
        sums.run(before, each_first, after)
    with jax.named_scope('gate_rest'):
        lax.fori_loop(len([turn for turn in gate_table if turn <= last]), 3 * tiles, gate_item, 0)
    shards = (me, mate, across, cross)

    def down_load(r, base):
        column = pl.ds(base, cols)
        sem = down_sem.at[0 if base else 1]
        return pltpu.make_async_copy(wd_ref if r == 0 else wdf_ref.at[shards[r]], w_buf.at[:, column], sem)

    def down_fetch(r, base):
        if isinstance(r, int):
            down_load(r, base).start()
            return
        for n in range(4):

            @pl.when(r == n)
            def _():
                down_load(n, base).start()

    def down_work(g, r, base):
        down_load(0, base).wait()
        parts = group_rows(g)
        gated = jnp.concatenate([z_buf[part, :] for part in parts], axis=0)
        down = jnp.dot(gated, w_buf[:, pl.ds(base, cols)], preferred_element_type=F32).astype(BF16)
        if isinstance(r, int):
            shard = shards[r]
        else:
            shard = jnp.where(r == 0, me, jnp.where(r == 1, mate, jnp.where(r == 2, across, cross)))
        for d, part in enumerate(parts):
            p_buf[part, shard_span(shard)] = down[d * span_rows:(d + 1) * span_rows]

    rows_each = wd_ref.shape[0] // (2 * pieces[DOWN])
    half_hidden = wd_ref.shape[0] // 2
    spans = (((0, edge * rows_each), (half_hidden, edge * rows_each)), ((edge * rows_each, late_pieces * rows_each), (half_hidden + edge * rows_each, late_pieces * rows_each)))

    def far_loads(r, base, late):
        column = pl.ds(base, cols)
        return [pltpu.make_async_copy(wdf_ref.at[shards[r], pl.ds(start, size)], w_buf.at[pl.ds(start, size), column], far_sem.at[r - 2, n]) for n, (start, size) in enumerate(spans[late])]

    def far_product(base, late):
        gated = [jnp.concatenate([z_buf[part, start:start + size] for part in group_rows(0)], axis=0) for start, size in spans[late]]
        return sum(jnp.dot(rows, w_buf[start:start + size, pl.ds(base, cols)], preferred_element_type=F32) for rows, (start, size) in zip(gated, spans[late]))

    def far_early(r, base):
        for load in far_loads(r, base, 0):
            load.wait()
        far_buf[r - 2] = far_product(base, 0)

    def far_late(r, base):
        for load in far_loads(r, base, 1):
            load.wait()
        down = (far_buf[r - 2] + far_product(base, 1)).astype(BF16)
        for d, part in enumerate(group_rows(0)):
            p_buf[part, shard_span(shards[r])] = down[d * span_rows:(d + 1) * span_rows]

    def far_start(r, base, late):
        for load in far_loads(r, base, late):
            load.start()

    early_moves = [move for (part, p), move in tail if part != DOWN or p < edge]
    late_moves = [move for (part, p), move in tail if part == DOWN and p >= edge]
    down_fetch(0, pair)
    with jax.named_scope('tail'):
        for move in early_moves:
            move()
        gather.own_landed(DOWN)
        down_fetch(1, 0)
        sums.settle()
    with jax.named_scope('down_near0'):
        down_work(0, 0, pair)
    with jax.named_scope('landed_early'):
        for p in range(edge):
            gather.landed(DOWN, p)
        far_start(2, pair, 0)
    with jax.named_scope('down_near1'):
        down_work(0, 1, 0)
        far_start(3, 0, 0)
    with jax.named_scope('pass_late0'):
        for move in late_moves[:len(late_moves) - 2]:
            move()
    with jax.named_scope('far_early0'):
        far_early(2, pair)
    with jax.named_scope('pass_late1'):
        for move in late_moves[len(late_moves) - 2:]:
            move()
    with jax.named_scope('far_early1'):
        far_early(3, 0)

    caches = ((k_buf, kf_ref), (v_buf, vf_ref))

    def rows_of(ref, shard):
        return ref.at[pl.ds(pl.multiple_of(shard * seq, seq), seq)]

    def kv_copy(i, hop):
        src, dst = caches[i]
        if hop == 0:
            return remote(src, rows_of(dst, me), kv_send.at[i, hop], kv_recv.at[i, hop], {'dm': across})
        if hop == 1:
            return remote(src, rows_of(dst, me), kv_send.at[i, hop], kv_recv.at[i, hop], {'dm': mate})
        return remote(rows_of(dst, across), rows_of(dst, across), kv_send.at[i, hop], kv_recv.at[i, hop], {'dm': mate})

    def kv_arrival(i, hop):
        region = rows_of(caches[i][1], (across, mate, cross)[hop])
        return remote(region, region, kv_send.at[i, hop], kv_recv.at[i, hop], {'dm': mate})

    with jax.named_scope('settle_down'):
        for p in range(edge, pieces[DOWN]):
            gather.landed(DOWN, p)
    far_start(2, pair, 1)
    far_start(3, 0, 1)
    kv_stores = [pltpu.make_async_copy(src, rows_of(dst, me), kv_store.at[i]) for i, (src, dst) in enumerate(caches)]
    for i in range(2):
        kv_copy(i, 0).start()
        kv_copy(i, 1).start()
        kv_stores[i].start()
    with jax.named_scope('far_late'):
        far_late(2, pair)
        down_fetch(0, pair)
        far_late(3, 0)
        gate_fetch(0, 0)

    def finish_last(out_rows, rows, total):
        xm_buf[out_rows, :] = (res_buf[rows, :].astype(F32) + unit_rows(total.astype(F32), gain_buf[3:4, :])).astype(BF16)

    def emit_last(out_rows):
        there = pl.ds(pl.multiple_of(me * seq + out_rows.start, CHUNK), CHUNK)
        for i, dev in enumerate((across, cross, mate)):
            remote(xm_buf.at[out_rows, shard_span(dev)], y_ref.at[there], fin_send.at[i], fin_recv.at[i], {'dm': dev}).start()
        pltpu.make_async_copy(xm_buf.at[out_rows, mine], y_ref.at[there], fin_own).start()

    last_sums = LineSum(p_buf, got, xm_buf, *line_sems[4:], finish_last, emit_last)

    def pass_kv(i):
        kv_arrival(i, 0).wait_recv()
        kv_copy(i, 2).start()

    late_gates = [int((f + 1) * 2 * ahead / (tiles + 1)) for f in range(tiles)]
    late_downs = [(n * ahead) // 4 + ahead // 8 for n in range(12)]

    def late_gate(f, carry):
        def refill(n):
            @pl.when(f + 1 < tiles)
            def _():
                gate_fetch(f + 1, 0, (n,))

        gate_work(3, f, 0, refill)
        return carry

    def late_down(n, carry):
        down_work(1 + lax.div(n, 4), lax.rem(n, 4), pair)

        @pl.when(n + 1 < 12)
        def _():
            down_fetch(lax.rem(n + 1, 4), pair)

        return carry

    def each_last(t):
        lax.fori_loop(*turns_of(late_gates, t), late_gate, 0)
        lax.fori_loop(*turns_of(late_downs, t), late_down, 0)

    with jax.named_scope('chain2'):
        last_sums.run({min(14, last - 1): [functools.partial(pass_kv, 0)], min(17, last): [functools.partial(pass_kv, 1)]}, each_last, {})
    with jax.named_scope('close'):
        last_sums.settle()
        for i in range(2):
            kv_stores[i].wait()
            for hop in range(3):
                kv_copy(i, hop).wait_send()
            kv_arrival(i, 1).wait_recv()
            kv_arrival(i, 2).wait_recv()
        for i, dev in enumerate((across, cross, mate)):
            done = remote(xm_buf.at[:, shard_span(dev)], rows_of(y_ref, dev), fin_send.at[i], fin_recv.at[i], {'dm': dev})
            done.wait_send()
            done.wait_recv()
        pltpu.make_async_copy(xm_buf.at[:, mine], rows_of(y_ref, me), fin_own).wait()
        for part in (GATE, UP):
            for p in range(tiles):
                gather.sent(part, p)
                gather.own_sent(part, p)
        for p in range(pieces[DOWN]):
            gather.sent(DOWN, p)
        gather.own_sent(DOWN)
        for copy in n_copies:
            copy.wait_send()
        x_copy(0, 0).wait_send()
        for s in range(2):
            x_copy(1, s).wait_send()
            x_copy(2, s).wait_send()


def like(*shape, dtype=BF16):
    return jax.ShapeDtypeStruct(shape, dtype)


def params(collective_id):
    return pltpu.CompilerParams(collective_id=collective_id, has_side_effects=True, vmem_limit_bytes=VMEM_BYTES)


def run_layer(x, norms, wq, wk, wv, wo, wg, wu, wd, cos_tab, sin_tab, pos, scale):
    seq = pos.shape[0]
    cols = x.shape[1]
    dim = 4 * cols
    kv_heads, head_dim = wk.shape[1:]
    width = wo.shape[0] + 2 * kv_heads * head_dim
    chunks = seq // 2 // CHUNK
    cache = (seq, kv_heads, head_dim)
    hidden = wg.shape[1]
    tile = min(hidden // 2, 512)
    tiles = hidden // tile

    def count(rows, most):
        return most if rows % (32 * most) == 0 else 2

    pieces = (count(cols, 7), 4, tiles, tiles, count(wd.shape[0], 14))
    units = sum(pieces)
    return pl.pallas_call(
        functools.partial(layer_kernel, scale, kv_heads, head_dim, pieces),
        name='layer',
        out_shape=(like(4 * seq, cols), like(4 * seq, kv_heads, head_dim), like(4 * seq, kv_heads, head_dim), like(tiles, dim, tile), like(tiles, dim, tile), like(4, *wd.shape)),
        in_specs=[ANY] * 9 + [VMEM] * 4,
        out_specs=(ANY,) * 6,
        scratch_shapes=[
            pltpu.VMEM((seq, dim), BF16), pltpu.VMEM((dim, width), BF16), pltpu.VMEM((wo.shape[0], dim), BF16), pltpu.VMEM((seq, width), BF16),
            pltpu.VMEM((seq, dim), BF16), pltpu.VMEM((2, seq // 2, dim), BF16), pltpu.VMEM((seq // 2, dim), BF16), pltpu.VMEM((4,) + norms.shape, F32), pltpu.VMEM((4, dim), F32),
            pltpu.VMEM(wq.shape, BF16), pltpu.VMEM(wk.shape, BF16), pltpu.VMEM(wv.shape, BF16), pltpu.VMEM(cache, BF16), pltpu.VMEM(cache, BF16), pltpu.VMEM((2, seq // 4, cols), F32), pltpu.VMEM((seq // 4, tile), BF16),
            DMA((3, 2)), DMA((3, 2)), DMA((3,)), DMA((3,)), DMA((2, 2 * LINE)), DMA((2 * LINE,)), DMA((3 + 2 * tiles,)), DMA((3 + 2 * tiles,)), DMA((units, 4)), DMA((units, 4)), DMA((6,)),
            DMA((2, 2, 4)), DMA((2,)), DMA((2, 2)), DMA((2,)), DMA((2, 3)), DMA((2, 3)), DMA((3,)), DMA((3,)), DMA,
        ] + [DMA((2, chunks))] * 8,
        compiler_params=params(0),
    )(x, norms, wq, wk, wv, wo, wg, wu, wd, cos_tab, sin_tab, pos[:, None], pos[None, :])


def solution(mesh):
    tp_size = mesh.shape['tp']

    def layer(tokens, positions, norm_pre_attn, w_query, w_key, w_value, w_out, norm_post_attn, norm_pre_ffw, w_gate, w_up, w_down, norm_post_ffw):
        seq = positions.shape[1]
        heads, head_dim, cols = w_out.shape
        dim = 4 * cols
        scale = (dim / (heads * tp_size)) ** -0.5
        norms = jnp.stack([norm_pre_attn, norm_post_attn, norm_pre_ffw, norm_post_ffw]).astype(F32)
        pos = lax.dynamic_index_in_dim(positions, lax.axis_index('dm'), 0, keepdims=False)
        half_dim = head_dim // 2
        inv_freq = ROPE_BASE ** (-2.0 * jnp.arange(half_dim, dtype=F32) / head_dim)
        angles = pos.astype(F32)[:, None] * inv_freq[None, :]
        outs = run_layer(tokens, norms, w_query, w_key, w_value, w_out.reshape(heads * head_dim, cols), w_gate, w_up, w_down, jnp.cos(angles), jnp.sin(angles), pos, scale)
        return outs[:3]

    width_spec = P('dm')
    in_specs = (P('dp', 'dm'), P('dp', None), width_spec, P('dm', 'tp', None), P('dm', 'tp', None), P('dm', 'tp', None), P('tp', None, 'dm'), width_spec, width_spec, P('dm', 'tp'), P('dm', 'tp'), P('tp', 'dm'), width_spec)
    out_specs = (P('dp', 'dm'), P('dp', 'tp', None), P('dp', 'tp', None))
    return jax.shard_map(layer, mesh=mesh, in_specs=in_specs, out_specs=out_specs, check_vma=False)
```

```python
import functools

import jax
import jax.numpy as jnp
from jax import lax
from jax.experimental import pallas as pl
from jax.experimental.pallas import tpu as pltpu
from jax.sharding import PartitionSpec as P

NORM_EPS = 1e-6
SOFT_CAP = 50.0
ROPE_BASE = 10000.0
WINDOW_LEN = 4096
BF16 = jnp.bfloat16
F32 = jnp.float32

CHUNK = 16
LAG = 2
LINE = 4
VMEM_BYTES = 67043328

PASS_Y = [(0, 0), (0, 1), (5, 0), (8, 0), (11, 0), (13, 0), (14, 0), (16, 0), (18, 0), (19, 1), (20, 1), (23, 0), (25, 0), (27, 0), (28, 0), (29, 0), (29, 1), (30, 1), (31, 1), (32, 1), (33, 1), (33, 1), (35, 1), (36, 1), (37, 1), (38, 1), (39, 1), (42, 0)]
PASS_X = [(2, 1), (5, 1), (9, 0), (12, 0), (13, 1), (16, 0), (17, 0), (19, 0), (20, 1), (23, 0), (24, 0), (26, 0), (28, 0), (29, 1), (30, 1), (31, 1), (32, 1), (33, 1), (33, 1), (35, 1), (36, 1), (37, 1), (38, 1), (39, 1), (42, 0), None, None, None]
GATE_TURNS = [20, 20, 25, 29, 29, 30, 30, 31, 31, 32, 32, 33, 33, 34, 36, 36, 37, 37, 38, 38, 39]

ANY = pl.BlockSpec(memory_space=pl.ANY)
VMEM = pl.BlockSpec(memory_space=pltpu.VMEM)
DMA = pltpu.SemaphoreType.DMA


def places():
    row = lax.axis_index('dp')
    line = lax.axis_index('tp')
    me = lax.axis_index('dm')
    side = lax.div(me, 2)
    core = me - 2 * side
    return row, line, me, 2 * side + 1 - core, 2 * (1 - side) + core, 2 * (1 - side) + 1 - core


def times(value, unit):
    return value if isinstance(value, int) else pl.multiple_of(value, unit)


def remote(src, dst, send_sem, recv_sem, device):
    return pltpu.make_async_remote_copy(src_ref=src, dst_ref=dst, send_sem=send_sem, recv_sem=recv_sem, device_id=device, device_id_type=pl.DeviceIdType.MESH)


def meet(peers):
    barrier = pltpu.get_barrier_semaphore()
    for peer in peers:
        pl.semaphore_signal(barrier, inc=1, device_id=peer, device_id_type=pl.DeviceIdType.MESH)
    pl.semaphore_wait(barrier, len(peers))


def line_peers(line):
    return [{'tp': lax.rem(line + 1, LINE)}, {'tp': lax.rem(line + LINE - 1, LINE)}]


QKV, OUT, GATE, UP, DOWN = range(5)


class WeightGather:
    def __init__(self, refs, pieces, tile, own_send, own_recv, send, recv):
        self.refs, self.pieces, self.tile = refs, pieces, tile
        self.own_send, self.own_recv, self.send, self.recv = own_send, own_recv, send, recv
        self.row, _, self.me, self.mate, self.across, self.cross = places()
        self.order = [(QKV, p) for p in range(pieces[QKV])] + [(OUT, p) for p in range(pieces[OUT])]
        self.order += [(part, p) for p in range(pieces[GATE]) for part in (GATE, UP)]
        self.order += [(DOWN, p) for p in range(pieces[DOWN])]

    def index(self, part, p):
        first = {QKV: 0, OUT: self.pieces[QKV]}
        ffw = self.pieces[QKV] + self.pieces[OUT]
        if part in first:
            return first[part] + p
        if part == DOWN:
            return ffw + 2 * self.pieces[GATE] + p
        return ffw + 2 * p + (part - GATE)

    def direct(self, part, p):
        return part == DOWN and p == self.pieces[DOWN] - 1

    def cut(self, part, half, p):
        size = self.refs[part][0].shape[0] // (2 * self.pieces[part])
        return pl.ds(pl.multiple_of((half * self.pieces[part] + p) * size, size), size)

    def own(self, part, half, p):
        src = self.refs[part][0]
        if part in (GATE, UP):
            size = self.tile // 2
            return src.at[:, pl.ds(pl.multiple_of(p * self.tile + half * size, size), size)]
        return src.at[self.cut(part, half, p)]

    def at(self, part, shard, half, p):
        src, dst = self.refs[part]
        if part == QKV:
            size = src.shape[0] // (2 * self.pieces[part])
            return dst.at[pl.ds(pl.multiple_of(shard * src.shape[0] + (half * self.pieces[part] + p) * size, size), size)]
        if part == OUT:
            return dst.at[self.cut(part, half, p), pl.ds(pl.multiple_of(shard * src.shape[1], src.shape[1]), src.shape[1])]
        if part == DOWN:
            return dst.at[shard, self.cut(part, half, p)]
        size = self.tile // 2
        return dst.at[p, pl.ds(pl.multiple_of(shard * src.shape[0], src.shape[0]), src.shape[0]), pl.ds(pl.multiple_of(half * size, size), size)]

    def copy(self, part, p, hop):
        mine, other = self.row, 1 - self.row
        k = self.index(part, p)
        device = {'dm': self.mate}
        if hop == 0 or (hop == 1 and self.direct(part, p)):
            half = mine if hop == 0 else other
            src, dst, device = self.own(part, half, p), self.at(part, self.me, half, p), {'dm': self.across}
        else:
            src = dst = self.at(part, self.across, other if hop == 3 else mine, p)
            if hop == 1:
                device = {'dp': other}
        return remote(src, dst, self.send.at[k, hop], self.recv.at[k, hop], device)

    def arrival(self, part, p, hop):
        k = self.index(part, p)
        region = self.at(part, self.across if hop < 2 else self.cross, 1 - self.row if hop % 2 else self.row, p)
        return remote(region, region, self.send.at[k, hop], self.recv.at[k, hop], {'dm': self.mate})

    def own_copy(self, part, p, shard):
        src, dst = self.refs[part]
        if part in (GATE, UP):
            src = src.at[:, pl.ds(times(p * self.tile, self.tile), self.tile)]
            dst = dst.at[p, pl.ds(pl.multiple_of(shard * src.shape[0], src.shape[0]), src.shape[0])]
            k = 3 + 2 * p + part - GATE
        else:
            k = (QKV, OUT, DOWN).index(part)
            if part == DOWN:
                dst = dst.at[shard]
            elif part == OUT:
                dst = dst.at[:, pl.ds(pl.multiple_of(shard * src.shape[1], src.shape[1]), src.shape[1])]
            else:
                dst = dst.at[pl.ds(pl.multiple_of(shard * src.shape[0], src.shape[0]), src.shape[0])]
        return remote(src, dst, self.own_send.at[k], self.own_recv.at[k], {'dm': self.mate})

    def start(self):
        for part, p in self.order:
            self.copy(part, p, 0).start()
            if self.direct(part, p):
                self.copy(part, p, 1).start()

    def pass_y(self, part, p):
        self.arrival(part, p, 0).wait_recv()
        if not self.direct(part, p):
            self.copy(part, p, 1).start()
        self.copy(part, p, 2).start()

    def pass_x(self, part, p):
        self.arrival(part, p, 1).wait_recv()
        self.copy(part, p, 3).start()

    def landed(self, part, p):
        self.arrival(part, p, 2).wait_recv()
        self.arrival(part, p, 3).wait_recv()

    def sent(self, part, p):
        for hop in range(4):
            self.copy(part, p, hop).wait_send()

    def own_start(self, part, p=0):
        self.own_copy(part, p, self.me).start()

    def own_landed(self, part, p=0):
        self.own_copy(part, p, self.mate).wait_recv()

    def own_sent(self, part, p=0):
        self.own_copy(part, p, self.me).wait_send()


class LineSum:
    def __init__(self, p_buf, got, out, sum_send, sum_recv, out_send, out_recv, finish, emit):
        self.p_buf, self.got, self.out = p_buf, got, out
        self.sum_send, self.sum_recv, self.out_send, self.out_recv = sum_send, sum_recv, out_send, out_recv
        self.finish, self.emit = finish, emit
        self.half = p_buf.shape[0] // 2
        self.chunks = self.half // CHUNK
        self.steps = self.chunks + 6 * LAG
        self.line = lax.axis_index('tp')

    def way(self, d):
        if d == 0:
            return self.line, {'tp': self.line + 1}, {'tp': self.line - 1}
        return LINE - 1 - self.line, {'tp': self.line - 1}, {'tp': self.line + 1}

    def rows(self, c):
        return pl.ds(pl.multiple_of(c * CHUNK, CHUNK), CHUNK)

    def out_rows(self, d, c):
        return pl.ds(pl.multiple_of(d * self.half + c * CHUNK, CHUNK), CHUNK)

    def sum_copy(self, d, c):
        return remote(self.p_buf.at[self.out_rows(d, c)], self.got.at[d, self.rows(c)], self.sum_send.at[d, c], self.sum_recv.at[d, c], self.way(d)[1])

    def out_copy(self, d, c):
        region = self.out.at[self.out_rows(d, c)]
        return remote(region, region, self.out_send.at[d, c], self.out_recv.at[d, c], self.way(d)[2])

    def step(self, t):
        for d in range(2):
            with jax.named_scope(f'sum{d}'):
                self.sum_step(d, t)
        for d in range(2):
            with jax.named_scope(f'out{d}'):
                self.out_step(d, t)

    def sum_step(self, d, t):
        pos = self.way(d)[0]
        c = t - LAG * pos

        @pl.when((c >= 0) & (c < self.chunks))
        def _():
            @pl.when(pos == 0)
            def _():
                self.sum_copy(d, c).start()

            @pl.when(pos > 0)
            def _():
                self.sum_copy(d, c).wait_recv()
                total = self.p_buf[self.out_rows(d, c), :].astype(F32) + self.got[d, self.rows(c), :].astype(F32)

                @pl.when(pos < LINE - 1)
                def _():
                    self.p_buf[self.out_rows(d, c), :] = total.astype(BF16)
                    self.sum_copy(d, c).start()

                @pl.when(pos == LINE - 1)
                def _():
                    self.finish(self.out_rows(d, c), self.rows(c), total.astype(BF16))
                    self.out_copy(d, c).start()
                    self.emit(self.out_rows(d, c))

    def out_step(self, d, t):
        pos = self.way(d)[0]
        c = t - 3 * LAG - LAG * (LINE - 1 - pos)

        @pl.when((c >= 0) & (c < self.chunks) & (pos < LINE - 1))
        def _():
            self.out_copy(d, c).wait_recv()

            @pl.when(pos > 0)
            def _():
                self.out_copy(d, c).start()

            self.emit(self.out_rows(d, c))

    def run(self, before, each, after):
        def body(t, carry):
            def act(actions):
                for turn in sorted(actions):

                    @pl.when(t == turn)
                    def _():
                        for action in actions[turn]:
                            action()

            with jax.named_scope('before'):
                act(before)
            with jax.named_scope('each'):
                each(t)
            with jax.named_scope('after'):
                act(after)
            self.step(t)
            return carry

        lax.fori_loop(0, self.steps, body, 0)

    def settle(self):
        def body(c, carry):
            for d in range(2):
                pos = self.way(d)[0]

                @pl.when(pos < LINE - 1)
                def _():
                    self.sum_copy(d, c).wait_send()

                @pl.when(pos > 0)
                def _():
                    self.out_copy(d, c).wait_send()

            return carry

        lax.fori_loop(0, self.chunks, body, 0)


def unit_rows(values, gain):
    mean_sq = jnp.mean(values * values, axis=-1, keepdims=True)
    return values * lax.rsqrt(mean_sq + NORM_EPS) * gain


def rotate(values, cos_tab, sin_tab):
    half_dim = values.shape[-1] // 2
    lower = values[:, :half_dim].astype(F32)
    upper = values[:, half_dim:].astype(F32)
    return jnp.concatenate([lower * cos_tab - upper * sin_tab, upper * cos_tab + lower * sin_tab], axis=-1).astype(BF16)


def turns_of(table, t):
    first = sum([jnp.where(t > turn, 1, 0) for turn in table], 0)
    return first, first + sum([jnp.where(t == turn, 1, 0) for turn in table], 0)


def layer_kernel(scale, kv_heads, head_dim, pieces, x_ref, n_ref, wq_ref, wk_ref, wv_ref, wo_ref, wg_ref, wu_ref, wd_ref, cos_ref, sin_ref, pos_col_ref, pos_row_ref, y_ref, kf_ref, vf_ref, wgf_ref, wuf_ref, wdf_ref, xm_buf, w_buf, wo_buf, qkv_buf, p_buf, got, res_buf, n_buf, gain_buf, wq_buf, wk_buf, wv_buf, k_buf, v_buf, far_buf, gate_tile, x_send, x_recv, n_send, n_recv, z_send, z_recv, own_send, own_recv, w_send, w_recv, load_sem, gate_sem, down_sem, far_sem, kv_store, kv_send, kv_recv, fin_send, fin_recv, fin_own, *line_sems):
    row, line, me, mate, across, cross = places()
    seq, dim = xm_buf.shape
    cols = dim // 4
    half = seq // 2
    quarter = seq // LINE
    sub = quarter // 2
    heads = wo_ref.shape[0] // head_dim
    group = heads // kv_heads
    tiles, _, tile = wgf_ref.shape
    peers = (mate, across, cross)

    def shard_span(shard):
        return pl.ds(pl.multiple_of(shard * cols, cols), cols)

    mine = shard_span(me)
    refs = ((w_buf.at[mine], w_buf), (wo_ref, wo_buf), (wg_ref, wgf_ref), (wu_ref, wuf_ref), (wd_ref, wdf_ref))
    gather = WeightGather(refs, pieces, tile, own_send, own_recv, w_send, w_recv)
    pass_y, pass_x = gather.pass_y, gather.pass_x

    def x_copy(hop, s):
        dev = peers[hop]
        if hop == 0:
            src, dst = x_ref.at[pl.ds(pl.multiple_of(dev * seq, seq), seq)], xm_buf.at[:, mine]
        else:
            start = line * quarter + s * sub
            src = x_ref.at[pl.ds(pl.multiple_of(dev * seq + start, sub), sub)]
            dst = xm_buf.at[pl.ds(pl.multiple_of(start, sub), sub), mine]
        return remote(src, dst, x_send.at[hop, s], x_recv.at[hop, s], {'dm': dev})

    def x_arrival(hop, s):
        theirs = shard_span(peers[hop])
        region = xm_buf.at[:, theirs] if hop == 0 else xm_buf.at[pl.ds(pl.multiple_of(line * quarter + s * sub, sub), sub), theirs]
        return remote(region, region, x_send.at[hop, s], x_recv.at[hop, s], {'dm': mate})

    far = pl.ds(pl.multiple_of((1 - lax.div(me, 2)) * 2 * cols, 2 * cols), 2 * cols)

    def z_copy(up, block, s):
        index = 2 * block + s
        region = xm_buf.at[pl.ds(pl.multiple_of(index * sub, sub), sub), far]
        device = {'tp': line + 1} if up else {'tp': line - 1}
        return remote(region, region, z_send.at[0 if up else 1, index], z_recv.at[index], device)

    def z_first(s):
        x_arrival(1, s).wait_recv()
        x_arrival(2, s).wait_recv()

        @pl.when(line < LINE - 1)
        def _():
            z_copy(True, line, s).start()

        @pl.when(line > 0)
        def _():
            z_copy(False, line, s).start()

    def z_step(step, s):
        below, above = line - step, line + step

        @pl.when(below >= 0)
        def _():
            z_copy(True, below, s).wait_recv()

            @pl.when(line < LINE - 1)
            def _():
                z_copy(True, below, s).start()

        @pl.when(above < LINE)
        def _():
            z_copy(False, above, s).wait_recv()

            @pl.when(line > 0)
            def _():
                z_copy(False, above, s).start()

    n_copies = [remote(n_ref, n_buf.at[me], n_send.at[i], n_recv.at[i], {'dm': dev}) for i, dev in enumerate(peers)]
    n_arrivals = [remote(n_ref, n_buf.at[dev], n_send.at[i], n_recv.at[i], {'dm': dev}) for i, dev in enumerate(peers)]
    loads = [
        pltpu.make_async_copy(x_ref.at[pl.ds(pl.multiple_of(me * seq, seq), seq)], xm_buf.at[:, mine], load_sem.at[0]),
        pltpu.make_async_copy(wo_ref, wo_buf.at[:, mine], load_sem.at[1]),
        pltpu.make_async_copy(n_ref, n_buf.at[me], load_sem.at[2]),
    ]
    thirds = ((wq_ref, wq_buf), (wk_ref, wk_buf), (wv_ref, wv_buf))
    third_loads = [pltpu.make_async_copy(src, buf, load_sem.at[3 + i]) for i, (src, buf) in enumerate(thirds)]

    def flatten_own():
        for load in third_loads:
            load.wait()
        flat_rows = min(cols, 64)

        def body(i, carry):
            part = pl.ds(pl.multiple_of(i * flat_rows, flat_rows), flat_rows)
            there = pl.ds(pl.multiple_of(me * cols + i * flat_rows, flat_rows), flat_rows)
            start = 0
            for _, buf in thirds:
                wide = buf.shape[1] * buf.shape[2]
                w_buf[there, start:start + wide] = buf[part].reshape(flat_rows, wide)
                start += wide
            return carry

        lax.fori_loop(0, cols // flat_rows, body, 0)

    def spread(part, share):
        count = pieces[part]
        return [p for p in range(count) if (4 * p) // count == share]

    for load in third_loads:
        load.start()
    with jax.named_scope('meet'):
        meet([{'dm': mate}, {'dm': across}, {'dm': cross}, {'dp': 1 - row}] + line_peers(line))
    for s in range(2):
        x_copy(1, s).start()
        x_copy(2, s).start()
    for copy in n_copies:
        copy.start()
    with jax.named_scope('flatten'):
        flatten_own()
    gather.start()
    x_copy(0, 0).start()
    for load in loads:
        load.start()
    gather.own_start(QKV)
    gather.own_start(OUT)
    with jax.named_scope('z0'):
        z_first(0)
        z_first(1)
        z_step(1, 0)
    with jax.named_scope('z1'):
        for p in spread(QKV, 0)[:1]:
            pass_y(QKV, p)
        z_step(1, 1)
        for p in spread(QKV, 0)[1:]:
            pass_y(QKV, p)
        for p in spread(QKV, 0)[:1]:
            pass_x(QKV, p)
        z_step(2, 0)
    with jax.named_scope('z2'):
        for p in spread(QKV, 1):
            pass_y(QKV, p)
        for p in spread(QKV, 0)[1:]:
            pass_x(QKV, p)
        z_step(2, 1)
        for p in spread(QKV, 2):
            pass_y(QKV, p)
        for p in spread(QKV, 1):
            pass_x(QKV, p)
        z_step(3, 0)
    with jax.named_scope('z3'):
        for p in spread(QKV, 3):
            pass_y(QKV, p)
        for p in spread(QKV, 2):
            pass_x(QKV, p)
        for copy in n_arrivals:
            copy.wait_recv()
        for load in loads:
            load.wait()
        for shard in range(4):
            gain_buf[:, shard * cols:(shard + 1) * cols] = 1.0 + n_buf[shard]
        x_arrival(0, 0).wait_recv()
        z_step(3, 1)

    for block in range(LINE):
        for s in range(2):

            @pl.when((block <= line) & (line < LINE - 1))
            def _():
                z_copy(True, block, s).wait_send()

            @pl.when((block >= line) & (line > 0))
            def _():
                z_copy(False, block, s).wait_send()

    first_row = pl.multiple_of(half * (1 - jnp.minimum(line, 1)), half)
    res_buf[...] = xm_buf[pl.ds(first_row, half), :]
    norm_rows = min(seq, 64)

    def norm_body(i, carry):
        part = pl.ds(pl.multiple_of(i * norm_rows, norm_rows), norm_rows)
        xm_buf[part, :] = unit_rows(xm_buf[part, :].astype(F32), gain_buf[0:1, :]).astype(BF16)
        return carry

    pass_y(OUT, 0)
    with jax.named_scope('norm'):
        lax.fori_loop(0, seq // norm_rows, norm_body, 0)
    with jax.named_scope('settle_qkv'):
        pass_y(OUT, 1)
        for p in spread(QKV, 3):
            pass_x(QKV, p)
        for p in range(pieces[QKV]):
            gather.landed(QKV, p)
            gather.sent(QKV, p)
        gather.own_landed(QKV)
        gather.own_sent(QKV)

    big = min(seq, 512)
    width = qkv_buf.shape[1]
    q_tile = min(width, 512)
    q_steps = (width // q_tile) * (seq // big)

    def qkv_body(i, carry):
        column = pl.ds(pl.multiple_of(lax.rem(i, width // q_tile) * q_tile, q_tile), q_tile)
        part = pl.ds(pl.multiple_of(lax.div(i, width // q_tile) * big, big), big)
        qkv_buf[part, column] = jnp.dot(xm_buf[part, :], w_buf[:, column], preferred_element_type=F32).astype(BF16)
        return carry

    with jax.named_scope('qkv'):
        lax.fori_loop(0, q_steps // 4, qkv_body, 0)
        pass_y(OUT, 2)
        pass_x(OUT, 0)
        lax.fori_loop(q_steps // 4, q_steps // 2, qkv_body, 0)
        pass_y(OUT, 3)
        pass_x(OUT, 1)
        lax.fori_loop(q_steps // 2, q_steps, qkv_body, 0)
        pass_x(OUT, 2)
        pass_y(GATE, 0)
    with jax.named_scope('pass_out'):
        pass_x(OUT, 3)

    def rotate_body(i, carry):
        column = pl.ds(pl.multiple_of(i * head_dim, head_dim), head_dim)
        qkv_buf[:, column] = rotate(qkv_buf[:, column], cos_ref[...], sin_ref[...])
        return carry

    with jax.named_scope('rotate'):
        lax.fori_loop(0, heads + kv_heads, rotate_body, 0)

    def keep_caches():
        def cache_body(i, carry):
            part = pl.ds(pl.multiple_of(i * norm_rows, norm_rows), norm_rows)
            wide = kv_heads * head_dim
            for n, buf in enumerate((k_buf, v_buf)):
                start = heads * head_dim + n * wide
                buf[part] = qkv_buf[part, start:start + wide].reshape(norm_rows, kv_heads, head_dim)
            return carry

        lax.fori_loop(0, seq // norm_rows, cache_body, 0)

    block = seq // 8
    d_tile = min(dim, 512)

    def attend_block(i):
        part = slice(i * block, (i + 1) * block)
        span = (i + 1) * block
        q_index = i * block + lax.broadcasted_iota(jnp.int32, (block, span), 0)
        key_index = lax.broadcasted_iota(jnp.int32, (block, span), 1)
        allowed = (key_index <= q_index) & (pos_col_ref[part, :] - pos_row_ref[:, :span] < WINDOW_LEN)

        def head_body(h, carry):
            q_cols = pl.ds(pl.multiple_of(h * head_dim, head_dim), head_dim)
            k_cols = pl.ds(pl.multiple_of((heads + lax.div(h, group)) * head_dim, head_dim), head_dim)
            v_cols = pl.ds(pl.multiple_of((heads + kv_heads + lax.div(h, group)) * head_dim, head_dim), head_dim)
            scores = lax.dot_general(qkv_buf[part, q_cols], qkv_buf[:span, k_cols], (((1,), (1,)), ((), ())), preferred_element_type=F32)
            capped = SOFT_CAP * jnp.tanh(scores * scale / SOFT_CAP)
            weights = jnp.where(allowed, jnp.exp(capped), 0.0)
            probs = (weights / jnp.sum(weights, axis=-1, keepdims=True)).astype(BF16)
            qkv_buf[part, q_cols] = jnp.dot(probs, qkv_buf[:span, v_cols], preferred_element_type=F32).astype(BF16)
            return carry

        lax.fori_loop(0, heads, head_body, 0)

    def out_pair(i):
        parts = [slice(n * block, (n + 1) * block) for n in (i, 4 + i)]

        def out_body(n, carry):
            column = pl.ds(pl.multiple_of(n * d_tile, d_tile), d_tile)
            rows = jnp.concatenate([qkv_buf[part, :heads * head_dim] for part in parts], axis=0)
            sums = jnp.dot(rows, wo_buf[:, column], preferred_element_type=F32).astype(BF16)
            for d, part in enumerate(parts):
                p_buf[part, column] = sums[d * block:(d + 1) * block]
            return carry

        lax.fori_loop(0, dim // d_tile, out_body, 0)

    def second(i):
        attend_block(4 + i)
        out_pair(i)

    with jax.named_scope('attend0'):
        attend_block(0)
        attend_block(4)
    with jax.named_scope('settle_out'):
        for p in range(pieces[OUT]):
            gather.landed(OUT, p)
            gather.sent(OUT, p)
        gather.own_landed(OUT)
        gather.own_sent(OUT)
        for part in (GATE, UP):
            for p in range(tiles):
                gather.own_start(part, p)
        gather.own_start(DOWN)
    with jax.named_scope('out0'):
        out_pair(0)

    def finish(out_rows, rows, total):
        hidden = (res_buf[rows, :].astype(F32) + unit_rows(total.astype(F32), gain_buf[1:2, :])).astype(BF16)
        res_buf[rows, :] = hidden
        xm_buf[out_rows, :] = unit_rows(hidden.astype(F32), gain_buf[2:3, :]).astype(BF16)

    sums = LineSum(p_buf, got, xm_buf, *line_sems[:4], finish, lambda out_rows: None)
    last = sums.steps - 1
    ahead = sums.chunks // 4

    span_rows = half // 4
    z_buf = wo_buf
    pair = 2 * tile

    def group_rows(g):
        return [pl.ds(times(d * half + g * span_rows, span_rows), span_rows) for d in range(2)]

    def gate_loads(f, base):
        copies = []
        for n, (src, dst) in enumerate(((wg_ref, wgf_ref), (wu_ref, wuf_ref))):
            column = pl.ds(times(base + n * tile, tile), tile)
            for r, shard in enumerate((me, mate, across, cross)):
                part = src.at[:, pl.ds(times(f * tile, tile), tile)] if r == 0 else dst.at[f, shard_span(shard)]
                copies.append(pltpu.make_async_copy(part, w_buf.at[shard_span(shard), column], gate_sem.at[base // pair if isinstance(base, int) else lax.div(base, pair), n, r]))
        return copies

    def gate_fetch(f, base, which=(0, 1)):
        for n in which:
            for load in gate_loads(f, base)[4 * n:4 * n + 4]:
                load.start()

    def gate_settle(f):
        for part in (GATE, UP):
            gather.landed(part, f)
            gather.own_landed(part, f)

    def gate_work(g, f, base, refill):
        parts = group_rows(g)
        ffw_in = jnp.concatenate([xm_buf[part, :] for part in parts], axis=0)
        for load in gate_loads(f, base)[:4]:
            load.wait()
        gate_tile[...] = jnp.dot(ffw_in, w_buf[:, pl.ds(times(base, tile), tile)], preferred_element_type=F32).astype(BF16)
        refill(0)
        for load in gate_loads(f, base)[4:]:
            load.wait()
        up = jnp.dot(ffw_in, w_buf[:, pl.ds(times(base + tile, tile), tile)], preferred_element_type=F32).astype(BF16).astype(F32)
        gated = (jax.nn.gelu(gate_tile[...].astype(F32), approximate=True) * up).astype(BF16)
        refill(1)
        for d, part in enumerate(parts):
            z_buf[part, pl.ds(times(f * tile, tile), tile)] = gated[d * span_rows:(d + 1) * span_rows]

    def gate_place(i):
        early = tiles - 1
        if isinstance(i, int):
            if i < 2 * early:
                return i // early, i % early
            return (i - 2 * early, early) if i < 2 * tiles else (2, i - 2 * tiles)
        g = jnp.where(i < 2 * early, lax.div(i, early), jnp.where(i < 2 * tiles, i - 2 * early, 2))
        return g, jnp.where(i < 2 * early, lax.rem(i, early), jnp.where(i < 2 * tiles, early, i - 2 * tiles))

    def gate_item(i, carry):
        base = lax.rem(i, 2) * pair
        ahead_g, ahead_f = gate_place(i + 2)

        @pl.when(ahead_g == 0)
        def _():
            gate_settle(ahead_f)

        def refill(n):
            @pl.when(i + 2 < 3 * tiles)
            def _():
                gate_fetch(ahead_f, base, (n,))

        gate_work(*gate_place(i), base, refill)
        return carry

    ffw = gather.order[pieces[QKV] + pieces[OUT]:]
    if len(ffw) == len(PASS_Y):
        y_turns, x_turns, gate_turns = PASS_Y, PASS_X, GATE_TURNS
    else:
        y_turns = [(min(3 + 2 * k, last), 0) for k in range(len(ffw))]
        x_turns = [(min(4 + 2 * k, last), 0) for k in range(len(ffw))]
        gate_turns = [0] * (3 * tiles)
    before, after, tail = {}, {}, []

    def at(turn, action):
        (after if turn[1] else before).setdefault(turn[0], []).append(action)

    late_pieces = max(1, min(2, pieces[DOWN] - 1))
    edge = pieces[DOWN] - late_pieces

    moves = [(turn, 0, k) for k, turn in enumerate(y_turns) if k > 0] + [(turn, 1, k) for k, turn in enumerate(x_turns)]
    for turn, way, k in sorted(moves, key=lambda move: ((99, 0) if move[0] is None else move[0], move[2] + move[1], move[1])):
        move = functools.partial((pass_y, pass_x)[way], *ffw[k])
        if turn is None:
            tail.append((ffw[k], move))
        else:
            at(turn, move)
    at((min(1, last), 1), keep_caches)
    for i in range(1, 4):
        early = (2 * ahead) // 8 if i == 3 else 0
        at((min(i * ahead - (5 * ahead) // 8 - early, last), 0), functools.partial(attend_block, i))
        at((min(i * ahead - (3 * ahead) // 8 - early, last), 0), functools.partial(second, i))
    gate_ready = [max(x_turns[k][0] + x_turns[k][1] for k in (2 * f, 2 * f + 1)) for f in range(tiles)]
    gate_table = []
    for i in range(3 * tiles):
        coming = [gate_place(min(i + n, 3 * tiles - 1)) for n in (0, 1, 2)]
        turn = max([gate_turns[i], (coming[0][0] + 1) * ahead + 6 * LAG] + [gate_ready[f] for g, f in coming if g == 0])
        gate_table.append(max(turn, gate_table[-1] if gate_table else 0))

    def open_gate():
        for i in range(2):
            if gate_place(i)[0] == 0:
                gate_settle(gate_place(i)[1])
            gate_fetch(gate_place(i)[1], i * pair)

    at((min(gate_table[0], last), 0), open_gate)

    def each_first(t):
        lax.fori_loop(*turns_of([turn for turn in gate_table if turn <= last], t), gate_item, 0)

    with jax.named_scope('chain1'):
        sums.run(before, each_first, after)
    with jax.named_scope('gate_rest'):
        lax.fori_loop(len([turn for turn in gate_table if turn <= last]), 3 * tiles, gate_item, 0)
    shards = (me, mate, across, cross)

    def down_load(r, base):
        column = pl.ds(base, cols)
        sem = down_sem.at[0 if base else 1]
        return pltpu.make_async_copy(wd_ref if r == 0 else wdf_ref.at[shards[r]], w_buf.at[:, column], sem)

    def down_fetch(r, base):
        if isinstance(r, int):
            down_load(r, base).start()
            return
        for n in range(4):

            @pl.when(r == n)
            def _():
                down_load(n, base).start()

    def down_work(g, r, base):
        down_load(0, base).wait()
        parts = group_rows(g)
        gated = jnp.concatenate([z_buf[part, :] for part in parts], axis=0)
        down = jnp.dot(gated, w_buf[:, pl.ds(base, cols)], preferred_element_type=F32).astype(BF16)
        if isinstance(r, int):
            shard = shards[r]
        else:
            shard = jnp.where(r == 0, me, jnp.where(r == 1, mate, jnp.where(r == 2, across, cross)))
        for d, part in enumerate(parts):
            p_buf[part, shard_span(shard)] = down[d * span_rows:(d + 1) * span_rows]

    rows_each = wd_ref.shape[0] // (2 * pieces[DOWN])
    half_hidden = wd_ref.shape[0] // 2
    spans = (((0, edge * rows_each), (half_hidden, edge * rows_each)), ((edge * rows_each, late_pieces * rows_each), (half_hidden + edge * rows_each, late_pieces * rows_each)))

    def far_loads(r, base, late):
        column = pl.ds(base, cols)
        return [pltpu.make_async_copy(wdf_ref.at[shards[r], pl.ds(start, size)], w_buf.at[pl.ds(start, size), column], far_sem.at[r - 2, n]) for n, (start, size) in enumerate(spans[late])]

    def far_product(base, late):
        gated = [jnp.concatenate([z_buf[part, start:start + size] for part in group_rows(0)], axis=0) for start, size in spans[late]]
        return sum(jnp.dot(rows, w_buf[start:start + size, pl.ds(base, cols)], preferred_element_type=F32) for rows, (start, size) in zip(gated, spans[late]))

    def far_early(r, base):
        for load in far_loads(r, base, 0):
            load.wait()
        far_buf[r - 2] = far_product(base, 0)

    def far_late(r, base):
        for load in far_loads(r, base, 1):
            load.wait()
        down = (far_buf[r - 2] + far_product(base, 1)).astype(BF16)
        for d, part in enumerate(group_rows(0)):
            p_buf[part, shard_span(shards[r])] = down[d * span_rows:(d + 1) * span_rows]

    def far_start(r, base, late):
        for load in far_loads(r, base, late):
            load.start()

    early_moves = [move for (part, p), move in tail if part != DOWN or p < edge]
    late_moves = [move for (part, p), move in tail if part == DOWN and p >= edge]
    down_fetch(0, pair)
    with jax.named_scope('tail'):
        gather.own_landed(DOWN)
        down_fetch(1, 0)
        sums.settle()
    with jax.named_scope('down_near0'):
        down_work(0, 0, pair)
    with jax.named_scope('pass_early'):
        for move in early_moves:
            move()
    with jax.named_scope('down_near1'):
        down_work(0, 1, 0)
    with jax.named_scope('landed_early'):
        for p in range(edge):
            gather.landed(DOWN, p)
        far_start(2, pair, 0)
        far_start(3, 0, 0)
    with jax.named_scope('pass_late0'):
        for move in late_moves[:len(late_moves) - 2]:
            move()
    with jax.named_scope('far_early0'):
        far_early(2, pair)
    with jax.named_scope('pass_late1'):
        for move in late_moves[len(late_moves) - 2:]:
            move()
    with jax.named_scope('far_early1'):
        far_early(3, 0)

    caches = ((k_buf, kf_ref), (v_buf, vf_ref))

    def rows_of(ref, shard):
        return ref.at[pl.ds(pl.multiple_of(shard * seq, seq), seq)]

    def kv_copy(i, hop):
        src, dst = caches[i]
        if hop == 0:
            return remote(src, rows_of(dst, me), kv_send.at[i, hop], kv_recv.at[i, hop], {'dm': across})
        if hop == 1:
            return remote(src, rows_of(dst, me), kv_send.at[i, hop], kv_recv.at[i, hop], {'dm': mate})
        return remote(rows_of(dst, across), rows_of(dst, across), kv_send.at[i, hop], kv_recv.at[i, hop], {'dm': mate})

    def kv_arrival(i, hop):
        region = rows_of(caches[i][1], (across, mate, cross)[hop])
        return remote(region, region, kv_send.at[i, hop], kv_recv.at[i, hop], {'dm': mate})

    with jax.named_scope('settle_down'):
        for p in range(edge, pieces[DOWN]):
            gather.landed(DOWN, p)
    far_start(2, pair, 1)
    far_start(3, 0, 1)
    kv_stores = [pltpu.make_async_copy(src, rows_of(dst, me), kv_store.at[i]) for i, (src, dst) in enumerate(caches)]
    for i in range(2):
        kv_copy(i, 0).start()
        kv_copy(i, 1).start()
        kv_stores[i].start()
    with jax.named_scope('far_late'):
        far_late(2, pair)
        down_fetch(0, pair)
        far_late(3, 0)
        gate_fetch(0, 0)

    def finish_last(out_rows, rows, total):
        xm_buf[out_rows, :] = (res_buf[rows, :].astype(F32) + unit_rows(total.astype(F32), gain_buf[3:4, :])).astype(BF16)

    def emit_last(out_rows):
        there = pl.ds(pl.multiple_of(me * seq + out_rows.start, CHUNK), CHUNK)
        for i, dev in enumerate((across, cross, mate)):
            remote(xm_buf.at[out_rows, shard_span(dev)], y_ref.at[there], fin_send.at[i], fin_recv.at[i], {'dm': dev}).start()
        pltpu.make_async_copy(xm_buf.at[out_rows, mine], y_ref.at[there], fin_own).start()

    last_sums = LineSum(p_buf, got, xm_buf, *line_sems[4:], finish_last, emit_last)

    def pass_kv(i):
        kv_arrival(i, 0).wait_recv()
        kv_copy(i, 2).start()

    late_gates = [int((f + 1) * 2 * ahead / (tiles + 1)) for f in range(tiles)]
    late_downs = [(n * ahead) // 4 + ahead // 8 for n in range(12)]

    def late_gate(f, carry):
        def refill(n):
            @pl.when(f + 1 < tiles)
            def _():
                gate_fetch(f + 1, 0, (n,))

        gate_work(3, f, 0, refill)
        return carry

    def late_down(n, carry):
        down_work(1 + lax.div(n, 4), lax.rem(n, 4), pair)

        @pl.when(n + 1 < 12)
        def _():
            down_fetch(lax.rem(n + 1, 4), pair)

        return carry

    def each_last(t):
        lax.fori_loop(*turns_of(late_gates, t), late_gate, 0)
        lax.fori_loop(*turns_of(late_downs, t), late_down, 0)

    with jax.named_scope('chain2'):
        last_sums.run({min(14, last - 1): [functools.partial(pass_kv, 0)], min(17, last): [functools.partial(pass_kv, 1)]}, each_last, {})
    with jax.named_scope('close'):
        last_sums.settle()
        for i in range(2):
            kv_stores[i].wait()
            for hop in range(3):
                kv_copy(i, hop).wait_send()
            kv_arrival(i, 1).wait_recv()
            kv_arrival(i, 2).wait_recv()
        for i, dev in enumerate((across, cross, mate)):
            done = remote(xm_buf.at[:, shard_span(dev)], rows_of(y_ref, dev), fin_send.at[i], fin_recv.at[i], {'dm': dev})
            done.wait_send()
            done.wait_recv()
        pltpu.make_async_copy(xm_buf.at[:, mine], rows_of(y_ref, me), fin_own).wait()
        for part in (GATE, UP):
            for p in range(tiles):
                gather.sent(part, p)
                gather.own_sent(part, p)
        for p in range(pieces[DOWN]):
            gather.sent(DOWN, p)
        gather.own_sent(DOWN)
        for copy in n_copies:
            copy.wait_send()
        x_copy(0, 0).wait_send()
        for s in range(2):
            x_copy(1, s).wait_send()
            x_copy(2, s).wait_send()


def like(*shape, dtype=BF16):
    return jax.ShapeDtypeStruct(shape, dtype)


def params(collective_id):
    return pltpu.CompilerParams(collective_id=collective_id, has_side_effects=True, vmem_limit_bytes=VMEM_BYTES)


def run_layer(x, norms, wq, wk, wv, wo, wg, wu, wd, cos_tab, sin_tab, pos, scale):
    seq = pos.shape[0]
    cols = x.shape[1]
    dim = 4 * cols
    kv_heads, head_dim = wk.shape[1:]
    width = wo.shape[0] + 2 * kv_heads * head_dim
    chunks = seq // 2 // CHUNK
    cache = (seq, kv_heads, head_dim)
    hidden = wg.shape[1]
    tile = min(hidden // 2, 512)
    tiles = hidden // tile

    def count(rows, most):
        return most if rows % (32 * most) == 0 else 2

    pieces = (count(cols, 7), 4, tiles, tiles, count(wd.shape[0], 14))
    units = sum(pieces)
    return pl.pallas_call(
        functools.partial(layer_kernel, scale, kv_heads, head_dim, pieces),
        name='layer',
        out_shape=(like(4 * seq, cols), like(4 * seq, kv_heads, head_dim), like(4 * seq, kv_heads, head_dim), like(tiles, dim, tile), like(tiles, dim, tile), like(4, *wd.shape)),
        in_specs=[ANY] * 9 + [VMEM] * 4,
        out_specs=(ANY,) * 6,
        scratch_shapes=[
            pltpu.VMEM((seq, dim), BF16), pltpu.VMEM((dim, width), BF16), pltpu.VMEM((wo.shape[0], dim), BF16), pltpu.VMEM((seq, width), BF16),
            pltpu.VMEM((seq, dim), BF16), pltpu.VMEM((2, seq // 2, dim), BF16), pltpu.VMEM((seq // 2, dim), BF16), pltpu.VMEM((4,) + norms.shape, F32), pltpu.VMEM((4, dim), F32),
            pltpu.VMEM(wq.shape, BF16), pltpu.VMEM(wk.shape, BF16), pltpu.VMEM(wv.shape, BF16), pltpu.VMEM(cache, BF16), pltpu.VMEM(cache, BF16), pltpu.VMEM((2, seq // 4, cols), F32), pltpu.VMEM((seq // 4, tile), BF16),
            DMA((3, 2)), DMA((3, 2)), DMA((3,)), DMA((3,)), DMA((2, 2 * LINE)), DMA((2 * LINE,)), DMA((3 + 2 * tiles,)), DMA((3 + 2 * tiles,)), DMA((units, 4)), DMA((units, 4)), DMA((6,)),
            DMA((2, 2, 4)), DMA((2,)), DMA((2, 2)), DMA((2,)), DMA((2, 3)), DMA((2, 3)), DMA((3,)), DMA((3,)), DMA,
        ] + [DMA((2, chunks))] * 8,
        compiler_params=params(0),
    )(x, norms, wq, wk, wv, wo, wg, wu, wd, cos_tab, sin_tab, pos[:, None], pos[None, :])


def solution(mesh):
    tp_size = mesh.shape['tp']

    def layer(tokens, positions, norm_pre_attn, w_query, w_key, w_value, w_out, norm_post_attn, norm_pre_ffw, w_gate, w_up, w_down, norm_post_ffw):
        seq = positions.shape[1]
        heads, head_dim, cols = w_out.shape
        dim = 4 * cols
        scale = (dim / (heads * tp_size)) ** -0.5
        norms = jnp.stack([norm_pre_attn, norm_post_attn, norm_pre_ffw, norm_post_ffw]).astype(F32)
        pos = lax.dynamic_index_in_dim(positions, lax.axis_index('dm'), 0, keepdims=False)
        half_dim = head_dim // 2
        inv_freq = ROPE_BASE ** (-2.0 * jnp.arange(half_dim, dtype=F32) / head_dim)
        angles = pos.astype(F32)[:, None] * inv_freq[None, :]
        outs = run_layer(tokens, norms, w_query, w_key, w_value, w_out.reshape(heads * head_dim, cols), w_gate, w_up, w_down, jnp.cos(angles), jnp.sin(angles), pos, scale)
        return outs[:3]

    width_spec = P('dm')
    in_specs = (P('dp', 'dm'), P('dp', None), width_spec, P('dm', 'tp', None), P('dm', 'tp', None), P('dm', 'tp', None), P('tp', None, 'dm'), width_spec, width_spec, P('dm', 'tp'), P('dm', 'tp'), P('tp', 'dm'), width_spec)
    out_specs = (P('dp', 'dm'), P('dp', 'tp', None), P('dp', 'tp', None))
    return jax.shard_map(layer, mesh=mesh, in_specs=in_specs, out_specs=out_specs, check_vma=False)
```

```python
import functools

import jax
import jax.numpy as jnp
from jax import lax
from jax.experimental import pallas as pl
from jax.experimental.pallas import tpu as pltpu
from jax.sharding import PartitionSpec as P

NORM_EPS = 1e-6
SOFT_CAP = 50.0
ROPE_BASE = 10000.0
WINDOW_LEN = 4096
BF16 = jnp.bfloat16
F32 = jnp.float32

CHUNK = 16
LAG = 2
LINE = 4
VMEM_BYTES = 67043328

PASS_Y = [(0, 0), (1, 1), (5, 0), (8, 0), (11, 1), (13, 0), (15, 1), (16, 0), (18, 0), (19, 1), (21, 0), (24, 0), (25, 1), (28, 0), (29, 0), (29, 1), (30, 1), (30, 1), (31, 1), (32, 1), (33, 1), (34, 1), (36, 1), (36, 1), (37, 1), (38, 1), (39, 1), (42, 0)]
PASS_X = [(2, 1), (5, 1), (9, 0), (12, 0), (13, 1), (16, 0), (17, 0), (19, 0), (20, 1), (23, 0), (25, 0), (27, 0), (29, 0), (30, 1), (31, 0), (31, 1), (32, 1), (33, 1), (34, 1), (36, 1), (37, 0), (37, 1), (38, 1), (39, 1), (42, 0), None, None, None]
GATE_TURNS = [20, 20, 25, 29, 29, 30, 30, 31, 31, 32, 32, 33, 33, 34, 36, 36, 37, 37, 38, 38, 39]

ANY = pl.BlockSpec(memory_space=pl.ANY)
VMEM = pl.BlockSpec(memory_space=pltpu.VMEM)
DMA = pltpu.SemaphoreType.DMA


def places():
    row = lax.axis_index('dp')
    line = lax.axis_index('tp')
    me = lax.axis_index('dm')
    side = lax.div(me, 2)
    core = me - 2 * side
    return row, line, me, 2 * side + 1 - core, 2 * (1 - side) + core, 2 * (1 - side) + 1 - core


def times(value, unit):
    return value if isinstance(value, int) else pl.multiple_of(value, unit)


def remote(src, dst, send_sem, recv_sem, device):
    return pltpu.make_async_remote_copy(src_ref=src, dst_ref=dst, send_sem=send_sem, recv_sem=recv_sem, device_id=device, device_id_type=pl.DeviceIdType.MESH)


def meet(peers):
    barrier = pltpu.get_barrier_semaphore()
    for peer in peers:
        pl.semaphore_signal(barrier, inc=1, device_id=peer, device_id_type=pl.DeviceIdType.MESH)
    pl.semaphore_wait(barrier, len(peers))


def line_peers(line):
    return [{'tp': lax.rem(line + 1, LINE)}, {'tp': lax.rem(line + LINE - 1, LINE)}]


QKV, OUT, GATE, UP, DOWN = range(5)


class WeightGather:
    def __init__(self, refs, pieces, tile, own_send, own_recv, send, recv):
        self.refs, self.pieces, self.tile = refs, pieces, tile
        self.own_send, self.own_recv, self.send, self.recv = own_send, own_recv, send, recv
        self.row, _, self.me, self.mate, self.across, self.cross = places()
        self.order = [(QKV, p) for p in range(pieces[QKV])] + [(OUT, p) for p in range(pieces[OUT])]
        self.order += [(part, p) for p in range(pieces[GATE]) for part in (GATE, UP)]
        self.order += [(DOWN, p) for p in range(pieces[DOWN])]

    def index(self, part, p):
        first = {QKV: 0, OUT: self.pieces[QKV]}
        ffw = self.pieces[QKV] + self.pieces[OUT]
        if part in first:
            return first[part] + p
        if part == DOWN:
            return ffw + 2 * self.pieces[GATE] + p
        return ffw + 2 * p + (part - GATE)

    def direct(self, part, p):
        return part == DOWN and p == self.pieces[DOWN] - 1

    def cut(self, part, half, p):
        size = self.refs[part][0].shape[0] // (2 * self.pieces[part])
        return pl.ds(pl.multiple_of((half * self.pieces[part] + p) * size, size), size)

    def own(self, part, half, p):
        src = self.refs[part][0]
        if part in (GATE, UP):
            size = self.tile // 2
            return src.at[:, pl.ds(pl.multiple_of(p * self.tile + half * size, size), size)]
        return src.at[self.cut(part, half, p)]

    def at(self, part, shard, half, p):
        src, dst = self.refs[part]
        if part == QKV:
            size = src.shape[0] // (2 * self.pieces[part])
            return dst.at[pl.ds(pl.multiple_of(shard * src.shape[0] + (half * self.pieces[part] + p) * size, size), size)]
        if part == OUT:
            return dst.at[self.cut(part, half, p), pl.ds(pl.multiple_of(shard * src.shape[1], src.shape[1]), src.shape[1])]
        if part == DOWN:
            return dst.at[shard, self.cut(part, half, p)]
        size = self.tile // 2
        return dst.at[p, pl.ds(pl.multiple_of(shard * src.shape[0], src.shape[0]), src.shape[0]), pl.ds(pl.multiple_of(half * size, size), size)]

    def copy(self, part, p, hop):
        mine, other = self.row, 1 - self.row
        k = self.index(part, p)
        device = {'dm': self.mate}
        if hop == 0 or (hop == 1 and self.direct(part, p)):
            half = mine if hop == 0 else other
            src, dst, device = self.own(part, half, p), self.at(part, self.me, half, p), {'dm': self.across}
        else:
            src = dst = self.at(part, self.across, other if hop == 3 else mine, p)
            if hop == 1:
                device = {'dp': other}
        return remote(src, dst, self.send.at[k, hop], self.recv.at[k, hop], device)

    def arrival(self, part, p, hop):
        k = self.index(part, p)
        region = self.at(part, self.across if hop < 2 else self.cross, 1 - self.row if hop % 2 else self.row, p)
        return remote(region, region, self.send.at[k, hop], self.recv.at[k, hop], {'dm': self.mate})

    def own_copy(self, part, p, shard):
        src, dst = self.refs[part]
        if part in (GATE, UP):
            src = src.at[:, pl.ds(times(p * self.tile, self.tile), self.tile)]
            dst = dst.at[p, pl.ds(pl.multiple_of(shard * src.shape[0], src.shape[0]), src.shape[0])]
            k = 3 + 2 * p + part - GATE
        else:
            k = (QKV, OUT, DOWN).index(part)
            if part == DOWN:
                dst = dst.at[shard]
            elif part == OUT:
                dst = dst.at[:, pl.ds(pl.multiple_of(shard * src.shape[1], src.shape[1]), src.shape[1])]
            else:
                dst = dst.at[pl.ds(pl.multiple_of(shard * src.shape[0], src.shape[0]), src.shape[0])]
        return remote(src, dst, self.own_send.at[k], self.own_recv.at[k], {'dm': self.mate})

    def start(self):
        for part, p in self.order:
            self.copy(part, p, 0).start()
            if self.direct(part, p):
                self.copy(part, p, 1).start()

    def pass_y(self, part, p):
        self.arrival(part, p, 0).wait_recv()
        if not self.direct(part, p):
            self.copy(part, p, 1).start()
        self.copy(part, p, 2).start()

    def pass_x(self, part, p):
        self.arrival(part, p, 1).wait_recv()
        self.copy(part, p, 3).start()

    def landed(self, part, p):
        self.arrival(part, p, 2).wait_recv()
        self.arrival(part, p, 3).wait_recv()

    def sent(self, part, p):
        for hop in range(4):
            self.copy(part, p, hop).wait_send()

    def own_start(self, part, p=0):
        self.own_copy(part, p, self.me).start()

    def own_landed(self, part, p=0):
        self.own_copy(part, p, self.mate).wait_recv()

    def own_sent(self, part, p=0):
        self.own_copy(part, p, self.me).wait_send()


class LineSum:
    def __init__(self, p_buf, got, out, sum_send, sum_recv, out_send, out_recv, finish, emit):
        self.p_buf, self.got, self.out = p_buf, got, out
        self.sum_send, self.sum_recv, self.out_send, self.out_recv = sum_send, sum_recv, out_send, out_recv
        self.finish, self.emit = finish, emit
        self.half = p_buf.shape[0] // 2
        self.chunks = self.half // CHUNK
        self.steps = self.chunks + 6 * LAG
        self.line = lax.axis_index('tp')

    def way(self, d):
        if d == 0:
            return self.line, {'tp': self.line + 1}, {'tp': self.line - 1}
        return LINE - 1 - self.line, {'tp': self.line - 1}, {'tp': self.line + 1}

    def rows(self, c):
        return pl.ds(pl.multiple_of(c * CHUNK, CHUNK), CHUNK)

    def out_rows(self, d, c):
        return pl.ds(pl.multiple_of(d * self.half + c * CHUNK, CHUNK), CHUNK)

    def sum_copy(self, d, c):
        return remote(self.p_buf.at[self.out_rows(d, c)], self.got.at[d, self.rows(c)], self.sum_send.at[d, c], self.sum_recv.at[d, c], self.way(d)[1])

    def out_copy(self, d, c):
        region = self.out.at[self.out_rows(d, c)]
        return remote(region, region, self.out_send.at[d, c], self.out_recv.at[d, c], self.way(d)[2])

    def step(self, t):
        for d in range(2):
            with jax.named_scope(f'sum{d}'):
                self.sum_step(d, t)
        for d in range(2):
            with jax.named_scope(f'out{d}'):
                self.out_step(d, t)

    def sum_step(self, d, t):
        pos = self.way(d)[0]
        c = t - LAG * pos

        @pl.when((c >= 0) & (c < self.chunks))
        def _():
            @pl.when(pos == 0)
            def _():
                self.sum_copy(d, c).start()

            @pl.when(pos > 0)
            def _():
                self.sum_copy(d, c).wait_recv()
                total = self.p_buf[self.out_rows(d, c), :].astype(F32) + self.got[d, self.rows(c), :].astype(F32)

                @pl.when(pos < LINE - 1)
                def _():
                    self.p_buf[self.out_rows(d, c), :] = total.astype(BF16)
                    self.sum_copy(d, c).start()

                @pl.when(pos == LINE - 1)
                def _():
                    self.finish(self.out_rows(d, c), self.rows(c), total.astype(BF16))
                    self.out_copy(d, c).start()
                    self.emit(self.out_rows(d, c))

    def out_step(self, d, t):
        pos = self.way(d)[0]
        c = t - 3 * LAG - LAG * (LINE - 1 - pos)

        @pl.when((c >= 0) & (c < self.chunks) & (pos < LINE - 1))
        def _():
            self.out_copy(d, c).wait_recv()

            @pl.when(pos > 0)
            def _():
                self.out_copy(d, c).start()

            self.emit(self.out_rows(d, c))

    def run(self, before, each, after):
        def body(t, carry):
            def act(actions):
                for turn in sorted(actions):

                    @pl.when(t == turn)
                    def _():
                        for action in actions[turn]:
                            action()

            with jax.named_scope('before'):
                act(before)
            with jax.named_scope('each'):
                each(t)
            with jax.named_scope('after'):
                act(after)
            self.step(t)
            return carry

        lax.fori_loop(0, self.steps, body, 0)

    def settle(self):
        def body(c, carry):
            for d in range(2):
                pos = self.way(d)[0]

                @pl.when(pos < LINE - 1)
                def _():
                    self.sum_copy(d, c).wait_send()

                @pl.when(pos > 0)
                def _():
                    self.out_copy(d, c).wait_send()

            return carry

        lax.fori_loop(0, self.chunks, body, 0)


def unit_rows(values, gain):
    mean_sq = jnp.mean(values * values, axis=-1, keepdims=True)
    return values * lax.rsqrt(mean_sq + NORM_EPS) * gain


def rotate(values, cos_tab, sin_tab):
    half_dim = values.shape[-1] // 2
    lower = values[:, :half_dim].astype(F32)
    upper = values[:, half_dim:].astype(F32)
    return jnp.concatenate([lower * cos_tab - upper * sin_tab, upper * cos_tab + lower * sin_tab], axis=-1).astype(BF16)


def turns_of(table, t):
    first = sum([jnp.where(t > turn, 1, 0) for turn in table], 0)
    return first, first + sum([jnp.where(t == turn, 1, 0) for turn in table], 0)


def layer_kernel(scale, kv_heads, head_dim, pieces, x_ref, n_ref, wq_ref, wk_ref, wv_ref, wo_ref, wg_ref, wu_ref, wd_ref, cos_ref, sin_ref, pos_col_ref, pos_row_ref, y_ref, kf_ref, vf_ref, wgf_ref, wuf_ref, wdf_ref, xm_buf, w_buf, wo_buf, qkv_buf, p_buf, got, res_buf, n_buf, gain_buf, wq_buf, wk_buf, wv_buf, k_buf, v_buf, far_buf, gate_tile, x_send, x_recv, n_send, n_recv, z_send, z_recv, own_send, own_recv, w_send, w_recv, load_sem, gate_sem, down_sem, far_sem, kv_store, kv_send, kv_recv, fin_send, fin_recv, fin_own, *line_sems):
    row, line, me, mate, across, cross = places()
    seq, dim = xm_buf.shape
    cols = dim // 4
    half = seq // 2
    quarter = seq // LINE
    sub = quarter // 2
    heads = wo_ref.shape[0] // head_dim
    group = heads // kv_heads
    tiles, _, tile = wgf_ref.shape
    peers = (mate, across, cross)

    def shard_span(shard):
        return pl.ds(pl.multiple_of(shard * cols, cols), cols)

    mine = shard_span(me)
    refs = ((w_buf.at[mine], w_buf), (wo_ref, wo_buf), (wg_ref, wgf_ref), (wu_ref, wuf_ref), (wd_ref, wdf_ref))
    gather = WeightGather(refs, pieces, tile, own_send, own_recv, w_send, w_recv)
    pass_y, pass_x = gather.pass_y, gather.pass_x

    def x_copy(hop, s):
        dev = peers[hop]
        if hop == 0:
            src, dst = x_ref.at[pl.ds(pl.multiple_of(dev * seq, seq), seq)], xm_buf.at[:, mine]
        else:
            start = line * quarter + s * sub
            src = x_ref.at[pl.ds(pl.multiple_of(dev * seq + start, sub), sub)]
            dst = xm_buf.at[pl.ds(pl.multiple_of(start, sub), sub), mine]
        return remote(src, dst, x_send.at[hop, s], x_recv.at[hop, s], {'dm': dev})

    def x_arrival(hop, s):
        theirs = shard_span(peers[hop])
        region = xm_buf.at[:, theirs] if hop == 0 else xm_buf.at[pl.ds(pl.multiple_of(line * quarter + s * sub, sub), sub), theirs]
        return remote(region, region, x_send.at[hop, s], x_recv.at[hop, s], {'dm': mate})

    far = pl.ds(pl.multiple_of((1 - lax.div(me, 2)) * 2 * cols, 2 * cols), 2 * cols)

    def z_copy(up, block, s):
        index = 2 * block + s
        region = xm_buf.at[pl.ds(pl.multiple_of(index * sub, sub), sub), far]
        device = {'tp': line + 1} if up else {'tp': line - 1}
        return remote(region, region, z_send.at[0 if up else 1, index], z_recv.at[index], device)

    def z_first(s):
        x_arrival(1, s).wait_recv()
        x_arrival(2, s).wait_recv()

        @pl.when(line < LINE - 1)
        def _():
            z_copy(True, line, s).start()

        @pl.when(line > 0)
        def _():
            z_copy(False, line, s).start()

    def z_step(step, s):
        below, above = line - step, line + step

        @pl.when(below >= 0)
        def _():
            z_copy(True, below, s).wait_recv()

            @pl.when(line < LINE - 1)
            def _():
                z_copy(True, below, s).start()

        @pl.when(above < LINE)
        def _():
            z_copy(False, above, s).wait_recv()

            @pl.when(line > 0)
            def _():
                z_copy(False, above, s).start()

    n_copies = [remote(n_ref, n_buf.at[me], n_send.at[i], n_recv.at[i], {'dm': dev}) for i, dev in enumerate(peers)]
    n_arrivals = [remote(n_ref, n_buf.at[dev], n_send.at[i], n_recv.at[i], {'dm': dev}) for i, dev in enumerate(peers)]
    loads = [
        pltpu.make_async_copy(x_ref.at[pl.ds(pl.multiple_of(me * seq, seq), seq)], xm_buf.at[:, mine], load_sem.at[0]),
        pltpu.make_async_copy(wo_ref, wo_buf.at[:, mine], load_sem.at[1]),
        pltpu.make_async_copy(n_ref, n_buf.at[me], load_sem.at[2]),
    ]
    thirds = ((wq_ref, wq_buf), (wk_ref, wk_buf), (wv_ref, wv_buf))
    third_loads = [pltpu.make_async_copy(src, buf, load_sem.at[3 + i]) for i, (src, buf) in enumerate(thirds)]

    def flatten_own():
        for load in third_loads:
            load.wait()
        flat_rows = min(cols, 64)

        def body(i, carry):
            part = pl.ds(pl.multiple_of(i * flat_rows, flat_rows), flat_rows)
            there = pl.ds(pl.multiple_of(me * cols + i * flat_rows, flat_rows), flat_rows)
            start = 0
            for _, buf in thirds:
                wide = buf.shape[1] * buf.shape[2]
                w_buf[there, start:start + wide] = buf[part].reshape(flat_rows, wide)
                start += wide
            return carry

        lax.fori_loop(0, cols // flat_rows, body, 0)

    def spread(part, share):
        count = pieces[part]
        return [p for p in range(count) if (4 * p) // count == share]

    for load in third_loads:
        load.start()
    with jax.named_scope('meet'):
        meet([{'dm': mate}, {'dm': across}, {'dm': cross}, {'dp': 1 - row}] + line_peers(line))
    for s in range(2):
        x_copy(1, s).start()
        x_copy(2, s).start()
    for copy in n_copies:
        copy.start()
    with jax.named_scope('flatten'):
        flatten_own()
    gather.start()
    x_copy(0, 0).start()
    for load in loads:
        load.start()
    gather.own_start(QKV)
    gather.own_start(OUT)
    with jax.named_scope('z0'):
        z_first(0)
        z_first(1)
        z_step(1, 0)
    with jax.named_scope('z1'):
        for p in spread(QKV, 0)[:1]:
            pass_y(QKV, p)
        z_step(1, 1)
        for p in spread(QKV, 0)[1:]:
            pass_y(QKV, p)
        for p in spread(QKV, 0)[:1]:
            pass_x(QKV, p)
        z_step(2, 0)
    with jax.named_scope('z2'):
        for p in spread(QKV, 1):
            pass_y(QKV, p)
        for p in spread(QKV, 0)[1:]:
            pass_x(QKV, p)
        z_step(2, 1)
        for p in spread(QKV, 2):
            pass_y(QKV, p)
        for p in spread(QKV, 1):
            pass_x(QKV, p)
        z_step(3, 0)
    with jax.named_scope('z3'):
        for p in spread(QKV, 3):
            pass_y(QKV, p)
        for p in spread(QKV, 2):
            pass_x(QKV, p)
        for copy in n_arrivals:
            copy.wait_recv()
        for load in loads:
            load.wait()
        for shard in range(4):
            gain_buf[:, shard * cols:(shard + 1) * cols] = 1.0 + n_buf[shard]
        x_arrival(0, 0).wait_recv()
        z_step(3, 1)

    for block in range(LINE):
        for s in range(2):

            @pl.when((block <= line) & (line < LINE - 1))
            def _():
                z_copy(True, block, s).wait_send()

            @pl.when((block >= line) & (line > 0))
            def _():
                z_copy(False, block, s).wait_send()

    first_row = pl.multiple_of(half * (1 - jnp.minimum(line, 1)), half)
    res_buf[...] = xm_buf[pl.ds(first_row, half), :]
    norm_rows = min(seq, 64)

    def norm_body(i, carry):
        part = pl.ds(pl.multiple_of(i * norm_rows, norm_rows), norm_rows)
        xm_buf[part, :] = unit_rows(xm_buf[part, :].astype(F32), gain_buf[0:1, :]).astype(BF16)
        return carry

    pass_y(OUT, 0)
    with jax.named_scope('norm'):
        lax.fori_loop(0, seq // norm_rows, norm_body, 0)
    with jax.named_scope('settle_qkv'):
        pass_y(OUT, 1)
        for p in spread(QKV, 3):
            pass_x(QKV, p)
        for p in range(pieces[QKV]):
            gather.landed(QKV, p)
            gather.sent(QKV, p)
        gather.own_landed(QKV)
        gather.own_sent(QKV)

    big = min(seq, 512)
    width = qkv_buf.shape[1]
    q_tile = min(width, 512)
    q_steps = (width // q_tile) * (seq // big)

    def qkv_body(i, carry):
        column = pl.ds(pl.multiple_of(lax.rem(i, width // q_tile) * q_tile, q_tile), q_tile)
        part = pl.ds(pl.multiple_of(lax.div(i, width // q_tile) * big, big), big)
        qkv_buf[part, column] = jnp.dot(xm_buf[part, :], w_buf[:, column], preferred_element_type=F32).astype(BF16)
        return carry

    with jax.named_scope('qkv'):
        lax.fori_loop(0, q_steps // 4, qkv_body, 0)
        pass_y(OUT, 2)
        pass_x(OUT, 0)
        lax.fori_loop(q_steps // 4, q_steps // 2, qkv_body, 0)
        pass_y(OUT, 3)
        pass_x(OUT, 1)
        lax.fori_loop(q_steps // 2, q_steps, qkv_body, 0)
        pass_x(OUT, 2)
        pass_y(GATE, 0)
    with jax.named_scope('pass_out'):
        pass_x(OUT, 3)

    def rotate_body(i, carry):
        column = pl.ds(pl.multiple_of(i * head_dim, head_dim), head_dim)
        qkv_buf[:, column] = rotate(qkv_buf[:, column], cos_ref[...], sin_ref[...])
        return carry

    with jax.named_scope('rotate'):
        lax.fori_loop(0, heads + kv_heads, rotate_body, 0)

    def keep_caches():
        def cache_body(i, carry):
            part = pl.ds(pl.multiple_of(i * norm_rows, norm_rows), norm_rows)
            wide = kv_heads * head_dim
            for n, buf in enumerate((k_buf, v_buf)):
                start = heads * head_dim + n * wide
                buf[part] = qkv_buf[part, start:start + wide].reshape(norm_rows, kv_heads, head_dim)
            return carry

        lax.fori_loop(0, seq // norm_rows, cache_body, 0)

    block = seq // 8
    d_tile = min(dim, 512)

    def attend_block(i):
        part = slice(i * block, (i + 1) * block)
        span = (i + 1) * block
        q_index = i * block + lax.broadcasted_iota(jnp.int32, (block, span), 0)
        key_index = lax.broadcasted_iota(jnp.int32, (block, span), 1)
        allowed = (key_index <= q_index) & (pos_col_ref[part, :] - pos_row_ref[:, :span] < WINDOW_LEN)

        def head_body(h, carry):
            q_cols = pl.ds(pl.multiple_of(h * head_dim, head_dim), head_dim)
            k_cols = pl.ds(pl.multiple_of((heads + lax.div(h, group)) * head_dim, head_dim), head_dim)
            v_cols = pl.ds(pl.multiple_of((heads + kv_heads + lax.div(h, group)) * head_dim, head_dim), head_dim)
            scores = lax.dot_general(qkv_buf[part, q_cols], qkv_buf[:span, k_cols], (((1,), (1,)), ((), ())), preferred_element_type=F32)
            capped = SOFT_CAP * jnp.tanh(scores * scale / SOFT_CAP)
            weights = jnp.where(allowed, jnp.exp(capped), 0.0)
            probs = (weights / jnp.sum(weights, axis=-1, keepdims=True)).astype(BF16)
            qkv_buf[part, q_cols] = jnp.dot(probs, qkv_buf[:span, v_cols], preferred_element_type=F32).astype(BF16)
            return carry

        lax.fori_loop(0, heads, head_body, 0)

    def out_pair(i):
        parts = [slice(n * block, (n + 1) * block) for n in (i, 4 + i)]

        def out_body(n, carry):
            column = pl.ds(pl.multiple_of(n * d_tile, d_tile), d_tile)
            rows = jnp.concatenate([qkv_buf[part, :heads * head_dim] for part in parts], axis=0)
            sums = jnp.dot(rows, wo_buf[:, column], preferred_element_type=F32).astype(BF16)
            for d, part in enumerate(parts):
                p_buf[part, column] = sums[d * block:(d + 1) * block]
            return carry

        lax.fori_loop(0, dim // d_tile, out_body, 0)

    def second(i):
        attend_block(4 + i)
        out_pair(i)

    with jax.named_scope('attend0'):
        attend_block(0)
        attend_block(4)
    with jax.named_scope('settle_out'):
        for p in range(pieces[OUT]):
            gather.landed(OUT, p)
            gather.sent(OUT, p)
        gather.own_landed(OUT)
        gather.own_sent(OUT)
        for part in (GATE, UP):
            for p in range(tiles):
                gather.own_start(part, p)
        gather.own_start(DOWN)
    with jax.named_scope('out0'):
        out_pair(0)

    def finish(out_rows, rows, total):
        hidden = (res_buf[rows, :].astype(F32) + unit_rows(total.astype(F32), gain_buf[1:2, :])).astype(BF16)
        res_buf[rows, :] = hidden
        xm_buf[out_rows, :] = unit_rows(hidden.astype(F32), gain_buf[2:3, :]).astype(BF16)

    sums = LineSum(p_buf, got, xm_buf, *line_sems[:4], finish, lambda out_rows: None)
    last = sums.steps - 1
    ahead = sums.chunks // 4

    span_rows = half // 4
    z_buf = wo_buf
    pair = 2 * tile

    def group_rows(g):
        return [pl.ds(times(d * half + g * span_rows, span_rows), span_rows) for d in range(2)]

    def gate_loads(f, base):
        copies = []
        for n, (src, dst) in enumerate(((wg_ref, wgf_ref), (wu_ref, wuf_ref))):
            column = pl.ds(times(base + n * tile, tile), tile)
            for r, shard in enumerate((me, mate, across, cross)):
                part = src.at[:, pl.ds(times(f * tile, tile), tile)] if r == 0 else dst.at[f, shard_span(shard)]
                copies.append(pltpu.make_async_copy(part, w_buf.at[shard_span(shard), column], gate_sem.at[base // pair if isinstance(base, int) else lax.div(base, pair), n, r]))
        return copies

    def gate_fetch(f, base, which=(0, 1)):
        for n in which:
            for load in gate_loads(f, base)[4 * n:4 * n + 4]:
                load.start()

    def gate_settle(f):
        for part in (GATE, UP):
            gather.landed(part, f)
            gather.own_landed(part, f)

    def gate_work(g, f, base, refill):
        parts = group_rows(g)
        ffw_in = jnp.concatenate([xm_buf[part, :] for part in parts], axis=0)
        for load in gate_loads(f, base)[:4]:
            load.wait()
        gate_tile[...] = jnp.dot(ffw_in, w_buf[:, pl.ds(times(base, tile), tile)], preferred_element_type=F32).astype(BF16)
        refill(0)
        for load in gate_loads(f, base)[4:]:
            load.wait()
        up = jnp.dot(ffw_in, w_buf[:, pl.ds(times(base + tile, tile), tile)], preferred_element_type=F32).astype(BF16).astype(F32)
        gated = (jax.nn.gelu(gate_tile[...].astype(F32), approximate=True) * up).astype(BF16)
        refill(1)
        for d, part in enumerate(parts):
            z_buf[part, pl.ds(times(f * tile, tile), tile)] = gated[d * span_rows:(d + 1) * span_rows]

    def gate_place(i):
        early = tiles - 1
        if isinstance(i, int):
            if i < 2 * early:
                return i // early, i % early
            return (i - 2 * early, early) if i < 2 * tiles else (2, i - 2 * tiles)
        g = jnp.where(i < 2 * early, lax.div(i, early), jnp.where(i < 2 * tiles, i - 2 * early, 2))
        return g, jnp.where(i < 2 * early, lax.rem(i, early), jnp.where(i < 2 * tiles, early, i - 2 * tiles))

    def gate_item(i, carry):
        base = lax.rem(i, 2) * pair
        ahead_g, ahead_f = gate_place(i + 2)

        @pl.when(ahead_g == 0)
        def _():
            gate_settle(ahead_f)

        def refill(n):
            @pl.when(i + 2 < 3 * tiles)
            def _():
                gate_fetch(ahead_f, base, (n,))

        gate_work(*gate_place(i), base, refill)
        return carry

    ffw = gather.order[pieces[QKV] + pieces[OUT]:]
    if len(ffw) == len(PASS_Y):
        y_turns, x_turns, gate_turns = PASS_Y, PASS_X, GATE_TURNS
    else:
        y_turns = [(min(3 + 2 * k, last), 0) for k in range(len(ffw))]
        x_turns = [(min(4 + 2 * k, last), 0) for k in range(len(ffw))]
        gate_turns = [0] * (3 * tiles)
    before, after, tail = {}, {}, []

    def at(turn, action):
        (after if turn[1] else before).setdefault(turn[0], []).append(action)

    late_pieces = max(1, min(2, pieces[DOWN] - 1))
    edge = pieces[DOWN] - late_pieces

    moves = [(turn, 0, k) for k, turn in enumerate(y_turns) if k > 0] + [(turn, 1, k) for k, turn in enumerate(x_turns)]
    for turn, way, k in sorted(moves, key=lambda move: ((99, 0) if move[0] is None else move[0], move[2] + move[1], move[1])):
        move = functools.partial((pass_y, pass_x)[way], *ffw[k])
        if turn is None:
            tail.append((ffw[k], move))
        else:
            at(turn, move)
    at((min(1, last), 1), keep_caches)
    for i in range(1, 4):
        early = (2 * ahead) // 8 if i == 3 else 0
        at((min(i * ahead - (5 * ahead) // 8 - early, last), 0), functools.partial(attend_block, i))
        at((min(i * ahead - (3 * ahead) // 8 - early, last), 0), functools.partial(second, i))
    gate_ready = [max(x_turns[k][0] + x_turns[k][1] for k in (2 * f, 2 * f + 1)) for f in range(tiles)]
    gate_table = []
    for i in range(3 * tiles):
        coming = [gate_place(min(i + n, 3 * tiles - 1)) for n in (0, 1, 2)]
        turn = max([gate_turns[i], (coming[0][0] + 1) * ahead + 6 * LAG] + [gate_ready[f] for g, f in coming if g == 0])
        gate_table.append(max(turn, gate_table[-1] if gate_table else 0))

    def open_gate():
        for i in range(2):
            if gate_place(i)[0] == 0:
                gate_settle(gate_place(i)[1])
            gate_fetch(gate_place(i)[1], i * pair)

    at((min(gate_table[0], last), 0), open_gate)

    def each_first(t):
        lax.fori_loop(*turns_of([turn for turn in gate_table if turn <= last], t), gate_item, 0)

    with jax.named_scope('chain1'):
        sums.run(before, each_first, after)
    with jax.named_scope('gate_rest'):
        lax.fori_loop(len([turn for turn in gate_table if turn <= last]), 3 * tiles, gate_item, 0)
    shards = (me, mate, across, cross)

    def down_load(r, base):
        column = pl.ds(base, cols)
        sem = down_sem.at[0 if base else 1]
        return pltpu.make_async_copy(wd_ref if r == 0 else wdf_ref.at[shards[r]], w_buf.at[:, column], sem)

    def down_fetch(r, base):
        if isinstance(r, int):
            down_load(r, base).start()
            return
        for n in range(4):

            @pl.when(r == n)
            def _():
                down_load(n, base).start()

    def down_work(g, r, base):
        down_load(0, base).wait()
        parts = group_rows(g)
        gated = jnp.concatenate([z_buf[part, :] for part in parts], axis=0)
        down = jnp.dot(gated, w_buf[:, pl.ds(base, cols)], preferred_element_type=F32).astype(BF16)
        if isinstance(r, int):
            shard = shards[r]
        else:
            shard = jnp.where(r == 0, me, jnp.where(r == 1, mate, jnp.where(r == 2, across, cross)))
        for d, part in enumerate(parts):
            p_buf[part, shard_span(shard)] = down[d * span_rows:(d + 1) * span_rows]

    rows_each = wd_ref.shape[0] // (2 * pieces[DOWN])
    half_hidden = wd_ref.shape[0] // 2
    spans = (((0, edge * rows_each), (half_hidden, edge * rows_each)), ((edge * rows_each, late_pieces * rows_each), (half_hidden + edge * rows_each, late_pieces * rows_each)))

    def far_loads(r, base, late):
        column = pl.ds(base, cols)
        return [pltpu.make_async_copy(wdf_ref.at[shards[r], pl.ds(start, size)], w_buf.at[pl.ds(start, size), column], far_sem.at[r - 2, n]) for n, (start, size) in enumerate(spans[late])]

    def far_product(base, late):
        gated = [jnp.concatenate([z_buf[part, start:start + size] for part in group_rows(0)], axis=0) for start, size in spans[late]]
        return sum(jnp.dot(rows, w_buf[start:start + size, pl.ds(base, cols)], preferred_element_type=F32) for rows, (start, size) in zip(gated, spans[late]))

    def far_early(r, base):
        for load in far_loads(r, base, 0):
            load.wait()
        far_buf[r - 2] = far_product(base, 0)

    def far_late(r, base):
        for load in far_loads(r, base, 1):
            load.wait()
        down = (far_buf[r - 2] + far_product(base, 1)).astype(BF16)
        for d, part in enumerate(group_rows(0)):
            p_buf[part, shard_span(shards[r])] = down[d * span_rows:(d + 1) * span_rows]

    def far_start(r, base, late):
        for load in far_loads(r, base, late):
            load.start()

    early_moves = [move for (part, p), move in tail if part != DOWN or p < edge]
    late_moves = [move for (part, p), move in tail if part == DOWN and p >= edge]
    down_fetch(0, pair)
    with jax.named_scope('tail'):
        gather.own_landed(DOWN)
        down_fetch(1, 0)
        sums.settle()
    with jax.named_scope('down_near0'):
        down_work(0, 0, pair)
    with jax.named_scope('pass_early'):
        for move in early_moves:
            move()
    with jax.named_scope('down_near1'):
        down_work(0, 1, 0)
    with jax.named_scope('landed_early'):
        for p in range(edge):
            gather.landed(DOWN, p)
        far_start(2, pair, 0)
        far_start(3, 0, 0)
    with jax.named_scope('pass_late0'):
        for move in late_moves[:len(late_moves) - 2]:
            move()
    with jax.named_scope('far_early0'):
        far_early(2, pair)
    with jax.named_scope('pass_late1'):
        for move in late_moves[len(late_moves) - 2:]:
            move()
    with jax.named_scope('far_early1'):
        far_early(3, 0)

    caches = ((k_buf, kf_ref), (v_buf, vf_ref))

    def rows_of(ref, shard):
        return ref.at[pl.ds(pl.multiple_of(shard * seq, seq), seq)]

    def kv_copy(i, hop):
        src, dst = caches[i]
        if hop == 0:
            return remote(src, rows_of(dst, me), kv_send.at[i, hop], kv_recv.at[i, hop], {'dm': across})
        if hop == 1:
            return remote(src, rows_of(dst, me), kv_send.at[i, hop], kv_recv.at[i, hop], {'dm': mate})
        return remote(rows_of(dst, across), rows_of(dst, across), kv_send.at[i, hop], kv_recv.at[i, hop], {'dm': mate})

    def kv_arrival(i, hop):
        region = rows_of(caches[i][1], (across, mate, cross)[hop])
        return remote(region, region, kv_send.at[i, hop], kv_recv.at[i, hop], {'dm': mate})

    with jax.named_scope('settle_down'):
        for p in range(edge, pieces[DOWN]):
            gather.landed(DOWN, p)
    far_start(2, pair, 1)
    far_start(3, 0, 1)
    kv_stores = [pltpu.make_async_copy(src, rows_of(dst, me), kv_store.at[i]) for i, (src, dst) in enumerate(caches)]
    for i in range(2):
        kv_copy(i, 0).start()
        kv_copy(i, 1).start()
        kv_stores[i].start()
    with jax.named_scope('far_late'):
        far_late(2, pair)
        down_fetch(0, pair)
        far_late(3, 0)
        gate_fetch(0, 0)

    def finish_last(out_rows, rows, total):
        xm_buf[out_rows, :] = (res_buf[rows, :].astype(F32) + unit_rows(total.astype(F32), gain_buf[3:4, :])).astype(BF16)

    def emit_last(out_rows):
        there = pl.ds(pl.multiple_of(me * seq + out_rows.start, CHUNK), CHUNK)
        for i, dev in enumerate((across, cross, mate)):
            remote(xm_buf.at[out_rows, shard_span(dev)], y_ref.at[there], fin_send.at[i], fin_recv.at[i], {'dm': dev}).start()
        pltpu.make_async_copy(xm_buf.at[out_rows, mine], y_ref.at[there], fin_own).start()

    last_sums = LineSum(p_buf, got, xm_buf, *line_sems[4:], finish_last, emit_last)

    def pass_kv(i):
        kv_arrival(i, 0).wait_recv()
        kv_copy(i, 2).start()

    late_gates = [int((f + 1) * 2 * ahead / (tiles + 1)) for f in range(tiles)]
    late_downs = [(n * ahead) // 4 + ahead // 8 for n in range(12)]

    def late_gate(f, carry):
        def refill(n):
            @pl.when(f + 1 < tiles)
            def _():
                gate_fetch(f + 1, 0, (n,))

        gate_work(3, f, 0, refill)
        return carry

    def late_down(n, carry):
        down_work(1 + lax.div(n, 4), lax.rem(n, 4), pair)

        @pl.when(n + 1 < 12)
        def _():
            down_fetch(lax.rem(n + 1, 4), pair)

        return carry

    def each_last(t):
        lax.fori_loop(*turns_of(late_gates, t), late_gate, 0)
        lax.fori_loop(*turns_of(late_downs, t), late_down, 0)

    with jax.named_scope('chain2'):
        last_sums.run({min(14, last - 1): [functools.partial(pass_kv, 0)], min(17, last): [functools.partial(pass_kv, 1)]}, each_last, {})
    with jax.named_scope('close'):
        last_sums.settle()
        for i in range(2):
            kv_stores[i].wait()
            for hop in range(3):
                kv_copy(i, hop).wait_send()
            kv_arrival(i, 1).wait_recv()
            kv_arrival(i, 2).wait_recv()
        for i, dev in enumerate((across, cross, mate)):
            done = remote(xm_buf.at[:, shard_span(dev)], rows_of(y_ref, dev), fin_send.at[i], fin_recv.at[i], {'dm': dev})
            done.wait_send()
            done.wait_recv()
        pltpu.make_async_copy(xm_buf.at[:, mine], rows_of(y_ref, me), fin_own).wait()
        for part in (GATE, UP):
            for p in range(tiles):
                gather.sent(part, p)
                gather.own_sent(part, p)
        for p in range(pieces[DOWN]):
            gather.sent(DOWN, p)
        gather.own_sent(DOWN)
        for copy in n_copies:
            copy.wait_send()
        x_copy(0, 0).wait_send()
        for s in range(2):
            x_copy(1, s).wait_send()
            x_copy(2, s).wait_send()


def like(*shape, dtype=BF16):
    return jax.ShapeDtypeStruct(shape, dtype)


def params(collective_id):
    return pltpu.CompilerParams(collective_id=collective_id, has_side_effects=True, vmem_limit_bytes=VMEM_BYTES)


def run_layer(x, norms, wq, wk, wv, wo, wg, wu, wd, cos_tab, sin_tab, pos, scale):
    seq = pos.shape[0]
    cols = x.shape[1]
    dim = 4 * cols
    kv_heads, head_dim = wk.shape[1:]
    width = wo.shape[0] + 2 * kv_heads * head_dim
    chunks = seq // 2 // CHUNK
    cache = (seq, kv_heads, head_dim)
    hidden = wg.shape[1]
    tile = min(hidden // 2, 512)
    tiles = hidden // tile

    def count(rows, most):
        return most if rows % (32 * most) == 0 else 2

    pieces = (count(cols, 7), 4, tiles, tiles, count(wd.shape[0], 14))
    units = sum(pieces)
    return pl.pallas_call(
        functools.partial(layer_kernel, scale, kv_heads, head_dim, pieces),
        name='layer',
        out_shape=(like(4 * seq, cols), like(4 * seq, kv_heads, head_dim), like(4 * seq, kv_heads, head_dim), like(tiles, dim, tile), like(tiles, dim, tile), like(4, *wd.shape)),
        in_specs=[ANY] * 9 + [VMEM] * 4,
        out_specs=(ANY,) * 6,
        scratch_shapes=[
            pltpu.VMEM((seq, dim), BF16), pltpu.VMEM((dim, width), BF16), pltpu.VMEM((wo.shape[0], dim), BF16), pltpu.VMEM((seq, width), BF16),
            pltpu.VMEM((seq, dim), BF16), pltpu.VMEM((2, seq // 2, dim), BF16), pltpu.VMEM((seq // 2, dim), BF16), pltpu.VMEM((4,) + norms.shape, F32), pltpu.VMEM((4, dim), F32),
            pltpu.VMEM(wq.shape, BF16), pltpu.VMEM(wk.shape, BF16), pltpu.VMEM(wv.shape, BF16), pltpu.VMEM(cache, BF16), pltpu.VMEM(cache, BF16), pltpu.VMEM((2, seq // 4, cols), F32), pltpu.VMEM((seq // 4, tile), BF16),
            DMA((3, 2)), DMA((3, 2)), DMA((3,)), DMA((3,)), DMA((2, 2 * LINE)), DMA((2 * LINE,)), DMA((3 + 2 * tiles,)), DMA((3 + 2 * tiles,)), DMA((units, 4)), DMA((units, 4)), DMA((6,)),
            DMA((2, 2, 4)), DMA((2,)), DMA((2, 2)), DMA((2,)), DMA((2, 3)), DMA((2, 3)), DMA((3,)), DMA((3,)), DMA,
        ] + [DMA((2, chunks))] * 8,
        compiler_params=params(0),
    )(x, norms, wq, wk, wv, wo, wg, wu, wd, cos_tab, sin_tab, pos[:, None], pos[None, :])


def solution(mesh):
    tp_size = mesh.shape['tp']

    def layer(tokens, positions, norm_pre_attn, w_query, w_key, w_value, w_out, norm_post_attn, norm_pre_ffw, w_gate, w_up, w_down, norm_post_ffw):
        seq = positions.shape[1]
        heads, head_dim, cols = w_out.shape
        dim = 4 * cols
        scale = (dim / (heads * tp_size)) ** -0.5
        norms = jnp.stack([norm_pre_attn, norm_post_attn, norm_pre_ffw, norm_post_ffw]).astype(F32)
        pos = lax.dynamic_index_in_dim(positions, lax.axis_index('dm'), 0, keepdims=False)
        half_dim = head_dim // 2
        inv_freq = ROPE_BASE ** (-2.0 * jnp.arange(half_dim, dtype=F32) / head_dim)
        angles = pos.astype(F32)[:, None] * inv_freq[None, :]
        outs = run_layer(tokens, norms, w_query, w_key, w_value, w_out.reshape(heads * head_dim, cols), w_gate, w_up, w_down, jnp.cos(angles), jnp.sin(angles), pos, scale)
        return outs[:3]

    width_spec = P('dm')
    in_specs = (P('dp', 'dm'), P('dp', None), width_spec, P('dm', 'tp', None), P('dm', 'tp', None), P('dm', 'tp', None), P('tp', None, 'dm'), width_spec, width_spec, P('dm', 'tp'), P('dm', 'tp'), P('tp', 'dm'), width_spec)
    out_specs = (P('dp', 'dm'), P('dp', 'tp', None), P('dp', 'tp', None))
    return jax.shard_map(layer, mesh=mesh, in_specs=in_specs, out_specs=out_specs, check_vma=False)
```
